32 devices in a mesh: dp: 8 (over y, x, core), tensor: 4 (over z).
Axes of the slice: x: 2, y: 2, z: 4, core: 2. Of those that a mesh axis runs over, the one named last changes fastest.
Arguments:
- tokens: bfloat16 [4096, 1024], P(('dp', 'tensor')), may hold values from -5 to 5
- lengths: int32 [8, 2], P('dp'), may hold values from 0 to 512, as said below
- w_query: bfloat16 [1024, 1024], P('dp', 'tensor'), may hold values from -0.1875 to 0.1875
- b_query: float32 [1024], replicated, may hold values from -3 to 3
- w_key: bfloat16 [1024, 1024], P('dp', 'tensor'), may hold values from -0.1875 to 0.1875
- w_value: bfloat16 [1024, 1024], P('dp', 'tensor'), may hold values from -0.1875 to 0.1875
- b_value: float32 [1024], replicated, may hold values from -3 to 3
- w_out: bfloat16 [1024, 1024], P('tensor', 'dp'), may hold values from -3 to 3
- b_out: float32 [1024], replicated, may hold values from -3 to 3
- gain_attn: float32 [1024], replicated, may hold values from 0.1 to 1.9
- shift_attn: float32 [1024], replicated, may hold values from -3 to 3
- w_in: bfloat16 [1024, 4096], P('dp', 'tensor'), may hold values from -0.1875 to 0.1875
- b_in: float32 [4096], replicated, may hold values from -3 to 3
- w_back: bfloat16 [4096, 1024], P('tensor', 'dp'), may hold values from -0.09375 to 0.09375
- b_back: float32 [1024], replicated, may hold values from -3 to 3
- gain_ffn: float32 [1024], replicated, may hold values from 0.1 to 1.9
- shift_ffn: float32 [1024], replicated, may hold values from -3 to 3
- cotangent: bfloat16 [4096, 1024], P(('dp', 'tensor')), may hold values from -6 to 6
Outputs:
- output: bfloat16 [4096, 1024], P(('dp', 'tensor'))
- grad_tokens: float32 [4096, 1024], P(('dp', 'tensor'))
- grad_w_query: float32 [1024, 1024], P('dp', 'tensor')
- grad_b_query: float32 [1024], replicated
- grad_w_key: float32 [1024, 1024], P('dp', 'tensor')
- grad_w_value: float32 [1024, 1024], P('dp', 'tensor')
- grad_b_value: float32 [1024], replicated
- grad_w_out: float32 [1024, 1024], P('tensor', 'dp')
- grad_b_out: float32 [1024], replicated
- grad_gain_attn: float32 [1024], replicated
- grad_shift_attn: float32 [1024], replicated
- grad_w_in: float32 [1024, 4096], P('dp', 'tensor')
- grad_b_in: float32 [4096], replicated
- grad_w_back: float32 [4096, 1024], P('tensor', 'dp')
- grad_b_back: float32 [1024], replicated
- grad_gain_ffn: float32 [1024], replicated
- grad_shift_ffn: float32 [1024], replicated
The draws below stay inside these ranges and needn't reach their ends.
Inputs may be any that keep to these rules, and one draw needn't show every extreme that they name: Each group's 2 lengths sum to at most 512; the first is 1 or more, the second may be 0; in every draw one group holds a single sequence of exactly 512 tokens.
All inputs are finite; a program needn't handle non-finite values.
Results may differ from the reference program's by a relative error of at most 0.02.
Values may be sent and summed in bfloat16 or wider, within the bound.
A program may use at most 128 MiB of HBM per device.

```python
import jax
import jax.numpy as jnp
from jax import lax

D = 1024
HEADS = 16
HD = 64
FF = 4096
TOK_G = 512
TOKENS = 4096
N_DP = 8
N_TENSOR = 4


def draw_lengths(key, part):
    key_used, key_first, key_full = jax.random.split(key, 3)
    used_rows = jax.random.randint(key_used, (N_DP,), TOK_G // 4, TOK_G + 1)
    raw_first = jax.random.randint(key_first, (N_DP,), 0, 1048576)
    first_len = 1 + raw_first % used_rows
    full_group = jax.random.randint(key_full, (), 0, N_DP)
    selected = jnp.arange(N_DP, dtype=jnp.int32) == full_group
    first_len = jnp.where(selected, TOK_G, first_len)
    used_rows = jnp.where(selected, TOK_G, used_rows)
    second_len = used_rows - first_len
    return jnp.stack([first_len, second_len], axis=1).astype(jnp.int32)


def draw_tokens(key, part):
    key_base = jax.random.fold_in(key, 0)
    return jax.random.truncated_normal(key_base, -4.0, 4.0, (TOKENS, D), jnp.float32).astype(jnp.bfloat16)


def with_spikes(entries, key, source, target, shards_of, factor):
    def block_of(axis_at):
        return (jnp.arange(entries.shape[axis_at]) // (entries.shape[axis_at] // shards_of)).reshape((-1,) + (1,) * (entries.ndim - 1 - axis_at))

    one_side = jax.random.permutation(key, shards_of)[block_of(target)]
    far = (block_of(target) + shards_of // 2) % shards_of
    return jnp.where((block_of(source) == one_side) | (block_of(source) == far), factor * entries, entries)


def steps_of(key, dims, pieces, least, high):
    gain, own = 1.0, jax.random.fold_in(key, 6)
    for dim, parts in pieces:
        heights = jnp.exp(jax.random.uniform(jax.random.fold_in(own, dim), (parts,), jnp.float32, least / len(pieces), high / len(pieces)))
        gain = gain * jnp.repeat(heights, dims[dim] // parts).reshape([-1 if axis == dim else 1 for axis in range(len(dims))])
    return gain


def normal_values(own_key, shape, width, limit, pieces=(), kind=jnp.bfloat16):
    level = steps_of(own_key, shape, pieces, -0.22, 0.18) if pieces else 1.0
    values = jax.random.normal(own_key, shape, jnp.float32) * width * level
    return jnp.minimum(jnp.maximum(values, -limit), limit).astype(kind)


def gaussian_with(key, shape, deviation, most, cuts, heavy, kind=jnp.bfloat16):
    drawn = deviation * jax.random.normal(key, shape, jnp.float32)
    if cuts:
        drawn = drawn * steps_of(key, shape, cuts, -0.22, 0.18)
    return jnp.clip(with_spikes(drawn, jax.random.fold_in(key, 3), *heavy), -most, most).astype(kind)


def setup_inputs(seed: int = 0) -> dict:
    key_list = jax.random.split(jax.random.key(seed), 19)
    tokens = draw_tokens(jax.random.fold_in(key_list[18], 71), 0)
    lengths = draw_lengths(jax.random.fold_in(key_list[18], 71), 0)
    w_query = normal_values(key_list[2], (D, D), D ** -0.5, 0.1875, ((0, 8), (1, 4)))
    b_query = normal_values(key_list[3], (D,), 0.5, 3.0, (), jnp.float32)
    w_key = normal_values(key_list[4], (D, D), D ** -0.5, 0.1875, ((0, 8), (1, 4)))
    w_value = normal_values(key_list[5], (D, D), D ** -0.5, 0.1875, ((0, 8), (1, 4)))
    b_value = normal_values(key_list[6], (D,), 0.5, 3.0, (), jnp.float32)
    w_out = normal_values(key_list[7], (D, D), 4 ** -0.5, 3.0, ((0, 4), (1, 8)))
    b_out = normal_values(key_list[8], (D,), 0.5, 3.0, (), jnp.float32)
    gain_attn = jnp.clip(1.0 + 0.18 * jax.random.normal(key_list[9], (D,), jnp.float32), 0.1, 1.9)
    shift_attn = normal_values(key_list[10], (D,), 0.5, 3.0, (), jnp.float32)
    w_in = normal_values(key_list[11], (D, FF), D ** -0.5, 0.1875, ((0, 8), (1, 4)))
    b_in = normal_values(key_list[12], (FF,), 0.5, 3.0, (), jnp.float32)
    w_back = normal_values(key_list[13], (FF, D), FF ** -0.5, 0.09375, ((0, 4), (1, 8)))
    b_back = normal_values(key_list[14], (D,), 0.5, 3.0, (), jnp.float32)
    gain_ffn = jnp.clip(1.0 + 0.18 * jax.random.normal(key_list[15], (D,), jnp.float32), 0.1, 1.9)
    shift_ffn = normal_values(key_list[16], (D,), 0.5, 3.0, (), jnp.float32)
    cotangent = gaussian_with(key_list[17], (TOKENS, D), 1.0, 6.0, ((0, 32),), (0, 1, 32, 2.75))
    return {"tokens": tokens, "lengths": lengths, "w_query": w_query, "b_query": b_query, "w_key": w_key, "w_value": w_value, "b_value": b_value, "w_out": w_out, "b_out": b_out, "gain_attn": gain_attn, "shift_attn": shift_attn, "w_in": w_in, "b_in": b_in, "w_back": w_back, "b_back": b_back, "gain_ffn": gain_ffn, "shift_ffn": shift_ffn, "cotangent": cotangent}


epsilon = 1e-06
masked_value = -1e+30

def layer_norm(residual, gain_vec, shift_vec):
    mean_val = lax.optimization_barrier(jnp.mean(residual, axis=-1, keepdims=True))
    centered = residual - mean_val
    inv_std = lax.rsqrt(lax.optimization_barrier(jnp.mean(centered * centered, axis=-1, keepdims=True)) + epsilon)
    normed = centered * inv_std
    return (normed * gain_vec + shift_vec, normed, inv_std)

def norm_back(grad_out, normed, inv_std, gain_vec):
    grad_norm = grad_out * gain_vec
    first_mean = lax.optimization_barrier(jnp.mean(grad_norm, axis=-1, keepdims=True))
    second_mean = lax.optimization_barrier(jnp.mean(grad_norm * normed, axis=-1, keepdims=True))
    return inv_std * (grad_norm - first_mean - normed * second_mean)

def gelu_parts(preact):
    cdf_val = 0.5 * (1.0 + lax.erf(preact * 0.7071067811865476))
    pdf_val = jnp.exp(-0.5 * preact * preact) * 0.3989422804014327
    return (preact * cdf_val, cdf_val + preact * pdf_val)

def partial_terms(left_side, right_side):
    inner_width = left_side.shape[1]
    part_width = inner_width // N_TENSOR
    left_split = left_side.reshape(left_side.shape[0], N_TENSOR, part_width).astype(jnp.float32)
    right_split = right_side.reshape(N_TENSOR, part_width, right_side.shape[1]).astype(jnp.float32)
    return jnp.einsum('tnk,nkd->ntd', left_split, right_split, precision=lax.Precision.HIGHEST)

def round_sum(terms_all):
    rounded = lax.optimization_barrier(terms_all.astype(jnp.bfloat16))
    return lax.optimization_barrier(jnp.sum(rounded.astype(jnp.float32), axis=0))

def reference(tokens, lengths, w_query, b_query, w_key, w_value, b_value, w_out, b_out, gain_attn, shift_attn, w_in, b_in, w_back, b_back, gain_ffn, shift_ffn, cotangent):
    score_scale = HD ** (-0.5)
    group_tokens = tokens.reshape(N_DP, TOK_G, D)
    group_cotan = cotangent.reshape(N_DP, TOK_G, D)

    def split_heads(matrix):
        return matrix.reshape(TOK_G, HEADS, HD).transpose(1, 0, 2)

    def merge_heads(matrix):
        return matrix.transpose(1, 0, 2).reshape(TOK_G, D)

    def one_group(totals_in, inputs):
        rows_in, seq_lens, grad_out = inputs
        positions = jnp.arange(TOK_G, dtype=jnp.int32)
        live_end = seq_lens[0] + seq_lens[1]
        seg_ids = (positions >= seq_lens[0]).astype(jnp.int32) + (positions >= live_end).astype(jnp.int32)
        live_rows = (positions < live_end).astype(jnp.float32)[:, None]
        same_seg = seg_ids[:, None] == seg_ids[None, :]
        query_rows = (jnp.dot(rows_in, w_query, preferred_element_type=jnp.float32) + b_query).astype(jnp.bfloat16)
        key_rows = jnp.dot(rows_in, w_key, preferred_element_type=jnp.float32).astype(jnp.bfloat16)
        value_rows = (jnp.dot(rows_in, w_value, preferred_element_type=jnp.float32) + b_value).astype(jnp.bfloat16)

        def head_forward(head_parts):
            query_head, key_head, value_head = head_parts
            scores = jnp.dot(query_head, key_head.T, preferred_element_type=jnp.float32) * score_scale
            scores = jnp.where(same_seg, scores, masked_value)
            row_max = lax.optimization_barrier(jnp.max(scores, axis=-1, keepdims=True))
            log_total = row_max + jnp.log(lax.optimization_barrier(jnp.sum(jnp.exp(scores - row_max), axis=-1, keepdims=True)))
            prob_bf = jnp.exp(scores - log_total).astype(jnp.bfloat16)
            context_head = jnp.dot(prob_bf, value_head, preferred_element_type=jnp.float32).astype(jnp.bfloat16)
            return (context_head, log_total[:, 0])
        heads_query = split_heads(query_rows)
        heads_key = split_heads(key_rows)
        heads_value = split_heads(value_rows)
        context_heads, totals_heads = lax.map(head_forward, (heads_query, heads_key, heads_value))
        context = merge_heads(context_heads)
        attn_sum = round_sum(partial_terms(context, w_out))
        resid_one = rows_in.astype(jnp.float32) + attn_sum + b_out
        hidden_one, normed_one, inv_one = layer_norm(resid_one, gain_attn, shift_attn)
        hidden_bf = hidden_one.astype(jnp.bfloat16)
        preact = jnp.dot(hidden_bf, w_in, preferred_element_type=jnp.float32) + b_in
        activ_val, gelu_slope = gelu_parts(preact)
        activation = activ_val.astype(jnp.bfloat16)
        ffn_sum = round_sum(partial_terms(activation, w_back))
        resid_two = hidden_one + ffn_sum + b_back
        normed_out, normed_two, inv_two = layer_norm(resid_two, gain_ffn, shift_ffn)
        output_rows = (normed_out * live_rows).astype(jnp.bfloat16)
        grad_final = grad_out.astype(jnp.float32) * live_rows
        grad_gain_ffn = lax.optimization_barrier(jnp.sum(grad_final * normed_two, axis=0))
        grad_shift_ffn = lax.optimization_barrier(jnp.sum(grad_final, axis=0))
        grad_two = norm_back(grad_final, normed_two, inv_two, gain_ffn)
        grad_b_back = lax.optimization_barrier(jnp.sum(grad_two, axis=0))
        grad_two_bf = grad_two.astype(jnp.bfloat16)
        grad_w_back = jnp.dot(activation.T, grad_two_bf, preferred_element_type=jnp.float32)
        grad_pre = jnp.dot(grad_two_bf, w_back.T, preferred_element_type=jnp.float32) * gelu_slope
        grad_b_in = lax.optimization_barrier(jnp.sum(grad_pre, axis=0))
        grad_pre_bf = grad_pre.astype(jnp.bfloat16)
        grad_w_in = jnp.dot(hidden_bf.T, grad_pre_bf, preferred_element_type=jnp.float32)
        grad_one_out = grad_two + round_sum(partial_terms(grad_pre_bf, w_in.T))
        grad_gain_attn = lax.optimization_barrier(jnp.sum(grad_one_out * normed_one, axis=0))
        grad_shift_attn = lax.optimization_barrier(jnp.sum(grad_one_out, axis=0))
        grad_one = norm_back(grad_one_out, normed_one, inv_one, gain_attn)
        grad_b_out = lax.optimization_barrier(jnp.sum(grad_one, axis=0))
        grad_one_bf = grad_one.astype(jnp.bfloat16)
        grad_w_out = jnp.dot(context.T, grad_one_bf, preferred_element_type=jnp.float32)
        grad_context = jnp.dot(grad_one_bf, w_out.T, preferred_element_type=jnp.float32).astype(jnp.bfloat16)

        def head_backward(head_parts):
            query_head, key_head, value_head, context_head, gctx_head, total_head = head_parts
            scores = jnp.dot(query_head, key_head.T, preferred_element_type=jnp.float32) * score_scale
            scores = jnp.where(same_seg, scores, masked_value)
            probs = jnp.exp(scores - total_head[:, None])
            prob_bf = probs.astype(jnp.bfloat16)
            grad_probs = jnp.dot(gctx_head, value_head.T, preferred_element_type=jnp.float32)
            delta_rows = lax.optimization_barrier(jnp.sum(gctx_head.astype(jnp.float32) * context_head.astype(jnp.float32), axis=-1, keepdims=True))
            grad_scores = (probs * (grad_probs - delta_rows) * score_scale).astype(jnp.bfloat16)
            grad_q_head = jnp.dot(grad_scores, key_head, preferred_element_type=jnp.float32)
            grad_k_head = jnp.dot(grad_scores.T, query_head, preferred_element_type=jnp.float32)
            grad_v_head = jnp.dot(prob_bf.T, gctx_head, preferred_element_type=jnp.float32)
            return (grad_q_head, grad_k_head, grad_v_head)
        grad_q_heads, grad_k_heads, grad_v_heads = lax.map(head_backward, (heads_query, heads_key, heads_value, context_heads, split_heads(grad_context), totals_heads))
        grad_query = merge_heads(grad_q_heads)
        grad_keys = merge_heads(grad_k_heads)
        grad_values = merge_heads(grad_v_heads)
        grad_b_query = lax.optimization_barrier(jnp.sum(grad_query, axis=0))
        grad_b_value = lax.optimization_barrier(jnp.sum(grad_values, axis=0))
        grad_query_bf = grad_query.astype(jnp.bfloat16)
        grad_keys_bf = grad_keys.astype(jnp.bfloat16)
        grad_values_bf = grad_values.astype(jnp.bfloat16)
        grad_w_query = jnp.dot(rows_in.T, grad_query_bf, preferred_element_type=jnp.float32)
        grad_w_key = jnp.dot(rows_in.T, grad_keys_bf, preferred_element_type=jnp.float32)
        grad_w_value = jnp.dot(rows_in.T, grad_values_bf, preferred_element_type=jnp.float32)
        grad_terms = partial_terms(grad_query_bf, w_query.T) + partial_terms(grad_keys_bf, w_key.T) + partial_terms(grad_values_bf, w_value.T)
        grad_in = grad_one + round_sum(grad_terms)
        group_terms = (grad_w_query, grad_b_query, grad_w_key, grad_w_value, grad_b_value, grad_w_out, grad_b_out, grad_gain_attn, grad_shift_attn, grad_w_in, grad_b_in, grad_w_back, grad_b_back, grad_gain_ffn, grad_shift_ffn)
        totals_out = tuple((total_sum + group_term for total_sum, group_term in zip(totals_in, group_terms)))
        return (totals_out, (output_rows, grad_in))
    start_totals = tuple((jnp.zeros(param_array.shape, jnp.float32) for param_array in (w_query, b_query, w_key, w_value, b_value, w_out, b_out, gain_attn, shift_attn, w_in, b_in, w_back, b_back, gain_ffn, shift_ffn)))
    totals_end, stacked = lax.scan(one_group, start_totals, (group_tokens, lengths, group_cotan))
    outputs_all, grads_all = stacked
    return (outputs_all.reshape(TOKENS, D), grads_all.reshape(TOKENS, D), totals_end[0], totals_end[1], totals_end[2], totals_end[3], totals_end[4], totals_end[5], totals_end[6], totals_end[7], totals_end[8], totals_end[9], totals_end[10], totals_end[11], totals_end[12], totals_end[13], totals_end[14])
```

```python
from types import SimpleNamespace

import jax
import jax.numpy as jnp
from jax import lax
from jax.experimental import pallas as pl
from jax.experimental.pallas import tpu as pltpu
from jax.sharding import PartitionSpec as P

HD = 64


epsilon = 1e-06
masked_value = -1e30


def matmul_plain(left_side, right_side):
    return jnp.dot(left_side, right_side, preferred_element_type=jnp.float32)


def matmul_over_rows(left_side, right_side):
    return lax.dot_general(
        left_side, right_side, (((0,), (0,)), ((), ())), preferred_element_type=jnp.float32
    )


def matmul_over_cols(left_side, right_side):
    return lax.dot_general(
        left_side, right_side, (((1,), (1,)), ((), ())), preferred_element_type=jnp.float32
    )


def layer_norm(residual, gain_vec, shift_vec):
    mean_val = jnp.mean(residual, axis=-1, keepdims=True)
    centered = residual - mean_val
    inv_std = lax.rsqrt(jnp.mean(centered * centered, axis=-1, keepdims=True) + epsilon)
    normed = centered * inv_std
    return (normed * gain_vec + shift_vec, normed, inv_std)


def norm_back(grad_out, normed, inv_std, gain_vec):
    grad_norm = grad_out * gain_vec
    first_mean = jnp.mean(grad_norm, axis=-1, keepdims=True)
    second_mean = jnp.mean(grad_norm * normed, axis=-1, keepdims=True)
    return inv_std * (grad_norm - first_mean - normed * second_mean)


def gelu_parts(preact):
    cdf_val = 0.5 * (1.0 + lax.erf(preact * 0.7071067811865476))
    pdf_val = jnp.exp(-0.5 * preact * preact) * 0.3989422804014327
    return (preact * cdf_val, cdf_val + preact * pdf_val)


def attend_forward(query_rows, key_rows, value_rows, seg_ids, head_dim, block_rows):
    group_rows, head_cols = query_rows.shape
    pair_width = 2 * head_dim
    block_count = group_rows // block_rows
    pair_count = head_cols // pair_width
    score_scale = head_dim ** (-0.5)

    def attend_step(step_index, loop_carry):
        context, log_total = loop_carry
        pair_index = step_index // block_count
        row_start = step_index % block_count * block_rows
        first_col = pair_index * pair_width
        query_block = lax.dynamic_slice(
            query_rows, (row_start, first_col), (block_rows, pair_width)
        ).reshape(block_rows, 2, head_dim)
        key_pair = lax.dynamic_slice(key_rows, (0, first_col), (group_rows, pair_width)).reshape(
            group_rows, 2, head_dim
        )
        value_pair = lax.dynamic_slice(
            value_rows, (0, first_col), (group_rows, pair_width)
        ).reshape(group_rows, 2, head_dim)
        same_seg = seg_ids[:, None] == seg_ids[None, :]
        scores = (
            jnp.einsum("qhd,khd->hqk", query_block, key_pair, preferred_element_type=jnp.float32)
            * score_scale
        )
        scores = jnp.where(same_seg[None], scores, masked_value)
        row_max = jnp.max(scores, axis=-1, keepdims=True)
        block_total = row_max + jnp.log(jnp.sum(jnp.exp(scores - row_max), axis=-1, keepdims=True))
        prob_bf = jnp.exp(scores - block_total).astype(jnp.bfloat16)
        context_block = jnp.einsum(
            "hqk,khd->qhd", prob_bf, value_pair, preferred_element_type=jnp.float32
        ).astype(jnp.bfloat16)
        context = lax.dynamic_update_slice(
            context, context_block.reshape(block_rows, pair_width), (row_start, first_col)
        )
        log_total = lax.dynamic_update_slice(
            log_total, block_total[:, :, 0], (2 * pair_index, row_start)
        )
        return (context, log_total)

    start_carry = (
        jnp.zeros((group_rows, head_cols), jnp.bfloat16),
        jnp.zeros((head_cols // head_dim, group_rows), jnp.float32),
    )
    return lax.fori_loop(0, pair_count * block_count, attend_step, start_carry)


def attend_backward(
    query_rows,
    key_rows,
    value_rows,
    context,
    grad_context,
    log_total,
    seg_ids,
    head_dim,
    block_rows,
):
    group_rows, head_cols = query_rows.shape
    pair_width = 2 * head_dim
    block_count = group_rows // block_rows
    pair_count = head_cols // pair_width
    score_scale = head_dim ** (-0.5)

    def back_step(step_index, loop_carry):
        grad_query, grad_keys, grad_values = loop_carry
        pair_index = step_index // block_count
        row_start = step_index % block_count * block_rows
        first_col = pair_index * pair_width
        query_block = lax.dynamic_slice(
            query_rows, (row_start, first_col), (block_rows, pair_width)
        ).reshape(block_rows, 2, head_dim)
        key_pair = lax.dynamic_slice(key_rows, (0, first_col), (group_rows, pair_width)).reshape(
            group_rows, 2, head_dim
        )
        value_pair = lax.dynamic_slice(
            value_rows, (0, first_col), (group_rows, pair_width)
        ).reshape(group_rows, 2, head_dim)
        context_block = lax.dynamic_slice(
            context, (row_start, first_col), (block_rows, pair_width)
        ).reshape(block_rows, 2, head_dim)
        gctx_block = lax.dynamic_slice(
            grad_context, (row_start, first_col), (block_rows, pair_width)
        ).reshape(block_rows, 2, head_dim)
        total_block = lax.dynamic_slice(log_total, (2 * pair_index, row_start), (2, block_rows))
        same_seg = seg_ids[:, None] == seg_ids[None, :]
        scores = (
            jnp.einsum("qhd,khd->hqk", query_block, key_pair, preferred_element_type=jnp.float32)
            * score_scale
        )
        scores = jnp.where(same_seg[None], scores, masked_value)
        probs = jnp.exp(scores - total_block[:, :, None])
        prob_bf = probs.astype(jnp.bfloat16)
        grad_probs = jnp.einsum(
            "qhd,khd->hqk", gctx_block, value_pair, preferred_element_type=jnp.float32
        )
        delta_rows = jnp.sum(
            gctx_block.astype(jnp.float32) * context_block.astype(jnp.float32), axis=-1
        ).T[:, :, None]
        grad_scores = (probs * (grad_probs - delta_rows) * score_scale).astype(jnp.bfloat16)
        grad_q_block = jnp.einsum(
            "hqk,khd->qhd", grad_scores, key_pair, preferred_element_type=jnp.float32
        ).reshape(block_rows, pair_width)
        grad_k_pair = jnp.einsum(
            "hqk,qhd->khd", grad_scores, query_block, preferred_element_type=jnp.float32
        ).reshape(group_rows, pair_width)
        grad_v_pair = jnp.einsum(
            "hqk,qhd->khd", prob_bf, gctx_block, preferred_element_type=jnp.float32
        ).reshape(group_rows, pair_width)
        grad_query = lax.dynamic_update_slice(grad_query, grad_q_block, (row_start, first_col))
        old_keys = lax.dynamic_slice(grad_keys, (0, first_col), (group_rows, pair_width))
        grad_keys = lax.dynamic_update_slice(grad_keys, old_keys + grad_k_pair, (0, first_col))
        old_values = lax.dynamic_slice(grad_values, (0, first_col), (group_rows, pair_width))
        grad_values = lax.dynamic_update_slice(
            grad_values, old_values + grad_v_pair, (0, first_col)
        )
        return (grad_query, grad_keys, grad_values)

    zero_grad = jnp.zeros((group_rows, head_cols), jnp.float32)
    return lax.fori_loop(0, pair_count * block_count, back_step, (zero_grad, zero_grad, zero_grad))


def on_device_plain(
    tokens,
    lengths,
    w_query,
    b_query,
    w_key,
    w_value,
    b_value,
    w_out,
    b_out,
    gain_attn,
    shift_attn,
    w_in,
    b_in,
    w_back,
    b_back,
    gain_ffn,
    shift_ffn,
    cotangent,
):
    tensor_size = lax.axis_size("tensor")
    tensor_index = lax.axis_index("tensor")
    local_rows = tokens.shape[0]
    group_rows = local_rows * tensor_size
    head_cols = w_query.shape[1]
    hidden_cols = w_in.shape[1]
    block_rows = min(512, group_rows)
    seq_lens = lengths[0]
    live_end = seq_lens[0] + seq_lens[1]
    positions = jnp.arange(group_rows, dtype=jnp.int32)
    seg_ids = (positions >= seq_lens[0]).astype(jnp.int32) + (positions >= live_end).astype(
        jnp.int32
    )
    local_pos = tensor_index * local_rows + jnp.arange(local_rows, dtype=jnp.int32)
    live_rows = (local_pos < live_end).astype(jnp.float32)[:, None]
    rows_full = lax.all_gather(tokens, "tensor", axis=0, tiled=True)
    attn_mats = (
        lax.all_gather(w_query, "dp", axis=0, tiled=True),
        lax.all_gather(w_key, "dp", axis=0, tiled=True),
        lax.all_gather(w_value, "dp", axis=0, tiled=True),
        lax.all_gather(w_out, "dp", axis=1, tiled=True),
    )
    mat_query, mat_key, mat_value, mat_out = attn_mats
    bias_query = lax.dynamic_slice_in_dim(b_query, tensor_index * head_cols, head_cols)
    bias_value = lax.dynamic_slice_in_dim(b_value, tensor_index * head_cols, head_cols)
    bias_in = lax.dynamic_slice_in_dim(b_in, tensor_index * hidden_cols, hidden_cols)
    query_rows = (matmul_plain(rows_full, mat_query) + bias_query).astype(jnp.bfloat16)
    key_rows = matmul_plain(rows_full, mat_key).astype(jnp.bfloat16)
    value_rows = (matmul_plain(rows_full, mat_value) + bias_value).astype(jnp.bfloat16)
    context, log_total = attend_forward(query_rows, key_rows, value_rows, seg_ids, HD, block_rows)
    attn_sum = lax.psum_scatter(
        matmul_plain(context, mat_out).astype(jnp.bfloat16),
        "tensor",
        scatter_dimension=0,
        tiled=True,
    ).astype(jnp.float32)
    resid_one = tokens.astype(jnp.float32) + attn_sum + b_out
    hidden_one, normed_one, inv_one = layer_norm(resid_one, gain_attn, shift_attn)
    hidden_bf = hidden_one.astype(jnp.bfloat16)
    hidden_full = lax.all_gather(hidden_bf, "tensor", axis=0, tiled=True)
    ffn_mats = (
        lax.all_gather(w_in, "dp", axis=0, tiled=True),
        lax.all_gather(w_back, "dp", axis=1, tiled=True),
    )
    mat_in, mat_back = ffn_mats
    preact = matmul_plain(hidden_full, mat_in) + bias_in
    activ_val, gelu_slope = gelu_parts(preact)
    activation = activ_val.astype(jnp.bfloat16)
    ffn_sum = lax.psum_scatter(
        matmul_plain(activation, mat_back).astype(jnp.bfloat16),
        "tensor",
        scatter_dimension=0,
        tiled=True,
    ).astype(jnp.float32)
    resid_two = hidden_one + ffn_sum + b_back
    normed_out, normed_two, inv_two = layer_norm(resid_two, gain_ffn, shift_ffn)
    output = (normed_out * live_rows).astype(jnp.bfloat16)
    grad_final = cotangent.astype(jnp.float32) * live_rows
    grad_gain_ffn = jnp.sum(grad_final * normed_two, axis=0)
    grad_shift_ffn = jnp.sum(grad_final, axis=0)
    grad_two = norm_back(grad_final, normed_two, inv_two, gain_ffn)
    grad_b_back = jnp.sum(grad_two, axis=0)
    mat_query, mat_key, mat_value, mat_out, mat_in, mat_back = (
        lax.all_gather(w_query, "dp", axis=0, tiled=True),
        lax.all_gather(w_key, "dp", axis=0, tiled=True),
        lax.all_gather(w_value, "dp", axis=0, tiled=True),
        lax.all_gather(w_out, "dp", axis=1, tiled=True),
        lax.all_gather(w_in, "dp", axis=0, tiled=True),
        lax.all_gather(w_back, "dp", axis=1, tiled=True),
    )
    grad_two_full = lax.all_gather(grad_two.astype(jnp.bfloat16), "tensor", axis=0, tiled=True)
    grad_w_back = matmul_over_rows(activation, grad_two_full)
    grad_pre = matmul_over_cols(grad_two_full, mat_back) * gelu_slope
    grad_b_in_part = jnp.sum(grad_pre, axis=0)
    grad_pre_bf = grad_pre.astype(jnp.bfloat16)
    grad_w_in = matmul_over_rows(hidden_full, grad_pre_bf)
    grad_one_out = grad_two + lax.psum_scatter(
        matmul_over_cols(grad_pre_bf, mat_in).astype(jnp.bfloat16),
        "tensor",
        scatter_dimension=0,
        tiled=True,
    ).astype(jnp.float32)
    grad_w_in, grad_w_back = (
        lax.psum_scatter(grad_w_in, "dp", scatter_dimension=0, tiled=True),
        lax.psum_scatter(grad_w_back, "dp", scatter_dimension=1, tiled=True),
    )
    grad_gain_attn = jnp.sum(grad_one_out * normed_one, axis=0)
    grad_shift_attn = jnp.sum(grad_one_out, axis=0)
    grad_one = norm_back(grad_one_out, normed_one, inv_one, gain_attn)
    grad_b_out = jnp.sum(grad_one, axis=0)
    grad_one_full = lax.all_gather(grad_one.astype(jnp.bfloat16), "tensor", axis=0, tiled=True)
    grad_w_out = matmul_over_rows(context, grad_one_full)
    grad_context = matmul_over_cols(grad_one_full, mat_out).astype(jnp.bfloat16)
    grad_query, grad_keys, grad_values = attend_backward(
        query_rows, key_rows, value_rows, context, grad_context, log_total, seg_ids, HD, block_rows
    )
    grad_b_query_part = jnp.sum(grad_query, axis=0)
    grad_b_value_part = jnp.sum(grad_values, axis=0)
    grad_query_bf = grad_query.astype(jnp.bfloat16)
    grad_keys_bf = grad_keys.astype(jnp.bfloat16)
    grad_values_bf = grad_values.astype(jnp.bfloat16)
    grad_w_query = matmul_over_rows(rows_full, grad_query_bf)
    grad_w_key = matmul_over_rows(rows_full, grad_keys_bf)
    grad_w_value = matmul_over_rows(rows_full, grad_values_bf)
    query_part = matmul_over_cols(grad_query_bf, mat_query)
    key_part = matmul_over_cols(grad_keys_bf, mat_key)
    value_part = matmul_over_cols(grad_values_bf, mat_value)
    grad_in = grad_one + lax.psum_scatter(
        (query_part + key_part + value_part).astype(jnp.bfloat16),
        "tensor",
        scatter_dimension=0,
        tiled=True,
    ).astype(jnp.float32)
    grad_w_query, grad_w_key, grad_w_value, grad_w_out = (
        lax.psum_scatter(grad_w_query, "dp", scatter_dimension=0, tiled=True),
        lax.psum_scatter(grad_w_key, "dp", scatter_dimension=0, tiled=True),
        lax.psum_scatter(grad_w_value, "dp", scatter_dimension=0, tiled=True),
        lax.psum_scatter(grad_w_out, "dp", scatter_dimension=1, tiled=True),
    )

    def widen(part_vec, full_width):
        return lax.dynamic_update_slice_in_dim(
            jnp.zeros((full_width,), jnp.float32), part_vec, tensor_index * part_vec.shape[0], 0
        )

    small_sums = lax.psum(
        (
            widen(grad_b_query_part, b_query.shape[0]),
            widen(grad_b_value_part, b_value.shape[0]),
            grad_b_out,
            grad_gain_attn,
            grad_shift_attn,
            widen(grad_b_in_part, b_in.shape[0]),
            grad_b_back,
            grad_gain_ffn,
            grad_shift_ffn,
        ),
        ("dp", "tensor"),
    )
    return (
        output,
        grad_in,
        grad_w_query,
        small_sums[0],
        grad_w_key,
        grad_w_value,
        small_sums[1],
        grad_w_out,
        small_sums[2],
        small_sums[3],
        small_sums[4],
        grad_w_in,
        small_sums[5],
        grad_w_back,
        small_sums[6],
        small_sums[7],
        small_sums[8],
    )


MESH_ID = pl.DeviceIdType.MESH
F32 = jnp.float32
BF16 = jnp.bfloat16

SLOTS = 4
BLOCK = 128
GROUP = 512
WIDTH = 1024
HEAD_COLS = 256
HIDDEN = 1024
N_SEM = 176
HALVES = dict(q=(128, 256), k=(128, 256), v=(128, 256), o=(256, 128), i=(128, 1024), b=(1024, 128))
STAGES = ("xa", "ya", "s2", "r2", "zs", "zr")


def flip(bit):
    return 1 - bit


def slot_step(t, j):
    return (t % 2 + j % 2) % 2 + 2 * ((t // 2 + j // 2) % 2)


def rows_of(r, count=BLOCK):
    return pl.ds(pl.multiple_of(r * BLOCK, BLOCK), count)


def cols_of(n, count=256):
    return pl.ds(pl.multiple_of(n * count, count), count)


def dot_nn(a, b):
    return jnp.dot(a, b, preferred_element_type=F32)


def dot_nt(a, b):
    return lax.dot_general(a, b, (((1,), (1,)), ((), ())), preferred_element_type=F32)


def dot_tn(a, b):
    return lax.dot_general(a, b, (((0,), (0,)), ((), ())), preferred_element_type=F32)


def scratch_table():
    act = lambda n: pltpu.VMEM((GROUP, n), BF16)
    table = dict(
        w3=pltpu.VMEM((3 * WIDTH, HEAD_COLS), BF16),
        wo=pltpu.VMEM((4, HEAD_COLS, 256), BF16),
        wi=pltpu.VMEM((WIDTH, HIDDEN), BF16),
        wb=pltpu.VMEM((4, HIDDEN, 256), BF16),
        lens_own=pltpu.VMEM((2, 8, 128), F32),
        lens_got=pltpu.VMEM((2, 8, 128), F32),
        lens_use=pltpu.VMEM((2, 8, 128), F32),
        tk=act(WIDTH),
        tkt=pltpu.VMEM((WIDTH, GROUP), BF16),
        cot_own=pltpu.VMEM((BLOCK, WIDTH), BF16),
        bias=pltpu.VMEM((GROUP, GROUP), F32),
        q=act(HEAD_COLS),
        qt=pltpu.VMEM((HEAD_COLS, GROUP), BF16),
        k=act(HEAD_COLS),
        ks=act(HEAD_COLS),
        v=act(HEAD_COLS),
        ps=pltpu.VMEM((4, GROUP, GROUP), BF16),
        ctx=act(HEAD_COLS),
        ctxt=pltpu.VMEM((HEAD_COLS, GROUP), BF16),
        hid=act(WIDTH),
        hidt=pltpu.VMEM((WIDTH, GROUP), BF16),
        act=act(HIDDEN),
        actt=pltpu.VMEM((HIDDEN, GROUP), BF16),
        slope=pltpu.VMEM((GROUP, HIDDEN), F32),
        g2=act(WIDTH),
        gpre=act(HIDDEN),
        g1=act(WIDTH),
        gctxt=pltpu.VMEM((HEAD_COLS, GROUP), BF16),
        dq=act(HEAD_COLS),
        dkt=pltpu.VMEM((HEAD_COLS, GROUP), F32),
        dvt=pltpu.VMEM((HEAD_COLS, GROUP), F32),
        dk=act(HEAD_COLS),
        dv=act(HEAD_COLS),
        hid1=pltpu.VMEM((BLOCK, WIDTH), F32),
        normed1=pltpu.VMEM((BLOCK, WIDTH), F32),
        inv1=pltpu.VMEM((BLOCK, 128), F32),
        g2f=pltpu.VMEM((BLOCK, WIDTH), F32),
        g1f=pltpu.VMEM((BLOCK, WIDTH), F32),
        out_own=pltpu.VMEM((BLOCK, WIDTH), BF16),
        gtok_own=pltpu.VMEM((BLOCK, WIDTH), BF16),
        gtok_got=pltpu.VMEM((BLOCK, WIDTH), BF16),
        rs_own=pltpu.VMEM((4, BLOCK, WIDTH), BF16),
        rs_out=pltpu.VMEM((4, 3, BLOCK, WIDTH), BF16),
        rs_got=pltpu.VMEM((4, 3, BLOCK, WIDTH), BF16),
        sums=pltpu.VMEM((6, 16, WIDTH), F32),
        sums_got=pltpu.VMEM((5, 16, WIDTH), F32),
        gb_in=pltpu.VMEM((1, HIDDEN), F32),
        g3=pltpu.VMEM((3 * WIDTH, HEAD_COLS), BF16),
        go=pltpu.VMEM((4, HEAD_COLS, 256), BF16),
        gi=pltpu.VMEM((WIDTH, HIDDEN), BF16),
        gb=pltpu.VMEM((4, HIDDEN, 256), BF16),
        stage={},
        ssem=pltpu.SemaphoreType.DMA((N_SEM,)),
        rsem=pltpu.SemaphoreType.DMA((N_SEM,)),
    )
    for name, dims in HALVES.items():
        table["stage"][name] = {part: pltpu.VMEM((2,) + dims, BF16) for part in STAGES}
    return table


def layer_kernel(tok, lens, wq, bq, wk, wv, bv, wo, bo, ga, sa, wi, bi, wb, bb, gf, sf, cot, out, gtok, gq, gk, gv, go, gi,
                 gb, sums, *scratch):
    a = SimpleNamespace(tok=tok, lens=lens, wq=wq, bq=bq, wk=wk, wv=wv, bv=bv, wo=wo, bo=bo, ga=ga, sa=sa, wi=wi, bi=bi,
                        wb=wb, bb=bb, gf=gf, sf=sf, cot=cot)
    o = SimpleNamespace(out=out, gtok=gtok, gq=gq, gk=gk, gv=gv, go=go, gi=gi, gb=gb, sums=sums)
    s = SimpleNamespace(**jax.tree.unflatten(jax.tree.structure(scratch_table()), scratch))
    ssem, rsem = s.ssem, s.rsem

    dp = lax.axis_index("dp")
    z = lax.axis_index("tensor")
    b, c = dp // 2, dp % 2
    zl, zh = z % 2, z // 2
    t = zl * 2 + c
    bx = b + 1 - 2 * (b % 2)
    by = (b + 2) % 4
    bd = 3 - b
    t1, t2, t3 = slot_step(t, 1), slot_step(t, 2), slot_step(t, 3)

    def dev(pos, core, zz):
        return (pos * 2 + core, zz)

    partner = dev(b, flip(c), z)
    z_near = z + 1 - 2 * (z % 2)
    z_far = (z + 2) % 4
    pair = dev(b, c, z_near)
    across = dev(b, c, z_far)
    x_near = dev(bx, c, z)
    y_near = dev(by, c, z)

    taken = {"s": 0, "r": 0}

    def take(kind, count=1):
        first = taken[kind]
        taken[kind] = first + count
        assert taken[kind] <= N_SEM
        return first

    to_drain = []

    def send(src, dst, device, sk, rk, cond=None):
        copy = pltpu.make_async_remote_copy(
            src_ref=src, dst_ref=dst, send_sem=ssem.at[sk], recv_sem=rsem.at[rk], device_id=device,
            device_id_type=MESH_ID)
        copy.start()
        if cond is None:
            to_drain.append((copy, None))

    def got(dst, rk):
        pltpu.make_async_copy(dst, dst, rsem.at[rk]).wait()

    def send_or_keep(src, dst, device, is_self, sk, rk):
        copy = pltpu.make_async_remote_copy(
            src_ref=src, dst_ref=dst, send_sem=ssem.at[sk], recv_sem=rsem.at[rk], device_id=device,
            device_id_type=MESH_ID)

        @pl.when(is_self)
        def _():
            pltpu.make_async_copy(src, dst, rsem.at[rk]).start()

        @pl.when(jnp.logical_not(is_self))
        def _():
            copy.start()

        to_drain.append((copy, is_self))

    barrier = pltpu.get_barrier_semaphore()
    peers = [x_near, y_near]
    for dz in range(4):
        for dc in range(2):
            if dz or dc:
                peers.append(dev(b, (c + dc) % 2, (z + dz) % 4))
    for peer in peers:
        pl.semaphore_signal(barrier, inc=1, device_id=peer, device_id_type=MESH_ID)
    pl.semaphore_wait(barrier, len(peers))

    def piece_qkv(m, home):
        base = m * WIDTH
        return SimpleNamespace(
            home=home,
            own=lambda bb, cc: s.w3.at[pl.ds(pl.multiple_of(base + bb * 256 + cc * 128, 128), 128), :],
            block=lambda bb: s.w3.at[pl.ds(pl.multiple_of(base + bb * 256, 256), 256), :],
            half=lambda bb, h: s.w3.at[pl.ds(pl.multiple_of(base + bb * 256 + h * 128, 128), 128), :])

    piece_o = SimpleNamespace(
        home=a.wo,
        own=lambda bb, cc: s.wo.at[bb, :, pl.ds(pl.multiple_of(cc * 128, 128), 128)],
        block=lambda bb: s.wo.at[bb],
        half=lambda bb, h: s.wo.at[bb, pl.ds(h * 128, 128), :])

    def piece_in(j):
        cols = pl.ds(j * 512, 512)
        return SimpleNamespace(
            home=a.wi.at[:, cols],
            own=lambda bb, cc: s.wi.at[pl.ds(pl.multiple_of(bb * 256 + cc * 128, 128), 128), cols],
            block=lambda bb: s.wi.at[pl.ds(pl.multiple_of(bb * 256, 256), 256), cols],
            half=lambda bb, h: s.wi.at[pl.ds(pl.multiple_of(bb * 256 + h * 128, 128), 128), cols])

    def piece_back(j):
        part = pl.ds(j * 512, 512)
        return SimpleNamespace(
            home=a.wb.at[part, :],
            own=lambda bb, cc: s.wb.at[bb, part, pl.ds(pl.multiple_of(cc * 128, 128), 128)],
            block=lambda bb: s.wb.at[bb, part, :],
            half=lambda bb, h: s.wb.at[bb, pl.ds(j * 512 + h * 256, 256), :])

    pieces = dict(q=piece_qkv(0, a.wq), k=piece_qkv(1, a.wk), v=piece_qkv(2, a.wv), o=piece_o,
                  i0=piece_in(0), i1=piece_in(1), b0=piece_back(0), b1=piece_back(1))
    for piece in pieces.values():
        piece.s1 = take("s", 2)
        piece.r1 = take("r", 2)
        piece.s2 = take("s", 4)
        piece.r2 = take("r", 4)

    def from_home(name):
        piece = pieces[name]
        for far in range(2):
            zt, ct = z // 2 + 2 * far, z % 2
            is_self = jnp.logical_and(zt == z, ct == c)
            send_or_keep(piece.home, piece.own(b, c), dev(b, ct, zt), is_self, piece.s1 + far,
                         piece.r1 + c)

    def over_plane(name):
        piece = pieces[name]
        for cc in range(2):
            got(piece.own(b, cc), piece.r1 + cc)
        send(piece.block(b), piece.block(b), x_near, piece.s2, piece.r2)
        send(piece.block(b), piece.block(b), y_near, piece.s2 + 1, piece.r2 + 1)

    def relay(name):
        piece = pieces[name]
        got(piece.block(bx), piece.r2)
        send(piece.half(bx, 0), piece.half(bx, 0), y_near, piece.s2 + 2, piece.r2 + 2)
        got(piece.block(by), piece.r2 + 1)
        send(piece.half(by, 1), piece.half(by, 1), x_near, piece.s2 + 3, piece.r2 + 3)

    def arrived(name):
        piece = pieces[name]
        got(piece.half(bd, 0), piece.r2 + 2)
        got(piece.half(bd, 1), piece.r2 + 3)

    tok_s, tok_r = take("s", 2), take("r", 4)
    fwd_s = take("s", 4)
    lens_s, lens_r = take("s"), take("r")
    cot_s, cot_r = take("s"), take("r")

    def send_lens():
        first = a.lens[0, 0].astype(F32)
        s.lens_own[0] = jnp.full((8, 128), first, F32)
        s.lens_own[1] = jnp.full((8, 128), first + a.lens[0, 1].astype(F32), F32)
        send(s.lens_own, s.lens_got, partner, lens_s, lens_r)

    def take_lens():
        got(s.lens_got, lens_r)

        @pl.when(c == zh)
        def _():
            s.lens_use[...] = s.lens_own[...]

        @pl.when(c != zh)
        def _():
            s.lens_use[...] = s.lens_got[...]

    def tok_block(r):
        return s.tk.at[rows_of(r), :]

    def send_tokens():
        for j in range(2):
            zt = 2 * c + j
            send_or_keep(a.tok, tok_block(z), dev(b, c, zt), zt == z, tok_s + j, tok_r + z)

    def share_tokens():
        for r in range(SLOTS):
            got(tok_block(r), tok_r + r)
            copy = pltpu.make_async_remote_copy(
                src_ref=tok_block(r), dst_ref=tok_block(r), send_sem=ssem.at[fwd_s + r], recv_sem=rsem.at[tok_r + r],
                device_id=partner, device_id_type=MESH_ID)

            @pl.when(c == zh)
            def _():
                copy.start()

            to_drain.append((copy, c != zh))

    def send_cotangent():
        zt, ct = 2 * c + z // 2, z % 2
        is_self = jnp.logical_and(zt == z, ct == c)
        send_or_keep(a.cot, s.cot_own, dev(b, ct, zt), is_self, cot_s, cot_r)

    gather_s = [take("s", 3) for _ in range(3)]
    gather_r = [take("r", 3) for _ in range(3)]
    scatter_s = [take("s", 3) for _ in range(4)]
    scatter_r = [take("r", 3) for _ in range(4)]

    def block_at(full, r):
        return full.at[rows_of(r), :]

    def gather_start(which, full):
        send(block_at(full, t), block_at(full, t), pair, gather_s[which], gather_r[which] + 1)
        send(block_at(full, t), block_at(full, t), partner, gather_s[which] + 1, gather_r[which])

    def gather_steps(which, full):
        forward = pltpu.make_async_remote_copy(
            src_ref=block_at(full, t2), dst_ref=block_at(full, t2), send_sem=ssem.at[gather_s[which] + 2],
            recv_sem=rsem.at[gather_r[which] + 2], device_id=partner, device_id_type=MESH_ID)
        to_drain.append((forward, None))

        def step(j):
            @pl.when(j == 1)
            def _():
                got(block_at(full, t1), gather_r[which])

            @pl.when(j == 2)
            def _():
                got(block_at(full, t2), gather_r[which] + 1)
                forward.start()

            @pl.when(j == 3)
            def _():
                got(block_at(full, t3), gather_r[which] + 2)

        return step

    def scatter(which, part):
        out, back = s.rs_out, s.rs_got
        ss, rr = scatter_s[which], scatter_r[which]
        part(t3, out.at[which, 0], None)
        send(out.at[which, 0], back.at[which, 0], partner, ss, rr)
        part(t1, out.at[which, 2], None)
        send(out.at[which, 2], back.at[which, 2], partner, ss + 2, rr + 2)
        got(back.at[which, 0], rr)
        part(t2, out.at[which, 1], back.at[which, 0])
        send(out.at[which, 1], back.at[which, 1], pair, ss + 1, rr + 1)
        part(t, s.rs_own.at[which], None)

    def scatter_wait(which):
        got(s.rs_got.at[which, 2], scatter_r[which] + 2)
        got(s.rs_got.at[which, 1], scatter_r[which] + 1)

    def scatter_rows(which, chunk):
        total = s.rs_own[which, chunk, :].astype(F32) + s.rs_got[which, 2, chunk, :].astype(F32)
        return total + s.rs_got[which, 1, chunk, :].astype(F32)

    def put_part(dst, add, n, value):
        value = value.astype(BF16)
        if add is not None:
            value = (value.astype(F32) + add[:, cols_of(n)].astype(F32)).astype(BF16)
        dst[:, cols_of(n)] = value

    def loop(count, body):
        lax.fori_loop(0, count, lambda i, _: (body(i), 0)[1], 0)

    def grad_qkv(m):
        base = m * WIDTH
        return lambda bb, h: s.g3.at[pl.ds(pl.multiple_of(base + bb * 256 + h * 128, 128), 128), :]

    grad_half = dict(
        q=grad_qkv(0), k=grad_qkv(1), v=grad_qkv(2),
        o=lambda bb, h: s.go.at[bb, :, pl.ds(h * 128, 128)],
        i=lambda bb, h: s.gi.at[pl.ds(pl.multiple_of(bb * 256 + h * 128, 128), 128), :],
        b=lambda bb, h: s.gb.at[bb, :, pl.ds(h * 128, 128)])
    grad_out = dict(q=o.gq, k=o.gk, v=o.gv, o=o.go, i=o.gi, b=o.gb)
    grad_chunk = dict(q=128, k=128, v=128, o=128, i=32, b=256)
    grad_s = {name: take("s", 8) for name in grad_half}
    grad_r = {name: take("r", 8) for name in grad_half}

    def stage(name, *which):
        return tuple(s.stage[name][STAGES[i]] for i in which)

    def chunks(name, body):
        size = grad_chunk[name]
        count = HALVES[name][0] // size
        loop(count, lambda i: body(pl.ds(pl.multiple_of(i * size, size), size)))

    def grad_first(name):
        half, ss, rr = grad_half[name], grad_s[name], grad_r[name]
        xa, ya = stage(name, 0, 1)
        send(half(bd, 0), xa.at[1], x_near, ss + 1, rr + 1)
        send(half(bd, 1), ya.at[1], y_near, ss + 3, rr + 3)
        send(half(bx, 0), xa.at[0], x_near, ss, rr)
        send(half(by, 1), ya.at[0], y_near, ss + 2, rr + 2)

    def grad_second(name):
        half, ss, rr = grad_half[name], grad_s[name], grad_r[name]
        xa, ya, s2, r2 = stage(name, 0, 1, 2, 3)
        got(xa.at[1], rr + 1)
        mine = half(by, 0)

        def add_x(ch):
            s2[0, ch, :] = (mine[ch, :].astype(F32) + xa[1, ch, :].astype(F32)).astype(BF16)
        chunks(name, add_x)
        send(s2.at[0], r2.at[0], y_near, ss + 4, rr + 4)
        got(ya.at[1], rr + 3)
        other = half(bx, 1)

        def add_y(ch):
            s2[1, ch, :] = (other[ch, :].astype(F32) + ya[1, ch, :].astype(F32)).astype(BF16)
        chunks(name, add_y)
        send(s2.at[1], r2.at[1], x_near, ss + 5, rr + 5)

    def grad_third(name):
        half, ss, rr = grad_half[name], grad_s[name], grad_r[name]
        xa, ya, r2 = stage(name, 0, 1, 3)
        zs, zr = stage(name, 4, 5)
        for h, first in ((0, xa), (1, ya)):
            got(first.at[0], rr + 2 * h)
            got(r2.at[h], rr + 4 + h)
            mine = half(b, h)

            def add_all(ch):
                total = mine[ch, :].astype(F32) + first[0, ch, :].astype(F32) + r2[h, ch, :].astype(F32)
                zs[h, ch, :] = total.astype(BF16)
            chunks(name, add_all)
            is_self = jnp.logical_and(c == h, z == t)
            send_or_keep(zs.at[h], zr.at[zh], dev(b, h, t), is_self, ss + 6 + h, rr + 6 + zh)

    def grad_final(name):
        rr, (zr,) = grad_r[name], stage(name, 5)
        got(zr.at[0], rr + 6)
        got(zr.at[1], rr + 7)

        def add_both(ch):
            grad_out[name][ch, :] = zr[0, ch, :].astype(F32) + zr[1, ch, :].astype(F32)
        chunks(name, add_both)

    from_home("q")
    from_home("k")
    from_home("v")
    send_lens()
    send_tokens()
    from_home("o")
    from_home("i0")
    from_home("i1")
    from_home("b0")
    from_home("b1")
    send_cotangent()
    s.sums[0] = jnp.zeros((16, WIDTH), F32)
    s.gb_in[...] = jnp.zeros((1, HIDDEN), F32)
    over_plane("q")
    over_plane("k")
    over_plane("v")
    relay("q")
    relay("k")
    relay("v")
    share_tokens()
    over_plane("o")
    take_lens()

    def make_bias(r):
        first, end = s.lens_use[0][0:1, 0:1], s.lens_use[1][0:1, 0:1]
        row = (lax.broadcasted_iota(jnp.int32, (BLOCK, GROUP), 0) + r * BLOCK).astype(F32)
        col = lax.broadcasted_iota(jnp.int32, (BLOCK, GROUP), 1).astype(F32)
        seg = lambda p: jnp.where(p >= end, 2.0, jnp.where(p >= first, 1.0, 0.0))
        s.bias[rows_of(r), :] = jnp.where(seg(row) == seg(col), 0.0, masked_value)
    loop(SLOTS, make_bias)

    def turn_tokens(r):
        s.tkt[:, rows_of(r)] = s.tk[rows_of(r), :].T
    loop(SLOTS, turn_tokens)

    head_cols = pl.ds(pl.multiple_of(t * HEAD_COLS, HEAD_COLS), HEAD_COLS)

    def project(m):
        def body(r):
            rows = rows_of(r)
            acc = dot_nn(s.tk[rows, :], s.w3[pl.ds(m * WIDTH, WIDTH), :])
            if m == 0:
                acc = acc + a.bq[:, head_cols]
                scaled = acc.astype(BF16).astype(F32) * 0.125
                s.q[rows, :] = scaled.astype(BF16)
                s.qt[:, rows] = scaled.astype(BF16).T
            elif m == 1:
                s.k[rows, :] = acc.astype(BF16)
                s.ks[rows, :] = (acc.astype(BF16).astype(F32) * 0.125).astype(BF16)
            else:
                acc = acc + a.bv[:, head_cols]
                s.v[rows, :] = acc.astype(BF16)
        loop(SLOTS, body)

    for m, name in enumerate("qkv"):
        arrived(name)
        project(m)
    relay("o")

    def attend(r):
        rows = rows_of(r)
        parts = []
        for h in range(4):
            cols = slice(64 * h, 64 * h + 64)
            scores = dot_nt(s.q[rows, cols], s.k[:, cols]) + s.bias[rows, :]
            top = jnp.max(scores, axis=-1, keepdims=True)
            weight = jnp.exp(scores - top)
            total = jnp.sum(weight, axis=-1, keepdims=True)
            prob = (weight * (1.0 / total)).astype(BF16)
            s.ps[h, rows, :] = prob
            parts.append(dot_nn(prob, s.v[:, cols]))
        context = jnp.concatenate(parts, axis=1).astype(BF16)
        s.ctx[rows, :] = context
        s.ctxt[:, rows] = context.T
    loop(SLOTS, attend)

    over_plane("i0")
    over_plane("i1")
    arrived("o")

    def attn_part(r, dst, add):
        rows = s.ctx[rows_of(r), :]
        loop(4, lambda n: put_part(dst, add, n, dot_nn(rows, s.wo[n])))
    scatter(0, attn_part)
    relay("i0")
    relay("i1")
    over_plane("b0")
    over_plane("b1")
    scatter_wait(0)

    CH = 32

    def own_chunk(i):
        return pl.ds(pl.multiple_of(i * CH, CH), CH)

    def group_chunk(i):
        return pl.ds(pl.multiple_of(t * BLOCK + i * CH, CH), CH)

    def norm_one(i):
        ch = own_chunk(i)
        resid = s.tk[group_chunk(i), :].astype(F32) + scatter_rows(0, ch) + a.bo[...]
        centered = resid - jnp.mean(resid, axis=-1, keepdims=True)
        inv = lax.rsqrt(jnp.mean(centered * centered, axis=-1, keepdims=True) + epsilon)
        normed = centered * inv
        hidden = normed * a.ga[...] + a.sa[...]
        s.normed1[ch, :] = normed
        s.inv1[ch, :] = jnp.broadcast_to(inv, (CH, 128))
        s.hid1[ch, :] = hidden
        s.hid[group_chunk(i), :] = hidden.astype(BF16)
    loop(BLOCK // CH, norm_one)
    gather_start(0, s.hid)
    arrived("i0")
    arrived("i1")

    next_hid = gather_steps(0, s.hid)

    def ffn_in(j):
        next_hid(j)
        r = slot_step(t, j)
        rows = rows_of(r)

        def body(n):
            cols = cols_of(n)
            bias = a.bi[:, pl.ds(pl.multiple_of(t * HIDDEN + n * 256, 256), 256)]
            pre = dot_nn(s.hid[rows, :], s.wi[:, cols]) + bias
            cdf = 0.5 * (1.0 + lax.erf(pre * 0.7071067811865476))
            pdf = jnp.exp(-0.5 * pre * pre) * 0.3989422804014327
            s.act[rows, cols] = (pre * cdf).astype(BF16)
            s.slope[rows, cols] = cdf + pre * pdf
        loop(4, body)
        s.actt[:, rows] = s.act[rows, :].T
        s.hidt[:, rows] = s.hid[rows, :].T
    loop(SLOTS, ffn_in)
    relay("b0")
    relay("b1")
    arrived("b0")
    arrived("b1")

    def ffn_part(r, dst, add):
        loop(4, lambda n: put_part(dst, add, n, dot_nn(s.act[rows_of(r), :], s.wb[n])))
    scatter(1, ffn_part)
    got(s.cot_own, cot_r)
    scatter_wait(1)

    def add_rows(row, value):
        s.sums[0, row:row + 1, :] += jnp.sum(value, axis=0, keepdims=True)

    def norm_two(i):
        ch = own_chunk(i)
        resid = s.hid1[ch, :] + scatter_rows(1, ch) + a.bb[...]
        centered = resid - jnp.mean(resid, axis=-1, keepdims=True)
        inv = lax.rsqrt(jnp.mean(centered * centered, axis=-1, keepdims=True) + epsilon)
        normed = centered * inv
        position = lax.broadcasted_iota(jnp.int32, (CH, 128), 0) + (t * BLOCK + i * CH)
        live = jnp.where(position.astype(F32) < s.lens_use[1][0:1, :], 1.0, 0.0)[:, 0:1]
        s.out_own[ch, :] = ((normed * a.gf[...] + a.sf[...]) * live).astype(BF16)
        grad = s.cot_own[ch, :].astype(F32) * live
        add_rows(4, grad * normed)
        add_rows(5, grad)
        u = grad * a.gf[...]
        first = jnp.mean(u, axis=-1, keepdims=True)
        second = jnp.mean(u * normed, axis=-1, keepdims=True)
        grad_two = inv * (u - first - normed * second)
        add_rows(3, grad_two)
        s.g2f[ch, :] = grad_two
        s.g2[group_chunk(i), :] = grad_two.astype(BF16)
    loop(BLOCK // CH, norm_two)
    gather_start(1, s.g2)
    out_s, out_r = take("s"), take("r")
    home_self = jnp.logical_and(zh == c, t == z)
    send_or_keep(s.out_own, o.out, dev(b, zh, t), home_self, out_s, out_r)

    next_g2 = gather_steps(1, s.g2)

    def ffn_back(j):
        next_g2(j)
        r = slot_step(t, j)
        rows = rows_of(r)

        def body(n):
            cols = cols_of(n)
            acc = dot_nt(s.g2[rows, 0:256], s.wb[0, cols, :])
            for k in range(1, 4):
                acc = acc + dot_nt(s.g2[rows, 256 * k:256 * k + 256], s.wb[k, cols, :])
            grad = acc * s.slope[rows, cols]
            s.gb_in[:, cols] += jnp.sum(grad, axis=0, keepdims=True)
            s.gpre[rows, cols] = grad.astype(BF16)
        loop(4, body)
    loop(SLOTS, ffn_back)

    def grad_back(n):
        def body(m):
            part = cols_of(m)
            s.gb[n, part, :] = dot_nn(s.actt[part, :], s.g2[:, cols_of(n)]).astype(BF16)
        loop(4, body)
    loop(4, grad_back)
    grad_first("b")

    def in_part(r, dst, add):
        loop(4, lambda n: put_part(dst, add, n, dot_nt(s.gpre[rows_of(r), :], s.wi[cols_of(n), :])))
    scatter(2, in_part)

    def grad_in(n):
        def body(m):
            part = cols_of(m)
            s.gi[part, cols_of(n)] = dot_nn(s.hidt[part, :], s.gpre[:, cols_of(n)]).astype(BF16)
        loop(4, body)
    loop(4, grad_in)
    grad_first("i")
    scatter_wait(2)

    def norm_one_back(i):
        ch = own_chunk(i)
        grad = s.g2f[ch, :] + scatter_rows(2, ch)
        normed = s.normed1[ch, :]
        add_rows(1, grad * normed)
        add_rows(2, grad)
        u = grad * a.ga[...]
        first = jnp.mean(u, axis=-1, keepdims=True)
        second = jnp.mean(u * normed, axis=-1, keepdims=True)
        grad_one = s.inv1[ch, 0:1] * (u - first - normed * second)
        add_rows(0, grad_one)
        s.g1f[ch, :] = grad_one
        s.g1[group_chunk(i), :] = grad_one.astype(BF16)
    loop(BLOCK // CH, norm_one_back)
    gather_start(2, s.g1)
    grad_second("b")
    s.dkt[...] = jnp.zeros((HEAD_COLS, GROUP), F32)
    s.dvt[...] = jnp.zeros((HEAD_COLS, GROUP), F32)

    next_g1 = gather_steps(2, s.g1)

    def attend_back(j):
        next_g1(j)
        r = slot_step(t, j)
        rows = rows_of(r)
        acc = dot_nt(s.g1[rows, 0:256], s.wo[0])
        for k in range(1, 4):
            acc = acc + dot_nt(s.g1[rows, 256 * k:256 * k + 256], s.wo[k])
        grad_ctx = acc.astype(BF16)
        s.gctxt[:, rows] = grad_ctx.T
        product = grad_ctx.astype(F32) * s.ctx[rows, :].astype(F32)
        parts = []
        for h in range(4):
            cols = slice(64 * h, 64 * h + 64)
            prob = s.ps[h, rows, :]
            delta = jnp.sum(product[:, cols], axis=-1, keepdims=True)
            grad_prob = dot_nt(grad_ctx[:, cols], s.v[:, cols])
            grad_score = (prob.astype(F32) * (grad_prob - delta)).astype(BF16)
            parts.append(dot_nn(grad_score, s.ks[:, cols]))
            s.dkt[cols, :] += dot_nn(s.qt[cols, rows], grad_score)
            s.dvt[cols, :] += dot_nn(s.gctxt[cols, rows], prob)
        grad_query = jnp.concatenate(parts, axis=1)
        for k in range(4):
            @pl.when(t == k)
            def _():
                s.sums[0, 6:7, 256 * k:256 * k + 256] += jnp.sum(grad_query, axis=0, keepdims=True)
        s.dq[rows, :] = grad_query.astype(BF16)
    loop(SLOTS, attend_back)

    grad_second("i")

    def turn_back(r):
        rows = rows_of(r)
        s.dk[rows, :] = s.dkt[:, rows].T.astype(BF16)
        grad_value = s.dvt[:, rows].T
        for k in range(4):
            @pl.when(t == k)
            def _():
                s.sums[0, 7:8, 256 * k:256 * k + 256] += jnp.sum(grad_value, axis=0, keepdims=True)
        s.dv[rows, :] = grad_value.astype(BF16)
    loop(SLOTS, turn_back)
    for k in range(4):
        @pl.when(t == k)
        def _():
            s.sums[0, 8 + k:9 + k, :] = s.gb_in[...]

    sums_s, sums_r = take("s", 5), take("r", 5)
    sums_to = [partner, x_near, y_near, pair, across]

    def sums_start(k):
        send(s.sums.at[k], s.sums_got.at[k], sums_to[k], sums_s + k, sums_r + k)

    def sums_finish(k):
        got(s.sums_got.at[k], sums_r + k)
        total = s.sums[k] + s.sums_got[k]
        if k == 4:
            o.sums[...] = total
        else:
            s.sums[k + 1] = total

    sums_start(0)

    def tok_part(r, dst, add):
        rows = rows_of(r)

        def body(n):
            acc = dot_nt(s.dq[rows, :], s.w3[cols_of(n), :])
            acc = acc + dot_nt(s.dk[rows, :], s.w3[pl.ds(pl.multiple_of(WIDTH + n * 256, 256), 256), :])
            acc = acc + dot_nt(s.dv[rows, :], s.w3[pl.ds(pl.multiple_of(2 * WIDTH + n * 256, 256), 256), :])
            put_part(dst, add, n, acc)
        loop(4, body)
    scatter(3, tok_part)
    sums_finish(0)
    sums_start(1)

    def grad_head(m, src):
        def body(n):
            part = cols_of(n)
            dst = pl.ds(pl.multiple_of(m * WIDTH + n * 256, 256), 256)
            s.g3[dst, :] = dot_nn(s.tkt[part, :], src[...]).astype(BF16)
        loop(4, body)

    def grad_o(n):
        s.go[n] = dot_nn(s.ctxt[...], s.g1[:, cols_of(n)]).astype(BF16)
    loop(4, grad_o)
    grad_first("o")
    sums_finish(1)
    sums_start(2)
    grad_head(0, s.dq)
    grad_first("q")
    grad_head(1, s.dk)
    grad_first("k")
    grad_head(2, s.dv)
    grad_first("v")
    sums_finish(2)
    sums_start(3)
    grad_third("b")
    grad_third("i")
    scatter_wait(3)

    def last_rows(i):
        ch = own_chunk(i)
        s.gtok_own[ch, :] = (s.g1f[ch, :] + scatter_rows(3, ch)).astype(BF16)
    loop(BLOCK // CH, last_rows)
    gtok_s, gtok_r = take("s"), take("r")
    send_or_keep(s.gtok_own, s.gtok_got, dev(b, zh, t), home_self, gtok_s, gtok_r)
    sums_finish(3)
    sums_start(4)
    for name in "oqkv":
        grad_second(name)
    grad_final("b")
    grad_final("i")
    got(s.gtok_got, gtok_r)

    def widen_rows(i):
        ch = own_chunk(i)
        o.gtok[ch, :] = s.gtok_got[ch, :].astype(F32)
    loop(BLOCK // CH, widen_rows)
    sums_finish(4)
    for name in "oqkv":
        grad_third(name)
    for name in "oqkv":
        grad_final(name)
    got(o.out, out_r)

    for copy, skipped in to_drain:
        if skipped is None:
            copy.wait_send()
        else:
            @pl.when(jnp.logical_not(skipped))
            def _():
                copy.wait_send()


def on_device_fused(tokens, lengths, w_query, b_query, w_key, w_value, b_value, w_out, b_out, gain_attn, shift_attn,
                    w_in, b_in, w_back, b_back, gain_ffn, shift_ffn, cotangent):
    row = lambda vec: vec.reshape(1, -1)
    operands = (tokens, lengths, w_query, row(b_query), w_key, w_value, row(b_value), w_out, row(b_out),
                row(gain_attn), row(shift_attn), w_in, row(b_in), w_back, row(b_back), row(gain_ffn),
                row(shift_ffn), cotangent)
    vmem = pl.BlockSpec(memory_space=pltpu.VMEM)
    in_specs = [vmem] * len(operands)
    in_specs[1] = pl.BlockSpec(memory_space=pltpu.SMEM)
    shape = lambda dims, dtype: jax.ShapeDtypeStruct(dims, dtype)
    out_shape = (
        shape(tokens.shape, BF16), shape(tokens.shape, F32), shape(w_query.shape, F32), shape(w_key.shape, F32),
        shape(w_value.shape, F32), shape(w_out.shape, F32), shape(w_in.shape, F32), shape(w_back.shape, F32),
        shape((16, WIDTH), F32))
    out, gtok, gq, gk, gv, go, gi, gb, sums = pl.pallas_call(
        layer_kernel,
        out_shape=out_shape,
        in_specs=in_specs,
        out_specs=(vmem,) * len(out_shape),
        scratch_shapes=jax.tree.leaves(scratch_table()),
        compiler_params=pltpu.CompilerParams(collective_id=0, has_side_effects=True, vmem_limit_bytes=64 * 1024 * 1000),
        name="layer",
    )(*operands)
    return (out, gtok, gq, sums[6], gk, gv, sums[7], go, sums[0], sums[1], sums[2], gi, sums[8:12].reshape(-1), gb,
            sums[3], sums[4], sums[5])


def fits_fused(mesh):
    return dict(mesh.shape) == {"dp": 8, "tensor": 4}


def solution(mesh):
    placed = (
        P(("dp", "tensor"), None),
        P("dp", None),
        P("dp", "tensor"),
        P(),
        P("dp", "tensor"),
        P("dp", "tensor"),
        P(),
        P("tensor", "dp"),
        P(),
        P(),
        P(),
        P("dp", "tensor"),
        P(),
        P("tensor", "dp"),
        P(),
        P(),
        P(),
        P(("dp", "tensor"), None),
    )
    on_device = on_device_fused if fits_fused(mesh) else on_device_plain
    return jax.shard_map(
        on_device,
        mesh=mesh,
        in_specs=placed,
        out_specs=(
            P(("dp", "tensor"), None),
            P(("dp", "tensor"), None),
            P("dp", "tensor"),
            P(),
            P("dp", "tensor"),
            P("dp", "tensor"),
            P(),
            P("tensor", "dp"),
            P(),
            P(),
            P(),
            P("dp", "tensor"),
            P(),
            P("tensor", "dp"),
            P(),
            P(),
            P(),
        ),
        check_vma=False,
    )
```

```python
from types import SimpleNamespace

import jax
import jax.numpy as jnp
from jax import lax
from jax.experimental import pallas as pl
from jax.experimental.pallas import tpu as pltpu
from jax.sharding import PartitionSpec as P

HD = 64


epsilon = 1e-06
masked_value = -1e30


def matmul_plain(left_side, right_side):
    return jnp.dot(left_side, right_side, preferred_element_type=jnp.float32)


def matmul_over_rows(left_side, right_side):
    return lax.dot_general(
        left_side, right_side, (((0,), (0,)), ((), ())), preferred_element_type=jnp.float32
    )


def matmul_over_cols(left_side, right_side):
    return lax.dot_general(
        left_side, right_side, (((1,), (1,)), ((), ())), preferred_element_type=jnp.float32
    )


def layer_norm(residual, gain_vec, shift_vec):
    mean_val = jnp.mean(residual, axis=-1, keepdims=True)
    centered = residual - mean_val
    inv_std = lax.rsqrt(jnp.mean(centered * centered, axis=-1, keepdims=True) + epsilon)
    normed = centered * inv_std
    return (normed * gain_vec + shift_vec, normed, inv_std)


def norm_back(grad_out, normed, inv_std, gain_vec):
    grad_norm = grad_out * gain_vec
    first_mean = jnp.mean(grad_norm, axis=-1, keepdims=True)
    second_mean = jnp.mean(grad_norm * normed, axis=-1, keepdims=True)
    return inv_std * (grad_norm - first_mean - normed * second_mean)


def gelu_parts(preact):
    cdf_val = 0.5 * (1.0 + lax.erf(preact * 0.7071067811865476))
    pdf_val = jnp.exp(-0.5 * preact * preact) * 0.3989422804014327
    return (preact * cdf_val, cdf_val + preact * pdf_val)


def attend_forward(query_rows, key_rows, value_rows, seg_ids, head_dim, block_rows):
    group_rows, head_cols = query_rows.shape
    pair_width = 2 * head_dim
    block_count = group_rows // block_rows
    pair_count = head_cols // pair_width
    score_scale = head_dim ** (-0.5)

    def attend_step(step_index, loop_carry):
        context, log_total = loop_carry
        pair_index = step_index // block_count
        row_start = step_index % block_count * block_rows
        first_col = pair_index * pair_width
        query_block = lax.dynamic_slice(
            query_rows, (row_start, first_col), (block_rows, pair_width)
        ).reshape(block_rows, 2, head_dim)
        key_pair = lax.dynamic_slice(key_rows, (0, first_col), (group_rows, pair_width)).reshape(
            group_rows, 2, head_dim
        )
        value_pair = lax.dynamic_slice(
            value_rows, (0, first_col), (group_rows, pair_width)
        ).reshape(group_rows, 2, head_dim)
        same_seg = seg_ids[:, None] == seg_ids[None, :]
        scores = (
            jnp.einsum("qhd,khd->hqk", query_block, key_pair, preferred_element_type=jnp.float32)
            * score_scale
        )
        scores = jnp.where(same_seg[None], scores, masked_value)
        row_max = jnp.max(scores, axis=-1, keepdims=True)
        block_total = row_max + jnp.log(jnp.sum(jnp.exp(scores - row_max), axis=-1, keepdims=True))
        prob_bf = jnp.exp(scores - block_total).astype(jnp.bfloat16)
        context_block = jnp.einsum(
            "hqk,khd->qhd", prob_bf, value_pair, preferred_element_type=jnp.float32
        ).astype(jnp.bfloat16)
        context = lax.dynamic_update_slice(
            context, context_block.reshape(block_rows, pair_width), (row_start, first_col)
        )
        log_total = lax.dynamic_update_slice(
            log_total, block_total[:, :, 0], (2 * pair_index, row_start)
        )
        return (context, log_total)

    start_carry = (
        jnp.zeros((group_rows, head_cols), jnp.bfloat16),
        jnp.zeros((head_cols // head_dim, group_rows), jnp.float32),
    )
    return lax.fori_loop(0, pair_count * block_count, attend_step, start_carry)


def attend_backward(
    query_rows,
    key_rows,
    value_rows,
    context,
    grad_context,
    log_total,
    seg_ids,
    head_dim,
    block_rows,
):
    group_rows, head_cols = query_rows.shape
    pair_width = 2 * head_dim
    block_count = group_rows // block_rows
    pair_count = head_cols // pair_width
    score_scale = head_dim ** (-0.5)

    def back_step(step_index, loop_carry):
        grad_query, grad_keys, grad_values = loop_carry
        pair_index = step_index // block_count
        row_start = step_index % block_count * block_rows
        first_col = pair_index * pair_width
        query_block = lax.dynamic_slice(
            query_rows, (row_start, first_col), (block_rows, pair_width)
        ).reshape(block_rows, 2, head_dim)
        key_pair = lax.dynamic_slice(key_rows, (0, first_col), (group_rows, pair_width)).reshape(
            group_rows, 2, head_dim
        )
        value_pair = lax.dynamic_slice(
            value_rows, (0, first_col), (group_rows, pair_width)
        ).reshape(group_rows, 2, head_dim)
        context_block = lax.dynamic_slice(
            context, (row_start, first_col), (block_rows, pair_width)
        ).reshape(block_rows, 2, head_dim)
        gctx_block = lax.dynamic_slice(
            grad_context, (row_start, first_col), (block_rows, pair_width)
        ).reshape(block_rows, 2, head_dim)
        total_block = lax.dynamic_slice(log_total, (2 * pair_index, row_start), (2, block_rows))
        same_seg = seg_ids[:, None] == seg_ids[None, :]
        scores = (
            jnp.einsum("qhd,khd->hqk", query_block, key_pair, preferred_element_type=jnp.float32)
            * score_scale
        )
        scores = jnp.where(same_seg[None], scores, masked_value)
        probs = jnp.exp(scores - total_block[:, :, None])
        prob_bf = probs.astype(jnp.bfloat16)
        grad_probs = jnp.einsum(
            "qhd,khd->hqk", gctx_block, value_pair, preferred_element_type=jnp.float32
        )
        delta_rows = jnp.sum(
            gctx_block.astype(jnp.float32) * context_block.astype(jnp.float32), axis=-1
        ).T[:, :, None]
        grad_scores = (probs * (grad_probs - delta_rows) * score_scale).astype(jnp.bfloat16)
        grad_q_block = jnp.einsum(
            "hqk,khd->qhd", grad_scores, key_pair, preferred_element_type=jnp.float32
        ).reshape(block_rows, pair_width)
        grad_k_pair = jnp.einsum(
            "hqk,qhd->khd", grad_scores, query_block, preferred_element_type=jnp.float32
        ).reshape(group_rows, pair_width)
        grad_v_pair = jnp.einsum(
            "hqk,qhd->khd", prob_bf, gctx_block, preferred_element_type=jnp.float32
        ).reshape(group_rows, pair_width)
        grad_query = lax.dynamic_update_slice(grad_query, grad_q_block, (row_start, first_col))
        old_keys = lax.dynamic_slice(grad_keys, (0, first_col), (group_rows, pair_width))
        grad_keys = lax.dynamic_update_slice(grad_keys, old_keys + grad_k_pair, (0, first_col))
        old_values = lax.dynamic_slice(grad_values, (0, first_col), (group_rows, pair_width))
        grad_values = lax.dynamic_update_slice(
            grad_values, old_values + grad_v_pair, (0, first_col)
        )
        return (grad_query, grad_keys, grad_values)

    zero_grad = jnp.zeros((group_rows, head_cols), jnp.float32)
    return lax.fori_loop(0, pair_count * block_count, back_step, (zero_grad, zero_grad, zero_grad))


def on_device_plain(
    tokens,
    lengths,
    w_query,
    b_query,
    w_key,
    w_value,
    b_value,
    w_out,
    b_out,
    gain_attn,
    shift_attn,
    w_in,
    b_in,
    w_back,
    b_back,
    gain_ffn,
    shift_ffn,
    cotangent,
):
    tensor_size = lax.axis_size("tensor")
    tensor_index = lax.axis_index("tensor")
    local_rows = tokens.shape[0]
    group_rows = local_rows * tensor_size
    head_cols = w_query.shape[1]
    hidden_cols = w_in.shape[1]
    block_rows = min(512, group_rows)
    seq_lens = lengths[0]
    live_end = seq_lens[0] + seq_lens[1]
    positions = jnp.arange(group_rows, dtype=jnp.int32)
    seg_ids = (positions >= seq_lens[0]).astype(jnp.int32) + (positions >= live_end).astype(
        jnp.int32
    )
    local_pos = tensor_index * local_rows + jnp.arange(local_rows, dtype=jnp.int32)
    live_rows = (local_pos < live_end).astype(jnp.float32)[:, None]
    rows_full = lax.all_gather(tokens, "tensor", axis=0, tiled=True)
    attn_mats = (
        lax.all_gather(w_query, "dp", axis=0, tiled=True),
        lax.all_gather(w_key, "dp", axis=0, tiled=True),
        lax.all_gather(w_value, "dp", axis=0, tiled=True),
        lax.all_gather(w_out, "dp", axis=1, tiled=True),
    )
    mat_query, mat_key, mat_value, mat_out = attn_mats
    bias_query = lax.dynamic_slice_in_dim(b_query, tensor_index * head_cols, head_cols)
    bias_value = lax.dynamic_slice_in_dim(b_value, tensor_index * head_cols, head_cols)
    bias_in = lax.dynamic_slice_in_dim(b_in, tensor_index * hidden_cols, hidden_cols)
    query_rows = (matmul_plain(rows_full, mat_query) + bias_query).astype(jnp.bfloat16)
    key_rows = matmul_plain(rows_full, mat_key).astype(jnp.bfloat16)
    value_rows = (matmul_plain(rows_full, mat_value) + bias_value).astype(jnp.bfloat16)
    context, log_total = attend_forward(query_rows, key_rows, value_rows, seg_ids, HD, block_rows)
    attn_sum = lax.psum_scatter(
        matmul_plain(context, mat_out).astype(jnp.bfloat16),
        "tensor",
        scatter_dimension=0,
        tiled=True,
    ).astype(jnp.float32)
    resid_one = tokens.astype(jnp.float32) + attn_sum + b_out
    hidden_one, normed_one, inv_one = layer_norm(resid_one, gain_attn, shift_attn)
    hidden_bf = hidden_one.astype(jnp.bfloat16)
    hidden_full = lax.all_gather(hidden_bf, "tensor", axis=0, tiled=True)
    ffn_mats = (
        lax.all_gather(w_in, "dp", axis=0, tiled=True),
        lax.all_gather(w_back, "dp", axis=1, tiled=True),
    )
    mat_in, mat_back = ffn_mats
    preact = matmul_plain(hidden_full, mat_in) + bias_in
    activ_val, gelu_slope = gelu_parts(preact)
    activation = activ_val.astype(jnp.bfloat16)
    ffn_sum = lax.psum_scatter(
        matmul_plain(activation, mat_back).astype(jnp.bfloat16),
        "tensor",
        scatter_dimension=0,
        tiled=True,
    ).astype(jnp.float32)
    resid_two = hidden_one + ffn_sum + b_back
    normed_out, normed_two, inv_two = layer_norm(resid_two, gain_ffn, shift_ffn)
    output = (normed_out * live_rows).astype(jnp.bfloat16)
    grad_final = cotangent.astype(jnp.float32) * live_rows
    grad_gain_ffn = jnp.sum(grad_final * normed_two, axis=0)
    grad_shift_ffn = jnp.sum(grad_final, axis=0)
    grad_two = norm_back(grad_final, normed_two, inv_two, gain_ffn)
    grad_b_back = jnp.sum(grad_two, axis=0)
    mat_query, mat_key, mat_value, mat_out, mat_in, mat_back = (
        lax.all_gather(w_query, "dp", axis=0, tiled=True),
        lax.all_gather(w_key, "dp", axis=0, tiled=True),
        lax.all_gather(w_value, "dp", axis=0, tiled=True),
        lax.all_gather(w_out, "dp", axis=1, tiled=True),
        lax.all_gather(w_in, "dp", axis=0, tiled=True),
        lax.all_gather(w_back, "dp", axis=1, tiled=True),
    )
    grad_two_full = lax.all_gather(grad_two.astype(jnp.bfloat16), "tensor", axis=0, tiled=True)
    grad_w_back = matmul_over_rows(activation, grad_two_full)
    grad_pre = matmul_over_cols(grad_two_full, mat_back) * gelu_slope
    grad_b_in_part = jnp.sum(grad_pre, axis=0)
    grad_pre_bf = grad_pre.astype(jnp.bfloat16)
    grad_w_in = matmul_over_rows(hidden_full, grad_pre_bf)
    grad_one_out = grad_two + lax.psum_scatter(
        matmul_over_cols(grad_pre_bf, mat_in).astype(jnp.bfloat16),
        "tensor",
        scatter_dimension=0,
        tiled=True,
    ).astype(jnp.float32)
    grad_w_in, grad_w_back = (
        lax.psum_scatter(grad_w_in, "dp", scatter_dimension=0, tiled=True),
        lax.psum_scatter(grad_w_back, "dp", scatter_dimension=1, tiled=True),
    )
    grad_gain_attn = jnp.sum(grad_one_out * normed_one, axis=0)
    grad_shift_attn = jnp.sum(grad_one_out, axis=0)
    grad_one = norm_back(grad_one_out, normed_one, inv_one, gain_attn)
    grad_b_out = jnp.sum(grad_one, axis=0)
    grad_one_full = lax.all_gather(grad_one.astype(jnp.bfloat16), "tensor", axis=0, tiled=True)
    grad_w_out = matmul_over_rows(context, grad_one_full)
    grad_context = matmul_over_cols(grad_one_full, mat_out).astype(jnp.bfloat16)
    grad_query, grad_keys, grad_values = attend_backward(
        query_rows, key_rows, value_rows, context, grad_context, log_total, seg_ids, HD, block_rows
    )
    grad_b_query_part = jnp.sum(grad_query, axis=0)
    grad_b_value_part = jnp.sum(grad_values, axis=0)
    grad_query_bf = grad_query.astype(jnp.bfloat16)
    grad_keys_bf = grad_keys.astype(jnp.bfloat16)
    grad_values_bf = grad_values.astype(jnp.bfloat16)
    grad_w_query = matmul_over_rows(rows_full, grad_query_bf)
    grad_w_key = matmul_over_rows(rows_full, grad_keys_bf)
    grad_w_value = matmul_over_rows(rows_full, grad_values_bf)
    query_part = matmul_over_cols(grad_query_bf, mat_query)
    key_part = matmul_over_cols(grad_keys_bf, mat_key)
    value_part = matmul_over_cols(grad_values_bf, mat_value)
    grad_in = grad_one + lax.psum_scatter(
        (query_part + key_part + value_part).astype(jnp.bfloat16),
        "tensor",
        scatter_dimension=0,
        tiled=True,
    ).astype(jnp.float32)
    grad_w_query, grad_w_key, grad_w_value, grad_w_out = (
        lax.psum_scatter(grad_w_query, "dp", scatter_dimension=0, tiled=True),
        lax.psum_scatter(grad_w_key, "dp", scatter_dimension=0, tiled=True),
        lax.psum_scatter(grad_w_value, "dp", scatter_dimension=0, tiled=True),
        lax.psum_scatter(grad_w_out, "dp", scatter_dimension=1, tiled=True),
    )

    def widen(part_vec, full_width):
        return lax.dynamic_update_slice_in_dim(
            jnp.zeros((full_width,), jnp.float32), part_vec, tensor_index * part_vec.shape[0], 0
        )

    small_sums = lax.psum(
        (
            widen(grad_b_query_part, b_query.shape[0]),
            widen(grad_b_value_part, b_value.shape[0]),
            grad_b_out,
            grad_gain_attn,
            grad_shift_attn,
            widen(grad_b_in_part, b_in.shape[0]),
            grad_b_back,
            grad_gain_ffn,
            grad_shift_ffn,
        ),
        ("dp", "tensor"),
    )
    return (
        output,
        grad_in,
        grad_w_query,
        small_sums[0],
        grad_w_key,
        grad_w_value,
        small_sums[1],
        grad_w_out,
        small_sums[2],
        small_sums[3],
        small_sums[4],
        grad_w_in,
        small_sums[5],
        grad_w_back,
        small_sums[6],
        small_sums[7],
        small_sums[8],
    )


MESH_ID = pl.DeviceIdType.MESH
F32 = jnp.float32
BF16 = jnp.bfloat16

SLOTS = 4
BLOCK = 128
GROUP = 512
WIDTH = 1024
HEAD_COLS = 256
HIDDEN = 1024
N_SEND = 58
N_GOT = 110
HALF = BLOCK // 2
HALVES = dict(q=(128, 256), k=(128, 256), v=(128, 256), o=(256, 128), i0=(128, 512), i1=(128, 512), b0=(512, 128),
              b1=(512, 128))
VECTORS = dict(bq=1024, bv=1024, bo=1024, ga=1024, sa=1024, bi=4096, bb=1024, gf=1024, sf=1024)


def flip(bit):
    return 1 - bit


def slot_step(t, j):
    return (t % 2 + j % 2) % 2 + 2 * ((t // 2 + j // 2) % 2)


def rows_of(r, count=BLOCK):
    return pl.ds(pl.multiple_of(r * BLOCK, BLOCK), count)


def cols_of(n, count=256):
    return pl.ds(pl.multiple_of(n * count, count), count)


def dot_nn(a, b):
    return jnp.dot(a, b, preferred_element_type=F32)


def dot_nt(a, b):
    return lax.dot_general(a, b, (((1,), (1,)), ((), ())), preferred_element_type=F32)


def dot_tn(a, b):
    return lax.dot_general(a, b, (((0,), (0,)), ((), ())), preferred_element_type=F32)


def scratch_table():
    act = lambda n: pltpu.VMEM((GROUP, n), BF16)
    table = dict(
        w3=pltpu.VMEM((3 * WIDTH, HEAD_COLS), BF16),
        wo=pltpu.VMEM((4, HEAD_COLS, 256), BF16),
        wi=pltpu.VMEM((WIDTH, HIDDEN), BF16),
        wb=pltpu.VMEM((4, HIDDEN, 256), BF16),
        w3t=pltpu.VMEM((3, HEAD_COLS, WIDTH), BF16),
        wot=pltpu.VMEM((WIDTH, HEAD_COLS), BF16),
        wit=pltpu.VMEM((HIDDEN, WIDTH), BF16),
        wbt=pltpu.VMEM((WIDTH, HIDDEN), BF16),
        lens_own=pltpu.VMEM((2, 8, 128), F32),
        lens_got=pltpu.VMEM((2, 8, 128), F32),
        lens_use=pltpu.VMEM((2, 8, 128), F32),
        tk=act(WIDTH),
        tkt=pltpu.VMEM((WIDTH, GROUP), BF16),
        cot_own=pltpu.VMEM((BLOCK, WIDTH), BF16),
        bias=pltpu.VMEM((GROUP, GROUP), F32),
        q=act(HEAD_COLS),
        qt=pltpu.VMEM((HEAD_COLS, GROUP), BF16),
        k=act(HEAD_COLS),
        ks=act(HEAD_COLS),
        v=act(HEAD_COLS),
        ps=pltpu.VMEM((4, GROUP, GROUP), BF16),
        ctx=act(HEAD_COLS),
        ctxt=pltpu.VMEM((HEAD_COLS, GROUP), BF16),
        hid=act(WIDTH),
        hidt=pltpu.VMEM((WIDTH, GROUP), BF16),
        act=act(HIDDEN),
        actt=pltpu.VMEM((HIDDEN, GROUP), BF16),
        slope=pltpu.VMEM((GROUP, HIDDEN), F32),
        g2=act(WIDTH),
        gpre=act(HIDDEN),
        g1=act(WIDTH),
        gctxt=pltpu.VMEM((HEAD_COLS, GROUP), BF16),
        dq=act(HEAD_COLS),
        dkt=pltpu.VMEM((HEAD_COLS, GROUP), F32),
        dvt=pltpu.VMEM((HEAD_COLS, GROUP), F32),
        dk=act(HEAD_COLS),
        dv=act(HEAD_COLS),
        hid1=pltpu.VMEM((BLOCK, WIDTH), F32),
        normed1=pltpu.VMEM((BLOCK, WIDTH), F32),
        inv1=pltpu.VMEM((BLOCK, 128), F32),
        g2f=pltpu.VMEM((BLOCK, WIDTH), F32),
        g1f=pltpu.VMEM((BLOCK, WIDTH), F32),
        out_own=pltpu.VMEM((BLOCK, WIDTH), BF16),
        gtok_own=pltpu.VMEM((BLOCK, WIDTH), BF16),
        rs_own=pltpu.VMEM((4, BLOCK, WIDTH), BF16),
        rs_out=pltpu.VMEM((4, 3, BLOCK, WIDTH), BF16),
        rs_got=pltpu.VMEM((4, 3, BLOCK, WIDTH), BF16),
        sums=pltpu.VMEM((6, 16, WIDTH), F32),
        sums_got=pltpu.VMEM((5, 16, WIDTH), F32),
        gb_in=pltpu.VMEM((1, HIDDEN), F32),
        vectors={name: pltpu.VMEM((1, width), F32) for name, width in VECTORS.items()},
        vsem=pltpu.SemaphoreType.DMA((len(VECTORS),)),
        g3=pltpu.VMEM((3 * WIDTH, HEAD_COLS), BF16),
        go=pltpu.VMEM((4, HEAD_COLS, 256), BF16),
        gi=pltpu.VMEM((WIDTH, HIDDEN), BF16),
        gb=pltpu.VMEM((4, HIDDEN, 256), BF16),
        stage={},
        ssem=pltpu.SemaphoreType.DMA((N_SEND,)),
        rsem=pltpu.SemaphoreType.DMA((N_GOT,)),
    )
    for name, dims in HALVES.items():
        table["stage"][name] = pltpu.VMEM((10,) + dims, BF16)
    return table


def layer_kernel(tok, lens, wq, bq, wk, wv, bv, wo, bo, ga, sa, wi, bi, wb, bb, gf, sf, cot, out, gtok, sums, zq, zk, zv,
                 zo, zi0, zi1, zb0, zb1, *scratch):
    a = SimpleNamespace(tok=tok, lens=lens, wq=wq, bq=bq, wk=wk, wv=wv, bv=bv, wo=wo, bo=bo, ga=ga, sa=sa, wi=wi, bi=bi,
                        wb=wb, bb=bb, gf=gf, sf=sf, cot=cot)
    o = SimpleNamespace(out=out, gtok=gtok, sums=sums)
    landed = dict(q=zq, k=zk, v=zv, o=zo, i0=zi0, i1=zi1, b0=zb0, b1=zb1)
    s = SimpleNamespace(**jax.tree.unflatten(jax.tree.structure(scratch_table()), scratch))
    ssem, rsem, vsem, vectors = s.ssem, s.rsem, s.vsem, s.vectors

    dp = lax.axis_index("dp")
    z = lax.axis_index("tensor")
    b, c = dp // 2, dp % 2
    zl, zh = z % 2, z // 2
    t = zl * 2 + c
    bx = b + 1 - 2 * (b % 2)
    by = (b + 2) % 4
    bd = 3 - b
    t1, t2, t3 = slot_step(t, 1), slot_step(t, 2), slot_step(t, 3)

    def dev(pos, core, zz):
        return (pos * 2 + core, zz)

    partner = dev(b, flip(c), z)
    z_near = z + 1 - 2 * (z % 2)
    z_far = (z + 2) % 4
    pair = dev(b, c, z_near)
    across = dev(b, c, z_far)
    x_near = dev(bx, c, z)
    y_near = dev(by, c, z)

    taken = {"s": 0, "r": 0}

    def take(kind, count=1):
        first = taken[kind]
        taken[kind] = first + count
        assert taken[kind] <= (N_SEND if kind == "s" else N_GOT)
        return first

    to_drain = []

    def make_copy(src, dst, device, sk, rk):
        return pltpu.make_async_remote_copy(
            src_ref=src, dst_ref=dst, send_sem=ssem.at[sk], recv_sem=rsem.at[rk], device_id=device,
            device_id_type=MESH_ID)

    def send(src, dst, device, sk, rk):
        make_copy(src, dst, device, sk, rk).start()

    def got(dst, rk):
        pltpu.make_async_copy(dst, dst, rsem.at[rk]).wait()

    def left(size_of, sk):
        pltpu.make_async_copy(size_of, size_of, ssem.at[sk]).wait()

    def at_end(size_of, sk, skipped=None, instead=None):
        to_drain.append((size_of, sk, skipped, instead))

    def send_or_keep(src, dst, device, is_self, sk, rk):
        copy = make_copy(src, dst, device, sk, rk)

        @pl.when(is_self)
        def _():
            pltpu.make_async_copy(src, dst, rsem.at[rk]).start()

        @pl.when(jnp.logical_not(is_self))
        def _():
            copy.start()

    barrier = pltpu.get_barrier_semaphore()
    peers = [x_near, y_near]
    for dz in range(4):
        for dc in range(2):
            if dz or dc:
                peers.append(dev(b, (c + dc) % 2, (z + dz) % 4))
    for peer in peers:
        pl.semaphore_signal(barrier, inc=1, device_id=peer, device_id_type=MESH_ID)
    pl.semaphore_wait(barrier, len(peers))

    def piece_qkv(m, home):
        base = m * WIDTH
        return SimpleNamespace(
            home=home,
            own=lambda bb, cc: s.w3.at[pl.ds(pl.multiple_of(base + bb * 256 + cc * 128, 128), 128), :],
            block=lambda bb: s.w3.at[pl.ds(pl.multiple_of(base + bb * 256, 256), 256), :],
            half=lambda bb, h: s.w3.at[pl.ds(pl.multiple_of(base + bb * 256 + h * 128, 128), 128), :])

    piece_o = SimpleNamespace(
        home=a.wo,
        own=lambda bb, cc: s.wo.at[bb, :, pl.ds(pl.multiple_of(cc * 128, 128), 128)],
        block=lambda bb: s.wo.at[bb],
        half=lambda bb, h: s.wo.at[bb, pl.ds(h * 128, 128), :])

    def piece_in(j):
        cols = pl.ds(j * 512, 512)
        return SimpleNamespace(
            home=a.wi.at[:, cols],
            own=lambda bb, cc: s.wi.at[pl.ds(pl.multiple_of(bb * 256 + cc * 128, 128), 128), cols],
            block=lambda bb: s.wi.at[pl.ds(pl.multiple_of(bb * 256, 256), 256), cols],
            half=lambda bb, h: s.wi.at[pl.ds(pl.multiple_of(bb * 256 + h * 128, 128), 128), cols])

    def piece_back(j):
        part = pl.ds(j * 512, 512)
        return SimpleNamespace(
            home=a.wb.at[part, :],
            own=lambda bb, cc: s.wb.at[bb, part, pl.ds(pl.multiple_of(cc * 128, 128), 128)],
            block=lambda bb: s.wb.at[bb, part, :],
            half=lambda bb, h: s.wb.at[bb, pl.ds(j * 512 + h * 256, 256), :])

    pieces = dict(q=piece_qkv(0, a.wq), k=piece_qkv(1, a.wk), v=piece_qkv(2, a.wv), o=piece_o,
                  i0=piece_in(0), i1=piece_in(1), b0=piece_back(0), b1=piece_back(1))
    first_size = dict(
        q=s.w3.at[0:768, :], k=s.w3.at[0:768, :], v=s.w3.at[0:768, :], o=s.wo.at[0:3], i0=s.wi.at[0:768, 0:512],
        i1=s.wi.at[0:768, 0:512], b0=s.wb.at[0:3, 0:512, :], b1=s.wb.at[0:3, 0:512, :])
    for name, piece in pieces.items():
        piece.s1, piece.r1 = take("s"), take("r")
        piece.s2, piece.r2 = take("s"), take("r", 3)
        keeps_one = jnp.logical_or(jnp.logical_and(z == 0, c == 0), jnp.logical_and(z == 3, c == 1))
        at_end(piece.block(b), piece.s1, keeps_one, piece.own(b, 0))
        at_end(first_size[name], piece.s2)

    def from_home(name):
        piece = pieces[name]
        for far in range(2):
            zt, ct = z // 2 + 2 * far, z % 2
            is_self = jnp.logical_and(zt == z, ct == c)
            send_or_keep(piece.home, piece.own(b, c), dev(b, ct, zt), is_self, piece.s1, piece.r1)

    def over_plane(name):
        piece = pieces[name]
        got(piece.block(b), piece.r1)
        send(piece.block(b), piece.block(b), x_near, piece.s2, piece.r2)
        send(piece.block(b), piece.block(b), y_near, piece.s2, piece.r2 + 1)

    def relay(name):
        piece = pieces[name]
        got(piece.block(bx), piece.r2)
        send(piece.half(bx, 0), piece.half(bx, 0), y_near, piece.s2, piece.r2 + 2)
        got(piece.block(by), piece.r2 + 1)
        send(piece.half(by, 1), piece.half(by, 1), x_near, piece.s2, piece.r2 + 2)

    def arrived(name):
        piece = pieces[name]
        got(piece.block(bd), piece.r2 + 2)

    tok_s, tok_r = take("s", 2), take("r", 4)
    fwd_s = take("s", 6)
    lens_s, lens_r = take("s"), take("r")
    cot_s, cot_r = take("s"), take("r")

    def send_lens():
        first = a.lens[0, 0].astype(F32)
        s.lens_own[0] = jnp.full((8, 128), first, F32)
        s.lens_own[1] = jnp.full((8, 128), first + a.lens[0, 1].astype(F32), F32)
        send(s.lens_own, s.lens_got, partner, lens_s, lens_r)
        at_end(s.lens_own, lens_s)

    def take_lens():
        got(s.lens_got, lens_r)

        @pl.when(c == zh)
        def _():
            s.lens_use[...] = s.lens_own[...]

        @pl.when(c != zh)
        def _():
            s.lens_use[...] = s.lens_got[...]

    def tok_block(r):
        return s.tk.at[rows_of(r), :]

    inner, outer = 1 + c, 3 * c
    is_relay = jnp.logical_and(c == zh, z == inner)
    is_inner = jnp.logical_and(z >= 1, z <= 2)

    def send_tokens():
        near = z // 2 == c
        first = jnp.where(near, 2 * c, inner)
        send_or_keep(a.tok, tok_block(z), dev(b, c, first), first == z, tok_s, tok_r + z)
        at_end(tok_block(z), tok_s, first == z)
        second = make_copy(a.tok, tok_block(z), dev(b, c, 2 * c + 1), tok_s + 1, tok_r + z)
        keep = jnp.logical_and(near, z == 2 * c + 1)
        go = jnp.logical_and(near, z != 2 * c + 1)

        @pl.when(keep)
        def _():
            pltpu.make_async_copy(a.tok, tok_block(z), rsem.at[tok_r + z]).start()

        @pl.when(go)
        def _():
            second.start()

        at_end(tok_block(z), tok_s + 1, jnp.logical_not(go))

    def pass_on(half, far):
        for k in range(2):
            r = half * 2 + k
            block = tok_block(r)
            got(block, tok_r + r)
            if far:
                on = make_copy(block, block, dev(b, c, outer), fwd_s + k, tok_r + r)

                @pl.when(is_relay)
                def _():
                    on.start()
            copy = make_copy(block, block, partner, fwd_s + 2 + 2 * far + k, tok_r + r)

            @pl.when(c == zh)
            def _():
                copy.start()

    for k in range(6):
        at_end(s.tk.at[0:BLOCK, :], fwd_s + k, jnp.logical_not(is_relay) if k < 2 else c != zh)

    def send_cotangent():
        zt, ct = 2 * c + z // 2, z % 2
        is_self = jnp.logical_and(zt == z, ct == c)
        send_or_keep(a.cot, s.cot_own, dev(b, ct, zt), is_self, cot_s, cot_r)
        at_end(s.cot_own, cot_s, is_self)

    gather_s, gather_r = take("s", 3), take("r", 12)
    scatter_s, scatter_r = take("s", 4), take("r", 20)
    for k in range(3):
        at_end(s.tk.at[0:3 * BLOCK, :], gather_s + k)
    for k in range(4):
        at_end(s.tk.at[0:3 * BLOCK, :], scatter_s + k)

    def block_at(full, r):
        return full.at[rows_of(r), :]

    def half_at(full, r, k):
        return full.at[pl.ds(pl.multiple_of(r * BLOCK + k * HALF, HALF), HALF), :]

    def gather_start(which, full, k):
        mine = half_at(full, t, k)
        send(mine, mine, pair, gather_s + which, gather_r + 4 * which + 1 + k)
        send(mine, mine, partner, gather_s + which, gather_r + 4 * which)

    def gather_step(which, full, j):
        base = gather_r + 4 * which

        @pl.when(j == 1)
        def _():
            got(block_at(full, t1), base)

        @pl.when(j == 2)
        def _():
            for k in range(2):
                near = half_at(full, t2, k)
                got(near, base + 1 + k)
                send(near, near, partner, gather_s + which, base + 3)

        @pl.when(j == 3)
        def _():
            got(block_at(full, t3), base + 3)

    halves = [pl.ds(k * HALF, HALF) for k in range(2)]

    def scatter(which, part):
        out, back = s.rs_out, s.rs_got
        ss, rr = scatter_s + which, scatter_r + 5 * which
        for k in range(2):
            mine = out.at[which, 0, halves[k], :]
            part(t3 * BLOCK + k * HALF, HALF, mine, None)
            send(mine, back.at[which, 0, halves[k], :], partner, ss, rr + k)
        for k in range(2):
            mine, theirs = out.at[which, 1, halves[k], :], back.at[which, 0, halves[k], :]
            got(theirs, rr + k)
            part(t2 * BLOCK + k * HALF, HALF, mine, theirs)
            send(mine, back.at[which, 1, halves[k], :], pair, ss, rr + 2 + k)
        part(t1 * BLOCK, BLOCK, out.at[which, 2], None)
        send(out.at[which, 2], back.at[which, 2], partner, ss, rr + 4)
        part(t * BLOCK, BLOCK, s.rs_own.at[which], None)

    def scatter_wait(which, k):
        rr = scatter_r + 5 * which
        if k == 0:
            got(s.rs_got.at[which, 2], rr + 4)
        got(s.rs_got.at[which, 1, halves[k], :], rr + 2 + k)

    def scatter_rows(which, chunk):
        total = s.rs_own[which, chunk, :].astype(F32) + s.rs_got[which, 2, chunk, :].astype(F32)
        return total + s.rs_got[which, 1, chunk, :].astype(F32)

    def by_halves(which, body, after):
        for k in range(2):
            scatter_wait(which, k)
            loop(2, lambda i: body(2 * k + i))
            after(k)

    def put_part(dst, add, n, value):
        cols = slice(256 * n, 256 * n + 256)
        value = value.astype(BF16)
        if add is not None:
            value = (value.astype(F32) + add[:, cols].astype(F32)).astype(BF16)
        dst[:, cols] = value

    def loop(count, body):
        lax.fori_loop(0, count, lambda i, _: (body(i), 0)[1], 0)

    def grad_qkv(m):
        base = m * WIDTH
        return lambda bb, h: s.g3.at[pl.ds(pl.multiple_of(base + bb * 256 + h * 128, 128), 128), :]

    def grad_in_part(k):
        cols = pl.ds(k * 512, 512)
        return lambda bb, h: s.gi.at[pl.ds(pl.multiple_of(bb * 256 + h * 128, 128), 128), cols]

    def grad_back_part(k):
        part = pl.ds(k * 512, 512)
        return lambda bb, h: s.gb.at[bb, part, pl.ds(h * 128, 128)]

    grad_half = dict(
        q=grad_qkv(0), k=grad_qkv(1), v=grad_qkv(2), o=lambda bb, h: s.go.at[bb, :, pl.ds(h * 128, 128)],
        i0=grad_in_part(0), i1=grad_in_part(1), b0=grad_back_part(0), b1=grad_back_part(1))
    grad_s = {name: take("s", 2) for name in grad_half}
    grad_r = {name: take("r", 4) for name in grad_half}
    keeps_part = jnp.logical_or(jnp.logical_and(z == 0, c == 0), jnp.logical_and(z == 3, c == 1))
    for name in grad_half:
        at_end(s.stage[name].at[0:6], grad_s[name])
        at_end(s.stage[name].at[0:2], grad_s[name] + 1, keeps_part, s.stage[name].at[0])

    def chunks(name, body):
        size = 64 if name in ("i0", "i1") else 128
        count = HALVES[name][0] // size
        loop(count, lambda i: body(pl.ds(pl.multiple_of(i * size, size), size)))

    def grad_first(name):
        half, ss, rr, st = grad_half[name], grad_s[name], grad_r[name], s.stage[name]
        send(half(bd, 0), st.at[1], x_near, ss, rr)
        send(half(bd, 1), st.at[3], y_near, ss, rr + 1)
        send(half(bx, 0), st.at[0], x_near, ss, rr + 2)
        send(half(by, 1), st.at[2], y_near, ss, rr + 2)

    def grad_second(name):
        half, ss, rr, st = grad_half[name], grad_s[name], grad_r[name], s.stage[name]
        for h, block, to in ((0, by, y_near), (1, bx, x_near)):
            got(st.at[1 + 2 * h], rr + h)
            mine = half(block, h)

            def add(ch):
                st[4 + h, ch, :] = (mine[ch, :].astype(F32) + st[1 + 2 * h, ch, :].astype(F32)).astype(BF16)
            chunks(name, add)
            send(st.at[4 + h], st.at[6 + h], to, ss, rr + 2)

    def grad_third(name):
        half, ss, rr, st = grad_half[name], grad_s[name], grad_r[name], s.stage[name]
        zr = landed[name]
        got(st.at[0:4], rr + 2)
        for h in range(2):
            mine = half(b, h)

            def add_all(ch):
                total = mine[ch, :].astype(F32) + st[2 * h, ch, :].astype(F32) + st[6 + h, ch, :].astype(F32)
                st[8 + h, ch, :] = total.astype(BF16)
            chunks(name, add_all)
            is_self = jnp.logical_and(c == h, z == t)
            send_or_keep(st.at[8 + h], zr.at[zh], dev(b, h, t), is_self, ss + 1, rr + 3)

    def grad_final(name):
        got(landed[name], grad_r[name] + 3)

    send_tokens()
    send_lens()
    for name, ref in vectors.items():
        pltpu.make_async_copy(getattr(a, name), ref, vsem.at[list(vectors).index(name)]).start()
    s.sums[0] = jnp.zeros((16, WIDTH), F32)
    s.gb_in[...] = jnp.zeros((1, HIDDEN), F32)
    s.dkt[...] = jnp.zeros((HEAD_COLS, GROUP), F32)
    s.dvt[...] = jnp.zeros((HEAD_COLS, GROUP), F32)
    pass_on(zh, 0)
    from_home("q")
    from_home("k")
    from_home("v")

    @pl.when(is_inner)
    def _():
        pass_on(flip(zh), 1)

    over_plane("q")
    from_home("o")
    from_home("i0")
    over_plane("k")
    over_plane("v")
    from_home("i1")

    @pl.when(jnp.logical_not(is_inner))
    def _():
        pass_on(flip(zh), 1)

    take_lens()
    for name, ref in vectors.items():
        pltpu.make_async_copy(getattr(a, name), ref, vsem.at[list(vectors).index(name)]).wait()
        setattr(a, name, ref)

    def make_bias(r):
        first, end = s.lens_use[0][0:1, 0:1], s.lens_use[1][0:1, 0:1]
        row = (lax.broadcasted_iota(jnp.int32, (BLOCK, GROUP), 0) + r * BLOCK).astype(F32)
        col = lax.broadcasted_iota(jnp.int32, (BLOCK, GROUP), 1).astype(F32)
        seg = lambda p: jnp.where(p >= end, 2.0, jnp.where(p >= first, 1.0, 0.0))
        s.bias[rows_of(r), :] = jnp.where(seg(row) == seg(col), 0.0, masked_value)
    loop(SLOTS, make_bias)
    relay("q")
    relay("k")
    relay("v")

    def turn_tokens(r):
        s.tkt[:, rows_of(r)] = s.tk[rows_of(r), :].T
    loop(SLOTS, turn_tokens)

    head_cols = pl.ds(pl.multiple_of(t * HEAD_COLS, HEAD_COLS), HEAD_COLS)

    def project(m):
        acc = dot_nn(s.tk[...], s.w3[m * WIDTH:(m + 1) * WIDTH, :])
        if m == 0:
            value = (acc + a.bq[:, head_cols]).astype(BF16)
            scaled = (value.astype(F32) * 0.125).astype(BF16)
            s.q[...] = scaled
            s.qt[...] = scaled.T
        elif m == 1:
            value = acc.astype(BF16)
            s.k[...] = value
            s.ks[...] = (value.astype(F32) * 0.125).astype(BF16)
        else:
            s.v[...] = (acc + a.bv[:, head_cols]).astype(BF16)

    from_home("b0")
    over_plane("o")
    over_plane("i0")
    for m, name in enumerate("qkv"):
        arrived(name)
        project(m)
    from_home("b1")
    relay("o")

    def attend(r):
        rows = rows_of(r)
        parts = []
        for h in range(4):
            cols = slice(64 * h, 64 * h + 64)
            scores = dot_nt(s.q[rows, cols], s.k[:, cols]) + s.bias[rows, :]
            top = jnp.max(scores, axis=-1, keepdims=True)
            weight = jnp.exp(scores - top)
            total = jnp.sum(weight, axis=-1, keepdims=True)
            prob = (weight * (1.0 / total)).astype(BF16)
            s.ps[h, rows, :] = prob
            parts.append(dot_nn(prob, s.v[:, cols]))
        context = jnp.concatenate(parts, axis=1).astype(BF16)
        s.ctx[rows, :] = context
        s.ctxt[:, rows] = context.T
    loop(2, attend)
    over_plane("i1")
    loop(2, lambda r: attend(r + 2))
    relay("i0")
    over_plane("b0")
    arrived("o")

    def attn_part(first, count, dst, add):
        rows = s.ctx[pl.ds(pl.multiple_of(first, HALF), count), :]
        for n in range(4):
            put_part(dst, add, n, dot_nn(rows, s.wo[n]))
    scatter(0, attn_part)
    relay("i1")
    over_plane("b1")
    for m in range(3):
        for n in range(4):
            s.w3t[m, :, 256 * n:256 * n + 256] = s.w3[m * WIDTH + 256 * n:m * WIDTH + 256 * n + 256, :].T
    for n in range(4):
        s.wot[256 * n:256 * n + 256, :] = s.wo[n].T

    CH = 32

    def own_chunk(i):
        return pl.ds(pl.multiple_of(i * CH, CH), CH)

    def group_chunk(i):
        return pl.ds(pl.multiple_of(t * BLOCK + i * CH, CH), CH)

    def norm_one(i):
        ch = own_chunk(i)
        resid = s.tk[group_chunk(i), :].astype(F32) + scatter_rows(0, ch) + a.bo[...]
        centered = resid - jnp.mean(resid, axis=-1, keepdims=True)
        inv = lax.rsqrt(jnp.mean(centered * centered, axis=-1, keepdims=True) + epsilon)
        normed = centered * inv
        hidden = normed * a.ga[...] + a.sa[...]
        s.normed1[ch, :] = normed
        s.inv1[ch, :] = jnp.broadcast_to(inv, (CH, 128))
        s.hid1[ch, :] = hidden
        s.hid[group_chunk(i), :] = hidden.astype(BF16)
    by_halves(0, norm_one, lambda k: gather_start(0, s.hid, k))
    send_cotangent()
    arrived("i0")
    arrived("i1")

    def ffn_in(j):
        gather_step(0, s.hid, j)
        r = slot_step(t, j)
        rows = rows_of(r)
        for n in range(4):
            cols = slice(256 * n, 256 * n + 256)
            bias = a.bi[:, pl.ds(pl.multiple_of(t * HIDDEN + n * 256, 256), 256)]
            pre = dot_nn(s.hid[rows, :], s.wi[:, cols]) + bias
            cdf = 0.5 * (1.0 + lax.erf(pre * 0.7071067811865476))
            pdf = jnp.exp(-0.5 * pre * pre) * 0.3989422804014327
            s.act[rows, cols] = (pre * cdf).astype(BF16)
            s.slope[rows, cols] = cdf + pre * pdf
    loop(SLOTS, ffn_in)

    def turn_ffn(r):
        rows = rows_of(r)
        s.actt[:, rows] = s.act[rows, :].T
        s.hidt[:, rows] = s.hid[rows, :].T
    relay("b0")
    loop(SLOTS, turn_ffn)

    def turn_wi(r):
        rows = rows_of(r)
        s.wit[:, rows] = s.wi[rows, :].T
    loop(8, turn_wi)
    relay("b1")
    arrived("b0")
    arrived("b1")

    def ffn_part(first, count, dst, add):
        rows = pl.ds(pl.multiple_of(first, HALF), count)
        for n in range(4):
            put_part(dst, add, n, dot_nn(s.act[rows, :], s.wb[n]))
    scatter(1, ffn_part)

    def turn_wb(r):
        rows = rows_of(r)
        for n in range(4):
            s.wbt[256 * n:256 * n + 256, rows] = s.wb[n, rows, :].T
    loop(8, turn_wb)
    got(s.cot_own, cot_r)

    def add_rows(row, value):
        s.sums[0, row:row + 1, :] += jnp.sum(value, axis=0, keepdims=True)

    def norm_two(i):
        ch = own_chunk(i)
        resid = s.hid1[ch, :] + scatter_rows(1, ch) + a.bb[...]
        centered = resid - jnp.mean(resid, axis=-1, keepdims=True)
        inv = lax.rsqrt(jnp.mean(centered * centered, axis=-1, keepdims=True) + epsilon)
        normed = centered * inv
        position = lax.broadcasted_iota(jnp.int32, (CH, 128), 0) + (t * BLOCK + i * CH)
        live = jnp.where(position.astype(F32) < s.lens_use[1][0:1, :], 1.0, 0.0)[:, 0:1]
        s.out_own[ch, :] = ((normed * a.gf[...] + a.sf[...]) * live).astype(BF16)
        grad = s.cot_own[ch, :].astype(F32) * live
        add_rows(4, grad * normed)
        add_rows(5, grad)
        u = grad * a.gf[...]
        first = jnp.mean(u, axis=-1, keepdims=True)
        second = jnp.mean(u * normed, axis=-1, keepdims=True)
        grad_two = inv * (u - first - normed * second)
        add_rows(3, grad_two)
        s.g2f[ch, :] = grad_two
        s.g2[group_chunk(i), :] = grad_two.astype(BF16)
    by_halves(1, norm_two, lambda k: gather_start(1, s.g2, k))
    out_s, out_r = take("s"), take("r")
    home_self = jnp.logical_and(zh == c, t == z)

    def ffn_back(j):
        gather_step(1, s.g2, j)
        r = slot_step(t, j)
        rows = rows_of(r)
        for n in range(4):
            cols = slice(256 * n, 256 * n + 256)
            grad = dot_nn(s.g2[rows, :], s.wbt[:, cols]) * s.slope[rows, cols]
            s.gb_in[:, cols] += jnp.sum(grad, axis=0, keepdims=True)
            s.gpre[rows, cols] = grad.astype(BF16)
    loop(SLOTS, ffn_back)
    send_or_keep(s.out_own, o.out, dev(b, zh, t), home_self, out_s, out_r)
    at_end(s.out_own, out_s, home_self)

    def grad_back(k):
        part = slice(512 * k, 512 * k + 512)

        def body(n):
            for e in range(2):
                block = n * 2 + e
                s.gb[block, part, :] = dot_nn(s.actt[part, :], s.g2[:, cols_of(block)]).astype(BF16)
        loop(2, body)

    def grad_in(k):
        cols = slice(512 * k, 512 * k + 512)

        def body(m):
            part = rows_of(m * 4, 512)
            s.gi[part, cols] = dot_nn(s.hidt[part, :], s.gpre[:, cols]).astype(BF16)
        loop(2, body)

    grad_back(0)
    grad_first("b0")
    grad_back(1)
    grad_first("b1")

    def in_part(first, count, dst, add):
        rows = pl.ds(pl.multiple_of(first, HALF), count)
        for n in range(4):
            put_part(dst, add, n, dot_nn(s.gpre[rows, :], s.wit[:, 256 * n:256 * n + 256]))
    scatter(2, in_part)
    grad_in(0)
    grad_in(1)
    grad_second("b0")
    grad_first("i0")

    def norm_one_back(i):
        ch = own_chunk(i)
        grad = s.g2f[ch, :] + scatter_rows(2, ch)
        normed = s.normed1[ch, :]
        add_rows(1, grad * normed)
        add_rows(2, grad)
        u = grad * a.ga[...]
        first = jnp.mean(u, axis=-1, keepdims=True)
        second = jnp.mean(u * normed, axis=-1, keepdims=True)
        grad_one = s.inv1[ch, 0:1] * (u - first - normed * second)
        add_rows(0, grad_one)
        s.g1f[ch, :] = grad_one
        s.g1[group_chunk(i), :] = grad_one.astype(BF16)
    by_halves(2, norm_one_back, lambda k: gather_start(2, s.g1, k))
    grad_second("b1")
    grad_first("i1")

    def attend_back(j):
        gather_step(2, s.g1, j)
        r = slot_step(t, j)
        rows = rows_of(r)
        grad_ctx = dot_nn(s.g1[rows, :], s.wot[...]).astype(BF16)
        s.gctxt[:, rows] = grad_ctx.T
        product = grad_ctx.astype(F32) * s.ctx[rows, :].astype(F32)
        parts = []
        for h in range(4):
            cols = slice(64 * h, 64 * h + 64)
            prob = s.ps[h, rows, :]
            delta = jnp.sum(product[:, cols], axis=-1, keepdims=True)
            grad_prob = dot_nt(grad_ctx[:, cols], s.v[:, cols])
            grad_score = (prob.astype(F32) * (grad_prob - delta)).astype(BF16)
            parts.append(dot_nn(grad_score, s.ks[:, cols]))
            s.dkt[cols, :] += dot_nn(s.qt[cols, rows], grad_score)
            s.dvt[cols, :] += dot_nn(s.gctxt[cols, rows], prob)
        grad_query = jnp.concatenate(parts, axis=1)
        for k in range(4):
            @pl.when(t == k)
            def _():
                s.sums[0, 6:7, 256 * k:256 * k + 256] += jnp.sum(grad_query, axis=0, keepdims=True)
        s.dq[rows, :] = grad_query.astype(BF16)
    loop(2, attend_back)
    grad_third("b0")
    loop(2, lambda j: attend_back(j + 2))
    grad_second("i0")
    grad_third("b1")

    def turn_back(r):
        rows = rows_of(r)
        s.dk[rows, :] = s.dkt[:, rows].T.astype(BF16)
        grad_value = s.dvt[:, rows].T
        for k in range(4):
            @pl.when(t == k)
            def _():
                s.sums[0, 7:8, 256 * k:256 * k + 256] += jnp.sum(grad_value, axis=0, keepdims=True)
        s.dv[rows, :] = grad_value.astype(BF16)
    loop(SLOTS, turn_back)
    for k in range(4):
        @pl.when(t == k)
        def _():
            s.sums[0, 8 + k:9 + k, :] = s.gb_in[...]

    sums_s, sums_r = take("s", 5), take("r", 5)
    sums_to = [partner, across, pair, x_near, y_near]

    def sums_start(k):
        send(s.sums.at[k], s.sums_got.at[k], sums_to[k], sums_s + k, sums_r + k)
        at_end(s.sums.at[k], sums_s + k)

    def sums_finish(k):
        got(s.sums_got.at[k], sums_r + k)
        total = s.sums[k] + s.sums_got[k]
        if k == 4:
            o.sums[...] = total
        else:
            s.sums[k + 1] = total

    sums_start(0)

    def tok_part(first, count, dst, add):
        rows = pl.ds(pl.multiple_of(first, HALF), count)
        for n in range(4):
            cols = slice(256 * n, 256 * n + 256)
            acc = dot_nn(s.dq[rows, :], s.w3t[0, :, cols])
            acc = acc + dot_nn(s.dk[rows, :], s.w3t[1, :, cols])
            acc = acc + dot_nn(s.dv[rows, :], s.w3t[2, :, cols])
            put_part(dst, add, n, acc)
    scatter(3, tok_part)
    sums_finish(0)
    sums_start(1)

    def grad_head(m, src):
        s.g3[m * WIDTH:(m + 1) * WIDTH, :] = dot_nn(s.tkt[...], src[...]).astype(BF16)

    for n in range(4):
        s.go[n] = dot_nn(s.ctxt[...], s.g1[:, 256 * n:256 * n + 256]).astype(BF16)
    grad_head(0, s.dq)
    grad_head(1, s.dk)
    grad_head(2, s.dv)
    grad_second("i1")
    grad_first("o")
    grad_first("q")
    grad_third("i0")
    grad_third("i1")
    grad_second("o")
    grad_first("k")

    def last_rows(i):
        ch = own_chunk(i)
        s.gtok_own[ch, :] = (s.g1f[ch, :] + scatter_rows(3, ch)).astype(BF16)
    by_halves(3, last_rows, lambda k: None)
    gtok_s, gtok_r = take("s"), take("r")
    send_or_keep(s.gtok_own, o.gtok, dev(b, zh, t), home_self, gtok_s, gtok_r)
    at_end(s.gtok_own, gtok_s, home_self)
    grad_second("q")
    grad_first("v")
    grad_third("o")
    sums_finish(1)
    sums_start(2)
    grad_second("k")
    grad_third("q")
    sums_finish(2)
    sums_start(3)
    grad_second("v")
    grad_third("k")
    grad_third("v")
    sums_finish(3)
    sums_start(4)
    grad_final("b0")
    grad_final("b1")
    grad_final("i0")
    grad_final("i1")
    got(o.gtok, gtok_r)
    got(o.out, out_r)
    grad_final("o")
    grad_final("q")
    sums_finish(4)
    grad_final("k")
    grad_final("v")

    for size_of, sk, skipped, instead in to_drain:
        if skipped is None:
            left(size_of, sk)
        else:
            @pl.when(jnp.logical_not(skipped))
            def _():
                left(size_of, sk)
            if instead is not None:
                @pl.when(skipped)
                def _():
                    left(instead, sk)


def result_kernel(out, gtok, sums, zq, zk, zv, zo, zi0, zi1, zb0, zb1, o_out, o_gtok, o_gq, o_gbq, o_gk, o_gv, o_gbv, o_go,
                  o_gbo, o_gga, o_gsa, o_gi, o_gbi, o_gb, o_gbb, o_ggf, o_gsf):
    both = lambda ref: ref[0].astype(F32) + ref[1].astype(F32)
    o_out[...] = out[...]
    o_gtok[...] = gtok[...].astype(F32)
    o_gq[...], o_gk[...], o_gv[...], o_go[...] = both(zq), both(zk), both(zv), both(zo)
    o_gi[:, :512], o_gi[:, 512:] = both(zi0), both(zi1)
    o_gb[:512, :], o_gb[512:, :] = both(zb0), both(zb1)
    for row, ref in ((6, o_gbq), (7, o_gbv), (0, o_gbo), (1, o_gga), (2, o_gsa), (3, o_gbb), (4, o_ggf), (5, o_gsf)):
        ref[...] = sums[row:row + 1, :]
    for k in range(4):
        o_gbi[:, WIDTH * k:WIDTH * k + WIDTH] = sums[8 + k:9 + k, :]


def on_device_fused(tokens, lengths, w_query, b_query, w_key, w_value, b_value, w_out, b_out, gain_attn, shift_attn,
                    w_in, b_in, w_back, b_back, gain_ffn, shift_ffn, cotangent):
    row = lambda vec: vec.reshape(1, -1)
    operands = (tokens, lengths, w_query, row(b_query), w_key, w_value, row(b_value), w_out, row(b_out),
                row(gain_attn), row(shift_attn), w_in, row(b_in), w_back, row(b_back), row(gain_ffn),
                row(shift_ffn), cotangent)
    vmem = pl.BlockSpec(memory_space=pltpu.VMEM)
    stay = pl.BlockSpec(memory_space=pl.ANY)
    in_specs = [stay] * len(operands)
    in_specs[1] = pl.BlockSpec(memory_space=pltpu.SMEM)
    shape = lambda dims, dtype: jax.ShapeDtypeStruct(dims, dtype)
    between = [shape(tokens.shape, BF16), shape(tokens.shape, BF16), shape((16, WIDTH), F32)]
    between += [shape((2,) + HALVES[name], BF16) for name in ("q", "k", "v", "o", "i0", "i1", "b0", "b1")]
    parts = pl.pallas_call(
        layer_kernel,
        out_shape=between,
        in_specs=in_specs,
        out_specs=[stay, stay, vmem] + [stay] * 8,
        scratch_shapes=jax.tree.leaves(scratch_table()),
        compiler_params=pltpu.CompilerParams(collective_id=0, has_side_effects=True, vmem_limit_bytes=64 * 1024 * 1000),
        name="layer",
    )(*operands)
    line = shape((1, WIDTH), F32)
    results = (
        shape(tokens.shape, BF16), shape(tokens.shape, F32), shape(w_query.shape, F32), line, shape(w_key.shape, F32),
        shape(w_value.shape, F32), line, shape(w_out.shape, F32), line, line, line, shape(w_in.shape, F32),
        shape((1, b_in.shape[0]), F32), shape(w_back.shape, F32), line, line, line)
    outs = pl.pallas_call(
        result_kernel,
        out_shape=results,
        in_specs=[vmem] * len(between),
        out_specs=[vmem] * len(results),
        name="results",
    )(*parts)
    return tuple(v.reshape(-1) if v.shape[0] == 1 else v for v in outs)


def fits_fused(mesh):
    return dict(mesh.shape) == {"dp": 8, "tensor": 4}


def solution(mesh):
    placed = (
        P(("dp", "tensor"), None),
        P("dp", None),
        P("dp", "tensor"),
        P(),
        P("dp", "tensor"),
        P("dp", "tensor"),
        P(),
        P("tensor", "dp"),
        P(),
        P(),
        P(),
        P("dp", "tensor"),
        P(),
        P("tensor", "dp"),
        P(),
        P(),
        P(),
        P(("dp", "tensor"), None),
    )
    on_device = on_device_fused if fits_fused(mesh) else on_device_plain
    return jax.shard_map(
        on_device,
        mesh=mesh,
        in_specs=placed,
        out_specs=(
            P(("dp", "tensor"), None),
            P(("dp", "tensor"), None),
            P("dp", "tensor"),
            P(),
            P("dp", "tensor"),
            P("dp", "tensor"),
            P(),
            P("tensor", "dp"),
            P(),
            P(),
            P(),
            P("dp", "tensor"),
            P(),
            P("tensor", "dp"),
            P(),
            P(),
            P(),
        ),
        check_vma=False,
    )
```

```python
from types import SimpleNamespace

import jax
import jax.numpy as jnp
from jax import lax
from jax.experimental import pallas as pl
from jax.experimental.pallas import tpu as pltpu
from jax.sharding import PartitionSpec as P

HD = 64


epsilon = 1e-06
masked_value = -1e30


def matmul_plain(left_side, right_side):
    return jnp.dot(left_side, right_side, preferred_element_type=jnp.float32)


def matmul_over_rows(left_side, right_side):
    return lax.dot_general(
        left_side, right_side, (((0,), (0,)), ((), ())), preferred_element_type=jnp.float32
    )


def matmul_over_cols(left_side, right_side):
    return lax.dot_general(
        left_side, right_side, (((1,), (1,)), ((), ())), preferred_element_type=jnp.float32
    )


def layer_norm(residual, gain_vec, shift_vec):
    mean_val = jnp.mean(residual, axis=-1, keepdims=True)
    centered = residual - mean_val
    inv_std = lax.rsqrt(jnp.mean(centered * centered, axis=-1, keepdims=True) + epsilon)
    normed = centered * inv_std
    return (normed * gain_vec + shift_vec, normed, inv_std)


def norm_back(grad_out, normed, inv_std, gain_vec):
    grad_norm = grad_out * gain_vec
    first_mean = jnp.mean(grad_norm, axis=-1, keepdims=True)
    second_mean = jnp.mean(grad_norm * normed, axis=-1, keepdims=True)
    return inv_std * (grad_norm - first_mean - normed * second_mean)


def gelu_parts(preact):
    cdf_val = 0.5 * (1.0 + lax.erf(preact * 0.7071067811865476))
    pdf_val = jnp.exp(-0.5 * preact * preact) * 0.3989422804014327
    return (preact * cdf_val, cdf_val + preact * pdf_val)


def attend_forward(query_rows, key_rows, value_rows, seg_ids, head_dim, block_rows):
    group_rows, head_cols = query_rows.shape
    pair_width = 2 * head_dim
    block_count = group_rows // block_rows
    pair_count = head_cols // pair_width
    score_scale = head_dim ** (-0.5)

    def attend_step(step_index, loop_carry):
        context, log_total = loop_carry
        pair_index = step_index // block_count
        row_start = step_index % block_count * block_rows
        first_col = pair_index * pair_width
        query_block = lax.dynamic_slice(
            query_rows, (row_start, first_col), (block_rows, pair_width)
        ).reshape(block_rows, 2, head_dim)
        key_pair = lax.dynamic_slice(key_rows, (0, first_col), (group_rows, pair_width)).reshape(
            group_rows, 2, head_dim
        )
        value_pair = lax.dynamic_slice(
            value_rows, (0, first_col), (group_rows, pair_width)
        ).reshape(group_rows, 2, head_dim)
        same_seg = seg_ids[:, None] == seg_ids[None, :]
        scores = (
            jnp.einsum("qhd,khd->hqk", query_block, key_pair, preferred_element_type=jnp.float32)
            * score_scale
        )
        scores = jnp.where(same_seg[None], scores, masked_value)
        row_max = jnp.max(scores, axis=-1, keepdims=True)
        block_total = row_max + jnp.log(jnp.sum(jnp.exp(scores - row_max), axis=-1, keepdims=True))
        prob_bf = jnp.exp(scores - block_total).astype(jnp.bfloat16)
        context_block = jnp.einsum(
            "hqk,khd->qhd", prob_bf, value_pair, preferred_element_type=jnp.float32
        ).astype(jnp.bfloat16)
        context = lax.dynamic_update_slice(
            context, context_block.reshape(block_rows, pair_width), (row_start, first_col)
        )
        log_total = lax.dynamic_update_slice(
            log_total, block_total[:, :, 0], (2 * pair_index, row_start)
        )
        return (context, log_total)

    start_carry = (
        jnp.zeros((group_rows, head_cols), jnp.bfloat16),
        jnp.zeros((head_cols // head_dim, group_rows), jnp.float32),
    )
    return lax.fori_loop(0, pair_count * block_count, attend_step, start_carry)


def attend_backward(
    query_rows,
    key_rows,
    value_rows,
    context,
    grad_context,
    log_total,
    seg_ids,
    head_dim,
    block_rows,
):
    group_rows, head_cols = query_rows.shape
    pair_width = 2 * head_dim
    block_count = group_rows // block_rows
    pair_count = head_cols // pair_width
    score_scale = head_dim ** (-0.5)

    def back_step(step_index, loop_carry):
        grad_query, grad_keys, grad_values = loop_carry
        pair_index = step_index // block_count
        row_start = step_index % block_count * block_rows
        first_col = pair_index * pair_width
        query_block = lax.dynamic_slice(
            query_rows, (row_start, first_col), (block_rows, pair_width)
        ).reshape(block_rows, 2, head_dim)
        key_pair = lax.dynamic_slice(key_rows, (0, first_col), (group_rows, pair_width)).reshape(
            group_rows, 2, head_dim
        )
        value_pair = lax.dynamic_slice(
            value_rows, (0, first_col), (group_rows, pair_width)
        ).reshape(group_rows, 2, head_dim)
        context_block = lax.dynamic_slice(
            context, (row_start, first_col), (block_rows, pair_width)
        ).reshape(block_rows, 2, head_dim)
        gctx_block = lax.dynamic_slice(
            grad_context, (row_start, first_col), (block_rows, pair_width)
        ).reshape(block_rows, 2, head_dim)
        total_block = lax.dynamic_slice(log_total, (2 * pair_index, row_start), (2, block_rows))
        same_seg = seg_ids[:, None] == seg_ids[None, :]
        scores = (
            jnp.einsum("qhd,khd->hqk", query_block, key_pair, preferred_element_type=jnp.float32)
            * score_scale
        )
        scores = jnp.where(same_seg[None], scores, masked_value)
        probs = jnp.exp(scores - total_block[:, :, None])
        prob_bf = probs.astype(jnp.bfloat16)
        grad_probs = jnp.einsum(
            "qhd,khd->hqk", gctx_block, value_pair, preferred_element_type=jnp.float32
        )
        delta_rows = jnp.sum(
            gctx_block.astype(jnp.float32) * context_block.astype(jnp.float32), axis=-1
        ).T[:, :, None]
        grad_scores = (probs * (grad_probs - delta_rows) * score_scale).astype(jnp.bfloat16)
        grad_q_block = jnp.einsum(
            "hqk,khd->qhd", grad_scores, key_pair, preferred_element_type=jnp.float32
        ).reshape(block_rows, pair_width)
        grad_k_pair = jnp.einsum(
            "hqk,qhd->khd", grad_scores, query_block, preferred_element_type=jnp.float32
        ).reshape(group_rows, pair_width)
        grad_v_pair = jnp.einsum(
            "hqk,qhd->khd", prob_bf, gctx_block, preferred_element_type=jnp.float32
        ).reshape(group_rows, pair_width)
        grad_query = lax.dynamic_update_slice(grad_query, grad_q_block, (row_start, first_col))
        old_keys = lax.dynamic_slice(grad_keys, (0, first_col), (group_rows, pair_width))
        grad_keys = lax.dynamic_update_slice(grad_keys, old_keys + grad_k_pair, (0, first_col))
        old_values = lax.dynamic_slice(grad_values, (0, first_col), (group_rows, pair_width))
        grad_values = lax.dynamic_update_slice(
            grad_values, old_values + grad_v_pair, (0, first_col)
        )
        return (grad_query, grad_keys, grad_values)

    zero_grad = jnp.zeros((group_rows, head_cols), jnp.float32)
    return lax.fori_loop(0, pair_count * block_count, back_step, (zero_grad, zero_grad, zero_grad))


def on_device_plain(
    tokens,
    lengths,
    w_query,
    b_query,
    w_key,
    w_value,
    b_value,
    w_out,
    b_out,
    gain_attn,
    shift_attn,
    w_in,
    b_in,
    w_back,
    b_back,
    gain_ffn,
    shift_ffn,
    cotangent,
):
    tensor_size = lax.axis_size("tensor")
    tensor_index = lax.axis_index("tensor")
    local_rows = tokens.shape[0]
    group_rows = local_rows * tensor_size
    head_cols = w_query.shape[1]
    hidden_cols = w_in.shape[1]
    block_rows = min(512, group_rows)
    seq_lens = lengths[0]
    live_end = seq_lens[0] + seq_lens[1]
    positions = jnp.arange(group_rows, dtype=jnp.int32)
    seg_ids = (positions >= seq_lens[0]).astype(jnp.int32) + (positions >= live_end).astype(
        jnp.int32
    )
    local_pos = tensor_index * local_rows + jnp.arange(local_rows, dtype=jnp.int32)
    live_rows = (local_pos < live_end).astype(jnp.float32)[:, None]
    rows_full = lax.all_gather(tokens, "tensor", axis=0, tiled=True)
    attn_mats = (
        lax.all_gather(w_query, "dp", axis=0, tiled=True),
        lax.all_gather(w_key, "dp", axis=0, tiled=True),
        lax.all_gather(w_value, "dp", axis=0, tiled=True),
        lax.all_gather(w_out, "dp", axis=1, tiled=True),
    )
    mat_query, mat_key, mat_value, mat_out = attn_mats
    bias_query = lax.dynamic_slice_in_dim(b_query, tensor_index * head_cols, head_cols)
    bias_value = lax.dynamic_slice_in_dim(b_value, tensor_index * head_cols, head_cols)
    bias_in = lax.dynamic_slice_in_dim(b_in, tensor_index * hidden_cols, hidden_cols)
    query_rows = (matmul_plain(rows_full, mat_query) + bias_query).astype(jnp.bfloat16)
    key_rows = matmul_plain(rows_full, mat_key).astype(jnp.bfloat16)
    value_rows = (matmul_plain(rows_full, mat_value) + bias_value).astype(jnp.bfloat16)
    context, log_total = attend_forward(query_rows, key_rows, value_rows, seg_ids, HD, block_rows)
    attn_sum = lax.psum_scatter(
        matmul_plain(context, mat_out).astype(jnp.bfloat16),
        "tensor",
        scatter_dimension=0,
        tiled=True,
    ).astype(jnp.float32)
    resid_one = tokens.astype(jnp.float32) + attn_sum + b_out
    hidden_one, normed_one, inv_one = layer_norm(resid_one, gain_attn, shift_attn)
    hidden_bf = hidden_one.astype(jnp.bfloat16)
    hidden_full = lax.all_gather(hidden_bf, "tensor", axis=0, tiled=True)
    ffn_mats = (
        lax.all_gather(w_in, "dp", axis=0, tiled=True),
        lax.all_gather(w_back, "dp", axis=1, tiled=True),
    )
    mat_in, mat_back = ffn_mats
    preact = matmul_plain(hidden_full, mat_in) + bias_in
    activ_val, gelu_slope = gelu_parts(preact)
    activation = activ_val.astype(jnp.bfloat16)
    ffn_sum = lax.psum_scatter(
        matmul_plain(activation, mat_back).astype(jnp.bfloat16),
        "tensor",
        scatter_dimension=0,
        tiled=True,
    ).astype(jnp.float32)
    resid_two = hidden_one + ffn_sum + b_back
    normed_out, normed_two, inv_two = layer_norm(resid_two, gain_ffn, shift_ffn)
    output = (normed_out * live_rows).astype(jnp.bfloat16)
    grad_final = cotangent.astype(jnp.float32) * live_rows
    grad_gain_ffn = jnp.sum(grad_final * normed_two, axis=0)
    grad_shift_ffn = jnp.sum(grad_final, axis=0)
    grad_two = norm_back(grad_final, normed_two, inv_two, gain_ffn)
    grad_b_back = jnp.sum(grad_two, axis=0)
    mat_query, mat_key, mat_value, mat_out, mat_in, mat_back = (
        lax.all_gather(w_query, "dp", axis=0, tiled=True),
        lax.all_gather(w_key, "dp", axis=0, tiled=True),
        lax.all_gather(w_value, "dp", axis=0, tiled=True),
        lax.all_gather(w_out, "dp", axis=1, tiled=True),
        lax.all_gather(w_in, "dp", axis=0, tiled=True),
        lax.all_gather(w_back, "dp", axis=1, tiled=True),
    )
    grad_two_full = lax.all_gather(grad_two.astype(jnp.bfloat16), "tensor", axis=0, tiled=True)
    grad_w_back = matmul_over_rows(activation, grad_two_full)
    grad_pre = matmul_over_cols(grad_two_full, mat_back) * gelu_slope
    grad_b_in_part = jnp.sum(grad_pre, axis=0)
    grad_pre_bf = grad_pre.astype(jnp.bfloat16)
    grad_w_in = matmul_over_rows(hidden_full, grad_pre_bf)
    grad_one_out = grad_two + lax.psum_scatter(
        matmul_over_cols(grad_pre_bf, mat_in).astype(jnp.bfloat16),
        "tensor",
        scatter_dimension=0,
        tiled=True,
    ).astype(jnp.float32)
    grad_w_in, grad_w_back = (
        lax.psum_scatter(grad_w_in, "dp", scatter_dimension=0, tiled=True),
        lax.psum_scatter(grad_w_back, "dp", scatter_dimension=1, tiled=True),
    )
    grad_gain_attn = jnp.sum(grad_one_out * normed_one, axis=0)
    grad_shift_attn = jnp.sum(grad_one_out, axis=0)
    grad_one = norm_back(grad_one_out, normed_one, inv_one, gain_attn)
    grad_b_out = jnp.sum(grad_one, axis=0)
    grad_one_full = lax.all_gather(grad_one.astype(jnp.bfloat16), "tensor", axis=0, tiled=True)
    grad_w_out = matmul_over_rows(context, grad_one_full)
    grad_context = matmul_over_cols(grad_one_full, mat_out).astype(jnp.bfloat16)
    grad_query, grad_keys, grad_values = attend_backward(
        query_rows, key_rows, value_rows, context, grad_context, log_total, seg_ids, HD, block_rows
    )
    grad_b_query_part = jnp.sum(grad_query, axis=0)
    grad_b_value_part = jnp.sum(grad_values, axis=0)
    grad_query_bf = grad_query.astype(jnp.bfloat16)
    grad_keys_bf = grad_keys.astype(jnp.bfloat16)
    grad_values_bf = grad_values.astype(jnp.bfloat16)
    grad_w_query = matmul_over_rows(rows_full, grad_query_bf)
    grad_w_key = matmul_over_rows(rows_full, grad_keys_bf)
    grad_w_value = matmul_over_rows(rows_full, grad_values_bf)
    query_part = matmul_over_cols(grad_query_bf, mat_query)
    key_part = matmul_over_cols(grad_keys_bf, mat_key)
    value_part = matmul_over_cols(grad_values_bf, mat_value)
    grad_in = grad_one + lax.psum_scatter(
        (query_part + key_part + value_part).astype(jnp.bfloat16),
        "tensor",
        scatter_dimension=0,
        tiled=True,
    ).astype(jnp.float32)
    grad_w_query, grad_w_key, grad_w_value, grad_w_out = (
        lax.psum_scatter(grad_w_query, "dp", scatter_dimension=0, tiled=True),
        lax.psum_scatter(grad_w_key, "dp", scatter_dimension=0, tiled=True),
        lax.psum_scatter(grad_w_value, "dp", scatter_dimension=0, tiled=True),
        lax.psum_scatter(grad_w_out, "dp", scatter_dimension=1, tiled=True),
    )

    def widen(part_vec, full_width):
        return lax.dynamic_update_slice_in_dim(
            jnp.zeros((full_width,), jnp.float32), part_vec, tensor_index * part_vec.shape[0], 0
        )

    small_sums = lax.psum(
        (
            widen(grad_b_query_part, b_query.shape[0]),
            widen(grad_b_value_part, b_value.shape[0]),
            grad_b_out,
            grad_gain_attn,
            grad_shift_attn,
            widen(grad_b_in_part, b_in.shape[0]),
            grad_b_back,
            grad_gain_ffn,
            grad_shift_ffn,
        ),
        ("dp", "tensor"),
    )
    return (
        output,
        grad_in,
        grad_w_query,
        small_sums[0],
        grad_w_key,
        grad_w_value,
        small_sums[1],
        grad_w_out,
        small_sums[2],
        small_sums[3],
        small_sums[4],
        grad_w_in,
        small_sums[5],
        grad_w_back,
        small_sums[6],
        small_sums[7],
        small_sums[8],
    )


MESH_ID = pl.DeviceIdType.MESH
F32 = jnp.float32
BF16 = jnp.bfloat16

SLOTS = 4
BLOCK = 128
GROUP = 512
WIDTH = 1024
HEAD_COLS = 256
HIDDEN = 1024
N_SEND = 58
N_GOT = 110
HALF = BLOCK // 2
HALVES = dict(q=(128, 256), k=(128, 256), v=(128, 256), o=(256, 128), i0=(128, 512), i1=(128, 512), b0=(512, 128),
              b1=(512, 128))
VECTORS = dict(bq=1024, bv=1024, bo=1024, ga=1024, sa=1024, bi=4096, bb=1024, gf=1024, sf=1024)


def flip(bit):
    return 1 - bit


def slot_step(t, j):
    return (t % 2 + j % 2) % 2 + 2 * ((t // 2 + j // 2) % 2)


def rows_of(r, count=BLOCK):
    return pl.ds(pl.multiple_of(r * BLOCK, BLOCK), count)


def cols_of(n, count=256):
    return pl.ds(pl.multiple_of(n * count, count), count)


def dot_nn(a, b):
    return jnp.dot(a, b, preferred_element_type=F32)


def dot_nt(a, b):
    return lax.dot_general(a, b, (((1,), (1,)), ((), ())), preferred_element_type=F32)


def dot_tn(a, b):
    return lax.dot_general(a, b, (((0,), (0,)), ((), ())), preferred_element_type=F32)


def scratch_table():
    act = lambda n: pltpu.VMEM((GROUP, n), BF16)
    table = dict(
        w3=pltpu.VMEM((3 * WIDTH, HEAD_COLS), BF16),
        wo=pltpu.VMEM((4, HEAD_COLS, 256), BF16),
        wi=pltpu.VMEM((WIDTH, HIDDEN), BF16),
        wb=pltpu.VMEM((4, HIDDEN, 256), BF16),
        w3t=pltpu.VMEM((3, HEAD_COLS, WIDTH), BF16),
        wot=pltpu.VMEM((WIDTH, HEAD_COLS), BF16),
        wit=pltpu.VMEM((HIDDEN, WIDTH), BF16),
        wbt=pltpu.VMEM((WIDTH, HIDDEN), BF16),
        lens_own=pltpu.VMEM((2, 8, 128), F32),
        lens_got=pltpu.VMEM((2, 8, 128), F32),
        lens_use=pltpu.VMEM((2, 8, 128), F32),
        tk=act(WIDTH),
        tkt=pltpu.VMEM((WIDTH, GROUP), BF16),
        cot_own=pltpu.VMEM((BLOCK, WIDTH), BF16),
        bias=pltpu.VMEM((GROUP, GROUP), F32),
        q=act(HEAD_COLS),
        qt=pltpu.VMEM((HEAD_COLS, GROUP), BF16),
        k=act(HEAD_COLS),
        ks=act(HEAD_COLS),
        v=act(HEAD_COLS),
        ps=pltpu.VMEM((4, GROUP, GROUP), BF16),
        ctx=act(HEAD_COLS),
        ctxt=pltpu.VMEM((HEAD_COLS, GROUP), BF16),
        hid=act(WIDTH),
        hidt=pltpu.VMEM((WIDTH, GROUP), BF16),
        act=act(HIDDEN),
        actt=pltpu.VMEM((HIDDEN, GROUP), BF16),
        slope=pltpu.VMEM((GROUP, HIDDEN), F32),
        g2=act(WIDTH),
        gpre=act(HIDDEN),
        g1=act(WIDTH),
        gctxt=pltpu.VMEM((HEAD_COLS, GROUP), BF16),
        dq=act(HEAD_COLS),
        dkt=pltpu.VMEM((HEAD_COLS, GROUP), F32),
        dvt=pltpu.VMEM((HEAD_COLS, GROUP), F32),
        dk=act(HEAD_COLS),
        dv=act(HEAD_COLS),
        hid1=pltpu.VMEM((BLOCK, WIDTH), F32),
        normed1=pltpu.VMEM((BLOCK, WIDTH), F32),
        inv1=pltpu.VMEM((BLOCK, 128), F32),
        g2f=pltpu.VMEM((BLOCK, WIDTH), F32),
        g1f=pltpu.VMEM((BLOCK, WIDTH), F32),
        out_own=pltpu.VMEM((BLOCK, WIDTH), BF16),
        gtok_own=pltpu.VMEM((BLOCK, WIDTH), BF16),
        rs_own=pltpu.VMEM((4, BLOCK, WIDTH), BF16),
        rs_out=pltpu.VMEM((4, 3, BLOCK, WIDTH), BF16),
        rs_got=pltpu.VMEM((4, 3, BLOCK, WIDTH), BF16),
        sums=pltpu.VMEM((6, 16, WIDTH), F32),
        sums_got=pltpu.VMEM((5, 16, WIDTH), F32),
        gb_in=pltpu.VMEM((1, HIDDEN), F32),
        vectors={name: pltpu.VMEM((1, width), F32) for name, width in VECTORS.items()},
        vsem=pltpu.SemaphoreType.DMA((len(VECTORS),)),
        turn=pltpu.SemaphoreType.REGULAR((4,)),
        g3=pltpu.VMEM((3 * WIDTH, HEAD_COLS), BF16),
        go=pltpu.VMEM((4, HEAD_COLS, 256), BF16),
        gi=pltpu.VMEM((WIDTH, HIDDEN), BF16),
        gb=pltpu.VMEM((4, HIDDEN, 256), BF16),
        stage={},
        ssem=pltpu.SemaphoreType.DMA((N_SEND,)),
        rsem=pltpu.SemaphoreType.DMA((N_GOT,)),
    )
    for name, dims in HALVES.items():
        table["stage"][name] = pltpu.VMEM((10,) + dims, BF16)
    return table


def layer_kernel(tok, lens, wq, bq, wk, wv, bv, wo, bo, ga, sa, wi, bi, wb, bb, gf, sf, cot, out, gtok, sums, zq, zk, zv,
                 zo, zi0, zi1, zb0, zb1, *scratch):
    a = SimpleNamespace(tok=tok, lens=lens, wq=wq, bq=bq, wk=wk, wv=wv, bv=bv, wo=wo, bo=bo, ga=ga, sa=sa, wi=wi, bi=bi,
                        wb=wb, bb=bb, gf=gf, sf=sf, cot=cot)
    o = SimpleNamespace(out=out, gtok=gtok, sums=sums)
    landed = dict(q=zq, k=zk, v=zv, o=zo, i0=zi0, i1=zi1, b0=zb0, b1=zb1)
    s = SimpleNamespace(**jax.tree.unflatten(jax.tree.structure(scratch_table()), scratch))
    ssem, rsem, vsem, vectors = s.ssem, s.rsem, s.vsem, s.vectors

    dp = lax.axis_index("dp")
    z = lax.axis_index("tensor")
    b, c = dp // 2, dp % 2
    zl, zh = z % 2, z // 2
    t = zl * 2 + c
    bx = b + 1 - 2 * (b % 2)
    by = (b + 2) % 4
    bd = 3 - b
    t1, t2, t3 = slot_step(t, 1), slot_step(t, 2), slot_step(t, 3)

    def dev(pos, core, zz):
        return (pos * 2 + core, zz)

    partner = dev(b, flip(c), z)
    z_near = z + 1 - 2 * (z % 2)
    z_far = (z + 2) % 4
    pair = dev(b, c, z_near)
    across = dev(b, c, z_far)
    x_near = dev(bx, c, z)
    y_near = dev(by, c, z)

    taken = {"s": 0, "r": 0}

    def take(kind, count=1):
        first = taken[kind]
        taken[kind] = first + count
        assert taken[kind] <= (N_SEND if kind == "s" else N_GOT)
        return first

    to_drain = []

    def make_copy(src, dst, device, sk, rk):
        return pltpu.make_async_remote_copy(
            src_ref=src, dst_ref=dst, send_sem=ssem.at[sk], recv_sem=rsem.at[rk], device_id=device,
            device_id_type=MESH_ID)

    def send(src, dst, device, sk, rk):
        make_copy(src, dst, device, sk, rk).start()

    def got(dst, rk):
        pltpu.make_async_copy(dst, dst, rsem.at[rk]).wait()

    def left(size_of, sk):
        pltpu.make_async_copy(size_of, size_of, ssem.at[sk]).wait()

    def at_end(size_of, sk, skipped=None, instead=None):
        to_drain.append((size_of, sk, skipped, instead))

    def send_or_keep(src, dst, device, is_self, sk, rk):
        copy = make_copy(src, dst, device, sk, rk)

        @pl.when(is_self)
        def _():
            pltpu.make_async_copy(src, dst, rsem.at[rk]).start()

        @pl.when(jnp.logical_not(is_self))
        def _():
            copy.start()

    barrier = pltpu.get_barrier_semaphore()
    peers = [x_near, y_near]
    for dz in range(4):
        for dc in range(2):
            if dz or dc:
                peers.append(dev(b, (c + dc) % 2, (z + dz) % 4))
    for peer in peers:
        pl.semaphore_signal(barrier, inc=1, device_id=peer, device_id_type=MESH_ID)
    pl.semaphore_wait(barrier, len(peers))

    def piece_qkv(m, home):
        base = m * WIDTH
        return SimpleNamespace(
            home=home,
            own=lambda bb, cc: s.w3.at[pl.ds(pl.multiple_of(base + bb * 256 + cc * 128, 128), 128), :],
            block=lambda bb: s.w3.at[pl.ds(pl.multiple_of(base + bb * 256, 256), 256), :],
            half=lambda bb, h: s.w3.at[pl.ds(pl.multiple_of(base + bb * 256 + h * 128, 128), 128), :])

    piece_o = SimpleNamespace(
        home=a.wo,
        own=lambda bb, cc: s.wo.at[bb, :, pl.ds(pl.multiple_of(cc * 128, 128), 128)],
        block=lambda bb: s.wo.at[bb],
        half=lambda bb, h: s.wo.at[bb, pl.ds(h * 128, 128), :])

    def piece_in(j):
        cols = pl.ds(j * 512, 512)
        return SimpleNamespace(
            home=a.wi.at[:, cols],
            own=lambda bb, cc: s.wi.at[pl.ds(pl.multiple_of(bb * 256 + cc * 128, 128), 128), cols],
            block=lambda bb: s.wi.at[pl.ds(pl.multiple_of(bb * 256, 256), 256), cols],
            half=lambda bb, h: s.wi.at[pl.ds(pl.multiple_of(bb * 256 + h * 128, 128), 128), cols])

    def piece_back(j):
        part = pl.ds(j * 512, 512)
        return SimpleNamespace(
            home=a.wb.at[part, :],
            own=lambda bb, cc: s.wb.at[bb, part, pl.ds(pl.multiple_of(cc * 128, 128), 128)],
            block=lambda bb: s.wb.at[bb, part, :],
            half=lambda bb, h: s.wb.at[bb, pl.ds(j * 512 + h * 256, 256), :])

    pieces = dict(q=piece_qkv(0, a.wq), k=piece_qkv(1, a.wk), v=piece_qkv(2, a.wv), o=piece_o,
                  i0=piece_in(0), i1=piece_in(1), b0=piece_back(0), b1=piece_back(1))
    first_size = dict(
        q=s.w3.at[0:768, :], k=s.w3.at[0:768, :], v=s.w3.at[0:768, :], o=s.wo.at[0:3], i0=s.wi.at[0:768, 0:512],
        i1=s.wi.at[0:768, 0:512], b0=s.wb.at[0:3, 0:512, :], b1=s.wb.at[0:3, 0:512, :])
    for name, piece in pieces.items():
        piece.s1, piece.r1 = take("s"), take("r")
        piece.s2, piece.r2 = take("s"), take("r", 3)
        keeps_one = jnp.logical_or(jnp.logical_and(z == 0, c == 0), jnp.logical_and(z == 3, c == 1))
        at_end(piece.block(b), piece.s1, keeps_one, piece.own(b, 0))
        at_end(first_size[name], piece.s2)

    def to_outer(name):
        piece = pieces[name]
        is_self = jnp.logical_and(z == 3 * zh, z % 2 == c)
        send_or_keep(piece.home, piece.own(b, c), dev(b, z % 2, 3 * zh), is_self, piece.s1, piece.r1)

    def to_inner(name):
        piece = pieces[name]
        send(piece.home, piece.own(b, c), dev(b, z % 2, 2 - zh), piece.s1, piece.r1)

    def from_home(name):
        to_inner(name)
        to_outer(name)

    def over_plane(name):
        piece = pieces[name]
        got(piece.block(b), piece.r1)
        send(piece.block(b), piece.block(b), x_near, piece.s2, piece.r2)
        send(piece.block(b), piece.block(b), y_near, piece.s2, piece.r2 + 1)

    def relay(name):
        piece = pieces[name]
        got(piece.block(bx), piece.r2)
        send(piece.half(bx, 0), piece.half(bx, 0), y_near, piece.s2, piece.r2 + 2)
        got(piece.block(by), piece.r2 + 1)
        send(piece.half(by, 1), piece.half(by, 1), x_near, piece.s2, piece.r2 + 2)

    def arrived(name):
        piece = pieces[name]
        got(piece.block(bd), piece.r2 + 2)

    tok_s, tok_r = take("s", 2), take("r", 4)
    fwd_s = take("s", 6)
    lens_s, lens_r = take("s"), take("r")
    cot_s, cot_r = take("s"), take("r")

    def send_lens():
        first = a.lens[0, 0].astype(F32)
        s.lens_own[0] = jnp.full((8, 128), first, F32)
        s.lens_own[1] = jnp.full((8, 128), first + a.lens[0, 1].astype(F32), F32)
        send(s.lens_own, s.lens_got, partner, lens_s, lens_r)
        at_end(s.lens_own, lens_s)

    def take_lens():
        got(s.lens_got, lens_r)

        @pl.when(c == zh)
        def _():
            s.lens_use[...] = s.lens_own[...]

        @pl.when(c != zh)
        def _():
            s.lens_use[...] = s.lens_got[...]

    def tok_block(r):
        return s.tk.at[rows_of(r), :]

    inner, outer = 1 + c, 3 * c
    is_relay = jnp.logical_and(c == zh, z == inner)
    is_inner = jnp.logical_and(z >= 1, z <= 2)

    def send_tokens():
        near = z // 2 == c
        first = jnp.where(near, 2 * c, inner)
        send_or_keep(a.tok, tok_block(z), dev(b, c, first), first == z, tok_s, tok_r + z)
        at_end(tok_block(z), tok_s, first == z)
        second = make_copy(a.tok, tok_block(z), dev(b, c, 2 * c + 1), tok_s + 1, tok_r + z)
        keep = jnp.logical_and(near, z == 2 * c + 1)
        go = jnp.logical_and(near, z != 2 * c + 1)

        @pl.when(keep)
        def _():
            pltpu.make_async_copy(a.tok, tok_block(z), rsem.at[tok_r + z]).start()

        @pl.when(go)
        def _():
            second.start()

        at_end(tok_block(z), tok_s + 1, jnp.logical_not(go))

    def pass_on(half, far):
        for k in range(2):
            r = half * 2 + k
            block = tok_block(r)
            got(block, tok_r + r)
            if far:
                on = make_copy(block, block, dev(b, c, outer), fwd_s + k, tok_r + r)

                @pl.when(is_relay)
                def _():
                    on.start()
            copy = make_copy(block, block, partner, fwd_s + 2 + 2 * far + k, tok_r + r)

            @pl.when(c == zh)
            def _():
                copy.start()

    for k in range(6):
        at_end(s.tk.at[0:BLOCK, :], fwd_s + k, jnp.logical_not(is_relay) if k < 2 else c != zh)

    def send_cotangent():
        zt, ct = 2 * c + z // 2, z % 2
        is_self = jnp.logical_and(zt == z, ct == c)
        send_or_keep(a.cot, s.cot_own, dev(b, ct, zt), is_self, cot_s, cot_r)
        at_end(s.cot_own, cot_s, is_self)

    gather_s, gather_r = take("s", 3), take("r", 12)
    scatter_s, scatter_r = take("s", 4), take("r", 20)
    for k in range(3):
        at_end(s.tk.at[0:3 * BLOCK, :], gather_s + k)
    for k in range(4):
        at_end(s.tk.at[0:3 * BLOCK, :], scatter_s + k)

    def block_at(full, r):
        return full.at[rows_of(r), :]

    def half_at(full, r, k):
        return full.at[pl.ds(pl.multiple_of(r * BLOCK + k * HALF, HALF), HALF), :]

    def gather_start(which, full, k):
        mine = half_at(full, t, k)
        send(mine, mine, pair, gather_s + which, gather_r + 4 * which + 1 + k)
        send(mine, mine, partner, gather_s + which, gather_r + 4 * which)

    def gather_step(which, full, j):
        base = gather_r + 4 * which

        @pl.when(j == 1)
        def _():
            got(block_at(full, t1), base)

        @pl.when(j == 2)
        def _():
            for k in range(2):
                near = half_at(full, t2, k)
                got(near, base + 1 + k)
                send(near, near, partner, gather_s + which, base + 3)

        @pl.when(j == 3)
        def _():
            got(block_at(full, t3), base + 3)

    halves = [pl.ds(k * HALF, HALF) for k in range(2)]

    def scatter(which, part):
        out, back = s.rs_out, s.rs_got
        ss, rr = scatter_s + which, scatter_r + 5 * which
        for k in range(2):
            mine = out.at[which, 0, halves[k], :]
            part(t3 * BLOCK + k * HALF, HALF, mine, None)
            send(mine, back.at[which, 0, halves[k], :], partner, ss, rr + k)
        for k in range(2):
            mine, theirs = out.at[which, 1, halves[k], :], back.at[which, 0, halves[k], :]
            got(theirs, rr + k)
            part(t2 * BLOCK + k * HALF, HALF, mine, theirs)
            send(mine, back.at[which, 1, halves[k], :], pair, ss, rr + 2 + k)
        part(t1 * BLOCK, BLOCK, out.at[which, 2], None)
        send(out.at[which, 2], back.at[which, 2], partner, ss, rr + 4)
        part(t * BLOCK, BLOCK, s.rs_own.at[which], None)

    def scatter_cols(which, blocks, k):
        out, back = s.rs_out, s.rs_got
        ss, rr = scatter_s + which, scatter_r + 5 * which
        slots = [pl.ds(pl.multiple_of(block * 256, 256), 256) for block in blocks]
        size = s.rs_got.at[which, 0, :, 0:256 * len(blocks)]

        def product(row, block):
            rows = pl.ds(pl.multiple_of(row * BLOCK, BLOCK), BLOCK)
            return dot_nn(s.act[rows, :], s.wb[block])

        def cast(row, slot):
            for block, cols in zip(blocks, slots):
                out[which, slot, :, cols] = product(row, block).astype(BF16)

        cast(t3, 0)
        for cols in slots:
            send(out.at[which, 0, :, cols], back.at[which, 0, :, cols], partner, ss, rr + k)
        cast(t1, 2)
        for cols in slots:
            send(out.at[which, 2, :, cols], back.at[which, 2, :, cols], partner, ss, rr + 4)
        got(size, rr + k)
        for block, cols in zip(blocks, slots):
            total = product(t2, block).astype(BF16).astype(F32) + back[which, 0, :, cols].astype(F32)
            out[which, 1, :, cols] = total.astype(BF16)
            send(out.at[which, 1, :, cols], back.at[which, 1, :, cols], pair, ss, rr + 2)
        for block, cols in zip(blocks, slots):
            s.rs_own[which, :, cols] = product(t, block).astype(BF16)

    def scatter_cols_wait(which):
        rr = scatter_r + 5 * which
        got(s.rs_got.at[which, 2], rr + 4)
        got(s.rs_got.at[which, 1], rr + 2)

    def scatter_wait(which, k):
        rr = scatter_r + 5 * which
        if k == 0:
            got(s.rs_got.at[which, 2], rr + 4)
        got(s.rs_got.at[which, 1, halves[k], :], rr + 2 + k)

    def scatter_rows(which, chunk):
        total = s.rs_own[which, chunk, :].astype(F32) + s.rs_got[which, 2, chunk, :].astype(F32)
        return total + s.rs_got[which, 1, chunk, :].astype(F32)

    def by_halves(which, body, after):
        if which == 1:
            scatter_cols_wait(which)
        for k in range(2):
            if which != 1:
                scatter_wait(which, k)
            loop(2, lambda i: body(2 * k + i))
            after(k)

    def put_part(dst, add, n, value):
        cols = slice(256 * n, 256 * n + 256)
        value = value.astype(BF16)
        if add is not None:
            value = (value.astype(F32) + add[:, cols].astype(F32)).astype(BF16)
        dst[:, cols] = value

    def loop(count, body):
        lax.fori_loop(0, count, lambda i, _: (body(i), 0)[1], 0)

    def grad_qkv(m):
        base = m * WIDTH
        return lambda bb, h: s.g3.at[pl.ds(pl.multiple_of(base + bb * 256 + h * 128, 128), 128), :]

    def grad_in_part(k):
        cols = pl.ds(k * 512, 512)
        return lambda bb, h: s.gi.at[pl.ds(pl.multiple_of(bb * 256 + h * 128, 128), 128), cols]

    def grad_back_part(k):
        part = pl.ds(k * 512, 512)
        return lambda bb, h: s.gb.at[bb, part, pl.ds(h * 128, 128)]

    grad_half = dict(
        q=grad_qkv(0), k=grad_qkv(1), v=grad_qkv(2), o=lambda bb, h: s.go.at[bb, :, pl.ds(h * 128, 128)],
        i0=grad_in_part(0), i1=grad_in_part(1), b0=grad_back_part(0), b1=grad_back_part(1))
    grad_s = {name: take("s", 2) for name in grad_half}
    grad_r = {name: take("r", 4) for name in grad_half}
    keeps_part = jnp.logical_or(jnp.logical_and(z == 0, c == 0), jnp.logical_and(z == 3, c == 1))
    for name in grad_half:
        at_end(s.stage[name].at[0:6], grad_s[name])
        at_end(s.stage[name].at[0:2], grad_s[name] + 1, keeps_part, s.stage[name].at[0])

    def chunks(name, body):
        size = 64 if name in ("i0", "i1") else 128
        count = HALVES[name][0] // size
        loop(count, lambda i: body(pl.ds(pl.multiple_of(i * size, size), size)))

    def grad_first(name, part=2):
        half, ss, rr, st = grad_half[name], grad_s[name], grad_r[name], s.stage[name]
        if part in (0, 2):
            send(half(bd, 0), st.at[1], x_near, ss, rr)
            send(half(bd, 1), st.at[3], y_near, ss, rr + 1)
        if part == 0:
            return
        send(half(bx, 0), st.at[0], x_near, ss, rr + 2)
        send(half(by, 1), st.at[2], y_near, ss, rr + 2)

    def grad_second(name):
        half, ss, rr, st = grad_half[name], grad_s[name], grad_r[name], s.stage[name]
        for h, block, to in ((0, by, y_near), (1, bx, x_near)):
            got(st.at[1 + 2 * h], rr + h)
            mine = half(block, h)

            def add(ch):
                st[4 + h, ch, :] = (mine[ch, :].astype(F32) + st[1 + 2 * h, ch, :].astype(F32)).astype(BF16)
            chunks(name, add)
            send(st.at[4 + h], st.at[6 + h], to, ss, rr + 2)

    def grad_third(name):
        half, ss, rr, st = grad_half[name], grad_s[name], grad_r[name], s.stage[name]
        zr = landed[name]
        got(st.at[0:4], rr + 2)
        for h in range(2):
            mine = half(b, h)

            def add_all(ch):
                total = mine[ch, :].astype(F32) + st[2 * h, ch, :].astype(F32) + st[6 + h, ch, :].astype(F32)
                st[8 + h, ch, :] = total.astype(BF16)
            chunks(name, add_all)
            is_self = jnp.logical_and(c == h, z == t)
            send_or_keep(st.at[8 + h], zr.at[zh], dev(b, h, t), is_self, ss + 1, rr + 3)

    def grad_final(name):
        got(landed[name], grad_r[name] + 3)

    to_inner("q")
    to_inner("k")
    send_tokens()
    to_inner("v")
    for name in "qkv":
        to_outer(name)
    send_lens()
    for name, ref in vectors.items():
        pltpu.make_async_copy(getattr(a, name), ref, vsem.at[list(vectors).index(name)]).start()
    s.sums[0] = jnp.zeros((16, WIDTH), F32)
    s.gb_in[...] = jnp.zeros((1, HIDDEN), F32)
    s.dkt[...] = jnp.zeros((HEAD_COLS, GROUP), F32)
    s.dvt[...] = jnp.zeros((HEAD_COLS, GROUP), F32)
    def in_turn(k):
        @pl.when(is_inner)
        def _():
            pl.semaphore_signal(s.turn.at[k], inc=1, device_id=pair, device_id_type=MESH_ID)

        @pl.when(jnp.logical_not(is_inner))
        def _():
            pl.semaphore_wait(s.turn.at[k], 1)

    over_plane("q")
    over_plane("k")
    relay("q")
    pass_on(zh, 0)
    to_inner("o")

    @pl.when(is_inner)
    def _():
        pass_on(flip(zh), 1)

    in_turn(0)
    to_inner("i0")
    take_lens()

    def make_bias(r):
        first, end = s.lens_use[0][0:1, 0:1], s.lens_use[1][0:1, 0:1]
        row = (lax.broadcasted_iota(jnp.int32, (BLOCK, GROUP), 0) + r * BLOCK).astype(F32)
        col = lax.broadcasted_iota(jnp.int32, (BLOCK, GROUP), 1).astype(F32)
        seg = lambda p: jnp.where(p >= end, 2.0, jnp.where(p >= first, 1.0, 0.0))
        s.bias[rows_of(r), :] = jnp.where(seg(row) == seg(col), 0.0, masked_value)
    loop(SLOTS, make_bias)
    for name, ref in vectors.items():
        pltpu.make_async_copy(getattr(a, name), ref, vsem.at[list(vectors).index(name)]).wait()
        setattr(a, name, ref)
    relay("k")
    over_plane("v")
    relay("v")

    @pl.when(is_inner)
    def _():
        over_plane("o")

    @pl.when(jnp.logical_not(is_inner))
    def _():
        pass_on(flip(zh), 1)

    in_turn(1)
    to_outer("o")
    to_outer("i0")
    to_inner("i1")

    @pl.when(jnp.logical_not(is_inner))
    def _():
        over_plane("o")


    def turn_tokens(r):
        s.tkt[:, rows_of(r)] = s.tk[rows_of(r), :].T
    loop(SLOTS, turn_tokens)

    head_cols = pl.ds(pl.multiple_of(t * HEAD_COLS, HEAD_COLS), HEAD_COLS)

    def project(m):
        acc = dot_nn(s.tk[...], s.w3[m * WIDTH:(m + 1) * WIDTH, :])
        if m == 0:
            value = (acc + a.bq[:, head_cols]).astype(BF16)
            scaled = (value.astype(F32) * 0.125).astype(BF16)
            s.q[...] = scaled
            s.qt[...] = scaled.T
        elif m == 1:
            value = acc.astype(BF16)
            s.k[...] = value
            s.ks[...] = (value.astype(F32) * 0.125).astype(BF16)
        else:
            s.v[...] = (acc + a.bv[:, head_cols]).astype(BF16)

    arrived("q")
    project(0)
    arrived("k")
    project(1)
    over_plane("i0")
    in_turn(2)
    to_outer("i1")
    to_inner("b0")
    arrived("v")
    project(2)

    def attend(r):
        rows = rows_of(r)
        parts = []
        for h in range(4):
            cols = slice(64 * h, 64 * h + 64)
            scores = dot_nt(s.q[rows, cols], s.k[:, cols]) + s.bias[rows, :]
            top = jnp.max(scores, axis=-1, keepdims=True)
            weight = jnp.exp(scores - top)
            total = jnp.sum(weight, axis=-1, keepdims=True)
            prob = (weight * (1.0 / total)).astype(BF16)
            s.ps[h, rows, :] = prob
            parts.append(dot_nn(prob, s.v[:, cols]))
        context = jnp.concatenate(parts, axis=1).astype(BF16)
        s.ctx[rows, :] = context
        s.ctxt[:, rows] = context.T
    loop(2, attend)
    relay("o")
    over_plane("i1")
    in_turn(3)
    to_outer("b0")
    from_home("b1")
    loop(2, lambda r: attend(r + 2))
    relay("i0")
    over_plane("b0")
    arrived("o")

    def attn_part(first, count, dst, add):
        rows = s.ctx[pl.ds(pl.multiple_of(first, HALF), count), :]
        for n in range(4):
            put_part(dst, add, n, dot_nn(rows, s.wo[n]))
    scatter(0, attn_part)
    relay("i1")
    for m in range(3):
        for n in range(4):
            s.w3t[m, :, 256 * n:256 * n + 256] = s.w3[m * WIDTH + 256 * n:m * WIDTH + 256 * n + 256, :].T
    for n in range(4):
        s.wot[256 * n:256 * n + 256, :] = s.wo[n].T

    CH = 32

    def own_chunk(i):
        return pl.ds(pl.multiple_of(i * CH, CH), CH)

    def group_chunk(i):
        return pl.ds(pl.multiple_of(t * BLOCK + i * CH, CH), CH)

    def norm_one(i):
        ch = own_chunk(i)
        resid = s.tk[group_chunk(i), :].astype(F32) + scatter_rows(0, ch) + a.bo[...]
        centered = resid - jnp.mean(resid, axis=-1, keepdims=True)
        inv = lax.rsqrt(jnp.mean(centered * centered, axis=-1, keepdims=True) + epsilon)
        normed = centered * inv
        hidden = normed * a.ga[...] + a.sa[...]
        s.normed1[ch, :] = normed
        s.inv1[ch, :] = jnp.broadcast_to(inv, (CH, 128))
        s.hid1[ch, :] = hidden
        s.hid[group_chunk(i), :] = hidden.astype(BF16)
    over_plane("b1")
    by_halves(0, norm_one, lambda k: gather_start(0, s.hid, k))
    send_cotangent()
    relay("b0")
    arrived("i0")
    arrived("i1")

    def ffn_in(j):
        gather_step(0, s.hid, j)
        r = slot_step(t, j)
        rows = rows_of(r)
        for n in range(4):
            cols = slice(256 * n, 256 * n + 256)
            bias = a.bi[:, pl.ds(pl.multiple_of(t * HIDDEN + n * 256, 256), 256)]
            pre = dot_nn(s.hid[rows, :], s.wi[:, cols]) + bias
            cdf = 0.5 * (1.0 + lax.erf(pre * 0.7071067811865476))
            pdf = jnp.exp(-0.5 * pre * pre) * 0.3989422804014327
            s.act[rows, cols] = (pre * cdf).astype(BF16)
            s.slope[rows, cols] = cdf + pre * pdf
    loop(SLOTS, ffn_in)

    def turn_ffn(r):
        rows = rows_of(r)
        s.actt[:, rows] = s.act[rows, :].T
        s.hidt[:, rows] = s.hid[rows, :].T
    relay("b1")
    scatter_cols(1, (b, bx, by), 0)
    loop(SLOTS, turn_ffn)

    def turn_wi(r):
        rows = rows_of(r)
        s.wit[:, rows] = s.wi[rows, :].T
    loop(8, turn_wi)
    arrived("b0")
    arrived("b1")
    scatter_cols(1, (bd,), 1)

    def turn_wb(r):
        rows = rows_of(r)
        for n in range(4):
            s.wbt[256 * n:256 * n + 256, rows] = s.wb[n, rows, :].T
    loop(8, turn_wb)
    got(s.cot_own, cot_r)

    def add_rows(row, value):
        s.sums[0, row:row + 1, :] += jnp.sum(value, axis=0, keepdims=True)

    def norm_two(i):
        ch = own_chunk(i)
        resid = s.hid1[ch, :] + scatter_rows(1, ch) + a.bb[...]
        centered = resid - jnp.mean(resid, axis=-1, keepdims=True)
        inv = lax.rsqrt(jnp.mean(centered * centered, axis=-1, keepdims=True) + epsilon)
        normed = centered * inv
        position = lax.broadcasted_iota(jnp.int32, (CH, 128), 0) + (t * BLOCK + i * CH)
        live = jnp.where(position.astype(F32) < s.lens_use[1][0:1, :], 1.0, 0.0)[:, 0:1]
        s.out_own[ch, :] = ((normed * a.gf[...] + a.sf[...]) * live).astype(BF16)
        grad = s.cot_own[ch, :].astype(F32) * live
        add_rows(4, grad * normed)
        add_rows(5, grad)
        u = grad * a.gf[...]
        first = jnp.mean(u, axis=-1, keepdims=True)
        second = jnp.mean(u * normed, axis=-1, keepdims=True)
        grad_two = inv * (u - first - normed * second)
        add_rows(3, grad_two)
        s.g2f[ch, :] = grad_two
        s.g2[group_chunk(i), :] = grad_two.astype(BF16)
    by_halves(1, norm_two, lambda k: gather_start(1, s.g2, k))
    out_s, out_r = take("s"), take("r")
    home_self = jnp.logical_and(zh == c, t == z)

    def ffn_back(j):
        @pl.when(j < 3)
        def _():
            gather_step(1, s.g2, j)
        r = slot_step(t, j)
        rows = rows_of(r)
        for n in range(4):
            cols = slice(256 * n, 256 * n + 256)
            grad = dot_nn(s.g2[rows, :], s.wbt[:, cols]) * s.slope[rows, cols]
            s.gb_in[:, cols] += jnp.sum(grad, axis=0, keepdims=True)
            s.gpre[rows, cols] = grad.astype(BF16)
    loop(SLOTS - 1, ffn_back)
    send_or_keep(s.out_own, o.out, dev(b, zh, t), home_self, out_s, out_r)
    at_end(s.out_own, out_s, home_self)

    def grad_back(k):
        part = slice(512 * k, 512 * k + 512)

        def body(n):
            for e in range(2):
                block = n * 2 + e
                s.gb[block, part, :] = dot_nn(s.actt[part, :], s.g2[:, cols_of(block)]).astype(BF16)
        loop(2, body)

    def grad_in(k):
        cols = slice(512 * k, 512 * k + 512)

        def body(m):
            part = rows_of(m * 4, 512)
            s.gi[part, cols] = dot_nn(s.hidt[part, :], s.gpre[:, cols]).astype(BF16)
        loop(2, body)

    gather_step(1, s.g2, 3)
    grad_back(0)
    grad_first("b0")
    ffn_back(3)
    grad_back(1)
    grad_first("b1")

    def in_part(first, count, dst, add):
        rows = pl.ds(pl.multiple_of(first, HALF), count)
        for n in range(4):
            put_part(dst, add, n, dot_nn(s.gpre[rows, :], s.wit[:, 256 * n:256 * n + 256]))
    scatter(2, in_part)
    grad_in(0)
    grad_in(1)
    grad_second("b0")

    def norm_one_back(i):
        ch = own_chunk(i)
        grad = s.g2f[ch, :] + scatter_rows(2, ch)
        normed = s.normed1[ch, :]
        add_rows(1, grad * normed)
        add_rows(2, grad)
        u = grad * a.ga[...]
        first = jnp.mean(u, axis=-1, keepdims=True)
        second = jnp.mean(u * normed, axis=-1, keepdims=True)
        grad_one = s.inv1[ch, 0:1] * (u - first - normed * second)
        add_rows(0, grad_one)
        s.g1f[ch, :] = grad_one
        s.g1[group_chunk(i), :] = grad_one.astype(BF16)
    by_halves(2, norm_one_back, lambda k: gather_start(2, s.g1, k))
    grad_second("b1")
    grad_first("i0")
    grad_first("i1", 0)

    def attend_back(j):
        gather_step(2, s.g1, j)
        r = slot_step(t, j)
        rows = rows_of(r)
        grad_ctx = dot_nn(s.g1[rows, :], s.wot[...]).astype(BF16)
        s.gctxt[:, rows] = grad_ctx.T
        product = grad_ctx.astype(F32) * s.ctx[rows, :].astype(F32)
        parts = []
        for h in range(4):
            cols = slice(64 * h, 64 * h + 64)
            prob = s.ps[h, rows, :]
            delta = jnp.sum(product[:, cols], axis=-1, keepdims=True)
            grad_prob = dot_nt(grad_ctx[:, cols], s.v[:, cols])
            grad_score = (prob.astype(F32) * (grad_prob - delta)).astype(BF16)
            parts.append(dot_nn(grad_score, s.ks[:, cols]))
            s.dkt[cols, :] += dot_nn(s.qt[cols, rows], grad_score)
            s.dvt[cols, :] += dot_nn(s.gctxt[cols, rows], prob)
        grad_query = jnp.concatenate(parts, axis=1)
        for k in range(4):
            @pl.when(t == k)
            def _():
                s.sums[0, 6:7, 256 * k:256 * k + 256] += jnp.sum(grad_query, axis=0, keepdims=True)
        s.dq[rows, :] = grad_query.astype(BF16)
    loop(2, attend_back)
    grad_third("b0")
    loop(2, lambda j: attend_back(j + 2))
    grad_third("b1")

    def turn_back(r):
        rows = rows_of(r)
        s.dk[rows, :] = s.dkt[:, rows].T.astype(BF16)
        grad_value = s.dvt[:, rows].T
        for k in range(4):
            @pl.when(t == k)
            def _():
                s.sums[0, 7:8, 256 * k:256 * k + 256] += jnp.sum(grad_value, axis=0, keepdims=True)
        s.dv[rows, :] = grad_value.astype(BF16)
    loop(SLOTS, turn_back)
    for k in range(4):
        @pl.when(t == k)
        def _():
            s.sums[0, 8 + k:9 + k, :] = s.gb_in[...]

    sums_s, sums_r = take("s", 5), take("r", 5)
    sums_to = [partner, across, pair, x_near, y_near]

    def sums_start(k):
        send(s.sums.at[k], s.sums_got.at[k], sums_to[k], sums_s + k, sums_r + k)
        at_end(s.sums.at[k], sums_s + k)

    def sums_finish(k):
        got(s.sums_got.at[k], sums_r + k)
        total = s.sums[k] + s.sums_got[k]
        if k == 4:
            o.sums[...] = total
        else:
            s.sums[k + 1] = total

    sums_start(0)

    def tok_part(first, count, dst, add):
        rows = pl.ds(pl.multiple_of(first, HALF), count)
        for n in range(4):
            cols = slice(256 * n, 256 * n + 256)
            acc = dot_nn(s.dq[rows, :], s.w3t[0, :, cols])
            acc = acc + dot_nn(s.dk[rows, :], s.w3t[1, :, cols])
            acc = acc + dot_nn(s.dv[rows, :], s.w3t[2, :, cols])
            put_part(dst, add, n, acc)
    grad_second("i0")
    grad_first("i1", 1)
    scatter(3, tok_part)
    sums_finish(0)
    sums_start(1)

    def grad_head(m, src):
        s.g3[m * WIDTH:(m + 1) * WIDTH, :] = dot_nn(s.tkt[...], src[...]).astype(BF16)

    for n in range(4):
        s.go[n] = dot_nn(s.ctxt[...], s.g1[:, 256 * n:256 * n + 256]).astype(BF16)
    grad_head(0, s.dq)
    grad_head(1, s.dk)
    grad_head(2, s.dv)
    grad_second("i1")
    grad_first("o")
    grad_first("q")
    grad_third("i0")
    grad_third("i1")
    grad_second("o")
    grad_first("k")

    def last_rows(i):
        ch = own_chunk(i)
        s.gtok_own[ch, :] = (s.g1f[ch, :] + scatter_rows(3, ch)).astype(BF16)
    by_halves(3, last_rows, lambda k: None)
    gtok_s, gtok_r = take("s"), take("r")
    send_or_keep(s.gtok_own, o.gtok, dev(b, zh, t), home_self, gtok_s, gtok_r)
    at_end(s.gtok_own, gtok_s, home_self)
    grad_second("q")
    grad_first("v")
    grad_third("o")
    grad_second("k")
    grad_third("q")
    sums_finish(1)
    sums_start(2)
    grad_second("v")
    grad_third("k")
    sums_finish(2)
    sums_start(3)
    grad_third("v")
    sums_finish(3)
    sums_start(4)
    grad_final("b0")
    grad_final("b1")
    grad_final("i0")
    grad_final("i1")
    got(o.gtok, gtok_r)
    got(o.out, out_r)
    grad_final("o")
    grad_final("q")
    sums_finish(4)
    grad_final("k")
    grad_final("v")

    for size_of, sk, skipped, instead in to_drain:
        if skipped is None:
            left(size_of, sk)
        else:
            @pl.when(jnp.logical_not(skipped))
            def _():
                left(size_of, sk)
            if instead is not None:
                @pl.when(skipped)
                def _():
                    left(instead, sk)


def result_kernel(out, gtok, sums, zq, zk, zv, zo, zi0, zi1, zb0, zb1, o_out, o_gtok, o_gq, o_gbq, o_gk, o_gv, o_gbv, o_go,
                  o_gbo, o_gga, o_gsa, o_gi, o_gbi, o_gb, o_gbb, o_ggf, o_gsf):
    both = lambda ref: ref[0].astype(F32) + ref[1].astype(F32)
    o_out[...] = out[...]
    o_gtok[...] = gtok[...].astype(F32)
    o_gq[...], o_gk[...], o_gv[...], o_go[...] = both(zq), both(zk), both(zv), both(zo)
    o_gi[:, :512], o_gi[:, 512:] = both(zi0), both(zi1)
    o_gb[:512, :], o_gb[512:, :] = both(zb0), both(zb1)
    for row, ref in ((6, o_gbq), (7, o_gbv), (0, o_gbo), (1, o_gga), (2, o_gsa), (3, o_gbb), (4, o_ggf), (5, o_gsf)):
        ref[...] = sums[row:row + 1, :]
    for k in range(4):
        o_gbi[:, WIDTH * k:WIDTH * k + WIDTH] = sums[8 + k:9 + k, :]


def on_device_fused(tokens, lengths, w_query, b_query, w_key, w_value, b_value, w_out, b_out, gain_attn, shift_attn,
                    w_in, b_in, w_back, b_back, gain_ffn, shift_ffn, cotangent):
    row = lambda vec: vec.reshape(1, -1)
    operands = (tokens, lengths, w_query, row(b_query), w_key, w_value, row(b_value), w_out, row(b_out),
                row(gain_attn), row(shift_attn), w_in, row(b_in), w_back, row(b_back), row(gain_ffn),
                row(shift_ffn), cotangent)
    vmem = pl.BlockSpec(memory_space=pltpu.VMEM)
    stay = pl.BlockSpec(memory_space=pl.ANY)
    in_specs = [stay] * len(operands)
    in_specs[1] = pl.BlockSpec(memory_space=pltpu.SMEM)
    shape = lambda dims, dtype: jax.ShapeDtypeStruct(dims, dtype)
    between = [shape(tokens.shape, BF16), shape(tokens.shape, BF16), shape((16, WIDTH), F32)]
    between += [shape((2,) + HALVES[name], BF16) for name in ("q", "k", "v", "o", "i0", "i1", "b0", "b1")]
    parts = pl.pallas_call(
        layer_kernel,
        out_shape=between,
        in_specs=in_specs,
        out_specs=[stay, stay, vmem] + [stay] * 8,
        scratch_shapes=jax.tree.leaves(scratch_table()),
        compiler_params=pltpu.CompilerParams(collective_id=0, has_side_effects=True, vmem_limit_bytes=64 * 1024 * 1000),
        name="layer",
    )(*operands)
    line = shape((1, WIDTH), F32)
    results = (
        shape(tokens.shape, BF16), shape(tokens.shape, F32), shape(w_query.shape, F32), line, shape(w_key.shape, F32),
        shape(w_value.shape, F32), line, shape(w_out.shape, F32), line, line, line, shape(w_in.shape, F32),
        shape((1, b_in.shape[0]), F32), shape(w_back.shape, F32), line, line, line)
    outs = pl.pallas_call(
        result_kernel,
        out_shape=results,
        in_specs=[vmem] * len(between),
        out_specs=[vmem] * len(results),
        name="results",
    )(*parts)
    return tuple(v.reshape(-1) if v.shape[0] == 1 else v for v in outs)


def fits_fused(mesh):
    return dict(mesh.shape) == {"dp": 8, "tensor": 4}


def solution(mesh):
    placed = (
        P(("dp", "tensor"), None),
        P("dp", None),
        P("dp", "tensor"),
        P(),
        P("dp", "tensor"),
        P("dp", "tensor"),
        P(),
        P("tensor", "dp"),
        P(),
        P(),
        P(),
        P("dp", "tensor"),
        P(),
        P("tensor", "dp"),
        P(),
        P(),
        P(),
        P(("dp", "tensor"), None),
    )
    on_device = on_device_fused if fits_fused(mesh) else on_device_plain
    return jax.shard_map(
        on_device,
        mesh=mesh,
        in_specs=placed,
        out_specs=(
            P(("dp", "tensor"), None),
            P(("dp", "tensor"), None),
            P("dp", "tensor"),
            P(),
            P("dp", "tensor"),
            P("dp", "tensor"),
            P(),
            P("tensor", "dp"),
            P(),
            P(),
            P(),
            P("dp", "tensor"),
            P(),
            P("tensor", "dp"),
            P(),
            P(),
            P(),
        ),
        check_vma=False,
    )
```

```python
from types import SimpleNamespace

import jax
import jax.numpy as jnp
from jax import lax
from jax.experimental import pallas as pl
from jax.experimental.pallas import tpu as pltpu
from jax.sharding import PartitionSpec as P

HD = 64


epsilon = 1e-06
masked_value = -1e30


def matmul_plain(left_side, right_side):
    return jnp.dot(left_side, right_side, preferred_element_type=jnp.float32)


def matmul_over_rows(left_side, right_side):
    return lax.dot_general(
        left_side, right_side, (((0,), (0,)), ((), ())), preferred_element_type=jnp.float32
    )


def matmul_over_cols(left_side, right_side):
    return lax.dot_general(
        left_side, right_side, (((1,), (1,)), ((), ())), preferred_element_type=jnp.float32
    )


def layer_norm(residual, gain_vec, shift_vec):
    mean_val = jnp.mean(residual, axis=-1, keepdims=True)
    centered = residual - mean_val
    inv_std = lax.rsqrt(jnp.mean(centered * centered, axis=-1, keepdims=True) + epsilon)
    normed = centered * inv_std
    return (normed * gain_vec + shift_vec, normed, inv_std)


def norm_back(grad_out, normed, inv_std, gain_vec):
    grad_norm = grad_out * gain_vec
    first_mean = jnp.mean(grad_norm, axis=-1, keepdims=True)
    second_mean = jnp.mean(grad_norm * normed, axis=-1, keepdims=True)
    return inv_std * (grad_norm - first_mean - normed * second_mean)


def gelu_parts(preact):
    cdf_val = 0.5 * (1.0 + lax.erf(preact * 0.7071067811865476))
    pdf_val = jnp.exp(-0.5 * preact * preact) * 0.3989422804014327
    return (preact * cdf_val, cdf_val + preact * pdf_val)


def attend_forward(query_rows, key_rows, value_rows, seg_ids, head_dim, block_rows):
    group_rows, head_cols = query_rows.shape
    pair_width = 2 * head_dim
    block_count = group_rows // block_rows
    pair_count = head_cols // pair_width
    score_scale = head_dim ** (-0.5)

    def attend_step(step_index, loop_carry):
        context, log_total = loop_carry
        pair_index = step_index // block_count
        row_start = step_index % block_count * block_rows
        first_col = pair_index * pair_width
        query_block = lax.dynamic_slice(
            query_rows, (row_start, first_col), (block_rows, pair_width)
        ).reshape(block_rows, 2, head_dim)
        key_pair = lax.dynamic_slice(key_rows, (0, first_col), (group_rows, pair_width)).reshape(
            group_rows, 2, head_dim
        )
        value_pair = lax.dynamic_slice(
            value_rows, (0, first_col), (group_rows, pair_width)
        ).reshape(group_rows, 2, head_dim)
        same_seg = seg_ids[:, None] == seg_ids[None, :]
        scores = (
            jnp.einsum("qhd,khd->hqk", query_block, key_pair, preferred_element_type=jnp.float32)
            * score_scale
        )
        scores = jnp.where(same_seg[None], scores, masked_value)
        row_max = jnp.max(scores, axis=-1, keepdims=True)
        block_total = row_max + jnp.log(jnp.sum(jnp.exp(scores - row_max), axis=-1, keepdims=True))
        prob_bf = jnp.exp(scores - block_total).astype(jnp.bfloat16)
        context_block = jnp.einsum(
            "hqk,khd->qhd", prob_bf, value_pair, preferred_element_type=jnp.float32
        ).astype(jnp.bfloat16)
        context = lax.dynamic_update_slice(
            context, context_block.reshape(block_rows, pair_width), (row_start, first_col)
        )
        log_total = lax.dynamic_update_slice(
            log_total, block_total[:, :, 0], (2 * pair_index, row_start)
        )
        return (context, log_total)

    start_carry = (
        jnp.zeros((group_rows, head_cols), jnp.bfloat16),
        jnp.zeros((head_cols // head_dim, group_rows), jnp.float32),
    )
    return lax.fori_loop(0, pair_count * block_count, attend_step, start_carry)


def attend_backward(
    query_rows,
    key_rows,
    value_rows,
    context,
    grad_context,
    log_total,
    seg_ids,
    head_dim,
    block_rows,
):
    group_rows, head_cols = query_rows.shape
    pair_width = 2 * head_dim
    block_count = group_rows // block_rows
    pair_count = head_cols // pair_width
    score_scale = head_dim ** (-0.5)

    def back_step(step_index, loop_carry):
        grad_query, grad_keys, grad_values = loop_carry
        pair_index = step_index // block_count
        row_start = step_index % block_count * block_rows
        first_col = pair_index * pair_width
        query_block = lax.dynamic_slice(
            query_rows, (row_start, first_col), (block_rows, pair_width)
        ).reshape(block_rows, 2, head_dim)
        key_pair = lax.dynamic_slice(key_rows, (0, first_col), (group_rows, pair_width)).reshape(
            group_rows, 2, head_dim
        )
        value_pair = lax.dynamic_slice(
            value_rows, (0, first_col), (group_rows, pair_width)
        ).reshape(group_rows, 2, head_dim)
        context_block = lax.dynamic_slice(
            context, (row_start, first_col), (block_rows, pair_width)
        ).reshape(block_rows, 2, head_dim)
        gctx_block = lax.dynamic_slice(
            grad_context, (row_start, first_col), (block_rows, pair_width)
        ).reshape(block_rows, 2, head_dim)
        total_block = lax.dynamic_slice(log_total, (2 * pair_index, row_start), (2, block_rows))
        same_seg = seg_ids[:, None] == seg_ids[None, :]
        scores = (
            jnp.einsum("qhd,khd->hqk", query_block, key_pair, preferred_element_type=jnp.float32)
            * score_scale
        )
        scores = jnp.where(same_seg[None], scores, masked_value)
        probs = jnp.exp(scores - total_block[:, :, None])
        prob_bf = probs.astype(jnp.bfloat16)
        grad_probs = jnp.einsum(
            "qhd,khd->hqk", gctx_block, value_pair, preferred_element_type=jnp.float32
        )
        delta_rows = jnp.sum(
            gctx_block.astype(jnp.float32) * context_block.astype(jnp.float32), axis=-1
        ).T[:, :, None]
        grad_scores = (probs * (grad_probs - delta_rows) * score_scale).astype(jnp.bfloat16)
        grad_q_block = jnp.einsum(
            "hqk,khd->qhd", grad_scores, key_pair, preferred_element_type=jnp.float32
        ).reshape(block_rows, pair_width)
        grad_k_pair = jnp.einsum(
            "hqk,qhd->khd", grad_scores, query_block, preferred_element_type=jnp.float32
        ).reshape(group_rows, pair_width)
        grad_v_pair = jnp.einsum(
            "hqk,qhd->khd", prob_bf, gctx_block, preferred_element_type=jnp.float32
        ).reshape(group_rows, pair_width)
        grad_query = lax.dynamic_update_slice(grad_query, grad_q_block, (row_start, first_col))
        old_keys = lax.dynamic_slice(grad_keys, (0, first_col), (group_rows, pair_width))
        grad_keys = lax.dynamic_update_slice(grad_keys, old_keys + grad_k_pair, (0, first_col))
        old_values = lax.dynamic_slice(grad_values, (0, first_col), (group_rows, pair_width))
        grad_values = lax.dynamic_update_slice(
            grad_values, old_values + grad_v_pair, (0, first_col)
        )
        return (grad_query, grad_keys, grad_values)

    zero_grad = jnp.zeros((group_rows, head_cols), jnp.float32)
    return lax.fori_loop(0, pair_count * block_count, back_step, (zero_grad, zero_grad, zero_grad))


def on_device_plain(
    tokens,
    lengths,
    w_query,
    b_query,
    w_key,
    w_value,
    b_value,
    w_out,
    b_out,
    gain_attn,
    shift_attn,
    w_in,
    b_in,
    w_back,
    b_back,
    gain_ffn,
    shift_ffn,
    cotangent,
):
    tensor_size = lax.axis_size("tensor")
    tensor_index = lax.axis_index("tensor")
    local_rows = tokens.shape[0]
    group_rows = local_rows * tensor_size
    head_cols = w_query.shape[1]
    hidden_cols = w_in.shape[1]
    block_rows = min(512, group_rows)
    seq_lens = lengths[0]
    live_end = seq_lens[0] + seq_lens[1]
    positions = jnp.arange(group_rows, dtype=jnp.int32)
    seg_ids = (positions >= seq_lens[0]).astype(jnp.int32) + (positions >= live_end).astype(
        jnp.int32
    )
    local_pos = tensor_index * local_rows + jnp.arange(local_rows, dtype=jnp.int32)
    live_rows = (local_pos < live_end).astype(jnp.float32)[:, None]
    rows_full = lax.all_gather(tokens, "tensor", axis=0, tiled=True)
    attn_mats = (
        lax.all_gather(w_query, "dp", axis=0, tiled=True),
        lax.all_gather(w_key, "dp", axis=0, tiled=True),
        lax.all_gather(w_value, "dp", axis=0, tiled=True),
        lax.all_gather(w_out, "dp", axis=1, tiled=True),
    )
    mat_query, mat_key, mat_value, mat_out = attn_mats
    bias_query = lax.dynamic_slice_in_dim(b_query, tensor_index * head_cols, head_cols)
    bias_value = lax.dynamic_slice_in_dim(b_value, tensor_index * head_cols, head_cols)
    bias_in = lax.dynamic_slice_in_dim(b_in, tensor_index * hidden_cols, hidden_cols)
    query_rows = (matmul_plain(rows_full, mat_query) + bias_query).astype(jnp.bfloat16)
    key_rows = matmul_plain(rows_full, mat_key).astype(jnp.bfloat16)
    value_rows = (matmul_plain(rows_full, mat_value) + bias_value).astype(jnp.bfloat16)
    context, log_total = attend_forward(query_rows, key_rows, value_rows, seg_ids, HD, block_rows)
    attn_sum = lax.psum_scatter(
        matmul_plain(context, mat_out).astype(jnp.bfloat16),
        "tensor",
        scatter_dimension=0,
        tiled=True,
    ).astype(jnp.float32)
    resid_one = tokens.astype(jnp.float32) + attn_sum + b_out
    hidden_one, normed_one, inv_one = layer_norm(resid_one, gain_attn, shift_attn)
    hidden_bf = hidden_one.astype(jnp.bfloat16)
    hidden_full = lax.all_gather(hidden_bf, "tensor", axis=0, tiled=True)
    ffn_mats = (
        lax.all_gather(w_in, "dp", axis=0, tiled=True),
        lax.all_gather(w_back, "dp", axis=1, tiled=True),
    )
    mat_in, mat_back = ffn_mats
    preact = matmul_plain(hidden_full, mat_in) + bias_in
    activ_val, gelu_slope = gelu_parts(preact)
    activation = activ_val.astype(jnp.bfloat16)
    ffn_sum = lax.psum_scatter(
        matmul_plain(activation, mat_back).astype(jnp.bfloat16),
        "tensor",
        scatter_dimension=0,
        tiled=True,
    ).astype(jnp.float32)
    resid_two = hidden_one + ffn_sum + b_back
    normed_out, normed_two, inv_two = layer_norm(resid_two, gain_ffn, shift_ffn)
    output = (normed_out * live_rows).astype(jnp.bfloat16)
    grad_final = cotangent.astype(jnp.float32) * live_rows
    grad_gain_ffn = jnp.sum(grad_final * normed_two, axis=0)
    grad_shift_ffn = jnp.sum(grad_final, axis=0)
    grad_two = norm_back(grad_final, normed_two, inv_two, gain_ffn)
    grad_b_back = jnp.sum(grad_two, axis=0)
    mat_query, mat_key, mat_value, mat_out, mat_in, mat_back = (
        lax.all_gather(w_query, "dp", axis=0, tiled=True),
        lax.all_gather(w_key, "dp", axis=0, tiled=True),
        lax.all_gather(w_value, "dp", axis=0, tiled=True),
        lax.all_gather(w_out, "dp", axis=1, tiled=True),
        lax.all_gather(w_in, "dp", axis=0, tiled=True),
        lax.all_gather(w_back, "dp", axis=1, tiled=True),
    )
    grad_two_full = lax.all_gather(grad_two.astype(jnp.bfloat16), "tensor", axis=0, tiled=True)
    grad_w_back = matmul_over_rows(activation, grad_two_full)
    grad_pre = matmul_over_cols(grad_two_full, mat_back) * gelu_slope
    grad_b_in_part = jnp.sum(grad_pre, axis=0)
    grad_pre_bf = grad_pre.astype(jnp.bfloat16)
    grad_w_in = matmul_over_rows(hidden_full, grad_pre_bf)
    grad_one_out = grad_two + lax.psum_scatter(
        matmul_over_cols(grad_pre_bf, mat_in).astype(jnp.bfloat16),
        "tensor",
        scatter_dimension=0,
        tiled=True,
    ).astype(jnp.float32)
    grad_w_in, grad_w_back = (
        lax.psum_scatter(grad_w_in, "dp", scatter_dimension=0, tiled=True),
        lax.psum_scatter(grad_w_back, "dp", scatter_dimension=1, tiled=True),
    )
    grad_gain_attn = jnp.sum(grad_one_out * normed_one, axis=0)
    grad_shift_attn = jnp.sum(grad_one_out, axis=0)
    grad_one = norm_back(grad_one_out, normed_one, inv_one, gain_attn)
    grad_b_out = jnp.sum(grad_one, axis=0)
    grad_one_full = lax.all_gather(grad_one.astype(jnp.bfloat16), "tensor", axis=0, tiled=True)
    grad_w_out = matmul_over_rows(context, grad_one_full)
    grad_context = matmul_over_cols(grad_one_full, mat_out).astype(jnp.bfloat16)
    grad_query, grad_keys, grad_values = attend_backward(
        query_rows, key_rows, value_rows, context, grad_context, log_total, seg_ids, HD, block_rows
    )
    grad_b_query_part = jnp.sum(grad_query, axis=0)
    grad_b_value_part = jnp.sum(grad_values, axis=0)
    grad_query_bf = grad_query.astype(jnp.bfloat16)
    grad_keys_bf = grad_keys.astype(jnp.bfloat16)
    grad_values_bf = grad_values.astype(jnp.bfloat16)
    grad_w_query = matmul_over_rows(rows_full, grad_query_bf)
    grad_w_key = matmul_over_rows(rows_full, grad_keys_bf)
    grad_w_value = matmul_over_rows(rows_full, grad_values_bf)
    query_part = matmul_over_cols(grad_query_bf, mat_query)
    key_part = matmul_over_cols(grad_keys_bf, mat_key)
    value_part = matmul_over_cols(grad_values_bf, mat_value)
    grad_in = grad_one + lax.psum_scatter(
        (query_part + key_part + value_part).astype(jnp.bfloat16),
        "tensor",
        scatter_dimension=0,
        tiled=True,
    ).astype(jnp.float32)
    grad_w_query, grad_w_key, grad_w_value, grad_w_out = (
        lax.psum_scatter(grad_w_query, "dp", scatter_dimension=0, tiled=True),
        lax.psum_scatter(grad_w_key, "dp", scatter_dimension=0, tiled=True),
        lax.psum_scatter(grad_w_value, "dp", scatter_dimension=0, tiled=True),
        lax.psum_scatter(grad_w_out, "dp", scatter_dimension=1, tiled=True),
    )

    def widen(part_vec, full_width):
        return lax.dynamic_update_slice_in_dim(
            jnp.zeros((full_width,), jnp.float32), part_vec, tensor_index * part_vec.shape[0], 0
        )

    small_sums = lax.psum(
        (
            widen(grad_b_query_part, b_query.shape[0]),
            widen(grad_b_value_part, b_value.shape[0]),
            grad_b_out,
            grad_gain_attn,
            grad_shift_attn,
            widen(grad_b_in_part, b_in.shape[0]),
            grad_b_back,
            grad_gain_ffn,
            grad_shift_ffn,
        ),
        ("dp", "tensor"),
    )
    return (
        output,
        grad_in,
        grad_w_query,
        small_sums[0],
        grad_w_key,
        grad_w_value,
        small_sums[1],
        grad_w_out,
        small_sums[2],
        small_sums[3],
        small_sums[4],
        grad_w_in,
        small_sums[5],
        grad_w_back,
        small_sums[6],
        small_sums[7],
        small_sums[8],
    )


MESH_ID = pl.DeviceIdType.MESH
F32 = jnp.float32
BF16 = jnp.bfloat16

SLOTS = 4
BLOCK = 128
GROUP = 512
WIDTH = 1024
HEAD_COLS = 256
HIDDEN = 1024
N_SEND = 58
N_GOT = 110
HALF = BLOCK // 2
HALVES = dict(q=(128, 256), k=(128, 256), v=(128, 256), o=(256, 128), i0=(128, 512), i1=(128, 512), b0=(512, 128),
              b1=(512, 128))
VECTORS = dict(bq=1024, bv=1024, bo=1024, ga=1024, sa=1024, bi=4096, bb=1024, gf=1024, sf=1024)


def flip(bit):
    return 1 - bit


def slot_step(t, j):
    return (t % 2 + j % 2) % 2 + 2 * ((t // 2 + j // 2) % 2)


def rows_of(r, count=BLOCK):
    return pl.ds(pl.multiple_of(r * BLOCK, BLOCK), count)


def cols_of(n, count=256):
    return pl.ds(pl.multiple_of(n * count, count), count)


def dot_nn(a, b):
    return jnp.dot(a, b, preferred_element_type=F32)


def dot_nt(a, b):
    return lax.dot_general(a, b, (((1,), (1,)), ((), ())), preferred_element_type=F32)


def dot_tn(a, b):
    return lax.dot_general(a, b, (((0,), (0,)), ((), ())), preferred_element_type=F32)


def scratch_table():
    act = lambda n: pltpu.VMEM((GROUP, n), BF16)
    table = dict(
        w3=pltpu.VMEM((3 * WIDTH, HEAD_COLS), BF16),
        wo=pltpu.VMEM((4, HEAD_COLS, 256), BF16),
        wi=pltpu.VMEM((WIDTH, HIDDEN), BF16),
        wb=pltpu.VMEM((4, HIDDEN, 256), BF16),
        w3t=pltpu.VMEM((3, HEAD_COLS, WIDTH), BF16),
        wot=pltpu.VMEM((WIDTH, HEAD_COLS), BF16),
        wit=pltpu.VMEM((HIDDEN, WIDTH), BF16),
        wbt=pltpu.VMEM((WIDTH, HIDDEN), BF16),
        lens_own=pltpu.VMEM((2, 8, 128), F32),
        lens_got=pltpu.VMEM((2, 8, 128), F32),
        lens_use=pltpu.VMEM((2, 8, 128), F32),
        tk=act(WIDTH),
        tkt=pltpu.VMEM((WIDTH, GROUP), BF16),
        cot_own=pltpu.VMEM((BLOCK, WIDTH), BF16),
        bias=pltpu.VMEM((GROUP, GROUP), F32),
        q=act(HEAD_COLS),
        qt=pltpu.VMEM((HEAD_COLS, GROUP), BF16),
        k=act(HEAD_COLS),
        ks=act(HEAD_COLS),
        v=act(HEAD_COLS),
        ps=pltpu.VMEM((4, GROUP, GROUP), BF16),
        ctx=act(HEAD_COLS),
        ctxt=pltpu.VMEM((HEAD_COLS, GROUP), BF16),
        hid=act(WIDTH),
        hidt=pltpu.VMEM((WIDTH, GROUP), BF16),
        act=act(HIDDEN),
        actt=pltpu.VMEM((HIDDEN, GROUP), BF16),
        slope=pltpu.VMEM((GROUP, HIDDEN), F32),
        g2=act(WIDTH),
        gpre=act(HIDDEN),
        g1=act(WIDTH),
        gctxt=pltpu.VMEM((HEAD_COLS, GROUP), BF16),
        dq=act(HEAD_COLS),
        dkt=pltpu.VMEM((HEAD_COLS, GROUP), F32),
        dvt=pltpu.VMEM((HEAD_COLS, GROUP), F32),
        dk=act(HEAD_COLS),
        dv=act(HEAD_COLS),
        hid1=pltpu.VMEM((BLOCK, WIDTH), F32),
        normed1=pltpu.VMEM((BLOCK, WIDTH), F32),
        inv1=pltpu.VMEM((BLOCK, 128), F32),
        g2f=pltpu.VMEM((BLOCK, WIDTH), F32),
        g1f=pltpu.VMEM((BLOCK, WIDTH), F32),
        out_own=pltpu.VMEM((BLOCK, WIDTH), BF16),
        gtok_own=pltpu.VMEM((BLOCK, WIDTH), BF16),
        rs_own=pltpu.VMEM((4, BLOCK, WIDTH), BF16),
        rs_out=pltpu.VMEM((4, 3, BLOCK, WIDTH), BF16),
        rs_got=pltpu.VMEM((4, 3, BLOCK, WIDTH), BF16),
        sums=pltpu.VMEM((6, 16, WIDTH), F32),
        sums_got=pltpu.VMEM((5, 16, WIDTH), F32),
        gb_in=pltpu.VMEM((1, HIDDEN), F32),
        vectors={name: pltpu.VMEM((1, width), F32) for name, width in VECTORS.items()},
        vsem=pltpu.SemaphoreType.DMA((len(VECTORS),)),
        turn=pltpu.SemaphoreType.REGULAR((4,)),
        g3=pltpu.VMEM((3 * WIDTH, HEAD_COLS), BF16),
        go=pltpu.VMEM((4, HEAD_COLS, 256), BF16),
        gi=pltpu.VMEM((WIDTH, HIDDEN), BF16),
        gb=pltpu.VMEM((4, HIDDEN, 256), BF16),
        stage={},
        ssem=pltpu.SemaphoreType.DMA((N_SEND,)),
        rsem=pltpu.SemaphoreType.DMA((N_GOT,)),
    )
    for name, dims in HALVES.items():
        table["stage"][name] = pltpu.VMEM((10,) + dims, BF16)
    return table


def layer_kernel(tok, lens, wq, bq, wk, wv, bv, wo, bo, ga, sa, wi, bi, wb, bb, gf, sf, cot, out, gtok, sums, zq, zk, zv,
                 zo, zi0, zi1, zb0, zb1, *scratch):
    a = SimpleNamespace(tok=tok, lens=lens, wq=wq, bq=bq, wk=wk, wv=wv, bv=bv, wo=wo, bo=bo, ga=ga, sa=sa, wi=wi, bi=bi,
                        wb=wb, bb=bb, gf=gf, sf=sf, cot=cot)
    o = SimpleNamespace(out=out, gtok=gtok, sums=sums)
    landed = dict(q=zq, k=zk, v=zv, o=zo, i0=zi0, i1=zi1, b0=zb0, b1=zb1)
    s = SimpleNamespace(**jax.tree.unflatten(jax.tree.structure(scratch_table()), scratch))
    ssem, rsem, vsem, vectors = s.ssem, s.rsem, s.vsem, s.vectors

    dp = lax.axis_index("dp")
    z = lax.axis_index("tensor")
    b, c = dp // 2, dp % 2
    zl, zh = z % 2, z // 2
    t = zl * 2 + c
    bx = b + 1 - 2 * (b % 2)
    by = (b + 2) % 4
    bd = 3 - b
    t1, t2, t3 = slot_step(t, 1), slot_step(t, 2), slot_step(t, 3)

    def dev(pos, core, zz):
        return (pos * 2 + core, zz)

    partner = dev(b, flip(c), z)
    z_near = z + 1 - 2 * (z % 2)
    z_far = (z + 2) % 4
    pair = dev(b, c, z_near)
    across = dev(b, c, z_far)
    is_inner = jnp.logical_and(z >= 1, z <= 2)
    x_near = dev(bx, c, z)
    y_near = dev(by, c, z)

    taken = {"s": 0, "r": 0}

    def take(kind, count=1):
        first = taken[kind]
        taken[kind] = first + count
        assert taken[kind] <= (N_SEND if kind == "s" else N_GOT)
        return first

    to_drain = []

    def make_copy(src, dst, device, sk, rk):
        return pltpu.make_async_remote_copy(
            src_ref=src, dst_ref=dst, send_sem=ssem.at[sk], recv_sem=rsem.at[rk], device_id=device,
            device_id_type=MESH_ID)

    def send(src, dst, device, sk, rk):
        make_copy(src, dst, device, sk, rk).start()

    def got(dst, rk):
        pltpu.make_async_copy(dst, dst, rsem.at[rk]).wait()

    def left(size_of, sk):
        pltpu.make_async_copy(size_of, size_of, ssem.at[sk]).wait()

    def at_end(size_of, sk, skipped=None, instead=None):
        to_drain.append((size_of, sk, skipped, instead))

    def send_or_keep(src, dst, device, is_self, sk, rk):
        copy = make_copy(src, dst, device, sk, rk)

        @pl.when(is_self)
        def _():
            pltpu.make_async_copy(src, dst, rsem.at[rk]).start()

        @pl.when(jnp.logical_not(is_self))
        def _():
            copy.start()

    barrier = pltpu.get_barrier_semaphore()
    peers = [x_near, y_near]
    for dz in range(4):
        for dc in range(2):
            if dz or dc:
                peers.append(dev(b, (c + dc) % 2, (z + dz) % 4))
    for peer in peers:
        pl.semaphore_signal(barrier, inc=1, device_id=peer, device_id_type=MESH_ID)
    pl.semaphore_wait(barrier, len(peers))

    def piece_qkv(m, home):
        base = m * WIDTH
        return SimpleNamespace(
            home=home,
            own=lambda bb, cc: s.w3.at[pl.ds(pl.multiple_of(base + bb * 256 + cc * 128, 128), 128), :],
            block=lambda bb: s.w3.at[pl.ds(pl.multiple_of(base + bb * 256, 256), 256), :],
            half=lambda bb, h: s.w3.at[pl.ds(pl.multiple_of(base + bb * 256 + h * 128, 128), 128), :])

    piece_o = SimpleNamespace(
        home=a.wo,
        own=lambda bb, cc: s.wo.at[bb, :, pl.ds(pl.multiple_of(cc * 128, 128), 128)],
        block=lambda bb: s.wo.at[bb],
        half=lambda bb, h: s.wo.at[bb, pl.ds(h * 128, 128), :])

    def piece_in(j):
        cols = pl.ds(j * 512, 512)
        return SimpleNamespace(
            home=a.wi.at[:, cols],
            own=lambda bb, cc: s.wi.at[pl.ds(pl.multiple_of(bb * 256 + cc * 128, 128), 128), cols],
            block=lambda bb: s.wi.at[pl.ds(pl.multiple_of(bb * 256, 256), 256), cols],
            half=lambda bb, h: s.wi.at[pl.ds(pl.multiple_of(bb * 256 + h * 128, 128), 128), cols])

    def piece_back(j):
        part = pl.ds(j * 512, 512)
        return SimpleNamespace(
            home=a.wb.at[part, :],
            own=lambda bb, cc: s.wb.at[bb, part, pl.ds(pl.multiple_of(cc * 128, 128), 128)],
            block=lambda bb: s.wb.at[bb, part, :],
            half=lambda bb, h: s.wb.at[bb, pl.ds(j * 512 + h * 256, 256), :])

    pieces = dict(q=piece_qkv(0, a.wq), k=piece_qkv(1, a.wk), v=piece_qkv(2, a.wv), o=piece_o,
                  i0=piece_in(0), i1=piece_in(1), b0=piece_back(0), b1=piece_back(1))
    first_size = dict(
        q=s.w3.at[0:768, :], k=s.w3.at[0:768, :], v=s.w3.at[0:768, :], o=s.wo.at[0:3], i0=s.wi.at[0:768, 0:512],
        i1=s.wi.at[0:768, 0:512], b0=s.wb.at[0:3, 0:512, :], b1=s.wb.at[0:3, 0:512, :])
    for name, piece in pieces.items():
        piece.s1, piece.r1 = take("s"), take("r")
        piece.s2, piece.r2 = take("s"), take("r", 3)
        keeps_one = jnp.logical_or(jnp.logical_and(z == 0, c == 0), jnp.logical_and(z == 3, c == 1))
        at_end(piece.block(b), piece.s1, keeps_one, piece.own(b, 0))
        at_end(first_size[name], piece.s2)

    def to_outer(name):
        piece = pieces[name]
        is_self = jnp.logical_and(z == 3 * zh, z % 2 == c)
        send_or_keep(piece.home, piece.own(b, c), dev(b, z % 2, 3 * zh), is_self, piece.s1, piece.r1)

    def to_inner(name):
        piece = pieces[name]
        send(piece.home, piece.own(b, c), dev(b, z % 2, 2 - zh), piece.s1, piece.r1)

    def to_outer_in_turn(name):
        @pl.when(is_inner)
        def _():
            to_outer(name)

    def over_plane(name):
        piece = pieces[name]
        got(piece.block(b), piece.r1)
        send(piece.block(b), piece.block(b), x_near, piece.s2, piece.r2)
        send(piece.block(b), piece.block(b), y_near, piece.s2, piece.r2 + 1)

    def relay(name):
        piece = pieces[name]
        got(piece.block(bx), piece.r2)
        send(piece.half(bx, 0), piece.half(bx, 0), y_near, piece.s2, piece.r2 + 2)
        got(piece.block(by), piece.r2 + 1)
        send(piece.half(by, 1), piece.half(by, 1), x_near, piece.s2, piece.r2 + 2)

    def over_plane_now(names, chosen, relays=()):
        @pl.when(chosen)
        def _():
            for name in relays:
                relay(name)
            for name in names:
                over_plane(name)

    lives_here = jnp.logical_or(jnp.logical_and(z == 0, c == 0), jnp.logical_and(z == 3, c == 1))

    lives_away = jnp.logical_not(lives_here)

    def arrived(name):
        piece = pieces[name]
        got(piece.block(bd), piece.r2 + 2)

    tok_s, tok_r = take("s", 2), take("r", 4)
    fwd_s = take("s", 6)
    lens_s, lens_r = take("s"), take("r")
    cot_s, cot_r = take("s"), take("r")

    def send_lens():
        first = a.lens[0, 0].astype(F32)
        s.lens_own[0] = jnp.full((8, 128), first, F32)
        s.lens_own[1] = jnp.full((8, 128), first + a.lens[0, 1].astype(F32), F32)
        send(s.lens_own, s.lens_got, partner, lens_s, lens_r)
        at_end(s.lens_own, lens_s)

    def take_lens():
        got(s.lens_got, lens_r)

        @pl.when(c == zh)
        def _():
            s.lens_use[...] = s.lens_own[...]

        @pl.when(c != zh)
        def _():
            s.lens_use[...] = s.lens_got[...]

    def tok_block(r):
        return s.tk.at[rows_of(r), :]

    inner, outer = 1 + c, 3 * c
    is_relay = jnp.logical_and(c == zh, z == inner)

    def send_tokens():
        near = z // 2 == c
        first = jnp.where(near, 2 * c, inner)
        send_or_keep(a.tok, tok_block(z), dev(b, c, first), first == z, tok_s, tok_r + z)
        at_end(tok_block(z), tok_s, first == z)
        second = make_copy(a.tok, tok_block(z), dev(b, c, 2 * c + 1), tok_s + 1, tok_r + z)
        keep = jnp.logical_and(near, z == 2 * c + 1)
        go = jnp.logical_and(near, z != 2 * c + 1)

        @pl.when(keep)
        def _():
            pltpu.make_async_copy(a.tok, tok_block(z), rsem.at[tok_r + z]).start()

        @pl.when(go)
        def _():
            second.start()

        at_end(tok_block(z), tok_s + 1, jnp.logical_not(go))

    def pass_on(half, far):
        for k in range(2):
            r = half * 2 + k
            block = tok_block(r)
            got(block, tok_r + r)
            if far:
                on = make_copy(block, block, dev(b, c, outer), fwd_s + k, tok_r + r)

                @pl.when(is_relay)
                def _():
                    on.start()
            copy = make_copy(block, block, partner, fwd_s + 2 + 2 * far + k, tok_r + r)

            @pl.when(c == zh)
            def _():
                copy.start()

    for k in range(6):
        at_end(s.tk.at[0:BLOCK, :], fwd_s + k, jnp.logical_not(is_relay) if k < 2 else c != zh)

    def send_cotangent():
        zt, ct = 2 * c + z // 2, z % 2
        is_self = jnp.logical_and(zt == z, ct == c)
        send_or_keep(a.cot, s.cot_own, dev(b, ct, zt), is_self, cot_s, cot_r)
        at_end(s.cot_own, cot_s, is_self)

    gather_s, gather_r = take("s", 3), take("r", 12)
    scatter_s, scatter_r = take("s", 4), take("r", 20)
    for k in range(3):
        at_end(s.tk.at[0:3 * BLOCK, :], gather_s + k)
    for k in range(4):
        at_end(s.tk.at[0:3 * BLOCK, :], scatter_s + k)

    def block_at(full, r):
        return full.at[rows_of(r), :]

    def half_at(full, r, k):
        return full.at[pl.ds(pl.multiple_of(r * BLOCK + k * HALF, HALF), HALF), :]

    def gather_start(which, full, k):
        mine = half_at(full, t, k)
        send(mine, mine, pair, gather_s + which, gather_r + 4 * which + 1 + k)
        send(mine, mine, partner, gather_s + which, gather_r + 4 * which)

    def gather_step(which, full, j):
        base = gather_r + 4 * which

        @pl.when(j == 1)
        def _():
            got(block_at(full, t1), base)

        @pl.when(j == 2)
        def _():
            for k in range(2):
                near = half_at(full, t2, k)
                got(near, base + 1 + k)
                send(near, near, partner, gather_s + which, base + 3)

        @pl.when(j == 3)
        def _():
            got(block_at(full, t3), base + 3)

    halves = [pl.ds(k * HALF, HALF) for k in range(2)]

    def scatter(which, part):
        out, back = s.rs_out, s.rs_got
        ss, rr = scatter_s + which, scatter_r + 5 * which
        for k in range(2):
            mine = out.at[which, 0, halves[k], :]
            part(t3 * BLOCK + k * HALF, HALF, mine, None)
            send(mine, back.at[which, 0, halves[k], :], partner, ss, rr + k)
        for k in range(2):
            mine, theirs = out.at[which, 1, halves[k], :], back.at[which, 0, halves[k], :]
            got(theirs, rr + k)
            part(t2 * BLOCK + k * HALF, HALF, mine, theirs)
            send(mine, back.at[which, 1, halves[k], :], pair, ss, rr + 2 + k)
        part(t1 * BLOCK, BLOCK, out.at[which, 2], None)
        send(out.at[which, 2], back.at[which, 2], partner, ss, rr + 4)
        part(t * BLOCK, BLOCK, s.rs_own.at[which], None)

    def scatter_cols(which, blocks, k):
        out, back = s.rs_out, s.rs_got
        ss, rr = scatter_s + which, scatter_r + 5 * which
        slots = [pl.ds(pl.multiple_of(block * 256, 256), 256) for block in blocks]
        size = s.rs_got.at[which, 0, :, 0:256 * len(blocks)]

        def product(row, block):
            rows = pl.ds(pl.multiple_of(row * BLOCK, BLOCK), BLOCK)
            return dot_nn(s.act[rows, :], s.wb[block])

        def cast(row, slot):
            for block, cols in zip(blocks, slots):
                out[which, slot, :, cols] = product(row, block).astype(BF16)

        cast(t3, 0)
        for cols in slots:
            send(out.at[which, 0, :, cols], back.at[which, 0, :, cols], partner, ss, rr + k)
        cast(t1, 2)
        for cols in slots:
            send(out.at[which, 2, :, cols], back.at[which, 2, :, cols], partner, ss, rr + 4)
        got(size, rr + k)
        for block, cols in zip(blocks, slots):
            total = product(t2, block).astype(BF16).astype(F32) + back[which, 0, :, cols].astype(F32)
            out[which, 1, :, cols] = total.astype(BF16)
            send(out.at[which, 1, :, cols], back.at[which, 1, :, cols], pair, ss, rr + 2)
        for block, cols in zip(blocks, slots):
            s.rs_own[which, :, cols] = product(t, block).astype(BF16)

    def scatter_cols_wait(which):
        rr = scatter_r + 5 * which
        got(s.rs_got.at[which, 2], rr + 4)
        got(s.rs_got.at[which, 1], rr + 2)

    def scatter_wait(which, k):
        rr = scatter_r + 5 * which
        if k == 0:
            got(s.rs_got.at[which, 2], rr + 4)
        got(s.rs_got.at[which, 1, halves[k], :], rr + 2 + k)

    def scatter_rows(which, chunk):
        total = s.rs_own[which, chunk, :].astype(F32) + s.rs_got[which, 2, chunk, :].astype(F32)
        return total + s.rs_got[which, 1, chunk, :].astype(F32)

    def by_halves(which, body, after):
        if which == 1:
            scatter_cols_wait(which)
        for k in range(2):
            if which != 1:
                scatter_wait(which, k)
            loop(2, lambda i: body(2 * k + i))
            after(k)

    def put_part(dst, add, n, value):
        cols = slice(256 * n, 256 * n + 256)
        value = value.astype(BF16)
        if add is not None:
            value = (value.astype(F32) + add[:, cols].astype(F32)).astype(BF16)
        dst[:, cols] = value

    def loop(count, body):
        lax.fori_loop(0, count, lambda i, _: (body(i), 0)[1], 0)

    def grad_qkv(m):
        base = m * WIDTH
        return lambda bb, h: s.g3.at[pl.ds(pl.multiple_of(base + bb * 256 + h * 128, 128), 128), :]

    def grad_in_part(k):
        cols = pl.ds(k * 512, 512)
        return lambda bb, h: s.gi.at[pl.ds(pl.multiple_of(bb * 256 + h * 128, 128), 128), cols]

    def grad_back_part(k):
        part = pl.ds(k * 512, 512)
        return lambda bb, h: s.gb.at[bb, part, pl.ds(h * 128, 128)]

    grad_half = dict(
        q=grad_qkv(0), k=grad_qkv(1), v=grad_qkv(2), o=lambda bb, h: s.go.at[bb, :, pl.ds(h * 128, 128)],
        i0=grad_in_part(0), i1=grad_in_part(1), b0=grad_back_part(0), b1=grad_back_part(1))
    grad_s = {name: take("s", 2) for name in grad_half}
    grad_r = {name: take("r", 4) for name in grad_half}
    keeps_part = jnp.logical_or(jnp.logical_and(z == 0, c == 0), jnp.logical_and(z == 3, c == 1))
    for name in grad_half:
        at_end(s.stage[name].at[0:6], grad_s[name])
        at_end(s.stage[name].at[0:2], grad_s[name] + 1, keeps_part, s.stage[name].at[0])

    def chunks(name, body):
        size = 64 if name in ("i0", "i1") else 128
        count = HALVES[name][0] // size
        loop(count, lambda i: body(pl.ds(pl.multiple_of(i * size, size), size)))

    def grad_first(name, part=2):
        half, ss, rr, st = grad_half[name], grad_s[name], grad_r[name], s.stage[name]
        if part in (0, 2):
            send(half(bd, 0), st.at[1], x_near, ss, rr)
            send(half(bd, 1), st.at[3], y_near, ss, rr + 1)
        if part == 0:
            return
        send(half(bx, 0), st.at[0], x_near, ss, rr + 2)
        send(half(by, 1), st.at[2], y_near, ss, rr + 2)

    def grad_second(name):
        half, ss, rr, st = grad_half[name], grad_s[name], grad_r[name], s.stage[name]
        for h, block, to in ((0, by, y_near), (1, bx, x_near)):
            got(st.at[1 + 2 * h], rr + h)
            mine = half(block, h)

            def add(ch):
                st[4 + h, ch, :] = (mine[ch, :].astype(F32) + st[1 + 2 * h, ch, :].astype(F32)).astype(BF16)
            chunks(name, add)
            send(st.at[4 + h], st.at[6 + h], to, ss, rr + 2)

    def grad_third(name):
        half, ss, rr, st = grad_half[name], grad_s[name], grad_r[name], s.stage[name]
        zr = landed[name]
        got(st.at[0:4], rr + 2)
        for h in range(2):
            mine = half(b, h)

            def add_all(ch):
                total = mine[ch, :].astype(F32) + st[2 * h, ch, :].astype(F32) + st[6 + h, ch, :].astype(F32)
                st[8 + h, ch, :] = total.astype(BF16)
            chunks(name, add_all)
            is_self = jnp.logical_and(c == h, z == t)
            send_or_keep(st.at[8 + h], zr.at[zh], dev(b, h, t), is_self, ss + 1, rr + 3)

    def grad_final(name):
        got(landed[name], grad_r[name] + 3)

    to_inner("q")
    to_inner("k")
    send_tokens()
    to_inner("v")
    for name in "qkv":
        to_outer(name)

    @pl.when(jnp.logical_not(is_inner))
    def _():
        for name in ("o", "i0", "i1", "b0", "b1"):
            to_outer(name)

    send_lens()
    for name, ref in vectors.items():
        pltpu.make_async_copy(getattr(a, name), ref, vsem.at[list(vectors).index(name)]).start()
    s.sums[0] = jnp.zeros((16, WIDTH), F32)
    s.gb_in[...] = jnp.zeros((1, HIDDEN), F32)
    s.dkt[...] = jnp.zeros((HEAD_COLS, GROUP), F32)
    s.dvt[...] = jnp.zeros((HEAD_COLS, GROUP), F32)
    def in_turn(k):
        @pl.when(is_inner)
        def _():
            pl.semaphore_signal(s.turn.at[k], inc=1, device_id=pair, device_id_type=MESH_ID)

        @pl.when(jnp.logical_not(is_inner))
        def _():
            pl.semaphore_wait(s.turn.at[k], 1)

    over_plane("q")
    over_plane("k")
    relay("q")
    pass_on(zh, 0)
    to_inner("o")

    @pl.when(is_inner)
    def _():
        pass_on(flip(zh), 1)

    in_turn(0)
    to_inner("i0")
    take_lens()

    def make_bias(r):
        first, end = s.lens_use[0][0:1, 0:1], s.lens_use[1][0:1, 0:1]
        row = (lax.broadcasted_iota(jnp.int32, (BLOCK, GROUP), 0) + r * BLOCK).astype(F32)
        col = lax.broadcasted_iota(jnp.int32, (BLOCK, GROUP), 1).astype(F32)
        seg = lambda p: jnp.where(p >= end, 2.0, jnp.where(p >= first, 1.0, 0.0))
        s.bias[rows_of(r), :] = jnp.where(seg(row) == seg(col), 0.0, masked_value)
    loop(SLOTS, make_bias)
    for name, ref in vectors.items():
        pltpu.make_async_copy(getattr(a, name), ref, vsem.at[list(vectors).index(name)]).wait()
        setattr(a, name, ref)
    relay("k")
    over_plane("v")
    over_plane_now(("o", "i0"), lives_here)
    over_plane_now(("o",), is_inner)
    relay("v")
    over_plane_now(("i1",), lives_here, relays=("o",))

    @pl.when(jnp.logical_not(is_inner))
    def _():
        pass_on(flip(zh), 1)

    in_turn(1)
    to_outer_in_turn("o")
    to_outer_in_turn("i0")
    to_inner("i1")
    over_plane_now(("o",), jnp.logical_not(jnp.logical_or(is_inner, lives_here)))


    def turn_tokens(r):
        s.tkt[:, rows_of(r)] = s.tk[rows_of(r), :].T
    loop(SLOTS, turn_tokens)

    head_cols = pl.ds(pl.multiple_of(t * HEAD_COLS, HEAD_COLS), HEAD_COLS)

    def project(m):
        acc = dot_nn(s.tk[...], s.w3[m * WIDTH:(m + 1) * WIDTH, :])
        if m == 0:
            value = (acc + a.bq[:, head_cols]).astype(BF16)
            scaled = (value.astype(F32) * 0.125).astype(BF16)
            s.q[...] = scaled
            s.qt[...] = scaled.T
        elif m == 1:
            value = acc.astype(BF16)
            s.k[...] = value
            s.ks[...] = (value.astype(F32) * 0.125).astype(BF16)
        else:
            s.v[...] = (acc + a.bv[:, head_cols]).astype(BF16)

    arrived("q")
    project(0)
    arrived("k")
    project(1)
    over_plane_now(("i0",), lives_away)
    over_plane_now(("b0",), lives_here, relays=("i0",))
    in_turn(2)
    to_outer_in_turn("i1")
    to_inner("b0")
    arrived("v")
    project(2)

    def attend(r):
        rows = rows_of(r)
        parts = []
        for h in range(4):
            cols = slice(64 * h, 64 * h + 64)
            scores = dot_nt(s.q[rows, cols], s.k[:, cols]) + s.bias[rows, :]
            top = jnp.max(scores, axis=-1, keepdims=True)
            weight = jnp.exp(scores - top)
            total = jnp.sum(weight, axis=-1, keepdims=True)
            prob = (weight * (1.0 / total)).astype(BF16)
            s.ps[h, rows, :] = prob
            parts.append(dot_nn(prob, s.v[:, cols]))
        context = jnp.concatenate(parts, axis=1).astype(BF16)
        s.ctx[rows, :] = context
        s.ctxt[:, rows] = context.T
    loop(2, attend)
    over_plane_now((), lives_away, relays=("o",))
    over_plane_now(("i1",), lives_away)
    over_plane_now(("b1",), lives_here)
    in_turn(3)
    to_outer_in_turn("b0")
    to_outer_in_turn("b1")
    to_inner("b1")
    loop(2, lambda r: attend(r + 2))
    over_plane_now((), lives_away, relays=("i0",))
    over_plane_now(("b0",), lives_away)
    arrived("o")

    def attn_part(first, count, dst, add):
        rows = s.ctx[pl.ds(pl.multiple_of(first, HALF), count), :]
        for n in range(4):
            put_part(dst, add, n, dot_nn(rows, s.wo[n]))
    scatter(0, attn_part)
    relay("i1")
    for m in range(3):
        for n in range(4):
            s.w3t[m, :, 256 * n:256 * n + 256] = s.w3[m * WIDTH + 256 * n:m * WIDTH + 256 * n + 256, :].T
    for n in range(4):
        s.wot[256 * n:256 * n + 256, :] = s.wo[n].T

    CH = 32

    def own_chunk(i):
        return pl.ds(pl.multiple_of(i * CH, CH), CH)

    def group_chunk(i):
        return pl.ds(pl.multiple_of(t * BLOCK + i * CH, CH), CH)

    def norm_one(i):
        ch = own_chunk(i)
        resid = s.tk[group_chunk(i), :].astype(F32) + scatter_rows(0, ch) + a.bo[...]
        centered = resid - jnp.mean(resid, axis=-1, keepdims=True)
        inv = lax.rsqrt(jnp.mean(centered * centered, axis=-1, keepdims=True) + epsilon)
        normed = centered * inv
        hidden = normed * a.ga[...] + a.sa[...]
        s.normed1[ch, :] = normed
        s.inv1[ch, :] = jnp.broadcast_to(inv, (CH, 128))
        s.hid1[ch, :] = hidden
        s.hid[group_chunk(i), :] = hidden.astype(BF16)
    over_plane_now(("b1",), lives_away)
    by_halves(0, norm_one, lambda k: gather_start(0, s.hid, k))
    send_cotangent()
    relay("b0")
    arrived("i0")
    arrived("i1")

    def ffn_in(j):
        gather_step(0, s.hid, j)
        r = slot_step(t, j)
        rows = rows_of(r)
        for n in range(4):
            cols = slice(256 * n, 256 * n + 256)
            bias = a.bi[:, pl.ds(pl.multiple_of(t * HIDDEN + n * 256, 256), 256)]
            pre = dot_nn(s.hid[rows, :], s.wi[:, cols]) + bias
            cdf = 0.5 * (1.0 + lax.erf(pre * 0.7071067811865476))
            pdf = jnp.exp(-0.5 * pre * pre) * 0.3989422804014327
            s.act[rows, cols] = (pre * cdf).astype(BF16)
            s.slope[rows, cols] = cdf + pre * pdf
    loop(SLOTS, ffn_in)

    def turn_ffn(r):
        rows = rows_of(r)
        s.actt[:, rows] = s.act[rows, :].T
        s.hidt[:, rows] = s.hid[rows, :].T
    relay("b1")
    scatter_cols(1, (b, bx, by), 0)
    loop(SLOTS, turn_ffn)

    def turn_wi(r):
        rows = rows_of(r)
        s.wit[:, rows] = s.wi[rows, :].T
    loop(8, turn_wi)
    arrived("b0")
    arrived("b1")
    scatter_cols(1, (bd,), 1)

    def turn_wb(r):
        rows = rows_of(r)
        for n in range(4):
            s.wbt[256 * n:256 * n + 256, rows] = s.wb[n, rows, :].T
    loop(8, turn_wb)
    got(s.cot_own, cot_r)

    def add_rows(row, value):
        s.sums[0, row:row + 1, :] += jnp.sum(value, axis=0, keepdims=True)

    def norm_two(i):
        ch = own_chunk(i)
        resid = s.hid1[ch, :] + scatter_rows(1, ch) + a.bb[...]
        centered = resid - jnp.mean(resid, axis=-1, keepdims=True)
        inv = lax.rsqrt(jnp.mean(centered * centered, axis=-1, keepdims=True) + epsilon)
        normed = centered * inv
        position = lax.broadcasted_iota(jnp.int32, (CH, 128), 0) + (t * BLOCK + i * CH)
        live = jnp.where(position.astype(F32) < s.lens_use[1][0:1, :], 1.0, 0.0)[:, 0:1]
        s.out_own[ch, :] = ((normed * a.gf[...] + a.sf[...]) * live).astype(BF16)
        grad = s.cot_own[ch, :].astype(F32) * live
        add_rows(4, grad * normed)
        add_rows(5, grad)
        u = grad * a.gf[...]
        first = jnp.mean(u, axis=-1, keepdims=True)
        second = jnp.mean(u * normed, axis=-1, keepdims=True)
        grad_two = inv * (u - first - normed * second)
        add_rows(3, grad_two)
        s.g2f[ch, :] = grad_two
        s.g2[group_chunk(i), :] = grad_two.astype(BF16)
    by_halves(1, norm_two, lambda k: gather_start(1, s.g2, k))
    out_s, out_r = take("s"), take("r")
    home_self = jnp.logical_and(zh == c, t == z)

    def ffn_back(j):
        @pl.when(j < 3)
        def _():
            gather_step(1, s.g2, j)
        r = slot_step(t, j)
        rows = rows_of(r)
        for n in range(4):
            cols = slice(256 * n, 256 * n + 256)
            grad = dot_nn(s.g2[rows, :], s.wbt[:, cols]) * s.slope[rows, cols]
            s.gb_in[:, cols] += jnp.sum(grad, axis=0, keepdims=True)
            s.gpre[rows, cols] = grad.astype(BF16)
    loop(SLOTS - 1, ffn_back)

    def grad_back(k):
        part = slice(512 * k, 512 * k + 512)

        def body(n):
            for e in range(2):
                block = n * 2 + e
                s.gb[block, part, :] = dot_nn(s.actt[part, :], s.g2[:, cols_of(block)]).astype(BF16)
        loop(2, body)

    def grad_in(k):
        cols = slice(512 * k, 512 * k + 512)

        def body(m):
            part = rows_of(m * 4, 512)
            s.gi[part, cols] = dot_nn(s.hidt[part, :], s.gpre[:, cols]).astype(BF16)
        loop(2, body)

    gather_step(1, s.g2, 3)
    grad_back(0)
    grad_first("b0")
    ffn_back(3)
    grad_back(1)
    grad_first("b1", 0)
    send_or_keep(s.out_own, o.out, dev(b, zh, t), home_self, out_s, out_r)
    at_end(s.out_own, out_s, home_self)

    def in_part(first, count, dst, add):
        rows = pl.ds(pl.multiple_of(first, HALF), count)
        for n in range(4):
            put_part(dst, add, n, dot_nn(s.gpre[rows, :], s.wit[:, 256 * n:256 * n + 256]))
    scatter(2, in_part)
    grad_in(0)
    grad_in(1)
    grad_second("b0")
    grad_first("b1", 1)
    grad_second("b1")
    grad_first("i0", 0)

    def norm_one_back(i):
        ch = own_chunk(i)
        grad = s.g2f[ch, :] + scatter_rows(2, ch)
        normed = s.normed1[ch, :]
        add_rows(1, grad * normed)
        add_rows(2, grad)
        u = grad * a.ga[...]
        first = jnp.mean(u, axis=-1, keepdims=True)
        second = jnp.mean(u * normed, axis=-1, keepdims=True)
        grad_one = s.inv1[ch, 0:1] * (u - first - normed * second)
        add_rows(0, grad_one)
        s.g1f[ch, :] = grad_one
        s.g1[group_chunk(i), :] = grad_one.astype(BF16)
    by_halves(2, norm_one_back, lambda k: gather_start(2, s.g1, k))
    grad_first("i0", 1)
    grad_third("b0")

    def attend_back(j):
        gather_step(2, s.g1, j)
        r = slot_step(t, j)
        rows = rows_of(r)
        grad_ctx = dot_nn(s.g1[rows, :], s.wot[...]).astype(BF16)
        s.gctxt[:, rows] = grad_ctx.T
        product = grad_ctx.astype(F32) * s.ctx[rows, :].astype(F32)
        parts = []
        for h in range(4):
            cols = slice(64 * h, 64 * h + 64)
            prob = s.ps[h, rows, :]
            delta = jnp.sum(product[:, cols], axis=-1, keepdims=True)
            grad_prob = dot_nt(grad_ctx[:, cols], s.v[:, cols])
            grad_score = (prob.astype(F32) * (grad_prob - delta)).astype(BF16)
            parts.append(dot_nn(grad_score, s.ks[:, cols]))
            s.dkt[cols, :] += dot_nn(s.qt[cols, rows], grad_score)
            s.dvt[cols, :] += dot_nn(s.gctxt[cols, rows], prob)
        grad_query = jnp.concatenate(parts, axis=1)
        for k in range(4):
            @pl.when(t == k)
            def _():
                s.sums[0, 6:7, 256 * k:256 * k + 256] += jnp.sum(grad_query, axis=0, keepdims=True)
        s.dq[rows, :] = grad_query.astype(BF16)
    loop(2, attend_back)
    grad_third("b1")
    loop(1, lambda j: attend_back(j + 2))
    grad_second("i0")
    grad_first("i1")
    loop(1, lambda j: attend_back(j + 3))

    def turn_back(r):
        rows = rows_of(r)
        s.dk[rows, :] = s.dkt[:, rows].T.astype(BF16)
        grad_value = s.dvt[:, rows].T
        for k in range(4):
            @pl.when(t == k)
            def _():
                s.sums[0, 7:8, 256 * k:256 * k + 256] += jnp.sum(grad_value, axis=0, keepdims=True)
        s.dv[rows, :] = grad_value.astype(BF16)
    loop(SLOTS, turn_back)
    for k in range(4):
        @pl.when(t == k)
        def _():
            s.sums[0, 8 + k:9 + k, :] = s.gb_in[...]

    sums_s, sums_r = take("s", 5), take("r", 5)
    sums_to = [partner, across, pair, x_near, y_near]

    def sums_start(k):
        send(s.sums.at[k], s.sums_got.at[k], sums_to[k], sums_s + k, sums_r + k)
        at_end(s.sums.at[k], sums_s + k)

    def sums_finish(k):
        got(s.sums_got.at[k], sums_r + k)
        total = s.sums[k] + s.sums_got[k]
        s.sums[k + 1] = total
        if k == 4:
            pltpu.make_async_copy(s.sums.at[5], o.sums, vsem.at[0]).start()

    sums_start(0)

    def tok_part(first, count, dst, add):
        rows = pl.ds(pl.multiple_of(first, HALF), count)
        for n in range(4):
            cols = slice(256 * n, 256 * n + 256)
            acc = dot_nn(s.dq[rows, :], s.w3t[0, :, cols])
            acc = acc + dot_nn(s.dk[rows, :], s.w3t[1, :, cols])
            acc = acc + dot_nn(s.dv[rows, :], s.w3t[2, :, cols])
            put_part(dst, add, n, acc)
    scatter(3, tok_part)
    sums_finish(0)
    sums_start(1)

    def grad_head(m, src):
        s.g3[m * WIDTH:(m + 1) * WIDTH, :] = dot_nn(s.tkt[...], src[...]).astype(BF16)

    grad_third("i0")
    for n in range(4):
        s.go[n] = dot_nn(s.ctxt[...], s.g1[:, 256 * n:256 * n + 256]).astype(BF16)
    grad_head(0, s.dq)
    grad_head(1, s.dk)
    grad_head(2, s.dv)
    grad_second("i1")
    grad_first("o")
    grad_first("q")
    grad_third("i1")
    grad_second("o")
    grad_first("k")

    def last_rows(i):
        ch = own_chunk(i)
        s.gtok_own[ch, :] = (s.g1f[ch, :] + scatter_rows(3, ch)).astype(BF16)
    by_halves(3, last_rows, lambda k: None)
    gtok_s, gtok_r = take("s"), take("r")
    send_or_keep(s.gtok_own, o.gtok, dev(b, zh, t), home_self, gtok_s, gtok_r)
    at_end(s.gtok_own, gtok_s, home_self)
    grad_second("q")
    grad_first("v")
    sums_finish(1)
    sums_start(2)
    grad_third("o")
    grad_second("k")
    grad_third("q")
    sums_finish(2)
    grad_second("v")
    sums_start(3)
    grad_third("k")
    grad_third("v")
    sums_finish(3)
    sums_start(4)
    grad_final("b0")
    grad_final("b1")
    grad_final("i0")
    grad_final("i1")
    got(o.gtok, gtok_r)
    got(o.out, out_r)
    grad_final("o")
    grad_final("q")
    sums_finish(4)
    grad_final("k")
    grad_final("v")

    pltpu.make_async_copy(s.sums.at[5], o.sums, vsem.at[0]).wait()
    for size_of, sk, skipped, instead in to_drain:
        if skipped is None:
            left(size_of, sk)
        else:
            @pl.when(jnp.logical_not(skipped))
            def _():
                left(size_of, sk)
            if instead is not None:
                @pl.when(skipped)
                def _():
                    left(instead, sk)


def result_kernel(out, gtok, sums, zq, zk, zv, zo, zi0, zi1, zb0, zb1, o_out, o_gtok, o_gq, o_gbq, o_gk, o_gv, o_gbv, o_go,
                  o_gbo, o_gga, o_gsa, o_gi, o_gbi, o_gb, o_gbb, o_ggf, o_gsf):
    both = lambda ref: ref[0].astype(F32) + ref[1].astype(F32)
    o_out[...] = out[...]
    o_gtok[...] = gtok[...].astype(F32)
    o_gq[...], o_gk[...], o_gv[...], o_go[...] = both(zq), both(zk), both(zv), both(zo)
    o_gi[:, :512], o_gi[:, 512:] = both(zi0), both(zi1)
    o_gb[:512, :], o_gb[512:, :] = both(zb0), both(zb1)
    for row, ref in ((6, o_gbq), (7, o_gbv), (0, o_gbo), (1, o_gga), (2, o_gsa), (3, o_gbb), (4, o_ggf), (5, o_gsf)):
        ref[...] = sums[row:row + 1, :]
    for k in range(4):
        o_gbi[:, WIDTH * k:WIDTH * k + WIDTH] = sums[8 + k:9 + k, :]


def on_device_fused(tokens, lengths, w_query, b_query, w_key, w_value, b_value, w_out, b_out, gain_attn, shift_attn,
                    w_in, b_in, w_back, b_back, gain_ffn, shift_ffn, cotangent):
    row = lambda vec: vec.reshape(1, -1)
    operands = (tokens, lengths, w_query, row(b_query), w_key, w_value, row(b_value), w_out, row(b_out),
                row(gain_attn), row(shift_attn), w_in, row(b_in), w_back, row(b_back), row(gain_ffn),
                row(shift_ffn), cotangent)
    vmem = pl.BlockSpec(memory_space=pltpu.VMEM)
    stay = pl.BlockSpec(memory_space=pl.ANY)
    in_specs = [stay] * len(operands)
    in_specs[1] = pl.BlockSpec(memory_space=pltpu.SMEM)
    shape = lambda dims, dtype: jax.ShapeDtypeStruct(dims, dtype)
    between = [shape(tokens.shape, BF16), shape(tokens.shape, BF16), shape((16, WIDTH), F32)]
    between += [shape((2,) + HALVES[name], BF16) for name in ("q", "k", "v", "o", "i0", "i1", "b0", "b1")]
    parts = pl.pallas_call(
        layer_kernel,
        out_shape=between,
        in_specs=in_specs,
        out_specs=[stay] * len(between),
        scratch_shapes=jax.tree.leaves(scratch_table()),
        compiler_params=pltpu.CompilerParams(collective_id=0, has_side_effects=True, vmem_limit_bytes=64 * 1024 * 1000),
        name="layer",
    )(*operands)
    line = shape((1, WIDTH), F32)
    results = (
        shape(tokens.shape, BF16), shape(tokens.shape, F32), shape(w_query.shape, F32), line, shape(w_key.shape, F32),
        shape(w_value.shape, F32), line, shape(w_out.shape, F32), line, line, line, shape(w_in.shape, F32),
        shape((1, b_in.shape[0]), F32), shape(w_back.shape, F32), line, line, line)
    outs = pl.pallas_call(
        result_kernel,
        out_shape=results,
        in_specs=[vmem] * len(between),
        out_specs=[vmem] * len(results),
        name="results",
    )(*parts)
    return tuple(v.reshape(-1) if v.shape[0] == 1 else v for v in outs)


def fits_fused(mesh):
    return dict(mesh.shape) == {"dp": 8, "tensor": 4}


def solution(mesh):
    placed = (
        P(("dp", "tensor"), None),
        P("dp", None),
        P("dp", "tensor"),
        P(),
        P("dp", "tensor"),
        P("dp", "tensor"),
        P(),
        P("tensor", "dp"),
        P(),
        P(),
        P(),
        P("dp", "tensor"),
        P(),
        P("tensor", "dp"),
        P(),
        P(),
        P(),
        P(("dp", "tensor"), None),
    )
    on_device = on_device_fused if fits_fused(mesh) else on_device_plain
    return jax.shard_map(
        on_device,
        mesh=mesh,
        in_specs=placed,
        out_specs=(
            P(("dp", "tensor"), None),
            P(("dp", "tensor"), None),
            P("dp", "tensor"),
            P(),
            P("dp", "tensor"),
            P("dp", "tensor"),
            P(),
            P("tensor", "dp"),
            P(),
            P(),
            P(),
            P("dp", "tensor"),
            P(),
            P("tensor", "dp"),
            P(),
            P(),
            P(),
        ),
        check_vma=False,
    )
```

```python
from types import SimpleNamespace

import jax
import jax.numpy as jnp
from jax import lax
from jax.experimental import pallas as pl
from jax.experimental.pallas import tpu as pltpu
from jax.sharding import PartitionSpec as P

HD = 64


epsilon = 1e-06
masked_value = -1e30


def matmul_plain(left_side, right_side):
    return jnp.dot(left_side, right_side, preferred_element_type=jnp.float32)


def matmul_over_rows(left_side, right_side):
    return lax.dot_general(
        left_side, right_side, (((0,), (0,)), ((), ())), preferred_element_type=jnp.float32
    )


def matmul_over_cols(left_side, right_side):
    return lax.dot_general(
        left_side, right_side, (((1,), (1,)), ((), ())), preferred_element_type=jnp.float32
    )


def layer_norm(residual, gain_vec, shift_vec):
    mean_val = jnp.mean(residual, axis=-1, keepdims=True)
    centered = residual - mean_val
    inv_std = lax.rsqrt(jnp.mean(centered * centered, axis=-1, keepdims=True) + epsilon)
    normed = centered * inv_std
    return (normed * gain_vec + shift_vec, normed, inv_std)


def norm_back(grad_out, normed, inv_std, gain_vec):
    grad_norm = grad_out * gain_vec
    first_mean = jnp.mean(grad_norm, axis=-1, keepdims=True)
    second_mean = jnp.mean(grad_norm * normed, axis=-1, keepdims=True)
    return inv_std * (grad_norm - first_mean - normed * second_mean)


def gelu_parts(preact):
    cdf_val = 0.5 * (1.0 + lax.erf(preact * 0.7071067811865476))
    pdf_val = jnp.exp(-0.5 * preact * preact) * 0.3989422804014327
    return (preact * cdf_val, cdf_val + preact * pdf_val)


def attend_forward(query_rows, key_rows, value_rows, seg_ids, head_dim, block_rows):
    group_rows, head_cols = query_rows.shape
    pair_width = 2 * head_dim
    block_count = group_rows // block_rows
    pair_count = head_cols // pair_width
    score_scale = head_dim ** (-0.5)

    def attend_step(step_index, loop_carry):
        context, log_total = loop_carry
        pair_index = step_index // block_count
        row_start = step_index % block_count * block_rows
        first_col = pair_index * pair_width
        query_block = lax.dynamic_slice(
            query_rows, (row_start, first_col), (block_rows, pair_width)
        ).reshape(block_rows, 2, head_dim)
        key_pair = lax.dynamic_slice(key_rows, (0, first_col), (group_rows, pair_width)).reshape(
            group_rows, 2, head_dim
        )
        value_pair = lax.dynamic_slice(
            value_rows, (0, first_col), (group_rows, pair_width)
        ).reshape(group_rows, 2, head_dim)
        same_seg = seg_ids[:, None] == seg_ids[None, :]
        scores = (
            jnp.einsum("qhd,khd->hqk", query_block, key_pair, preferred_element_type=jnp.float32)
            * score_scale
        )
        scores = jnp.where(same_seg[None], scores, masked_value)
        row_max = jnp.max(scores, axis=-1, keepdims=True)
        block_total = row_max + jnp.log(jnp.sum(jnp.exp(scores - row_max), axis=-1, keepdims=True))
        prob_bf = jnp.exp(scores - block_total).astype(jnp.bfloat16)
        context_block = jnp.einsum(
            "hqk,khd->qhd", prob_bf, value_pair, preferred_element_type=jnp.float32
        ).astype(jnp.bfloat16)
        context = lax.dynamic_update_slice(
            context, context_block.reshape(block_rows, pair_width), (row_start, first_col)
        )
        log_total = lax.dynamic_update_slice(
            log_total, block_total[:, :, 0], (2 * pair_index, row_start)
        )
        return (context, log_total)

    start_carry = (
        jnp.zeros((group_rows, head_cols), jnp.bfloat16),
        jnp.zeros((head_cols // head_dim, group_rows), jnp.float32),
    )
    return lax.fori_loop(0, pair_count * block_count, attend_step, start_carry)


def attend_backward(
    query_rows,
    key_rows,
    value_rows,
    context,
    grad_context,
    log_total,
    seg_ids,
    head_dim,
    block_rows,
):
    group_rows, head_cols = query_rows.shape
    pair_width = 2 * head_dim
    block_count = group_rows // block_rows
    pair_count = head_cols // pair_width
    score_scale = head_dim ** (-0.5)

    def back_step(step_index, loop_carry):
        grad_query, grad_keys, grad_values = loop_carry
        pair_index = step_index // block_count
        row_start = step_index % block_count * block_rows
        first_col = pair_index * pair_width
        query_block = lax.dynamic_slice(
            query_rows, (row_start, first_col), (block_rows, pair_width)
        ).reshape(block_rows, 2, head_dim)
        key_pair = lax.dynamic_slice(key_rows, (0, first_col), (group_rows, pair_width)).reshape(
            group_rows, 2, head_dim
        )
        value_pair = lax.dynamic_slice(
            value_rows, (0, first_col), (group_rows, pair_width)
        ).reshape(group_rows, 2, head_dim)
        context_block = lax.dynamic_slice(
            context, (row_start, first_col), (block_rows, pair_width)
        ).reshape(block_rows, 2, head_dim)
        gctx_block = lax.dynamic_slice(
            grad_context, (row_start, first_col), (block_rows, pair_width)
        ).reshape(block_rows, 2, head_dim)
        total_block = lax.dynamic_slice(log_total, (2 * pair_index, row_start), (2, block_rows))
        same_seg = seg_ids[:, None] == seg_ids[None, :]
        scores = (
            jnp.einsum("qhd,khd->hqk", query_block, key_pair, preferred_element_type=jnp.float32)
            * score_scale
        )
        scores = jnp.where(same_seg[None], scores, masked_value)
        probs = jnp.exp(scores - total_block[:, :, None])
        prob_bf = probs.astype(jnp.bfloat16)
        grad_probs = jnp.einsum(
            "qhd,khd->hqk", gctx_block, value_pair, preferred_element_type=jnp.float32
        )
        delta_rows = jnp.sum(
            gctx_block.astype(jnp.float32) * context_block.astype(jnp.float32), axis=-1
        ).T[:, :, None]
        grad_scores = (probs * (grad_probs - delta_rows) * score_scale).astype(jnp.bfloat16)
        grad_q_block = jnp.einsum(
            "hqk,khd->qhd", grad_scores, key_pair, preferred_element_type=jnp.float32
        ).reshape(block_rows, pair_width)
        grad_k_pair = jnp.einsum(
            "hqk,qhd->khd", grad_scores, query_block, preferred_element_type=jnp.float32
        ).reshape(group_rows, pair_width)
        grad_v_pair = jnp.einsum(
            "hqk,qhd->khd", prob_bf, gctx_block, preferred_element_type=jnp.float32
        ).reshape(group_rows, pair_width)
        grad_query = lax.dynamic_update_slice(grad_query, grad_q_block, (row_start, first_col))
        old_keys = lax.dynamic_slice(grad_keys, (0, first_col), (group_rows, pair_width))
        grad_keys = lax.dynamic_update_slice(grad_keys, old_keys + grad_k_pair, (0, first_col))
        old_values = lax.dynamic_slice(grad_values, (0, first_col), (group_rows, pair_width))
        grad_values = lax.dynamic_update_slice(
            grad_values, old_values + grad_v_pair, (0, first_col)
        )
        return (grad_query, grad_keys, grad_values)

    zero_grad = jnp.zeros((group_rows, head_cols), jnp.float32)
    return lax.fori_loop(0, pair_count * block_count, back_step, (zero_grad, zero_grad, zero_grad))


def on_device_plain(
    tokens,
    lengths,
    w_query,
    b_query,
    w_key,
    w_value,
    b_value,
    w_out,
    b_out,
    gain_attn,
    shift_attn,
    w_in,
    b_in,
    w_back,
    b_back,
    gain_ffn,
    shift_ffn,
    cotangent,
):
    tensor_size = lax.axis_size("tensor")
    tensor_index = lax.axis_index("tensor")
    local_rows = tokens.shape[0]
    group_rows = local_rows * tensor_size
    head_cols = w_query.shape[1]
    hidden_cols = w_in.shape[1]
    block_rows = min(512, group_rows)
    seq_lens = lengths[0]
    live_end = seq_lens[0] + seq_lens[1]
    positions = jnp.arange(group_rows, dtype=jnp.int32)
    seg_ids = (positions >= seq_lens[0]).astype(jnp.int32) + (positions >= live_end).astype(
        jnp.int32
    )
    local_pos = tensor_index * local_rows + jnp.arange(local_rows, dtype=jnp.int32)
    live_rows = (local_pos < live_end).astype(jnp.float32)[:, None]
    rows_full = lax.all_gather(tokens, "tensor", axis=0, tiled=True)
    attn_mats = (
        lax.all_gather(w_query, "dp", axis=0, tiled=True),
        lax.all_gather(w_key, "dp", axis=0, tiled=True),
        lax.all_gather(w_value, "dp", axis=0, tiled=True),
        lax.all_gather(w_out, "dp", axis=1, tiled=True),
    )
    mat_query, mat_key, mat_value, mat_out = attn_mats
    bias_query = lax.dynamic_slice_in_dim(b_query, tensor_index * head_cols, head_cols)
    bias_value = lax.dynamic_slice_in_dim(b_value, tensor_index * head_cols, head_cols)
    bias_in = lax.dynamic_slice_in_dim(b_in, tensor_index * hidden_cols, hidden_cols)
    query_rows = (matmul_plain(rows_full, mat_query) + bias_query).astype(jnp.bfloat16)
    key_rows = matmul_plain(rows_full, mat_key).astype(jnp.bfloat16)
    value_rows = (matmul_plain(rows_full, mat_value) + bias_value).astype(jnp.bfloat16)
    context, log_total = attend_forward(query_rows, key_rows, value_rows, seg_ids, HD, block_rows)
    attn_sum = lax.psum_scatter(
        matmul_plain(context, mat_out).astype(jnp.bfloat16),
        "tensor",
        scatter_dimension=0,
        tiled=True,
    ).astype(jnp.float32)
    resid_one = tokens.astype(jnp.float32) + attn_sum + b_out
    hidden_one, normed_one, inv_one = layer_norm(resid_one, gain_attn, shift_attn)
    hidden_bf = hidden_one.astype(jnp.bfloat16)
    hidden_full = lax.all_gather(hidden_bf, "tensor", axis=0, tiled=True)
    ffn_mats = (
        lax.all_gather(w_in, "dp", axis=0, tiled=True),
        lax.all_gather(w_back, "dp", axis=1, tiled=True),
    )
    mat_in, mat_back = ffn_mats
    preact = matmul_plain(hidden_full, mat_in) + bias_in
    activ_val, gelu_slope = gelu_parts(preact)
    activation = activ_val.astype(jnp.bfloat16)
    ffn_sum = lax.psum_scatter(
        matmul_plain(activation, mat_back).astype(jnp.bfloat16),
        "tensor",
        scatter_dimension=0,
        tiled=True,
    ).astype(jnp.float32)
    resid_two = hidden_one + ffn_sum + b_back
    normed_out, normed_two, inv_two = layer_norm(resid_two, gain_ffn, shift_ffn)
    output = (normed_out * live_rows).astype(jnp.bfloat16)
    grad_final = cotangent.astype(jnp.float32) * live_rows
    grad_gain_ffn = jnp.sum(grad_final * normed_two, axis=0)
    grad_shift_ffn = jnp.sum(grad_final, axis=0)
    grad_two = norm_back(grad_final, normed_two, inv_two, gain_ffn)
    grad_b_back = jnp.sum(grad_two, axis=0)
    mat_query, mat_key, mat_value, mat_out, mat_in, mat_back = (
        lax.all_gather(w_query, "dp", axis=0, tiled=True),
        lax.all_gather(w_key, "dp", axis=0, tiled=True),
        lax.all_gather(w_value, "dp", axis=0, tiled=True),
        lax.all_gather(w_out, "dp", axis=1, tiled=True),
        lax.all_gather(w_in, "dp", axis=0, tiled=True),
        lax.all_gather(w_back, "dp", axis=1, tiled=True),
    )
    grad_two_full = lax.all_gather(grad_two.astype(jnp.bfloat16), "tensor", axis=0, tiled=True)
    grad_w_back = matmul_over_rows(activation, grad_two_full)
    grad_pre = matmul_over_cols(grad_two_full, mat_back) * gelu_slope
    grad_b_in_part = jnp.sum(grad_pre, axis=0)
    grad_pre_bf = grad_pre.astype(jnp.bfloat16)
    grad_w_in = matmul_over_rows(hidden_full, grad_pre_bf)
    grad_one_out = grad_two + lax.psum_scatter(
        matmul_over_cols(grad_pre_bf, mat_in).astype(jnp.bfloat16),
        "tensor",
        scatter_dimension=0,
        tiled=True,
    ).astype(jnp.float32)
    grad_w_in, grad_w_back = (
        lax.psum_scatter(grad_w_in, "dp", scatter_dimension=0, tiled=True),
        lax.psum_scatter(grad_w_back, "dp", scatter_dimension=1, tiled=True),
    )
    grad_gain_attn = jnp.sum(grad_one_out * normed_one, axis=0)
    grad_shift_attn = jnp.sum(grad_one_out, axis=0)
    grad_one = norm_back(grad_one_out, normed_one, inv_one, gain_attn)
    grad_b_out = jnp.sum(grad_one, axis=0)
    grad_one_full = lax.all_gather(grad_one.astype(jnp.bfloat16), "tensor", axis=0, tiled=True)
    grad_w_out = matmul_over_rows(context, grad_one_full)
    grad_context = matmul_over_cols(grad_one_full, mat_out).astype(jnp.bfloat16)
    grad_query, grad_keys, grad_values = attend_backward(
        query_rows, key_rows, value_rows, context, grad_context, log_total, seg_ids, HD, block_rows
    )
    grad_b_query_part = jnp.sum(grad_query, axis=0)
    grad_b_value_part = jnp.sum(grad_values, axis=0)
    grad_query_bf = grad_query.astype(jnp.bfloat16)
    grad_keys_bf = grad_keys.astype(jnp.bfloat16)
    grad_values_bf = grad_values.astype(jnp.bfloat16)
    grad_w_query = matmul_over_rows(rows_full, grad_query_bf)
    grad_w_key = matmul_over_rows(rows_full, grad_keys_bf)
    grad_w_value = matmul_over_rows(rows_full, grad_values_bf)
    query_part = matmul_over_cols(grad_query_bf, mat_query)
    key_part = matmul_over_cols(grad_keys_bf, mat_key)
    value_part = matmul_over_cols(grad_values_bf, mat_value)
    grad_in = grad_one + lax.psum_scatter(
        (query_part + key_part + value_part).astype(jnp.bfloat16),
        "tensor",
        scatter_dimension=0,
        tiled=True,
    ).astype(jnp.float32)
    grad_w_query, grad_w_key, grad_w_value, grad_w_out = (
        lax.psum_scatter(grad_w_query, "dp", scatter_dimension=0, tiled=True),
        lax.psum_scatter(grad_w_key, "dp", scatter_dimension=0, tiled=True),
        lax.psum_scatter(grad_w_value, "dp", scatter_dimension=0, tiled=True),
        lax.psum_scatter(grad_w_out, "dp", scatter_dimension=1, tiled=True),
    )

    def widen(part_vec, full_width):
        return lax.dynamic_update_slice_in_dim(
            jnp.zeros((full_width,), jnp.float32), part_vec, tensor_index * part_vec.shape[0], 0
        )

    small_sums = lax.psum(
        (
            widen(grad_b_query_part, b_query.shape[0]),
            widen(grad_b_value_part, b_value.shape[0]),
            grad_b_out,
            grad_gain_attn,
            grad_shift_attn,
            widen(grad_b_in_part, b_in.shape[0]),
            grad_b_back,
            grad_gain_ffn,
            grad_shift_ffn,
        ),
        ("dp", "tensor"),
    )
    return (
        output,
        grad_in,
        grad_w_query,
        small_sums[0],
        grad_w_key,
        grad_w_value,
        small_sums[1],
        grad_w_out,
        small_sums[2],
        small_sums[3],
        small_sums[4],
        grad_w_in,
        small_sums[5],
        grad_w_back,
        small_sums[6],
        small_sums[7],
        small_sums[8],
    )


MESH_ID = pl.DeviceIdType.MESH
F32 = jnp.float32
BF16 = jnp.bfloat16

SLOTS = 4
BLOCK = 128
GROUP = 512
WIDTH = 1024
HEAD_COLS = 256
HIDDEN = 1024
N_SEND = 58
N_GOT = 110
HALF = BLOCK // 2
HALVES = dict(q=(128, 256), k=(128, 256), v=(128, 256), o=(256, 128), i0=(128, 512), i1=(128, 512), b0=(512, 128),
              b1=(512, 128))
VECTORS = dict(bq=1024, bv=1024, bo=1024, ga=1024, sa=1024, bi=4096, bb=1024, gf=1024, sf=1024)


def flip(bit):
    return 1 - bit


def slot_step(t, j):
    return (t % 2 + j % 2) % 2 + 2 * ((t // 2 + j // 2) % 2)


def rows_of(r, count=BLOCK):
    return pl.ds(pl.multiple_of(r * BLOCK, BLOCK), count)


def cols_of(n, count=256):
    return pl.ds(pl.multiple_of(n * count, count), count)


def dot_nn(a, b):
    return jnp.dot(a, b, preferred_element_type=F32)


def dot_nt(a, b):
    return lax.dot_general(a, b, (((1,), (1,)), ((), ())), preferred_element_type=F32)


def dot_tn(a, b):
    return lax.dot_general(a, b, (((0,), (0,)), ((), ())), preferred_element_type=F32)


def scratch_table():
    act = lambda n: pltpu.VMEM((GROUP, n), BF16)
    table = dict(
        w3=pltpu.VMEM((3 * WIDTH, HEAD_COLS), BF16),
        wo=pltpu.VMEM((4, HEAD_COLS, 256), BF16),
        wi=pltpu.VMEM((WIDTH, HIDDEN), BF16),
        wb=pltpu.VMEM((4, HIDDEN, 256), BF16),
        w3t=pltpu.VMEM((3, HEAD_COLS, WIDTH), BF16),
        wot=pltpu.VMEM((WIDTH, HEAD_COLS), BF16),
        wit=pltpu.VMEM((HIDDEN, WIDTH), BF16),
        wbt=pltpu.VMEM((WIDTH, HIDDEN), BF16),
        lens_own=pltpu.VMEM((2, 8, 128), F32),
        lens_got=pltpu.VMEM((2, 8, 128), F32),
        lens_use=pltpu.VMEM((2, 8, 128), F32),
        tk=act(WIDTH),
        tkt=pltpu.VMEM((WIDTH, GROUP), BF16),
        cot_own=pltpu.VMEM((BLOCK, WIDTH), BF16),
        bias=pltpu.VMEM((GROUP, GROUP), F32),
        q=act(HEAD_COLS),
        qt=pltpu.VMEM((HEAD_COLS, GROUP), BF16),
        k=act(HEAD_COLS),
        ks=act(HEAD_COLS),
        v=act(HEAD_COLS),
        ps=pltpu.VMEM((4, GROUP, GROUP), BF16),
        ctx=act(HEAD_COLS),
        ctxt=pltpu.VMEM((HEAD_COLS, GROUP), BF16),
        hid=act(WIDTH),
        hidt=pltpu.VMEM((WIDTH, GROUP), BF16),
        act=act(HIDDEN),
        actt=pltpu.VMEM((HIDDEN, GROUP), BF16),
        slope=pltpu.VMEM((GROUP, HIDDEN), F32),
        g2=act(WIDTH),
        gpre=act(HIDDEN),
        g1=act(WIDTH),
        gctxt=pltpu.VMEM((HEAD_COLS, GROUP), BF16),
        dq=act(HEAD_COLS),
        dkt=pltpu.VMEM((HEAD_COLS, GROUP), F32),
        dvt=pltpu.VMEM((HEAD_COLS, GROUP), F32),
        dk=act(HEAD_COLS),
        dv=act(HEAD_COLS),
        hid1=pltpu.VMEM((BLOCK, WIDTH), F32),
        normed1=pltpu.VMEM((BLOCK, WIDTH), F32),
        inv1=pltpu.VMEM((BLOCK, 128), F32),
        g2f=pltpu.VMEM((BLOCK, WIDTH), F32),
        g1f=pltpu.VMEM((BLOCK, WIDTH), F32),
        out_own=pltpu.VMEM((BLOCK, WIDTH), BF16),
        gtok_own=pltpu.VMEM((BLOCK, WIDTH), BF16),
        rs_own=pltpu.VMEM((4, BLOCK, WIDTH), BF16),
        rs_out=pltpu.VMEM((4, 3, BLOCK, WIDTH), BF16),
        rs_got=pltpu.VMEM((4, 3, BLOCK, WIDTH), BF16),
        sums=pltpu.VMEM((6, 16, WIDTH), F32),
        sums_got=pltpu.VMEM((5, 16, WIDTH), F32),
        gb_in=pltpu.VMEM((1, HIDDEN), F32),
        vectors={name: pltpu.VMEM((1, width), F32) for name, width in VECTORS.items()},
        vsem=pltpu.SemaphoreType.DMA((len(VECTORS),)),
        turn=pltpu.SemaphoreType.REGULAR((5,)),
        g3=pltpu.VMEM((3 * WIDTH, HEAD_COLS), BF16),
        go=pltpu.VMEM((4, HEAD_COLS, 256), BF16),
        gi=pltpu.VMEM((WIDTH, HIDDEN), BF16),
        gb=pltpu.VMEM((4, HIDDEN, 256), BF16),
        stage={},
        ssem=pltpu.SemaphoreType.DMA((N_SEND,)),
        rsem=pltpu.SemaphoreType.DMA((N_GOT,)),
    )
    for name, dims in HALVES.items():
        table["stage"][name] = pltpu.VMEM((10,) + dims, BF16)
    return table


def layer_kernel(tok, lens, wq, bq, wk, wv, bv, wo, bo, ga, sa, wi, bi, wb, bb, gf, sf, cot, out, gtok, sums, zq, zk, zv,
                 zo, zi0, zi1, zb0, zb1, *scratch):
    a = SimpleNamespace(tok=tok, lens=lens, wq=wq, bq=bq, wk=wk, wv=wv, bv=bv, wo=wo, bo=bo, ga=ga, sa=sa, wi=wi, bi=bi,
                        wb=wb, bb=bb, gf=gf, sf=sf, cot=cot)
    o = SimpleNamespace(out=out, gtok=gtok, sums=sums)
    landed = dict(q=zq, k=zk, v=zv, o=zo, i0=zi0, i1=zi1, b0=zb0, b1=zb1)
    s = SimpleNamespace(**jax.tree.unflatten(jax.tree.structure(scratch_table()), scratch))
    ssem, rsem, vsem, vectors = s.ssem, s.rsem, s.vsem, s.vectors

    dp = lax.axis_index("dp")
    z = lax.axis_index("tensor")
    b, c = dp // 2, dp % 2
    zl, zh = z % 2, z // 2
    t = zl * 2 + c
    sl = (z + 2 * c) % 4
    here, away = c == 0, c == 1
    bx = b + 1 - 2 * (b % 2)
    by = (b + 2) % 4
    bd = 3 - b
    t1, t2, t3 = slot_step(t, 1), slot_step(t, 2), slot_step(t, 3)

    def dev(pos, core, zz):
        return (pos * 2 + core, zz)

    partner = dev(b, flip(c), z)
    z_near = z + 1 - 2 * (z % 2)
    z_far = (z + 2) % 4
    pair = dev(b, c, z_near)
    across = dev(b, c, z_far)
    is_inner = jnp.logical_and(z >= 1, z <= 2)
    inner_away = jnp.logical_and(is_inner, away)
    outer_away = jnp.logical_and(jnp.logical_not(is_inner), away)
    x_near = dev(bx, c, z)
    y_near = dev(by, c, z)

    taken = {"s": 0, "r": 0}

    def take(kind, count=1):
        first = taken[kind]
        taken[kind] = first + count
        assert taken[kind] <= (N_SEND if kind == "s" else N_GOT)
        return first

    to_drain = []

    def make_copy(src, dst, device, sk, rk):
        return pltpu.make_async_remote_copy(
            src_ref=src, dst_ref=dst, send_sem=ssem.at[sk], recv_sem=rsem.at[rk], device_id=device,
            device_id_type=MESH_ID)

    def send(src, dst, device, sk, rk):
        make_copy(src, dst, device, sk, rk).start()

    def got(dst, rk):
        pltpu.make_async_copy(dst, dst, rsem.at[rk]).wait()

    def left(size_of, sk):
        pltpu.make_async_copy(size_of, size_of, ssem.at[sk]).wait()

    def at_end(size_of, sk, skipped=None, instead=None):
        to_drain.append((size_of, sk, skipped, instead))

    def send_or_keep(src, dst, device, is_self, sk, rk):
        copy = make_copy(src, dst, device, sk, rk)

        @pl.when(is_self)
        def _():
            pltpu.make_async_copy(src, dst, rsem.at[rk]).start()

        @pl.when(jnp.logical_not(is_self))
        def _():
            copy.start()

    barrier = pltpu.get_barrier_semaphore()
    peers = [x_near, y_near]
    for dz in range(4):
        for dc in range(2):
            if dz or dc:
                peers.append(dev(b, (c + dc) % 2, (z + dz) % 4))
    for peer in peers:
        pl.semaphore_signal(barrier, inc=1, device_id=peer, device_id_type=MESH_ID)
    pl.semaphore_wait(barrier, len(peers))

    def piece_qkv(m, home):
        base = m * WIDTH
        return SimpleNamespace(
            home=home,
            own=lambda bb, cc: s.w3.at[pl.ds(pl.multiple_of(base + bb * 256 + cc * 128, 128), 128), :],
            block=lambda bb: s.w3.at[pl.ds(pl.multiple_of(base + bb * 256, 256), 256), :],
            half=lambda bb, h: s.w3.at[pl.ds(pl.multiple_of(base + bb * 256 + h * 128, 128), 128), :])

    piece_o = SimpleNamespace(
        home=a.wo,
        own=lambda bb, cc: s.wo.at[bb, :, pl.ds(pl.multiple_of(cc * 128, 128), 128)],
        block=lambda bb: s.wo.at[bb],
        half=lambda bb, h: s.wo.at[bb, pl.ds(h * 128, 128), :])

    def piece_in(j):
        cols = pl.ds(j * 512, 512)
        return SimpleNamespace(
            home=a.wi.at[:, cols],
            own=lambda bb, cc: s.wi.at[pl.ds(pl.multiple_of(bb * 256 + cc * 128, 128), 128), cols],
            block=lambda bb: s.wi.at[pl.ds(pl.multiple_of(bb * 256, 256), 256), cols],
            half=lambda bb, h: s.wi.at[pl.ds(pl.multiple_of(bb * 256 + h * 128, 128), 128), cols])

    def piece_back(j):
        part = pl.ds(j * 512, 512)
        return SimpleNamespace(
            home=a.wb.at[part, :],
            own=lambda bb, cc: s.wb.at[bb, part, pl.ds(pl.multiple_of(cc * 128, 128), 128)],
            block=lambda bb: s.wb.at[bb, part, :],
            half=lambda bb, h: s.wb.at[bb, pl.ds(j * 512 + h * 256, 256), :])

    pieces = dict(q=piece_qkv(0, a.wq), k=piece_qkv(1, a.wk), v=piece_qkv(2, a.wv), o=piece_o,
                  i0=piece_in(0), i1=piece_in(1), b0=piece_back(0), b1=piece_back(1))
    first_size = dict(
        q=s.w3.at[0:768, :], k=s.w3.at[0:768, :], v=s.w3.at[0:768, :], o=s.wo.at[0:3], i0=s.wi.at[0:768, 0:512],
        i1=s.wi.at[0:768, 0:512], b0=s.wb.at[0:3, 0:512, :], b1=s.wb.at[0:3, 0:512, :])
    for name, piece in pieces.items():
        piece.s1, piece.r1 = take("s"), take("r")
        piece.s2, piece.r2 = take("s"), take("r", 3)
        at_end(piece.block(b), piece.s1, here, piece.own(b, 0))
        at_end(first_size[name], piece.s2)

    def to_local(name):
        piece = pieces[name]
        send_or_keep(piece.home, piece.own(b, c), dev(b, 0, z), here, piece.s1, piece.r1)

    def to_across(name):
        piece = pieces[name]
        send(piece.home, piece.own(b, c), dev(b, 1, z_far), piece.s1, piece.r1)

    def over_plane(name):
        piece = pieces[name]
        got(piece.block(b), piece.r1)
        send(piece.block(b), piece.block(b), x_near, piece.s2, piece.r2)
        send(piece.block(b), piece.block(b), y_near, piece.s2, piece.r2 + 1)

    def relay(name):
        piece = pieces[name]
        got(piece.block(bx), piece.r2)
        send(piece.half(bx, 0), piece.half(bx, 0), y_near, piece.s2, piece.r2 + 2)
        got(piece.block(by), piece.r2 + 1)
        send(piece.half(by, 1), piece.half(by, 1), x_near, piece.s2, piece.r2 + 2)

    def over_plane_now(names, chosen, relays=()):
        @pl.when(chosen)
        def _():
            for name in relays:
                relay(name)
            for name in names:
                over_plane(name)

    def arrived(name):
        piece = pieces[name]
        got(piece.block(bd), piece.r2 + 2)

    tok_s, tok_r = take("s", 2), take("r", 4)
    fwd_s = take("s", 6)
    lens_s, lens_r = take("s"), take("r")
    cot_s, cot_r = take("s"), take("r")

    def send_lens():
        first = a.lens[0, 0].astype(F32)
        s.lens_own[0] = jnp.full((8, 128), first, F32)
        s.lens_own[1] = jnp.full((8, 128), first + a.lens[0, 1].astype(F32), F32)
        send(s.lens_own, s.lens_got, partner, lens_s, lens_r)
        at_end(s.lens_own, lens_s)

    def take_lens():
        got(s.lens_got, lens_r)

        @pl.when(c == zh)
        def _():
            s.lens_use[...] = s.lens_own[...]

        @pl.when(c != zh)
        def _():
            s.lens_use[...] = s.lens_got[...]

    def tok_block(r):
        return s.tk.at[rows_of(r), :]

    inner, outer = 1 + c, 3 * c
    is_relay = jnp.logical_and(c == zh, z == inner)

    def send_tokens():
        near = z // 2 == c
        first = jnp.where(near, 2 * c, inner)
        send_or_keep(a.tok, tok_block(z), dev(b, c, first), first == z, tok_s, tok_r + z)
        at_end(tok_block(z), tok_s, first == z)
        second = make_copy(a.tok, tok_block(z), dev(b, c, 2 * c + 1), tok_s + 1, tok_r + z)
        keep = jnp.logical_and(near, z == 2 * c + 1)
        go = jnp.logical_and(near, z != 2 * c + 1)

        @pl.when(keep)
        def _():
            pltpu.make_async_copy(a.tok, tok_block(z), rsem.at[tok_r + z]).start()

        @pl.when(go)
        def _():
            second.start()

        at_end(tok_block(z), tok_s + 1, jnp.logical_not(go))

    def pass_on(half, far):
        for k in range(2):
            r = half * 2 + k
            block = tok_block(r)
            got(block, tok_r + r)
            if far:
                on = make_copy(block, block, dev(b, c, outer), fwd_s + k, tok_r + r)

                @pl.when(is_relay)
                def _():
                    on.start()
            copy = make_copy(block, block, partner, fwd_s + 2 + 2 * far + k, tok_r + r)

            @pl.when(c == zh)
            def _():
                copy.start()

    for k in range(6):
        at_end(s.tk.at[0:BLOCK, :], fwd_s + k, jnp.logical_not(is_relay) if k < 2 else c != zh)

    def send_cotangent():
        zt, ct = 2 * c + z // 2, z % 2
        is_self = jnp.logical_and(zt == z, ct == c)
        send_or_keep(a.cot, s.cot_own, dev(b, ct, zt), is_self, cot_s, cot_r)
        at_end(s.cot_own, cot_s, is_self)

    gather_s, gather_r = take("s", 3), take("r", 12)
    scatter_s, scatter_r = take("s", 4), take("r", 20)
    for k in range(3):
        at_end(s.tk.at[0:3 * BLOCK, :], gather_s + k)
    for k in range(4):
        at_end(s.tk.at[0:3 * BLOCK, :], scatter_s + k)

    def block_at(full, r):
        return full.at[rows_of(r), :]

    def half_at(full, r, k):
        return full.at[pl.ds(pl.multiple_of(r * BLOCK + k * HALF, HALF), HALF), :]

    def gather_start(which, full, k):
        mine = half_at(full, t, k)
        send(mine, mine, pair, gather_s + which, gather_r + 4 * which + 1 + k)
        send(mine, mine, partner, gather_s + which, gather_r + 4 * which)

    def gather_step(which, full, j):
        base = gather_r + 4 * which

        @pl.when(j == 1)
        def _():
            got(block_at(full, t1), base)

        @pl.when(j == 2)
        def _():
            for k in range(2):
                near = half_at(full, t2, k)
                got(near, base + 1 + k)
                send(near, near, partner, gather_s + which, base + 3)

        @pl.when(j == 3)
        def _():
            if which == 0:
                over_plane_now((), inner_away, relays=("b0", "b1"))
            got(block_at(full, t3), base + 3)

    halves = [pl.ds(k * HALF, HALF) for k in range(2)]

    def scatter(which, part):
        out, back = s.rs_out, s.rs_got
        ss, rr = scatter_s + which, scatter_r + 5 * which
        part(t3 * BLOCK, BLOCK, out.at[which, 0])
        send(out.at[which, 0], back.at[which, 0], partner, ss, rr)
        part(t2 * BLOCK, BLOCK, out.at[which, 1])
        got(back.at[which, 0], rr)
        for k in range(2):
            rows = halves[k]
            total = out[which, 1, rows, :].astype(F32) + back[which, 0, rows, :].astype(F32)
            out[which, 1, rows, :] = total.astype(BF16)
            send(out.at[which, 1, rows, :], back.at[which, 1, rows, :], pair, ss, rr + 2 + k)
        part(t1 * BLOCK, BLOCK, out.at[which, 2])
        send(out.at[which, 2], back.at[which, 2], partner, ss, rr + 4)
        part(t * BLOCK, BLOCK, s.rs_own.at[which])

    def scatter_wait(which, k):
        rr = scatter_r + 5 * which
        if k == 0:
            got(s.rs_got.at[which, 2], rr + 4)
        got(s.rs_got.at[which, 1, halves[k], :], rr + 2 + k)

    def scatter_rows(which, chunk):
        total = s.rs_own[which, chunk, :].astype(F32) + s.rs_got[which, 2, chunk, :].astype(F32)
        return total + s.rs_got[which, 1, chunk, :].astype(F32)

    def by_halves(which, body, after):
        for k in range(2):
            scatter_wait(which, k)
            loop(2, lambda i: body(2 * k + i))
            after(k)

    def put_part(dst, n, value):
        dst[:, 256 * n:256 * n + 256] = value.astype(BF16)

    def loop(count, body):
        lax.fori_loop(0, count, lambda i, _: (body(i), 0)[1], 0)

    def grad_qkv(m):
        base = m * WIDTH
        return lambda bb, h: s.g3.at[pl.ds(pl.multiple_of(base + bb * 256 + h * 128, 128), 128), :]

    def grad_in_part(k):
        cols = pl.ds(k * 512, 512)
        return lambda bb, h: s.gi.at[pl.ds(pl.multiple_of(bb * 256 + h * 128, 128), 128), cols]

    def grad_back_part(k):
        part = pl.ds(k * 512, 512)
        return lambda bb, h: s.gb.at[bb, part, pl.ds(h * 128, 128)]

    grad_half = dict(
        q=grad_qkv(0), k=grad_qkv(1), v=grad_qkv(2), o=lambda bb, h: s.go.at[bb, :, pl.ds(h * 128, 128)],
        i0=grad_in_part(0), i1=grad_in_part(1), b0=grad_back_part(0), b1=grad_back_part(1))
    grad_s = {name: take("s", 2) for name in grad_half}
    grad_r = {name: take("r", 4) for name in grad_half}
    for name in grad_half:
        at_end(s.stage[name].at[0:6], grad_s[name])
        at_end(s.stage[name].at[0:2], grad_s[name] + 1, here, s.stage[name].at[0])

    def chunks(name, body):
        size = 64 if name in ("i0", "i1") else 128
        count = HALVES[name][0] // size
        loop(count, lambda i: body(pl.ds(pl.multiple_of(i * size, size), size)))

    def grad_first(name, part=2):
        half, ss, rr, st = grad_half[name], grad_s[name], grad_r[name], s.stage[name]
        if part in (0, 2):
            send(half(bd, 0), st.at[1], x_near, ss, rr)
            send(half(bd, 1), st.at[3], y_near, ss, rr + 1)
        if part == 0:
            return
        send(half(bx, 0), st.at[0], x_near, ss, rr + 2)
        send(half(by, 1), st.at[2], y_near, ss, rr + 2)

    def grad_second(name):
        half, ss, rr, st = grad_half[name], grad_s[name], grad_r[name], s.stage[name]
        for h, block, to in ((0, by, y_near), (1, bx, x_near)):
            got(st.at[1 + 2 * h], rr + h)
            mine = half(block, h)

            def add(ch):
                st[4 + h, ch, :] = (mine[ch, :].astype(F32) + st[1 + 2 * h, ch, :].astype(F32)).astype(BF16)
            chunks(name, add)
            send(st.at[4 + h], st.at[6 + h], to, ss, rr + 2)

    def grad_third(name):
        half, ss, rr, st = grad_half[name], grad_s[name], grad_r[name], s.stage[name]
        zr = landed[name]
        got(st.at[0:4], rr + 2)
        for h in range(2):
            mine = half(b, h)

            def add_all(ch):
                total = mine[ch, :].astype(F32) + st[2 * h, ch, :].astype(F32) + st[6 + h, ch, :].astype(F32)
                st[8 + h, ch, :] = total.astype(BF16)
            chunks(name, add_all)
            is_self = here if h == 0 else c < 0
            send_or_keep(st.at[8 + h], zr.at[zh], dev(b, h, sl), is_self, ss + 1, rr + 3)

    def grad_final(name):
        got(landed[name], grad_r[name] + 3)

    to_across("q")
    to_across("k")
    send_tokens()
    to_across("v")
    for name in pieces:
        to_local(name)
    send_lens()
    for name, ref in vectors.items():
        pltpu.make_async_copy(getattr(a, name), ref, vsem.at[list(vectors).index(name)]).start()
    s.sums[0] = jnp.zeros((16, WIDTH), F32)
    s.gb_in[...] = jnp.zeros((1, HIDDEN), F32)
    leads = jnp.logical_and(is_inner, away)

    def in_turn(k, inner_next, outer_next):
        @pl.when(leads)
        def _():
            for device in (partner, pair, dev(b, 0, z_near)):
                pl.semaphore_signal(s.turn.at[k], inc=1, device_id=device, device_id_type=MESH_ID)

        @pl.when(jnp.logical_not(leads))
        def _():
            pl.semaphore_wait(s.turn.at[k], 1)

        for chosen, names in ((is_inner, inner_next), (jnp.logical_not(is_inner), outer_next)):
            if names:
                @pl.when(chosen)
                def _():
                    for name in names:
                        to_across(name)

    over_plane_now(("q", "k", "v", "o"), here)
    over_plane_now(("q", "k"), away)
    relay("q")
    over_plane_now(("i0",), here, relays=("k", "v"))
    pass_on(zh, 0)
    to_across("o")

    @pl.when(is_inner)
    def _():
        pass_on(flip(zh), 1)

    in_turn(0, (), ("i0",))
    take_lens()

    def make_bias(r):
        first, end = s.lens_use[0][0:1, 0:1], s.lens_use[1][0:1, 0:1]
        row = (lax.broadcasted_iota(jnp.int32, (BLOCK, GROUP), 0) + r * BLOCK).astype(F32)
        col = lax.broadcasted_iota(jnp.int32, (BLOCK, GROUP), 1).astype(F32)
        seg = lambda p: jnp.where(p >= end, 2.0, jnp.where(p >= first, 1.0, 0.0))
        s.bias[rows_of(r), :] = jnp.where(seg(row) == seg(col), 0.0, masked_value)
    loop(SLOTS, make_bias)
    for name, ref in vectors.items():
        pltpu.make_async_copy(getattr(a, name), ref, vsem.at[list(vectors).index(name)]).wait()
        setattr(a, name, ref)
    over_plane_now(("v", "o"), away, relays=("k",))
    over_plane_now(("i1",), here, relays=("o",))
    over_plane_now((), away, relays=("v",))
    over_plane_now(("b0",), here, relays=("i0",))
    in_turn(1, ("i0", "i1"), ("i1",))

    @pl.when(jnp.logical_not(is_inner))
    def _():
        pass_on(flip(zh), 1)


    def turn_tokens(r):
        s.tkt[:, rows_of(r)] = s.tk[rows_of(r), :].T
    loop(SLOTS, turn_tokens)

    head_cols = pl.ds(pl.multiple_of(sl * HEAD_COLS, HEAD_COLS), HEAD_COLS)

    def project(m):
        acc = dot_nn(s.tk[...], s.w3[m * WIDTH:(m + 1) * WIDTH, :])
        if m == 0:
            value = (acc + a.bq[:, head_cols]).astype(BF16)
            scaled = (value.astype(F32) * 0.125).astype(BF16)
            s.q[...] = scaled
            s.qt[...] = scaled.T
        elif m == 1:
            value = acc.astype(BF16)
            s.k[...] = value
            s.ks[...] = (value.astype(F32) * 0.125).astype(BF16)
        else:
            s.v[...] = (acc + a.bv[:, head_cols]).astype(BF16)

    arrived("q")
    project(0)
    arrived("k")
    project(1)
    in_turn(2, ("b0", "b1"), ())
    arrived("v")
    project(2)

    def attend():
        parts = []
        for h in range(4):
            cols = slice(64 * h, 64 * h + 64)
            scores = dot_nt(s.q[:, cols], s.k[:, cols]) + s.bias[...]
            top = jnp.max(scores, axis=-1, keepdims=True)
            weight = jnp.exp(scores - top)
            total = jnp.sum(weight, axis=-1, keepdims=True)
            prob = (weight * (1.0 / total)).astype(BF16)
            s.ps[h] = prob
            parts.append(dot_nn(prob, s.v[:, cols]))
        context = jnp.concatenate(parts, axis=1).astype(BF16)
        s.ctx[...] = context
        s.ctxt[...] = context.T
    over_plane_now((), away, relays=("o",))
    over_plane_now(("i0", "i1"), inner_away)
    over_plane_now(("b1",), here, relays=("i1",))
    attend()
    over_plane_now(("i0", "i1"), outer_away)
    arrived("o")

    def attn_part(first, count, dst):
        rows = s.ctx[pl.ds(pl.multiple_of(first, HALF), count), :]
        for n in range(4):
            put_part(dst, n, dot_nn(rows, s.wo[n]))
    scatter(0, attn_part)
    @pl.when(jnp.logical_not(is_inner))
    def _():
        to_across("b0")
        to_across("b1")

    for m in range(3):
        for n in range(4):
            s.w3t[m, :, 256 * n:256 * n + 256] = s.w3[m * WIDTH + 256 * n:m * WIDTH + 256 * n + 256, :].T
    for n in range(4):
        s.wot[256 * n:256 * n + 256, :] = s.wo[n].T

    CH = 32

    def own_chunk(i):
        return pl.ds(pl.multiple_of(i * CH, CH), CH)

    def group_chunk(i):
        return pl.ds(pl.multiple_of(t * BLOCK + i * CH, CH), CH)

    def norm_one(i):
        ch = own_chunk(i)
        resid = s.tk[group_chunk(i), :].astype(F32) + scatter_rows(0, ch) + a.bo[...]
        centered = resid - jnp.mean(resid, axis=-1, keepdims=True)
        inv = lax.rsqrt(jnp.mean(centered * centered, axis=-1, keepdims=True) + epsilon)
        normed = centered * inv
        hidden = normed * a.ga[...] + a.sa[...]
        s.normed1[ch, :] = normed
        s.inv1[ch, :] = jnp.broadcast_to(inv, (CH, 128))
        s.hid1[ch, :] = hidden
        s.hid[group_chunk(i), :] = hidden.astype(BF16)
    over_plane_now((), here, relays=("b0",))
    over_plane_now((), inner_away, relays=("i0", "i1"))
    over_plane_now(("b0", "b1"), outer_away, relays=("i0",))
    over_plane_now((), outer_away, relays=("i1",))
    by_halves(0, norm_one, lambda k: gather_start(0, s.hid, k))
    over_plane_now((), here, relays=("b1",))
    over_plane_now((), outer_away, relays=("b0", "b1"))
    arrived("i0")
    arrived("i1")

    over_plane_now(("b0", "b1"), inner_away)

    def ffn_in(j):
        gather_step(0, s.hid, j)
        r = slot_step(t, j)
        rows = rows_of(r)
        for n in range(4):
            cols = slice(256 * n, 256 * n + 256)
            bias = a.bi[:, pl.ds(pl.multiple_of(sl * HIDDEN + n * 256, 256), 256)]
            pre = dot_nn(s.hid[rows, :], s.wi[:, cols]) + bias
            cdf = 0.5 * (1.0 + lax.erf(pre * 0.7071067811865476))
            pdf = jnp.exp(-0.5 * pre * pre) * 0.3989422804014327
            s.act[rows, cols] = (pre * cdf).astype(BF16)
            s.slope[rows, cols] = cdf + pre * pdf
    loop(SLOTS, ffn_in)
    send_cotangent()

    def turn_ffn(r):
        rows = rows_of(r)
        s.actt[:, rows] = s.act[rows, :].T
        s.hidt[:, rows] = s.hid[rows, :].T
    arrived("b0")
    arrived("b1")

    def ffn_part(first, count, dst):
        rows = pl.ds(pl.multiple_of(first, HALF), count)
        for n in range(4):
            put_part(dst, n, dot_nn(s.act[rows, :], s.wb[n]))
    scatter(1, ffn_part)
    loop(SLOTS, turn_ffn)

    def turn_wi(r):
        rows = rows_of(r)
        s.wit[:, rows] = s.wi[rows, :].T
    loop(8, turn_wi)

    def turn_wb(r):
        rows = rows_of(r)
        for n in range(4):
            s.wbt[256 * n:256 * n + 256, rows] = s.wb[n, rows, :].T
    loop(8, turn_wb)
    got(s.cot_own, cot_r)

    def add_rows(row, value):
        s.sums[0, row:row + 1, :] += jnp.sum(value, axis=0, keepdims=True)

    def norm_two(i):
        ch = own_chunk(i)
        resid = s.hid1[ch, :] + scatter_rows(1, ch) + a.bb[...]
        centered = resid - jnp.mean(resid, axis=-1, keepdims=True)
        inv = lax.rsqrt(jnp.mean(centered * centered, axis=-1, keepdims=True) + epsilon)
        normed = centered * inv
        position = lax.broadcasted_iota(jnp.int32, (CH, 128), 0) + (t * BLOCK + i * CH)
        live = jnp.where(position.astype(F32) < s.lens_use[1][0:1, :], 1.0, 0.0)[:, 0:1]
        s.out_own[ch, :] = ((normed * a.gf[...] + a.sf[...]) * live).astype(BF16)
        grad = s.cot_own[ch, :].astype(F32) * live
        add_rows(4, grad * normed)
        add_rows(5, grad)
        u = grad * a.gf[...]
        first = jnp.mean(u, axis=-1, keepdims=True)
        second = jnp.mean(u * normed, axis=-1, keepdims=True)
        grad_two = inv * (u - first - normed * second)
        add_rows(3, grad_two)
        s.g2f[ch, :] = grad_two
        s.g2[group_chunk(i), :] = grad_two.astype(BF16)
    by_halves(1, norm_two, lambda k: gather_start(1, s.g2, k))
    out_s, out_r = take("s"), take("r")
    home_self = jnp.logical_and(zh == c, t == z)

    def ffn_back(j):
        @pl.when(j < 3)
        def _():
            gather_step(1, s.g2, j)
        r = slot_step(t, j)
        rows = rows_of(r)
        for n in range(4):
            cols = slice(256 * n, 256 * n + 256)
            grad = dot_nn(s.g2[rows, :], s.wbt[:, cols]) * s.slope[rows, cols]
            s.gb_in[:, cols] += jnp.sum(grad, axis=0, keepdims=True)
            s.gpre[rows, cols] = grad.astype(BF16)
    loop(SLOTS - 1, ffn_back)

    def grad_back(k):
        part = slice(512 * k, 512 * k + 512)

        def body(n):
            for e in range(2):
                block = n * 2 + e
                s.gb[block, part, :] = dot_nn(s.actt[part, :], s.g2[:, cols_of(block)]).astype(BF16)
        loop(2, body)

    def grad_in(k):
        cols = slice(512 * k, 512 * k + 512)

        def body(m):
            part = rows_of(m * 4, 512)
            s.gi[part, cols] = dot_nn(s.hidt[part, :], s.gpre[:, cols]).astype(BF16)
        loop(2, body)

    gather_step(1, s.g2, 3)
    grad_back(0)
    grad_first("b0")
    ffn_back(3)
    grad_back(1)
    grad_first("b1", 0)
    send_or_keep(s.out_own, o.out, dev(b, zh, t), home_self, out_s, out_r)
    at_end(s.out_own, out_s, home_self)

    def in_part(first, count, dst):
        rows = pl.ds(pl.multiple_of(first, HALF), count)
        for n in range(4):
            put_part(dst, n, dot_nn(s.gpre[rows, :], s.wit[:, 256 * n:256 * n + 256]))
    scatter(2, in_part)
    grad_in(0)
    grad_in(1)
    grad_second("b0")
    grad_first("b1", 1)
    grad_second("b1")
    grad_first("i0", 0)

    def norm_one_back(i):
        ch = own_chunk(i)
        grad = s.g2f[ch, :] + scatter_rows(2, ch)
        normed = s.normed1[ch, :]
        add_rows(1, grad * normed)
        add_rows(2, grad)
        u = grad * a.ga[...]
        first = jnp.mean(u, axis=-1, keepdims=True)
        second = jnp.mean(u * normed, axis=-1, keepdims=True)
        grad_one = s.inv1[ch, 0:1] * (u - first - normed * second)
        add_rows(0, grad_one)
        s.g1f[ch, :] = grad_one
        s.g1[group_chunk(i), :] = grad_one.astype(BF16)
    by_halves(2, norm_one_back, lambda k: gather_start(2, s.g1, k))
    grad_first("i0", 1)
    grad_third("b0")

    def attend_back(chip, add):
        rows = pl.ds(pl.multiple_of(chip * 2 * BLOCK, 2 * BLOCK), 2 * BLOCK)
        grad_ctx = dot_nn(s.g1[rows, :], s.wot[...]).astype(BF16)
        s.gctxt[:, rows] = grad_ctx.T
        product = grad_ctx.astype(F32) * s.ctx[rows, :].astype(F32)
        parts = []
        for h in range(4):
            cols = slice(64 * h, 64 * h + 64)
            prob = s.ps[h, rows, :]
            delta = jnp.sum(product[:, cols], axis=-1, keepdims=True)
            grad_prob = dot_nt(grad_ctx[:, cols], s.v[:, cols])
            grad_score = (prob.astype(F32) * (grad_prob - delta)).astype(BF16)
            parts.append(dot_nn(grad_score, s.ks[:, cols]))
            grad_key = dot_nn(s.qt[cols, rows], grad_score)
            grad_value = dot_nn(s.gctxt[cols, rows], prob)
            if add:
                grad_key, grad_value = s.dkt[cols, :] + grad_key, s.dvt[cols, :] + grad_value
            s.dkt[cols, :] = grad_key
            s.dvt[cols, :] = grad_value
        grad_query = jnp.concatenate(parts, axis=1)
        for k in range(4):
            @pl.when(sl == k)
            def _():
                s.sums[0, 6:7, 256 * k:256 * k + 256] += jnp.sum(grad_query, axis=0, keepdims=True)
        s.dq[rows, :] = grad_query.astype(BF16)
    gather_step(2, s.g1, 1)
    attend_back(zl, False)
    grad_third("b1")
    gather_step(2, s.g1, 2)
    gather_step(2, s.g1, 3)
    attend_back(flip(zl), True)
    grad_second("i0")
    grad_first("i1")
    s.dk[...] = s.dkt[...].T.astype(BF16)
    grad_value = s.dvt[...].T
    for k in range(4):
        @pl.when(sl == k)
        def _():
            s.sums[0, 7:8, 256 * k:256 * k + 256] += jnp.sum(grad_value, axis=0, keepdims=True)
    s.dv[...] = grad_value.astype(BF16)
    for k in range(4):
        @pl.when(sl == k)
        def _():
            s.sums[0, 8 + k:9 + k, :] = s.gb_in[...]

    sums_s, sums_r = take("s", 5), take("r", 5)
    sums_to = [partner, across, pair, x_near, y_near]

    def sums_start(k):
        send(s.sums.at[k], s.sums_got.at[k], sums_to[k], sums_s + k, sums_r + k)
        at_end(s.sums.at[k], sums_s + k)

    def sums_finish(k):
        got(s.sums_got.at[k], sums_r + k)
        total = s.sums[k] + s.sums_got[k]
        s.sums[k + 1] = total
        if k == 4:
            pltpu.make_async_copy(s.sums.at[5], o.sums, vsem.at[0]).start()

    sums_start(0)

    def tok_part(first, count, dst):
        rows = pl.ds(pl.multiple_of(first, HALF), count)
        for n in range(4):
            cols = slice(256 * n, 256 * n + 256)
            acc = dot_nn(s.dq[rows, :], s.w3t[0, :, cols])
            acc = acc + dot_nn(s.dk[rows, :], s.w3t[1, :, cols])
            acc = acc + dot_nn(s.dv[rows, :], s.w3t[2, :, cols])
            put_part(dst, n, acc)
    scatter(3, tok_part)
    sums_finish(0)
    sums_start(1)

    def grad_head(m, src):
        s.g3[m * WIDTH:(m + 1) * WIDTH, :] = dot_nn(s.tkt[...], src[...]).astype(BF16)

    grad_third("i0")
    for n in range(4):
        s.go[n] = dot_nn(s.ctxt[...], s.g1[:, 256 * n:256 * n + 256]).astype(BF16)
    grad_head(0, s.dq)
    grad_head(1, s.dk)
    grad_head(2, s.dv)
    grad_second("i1")
    grad_first("o")
    grad_first("q")
    gtok_s, gtok_r = take("s"), take("r")
    at_end(s.gtok_own, gtok_s, home_self)

    def last_rows(i):
        ch = own_chunk(i)
        s.gtok_own[ch, :] = (s.g1f[ch, :] + scatter_rows(3, ch)).astype(BF16)

    def rows_home(chosen):
        @pl.when(chosen)
        def _():
            by_halves(3, last_rows, lambda k: None)
            send_or_keep(s.gtok_own, o.gtok, dev(b, zh, t), home_self, gtok_s, gtok_r)

    rows_home(is_inner)
    grad_third("i1")
    grad_second("o")
    grad_first("k")
    grad_second("q")
    grad_first("v")
    rows_home(jnp.logical_not(is_inner))
    sums_finish(1)
    sums_start(2)
    grad_third("o")
    grad_second("k")
    grad_third("q")
    sums_finish(2)
    grad_second("v")
    sums_start(3)
    grad_third("k")
    grad_third("v")
    sums_finish(3)
    sums_start(4)
    grad_final("b0")
    grad_final("b1")
    grad_final("i0")
    grad_final("i1")
    got(o.gtok, gtok_r)
    got(o.out, out_r)
    grad_final("o")
    grad_final("q")
    sums_finish(4)
    grad_final("k")
    grad_final("v")

    pltpu.make_async_copy(s.sums.at[5], o.sums, vsem.at[0]).wait()
    for size_of, sk, skipped, instead in to_drain:
        if skipped is None:
            left(size_of, sk)
        else:
            @pl.when(jnp.logical_not(skipped))
            def _():
                left(size_of, sk)
            if instead is not None:
                @pl.when(skipped)
                def _():
                    left(instead, sk)


def result_kernel(out, gtok, sums, zq, zk, zv, zo, zi0, zi1, zb0, zb1, o_out, o_gtok, o_gq, o_gbq, o_gk, o_gv, o_gbv, o_go,
                  o_gbo, o_gga, o_gsa, o_gi, o_gbi, o_gb, o_gbb, o_ggf, o_gsf):
    both = lambda ref: ref[0].astype(F32) + ref[1].astype(F32)
    o_out[...] = out[...]
    o_gtok[...] = gtok[...].astype(F32)
    o_gq[...], o_gk[...], o_gv[...], o_go[...] = both(zq), both(zk), both(zv), both(zo)
    o_gi[:, :512], o_gi[:, 512:] = both(zi0), both(zi1)
    o_gb[:512, :], o_gb[512:, :] = both(zb0), both(zb1)
    for row, ref in ((6, o_gbq), (7, o_gbv), (0, o_gbo), (1, o_gga), (2, o_gsa), (3, o_gbb), (4, o_ggf), (5, o_gsf)):
        ref[...] = sums[row:row + 1, :]
    for k in range(4):
        o_gbi[:, WIDTH * k:WIDTH * k + WIDTH] = sums[8 + k:9 + k, :]


def on_device_fused(tokens, lengths, w_query, b_query, w_key, w_value, b_value, w_out, b_out, gain_attn, shift_attn,
                    w_in, b_in, w_back, b_back, gain_ffn, shift_ffn, cotangent):
    row = lambda vec: vec.reshape(1, -1)
    operands = (tokens, lengths, w_query, row(b_query), w_key, w_value, row(b_value), w_out, row(b_out),
                row(gain_attn), row(shift_attn), w_in, row(b_in), w_back, row(b_back), row(gain_ffn),
                row(shift_ffn), cotangent)
    vmem = pl.BlockSpec(memory_space=pltpu.VMEM)
    stay = pl.BlockSpec(memory_space=pl.ANY)
    in_specs = [stay] * len(operands)
    in_specs[1] = pl.BlockSpec(memory_space=pltpu.SMEM)
    shape = lambda dims, dtype: jax.ShapeDtypeStruct(dims, dtype)
    between = [shape(tokens.shape, BF16), shape(tokens.shape, BF16), shape((16, WIDTH), F32)]
    between += [shape((2,) + HALVES[name], BF16) for name in ("q", "k", "v", "o", "i0", "i1", "b0", "b1")]
    parts = pl.pallas_call(
        layer_kernel,
        out_shape=between,
        in_specs=in_specs,
        out_specs=[stay] * len(between),
        scratch_shapes=jax.tree.leaves(scratch_table()),
        compiler_params=pltpu.CompilerParams(collective_id=0, has_side_effects=True, vmem_limit_bytes=64 * 1024 * 1000),
        name="layer",
    )(*operands)
    line = shape((1, WIDTH), F32)
    results = (
        shape(tokens.shape, BF16), shape(tokens.shape, F32), shape(w_query.shape, F32), line, shape(w_key.shape, F32),
        shape(w_value.shape, F32), line, shape(w_out.shape, F32), line, line, line, shape(w_in.shape, F32),
        shape((1, b_in.shape[0]), F32), shape(w_back.shape, F32), line, line, line)
    outs = pl.pallas_call(
        result_kernel,
        out_shape=results,
        in_specs=[vmem] * len(between),
        out_specs=[vmem] * len(results),
        name="results",
    )(*parts)
    return tuple(v.reshape(-1) if v.shape[0] == 1 else v for v in outs)


def fits_fused(mesh):
    return dict(mesh.shape) == {"dp": 8, "tensor": 4}


def solution(mesh):
    placed = (
        P(("dp", "tensor"), None),
        P("dp", None),
        P("dp", "tensor"),
        P(),
        P("dp", "tensor"),
        P("dp", "tensor"),
        P(),
        P("tensor", "dp"),
        P(),
        P(),
        P(),
        P("dp", "tensor"),
        P(),
        P("tensor", "dp"),
        P(),
        P(),
        P(),
        P(("dp", "tensor"), None),
    )
    on_device = on_device_fused if fits_fused(mesh) else on_device_plain
    return jax.shard_map(
        on_device,
        mesh=mesh,
        in_specs=placed,
        out_specs=(
            P(("dp", "tensor"), None),
            P(("dp", "tensor"), None),
            P("dp", "tensor"),
            P(),
            P("dp", "tensor"),
            P("dp", "tensor"),
            P(),
            P("tensor", "dp"),
            P(),
            P(),
            P(),
            P("dp", "tensor"),
            P(),
            P("tensor", "dp"),
            P(),
            P(),
            P(),
        ),
        check_vma=False,
    )
```

```python
from types import SimpleNamespace

import jax
import jax.numpy as jnp
from jax import lax
from jax.experimental import pallas as pl
from jax.experimental.pallas import tpu as pltpu
from jax.sharding import PartitionSpec as P

HD = 64


epsilon = 1e-06
masked_value = -1e30


def matmul_plain(left_side, right_side):
    return jnp.dot(left_side, right_side, preferred_element_type=jnp.float32)


def matmul_over_rows(left_side, right_side):
    return lax.dot_general(
        left_side, right_side, (((0,), (0,)), ((), ())), preferred_element_type=jnp.float32
    )


def matmul_over_cols(left_side, right_side):
    return lax.dot_general(
        left_side, right_side, (((1,), (1,)), ((), ())), preferred_element_type=jnp.float32
    )


def layer_norm(residual, gain_vec, shift_vec):
    mean_val = jnp.mean(residual, axis=-1, keepdims=True)
    centered = residual - mean_val
    inv_std = lax.rsqrt(jnp.mean(centered * centered, axis=-1, keepdims=True) + epsilon)
    normed = centered * inv_std
    return (normed * gain_vec + shift_vec, normed, inv_std)


def norm_back(grad_out, normed, inv_std, gain_vec):
    grad_norm = grad_out * gain_vec
    first_mean = jnp.mean(grad_norm, axis=-1, keepdims=True)
    second_mean = jnp.mean(grad_norm * normed, axis=-1, keepdims=True)
    return inv_std * (grad_norm - first_mean - normed * second_mean)


def gelu_parts(preact):
    cdf_val = 0.5 * (1.0 + lax.erf(preact * 0.7071067811865476))
    pdf_val = jnp.exp(-0.5 * preact * preact) * 0.3989422804014327
    return (preact * cdf_val, cdf_val + preact * pdf_val)


def attend_forward(query_rows, key_rows, value_rows, seg_ids, head_dim, block_rows):
    group_rows, head_cols = query_rows.shape
    pair_width = 2 * head_dim
    block_count = group_rows // block_rows
    pair_count = head_cols // pair_width
    score_scale = head_dim ** (-0.5)

    def attend_step(step_index, loop_carry):
        context, log_total = loop_carry
        pair_index = step_index // block_count
        row_start = step_index % block_count * block_rows
        first_col = pair_index * pair_width
        query_block = lax.dynamic_slice(
            query_rows, (row_start, first_col), (block_rows, pair_width)
        ).reshape(block_rows, 2, head_dim)
        key_pair = lax.dynamic_slice(key_rows, (0, first_col), (group_rows, pair_width)).reshape(
            group_rows, 2, head_dim
        )
        value_pair = lax.dynamic_slice(
            value_rows, (0, first_col), (group_rows, pair_width)
        ).reshape(group_rows, 2, head_dim)
        same_seg = seg_ids[:, None] == seg_ids[None, :]
        scores = (
            jnp.einsum("qhd,khd->hqk", query_block, key_pair, preferred_element_type=jnp.float32)
            * score_scale
        )
        scores = jnp.where(same_seg[None], scores, masked_value)
        row_max = jnp.max(scores, axis=-1, keepdims=True)
        block_total = row_max + jnp.log(jnp.sum(jnp.exp(scores - row_max), axis=-1, keepdims=True))
        prob_bf = jnp.exp(scores - block_total).astype(jnp.bfloat16)
        context_block = jnp.einsum(
            "hqk,khd->qhd", prob_bf, value_pair, preferred_element_type=jnp.float32
        ).astype(jnp.bfloat16)
        context = lax.dynamic_update_slice(
            context, context_block.reshape(block_rows, pair_width), (row_start, first_col)
        )
        log_total = lax.dynamic_update_slice(
            log_total, block_total[:, :, 0], (2 * pair_index, row_start)
        )
        return (context, log_total)

    start_carry = (
        jnp.zeros((group_rows, head_cols), jnp.bfloat16),
        jnp.zeros((head_cols // head_dim, group_rows), jnp.float32),
    )
    return lax.fori_loop(0, pair_count * block_count, attend_step, start_carry)


def attend_backward(
    query_rows,
    key_rows,
    value_rows,
    context,
    grad_context,
    log_total,
    seg_ids,
    head_dim,
    block_rows,
):
    group_rows, head_cols = query_rows.shape
    pair_width = 2 * head_dim
    block_count = group_rows // block_rows
    pair_count = head_cols // pair_width
    score_scale = head_dim ** (-0.5)

    def back_step(step_index, loop_carry):
        grad_query, grad_keys, grad_values = loop_carry
        pair_index = step_index // block_count
        row_start = step_index % block_count * block_rows
        first_col = pair_index * pair_width
        query_block = lax.dynamic_slice(
            query_rows, (row_start, first_col), (block_rows, pair_width)
        ).reshape(block_rows, 2, head_dim)
        key_pair = lax.dynamic_slice(key_rows, (0, first_col), (group_rows, pair_width)).reshape(
            group_rows, 2, head_dim
        )
        value_pair = lax.dynamic_slice(
            value_rows, (0, first_col), (group_rows, pair_width)
        ).reshape(group_rows, 2, head_dim)
        context_block = lax.dynamic_slice(
            context, (row_start, first_col), (block_rows, pair_width)
        ).reshape(block_rows, 2, head_dim)
        gctx_block = lax.dynamic_slice(
            grad_context, (row_start, first_col), (block_rows, pair_width)
        ).reshape(block_rows, 2, head_dim)
        total_block = lax.dynamic_slice(log_total, (2 * pair_index, row_start), (2, block_rows))
        same_seg = seg_ids[:, None] == seg_ids[None, :]
        scores = (
            jnp.einsum("qhd,khd->hqk", query_block, key_pair, preferred_element_type=jnp.float32)
            * score_scale
        )
        scores = jnp.where(same_seg[None], scores, masked_value)
        probs = jnp.exp(scores - total_block[:, :, None])
        prob_bf = probs.astype(jnp.bfloat16)
        grad_probs = jnp.einsum(
            "qhd,khd->hqk", gctx_block, value_pair, preferred_element_type=jnp.float32
        )
        delta_rows = jnp.sum(
            gctx_block.astype(jnp.float32) * context_block.astype(jnp.float32), axis=-1
        ).T[:, :, None]
        grad_scores = (probs * (grad_probs - delta_rows) * score_scale).astype(jnp.bfloat16)
        grad_q_block = jnp.einsum(
            "hqk,khd->qhd", grad_scores, key_pair, preferred_element_type=jnp.float32
        ).reshape(block_rows, pair_width)
        grad_k_pair = jnp.einsum(
            "hqk,qhd->khd", grad_scores, query_block, preferred_element_type=jnp.float32
        ).reshape(group_rows, pair_width)
        grad_v_pair = jnp.einsum(
            "hqk,qhd->khd", prob_bf, gctx_block, preferred_element_type=jnp.float32
        ).reshape(group_rows, pair_width)
        grad_query = lax.dynamic_update_slice(grad_query, grad_q_block, (row_start, first_col))
        old_keys = lax.dynamic_slice(grad_keys, (0, first_col), (group_rows, pair_width))
        grad_keys = lax.dynamic_update_slice(grad_keys, old_keys + grad_k_pair, (0, first_col))
        old_values = lax.dynamic_slice(grad_values, (0, first_col), (group_rows, pair_width))
        grad_values = lax.dynamic_update_slice(
            grad_values, old_values + grad_v_pair, (0, first_col)
        )
        return (grad_query, grad_keys, grad_values)

    zero_grad = jnp.zeros((group_rows, head_cols), jnp.float32)
    return lax.fori_loop(0, pair_count * block_count, back_step, (zero_grad, zero_grad, zero_grad))


def on_device_plain(
    tokens,
    lengths,
    w_query,
    b_query,
    w_key,
    w_value,
    b_value,
    w_out,
    b_out,
    gain_attn,
    shift_attn,
    w_in,
    b_in,
    w_back,
    b_back,
    gain_ffn,
    shift_ffn,
    cotangent,
):
    tensor_size = lax.axis_size("tensor")
    tensor_index = lax.axis_index("tensor")
    local_rows = tokens.shape[0]
    group_rows = local_rows * tensor_size
    head_cols = w_query.shape[1]
    hidden_cols = w_in.shape[1]
    block_rows = min(512, group_rows)
    seq_lens = lengths[0]
    live_end = seq_lens[0] + seq_lens[1]
    positions = jnp.arange(group_rows, dtype=jnp.int32)
    seg_ids = (positions >= seq_lens[0]).astype(jnp.int32) + (positions >= live_end).astype(
        jnp.int32
    )
    local_pos = tensor_index * local_rows + jnp.arange(local_rows, dtype=jnp.int32)
    live_rows = (local_pos < live_end).astype(jnp.float32)[:, None]
    rows_full = lax.all_gather(tokens, "tensor", axis=0, tiled=True)
    attn_mats = (
        lax.all_gather(w_query, "dp", axis=0, tiled=True),
        lax.all_gather(w_key, "dp", axis=0, tiled=True),
        lax.all_gather(w_value, "dp", axis=0, tiled=True),
        lax.all_gather(w_out, "dp", axis=1, tiled=True),
    )
    mat_query, mat_key, mat_value, mat_out = attn_mats
    bias_query = lax.dynamic_slice_in_dim(b_query, tensor_index * head_cols, head_cols)
    bias_value = lax.dynamic_slice_in_dim(b_value, tensor_index * head_cols, head_cols)
    bias_in = lax.dynamic_slice_in_dim(b_in, tensor_index * hidden_cols, hidden_cols)
    query_rows = (matmul_plain(rows_full, mat_query) + bias_query).astype(jnp.bfloat16)
    key_rows = matmul_plain(rows_full, mat_key).astype(jnp.bfloat16)
    value_rows = (matmul_plain(rows_full, mat_value) + bias_value).astype(jnp.bfloat16)
    context, log_total = attend_forward(query_rows, key_rows, value_rows, seg_ids, HD, block_rows)
    attn_sum = lax.psum_scatter(
        matmul_plain(context, mat_out).astype(jnp.bfloat16),
        "tensor",
        scatter_dimension=0,
        tiled=True,
    ).astype(jnp.float32)
    resid_one = tokens.astype(jnp.float32) + attn_sum + b_out
    hidden_one, normed_one, inv_one = layer_norm(resid_one, gain_attn, shift_attn)
    hidden_bf = hidden_one.astype(jnp.bfloat16)
    hidden_full = lax.all_gather(hidden_bf, "tensor", axis=0, tiled=True)
    ffn_mats = (
        lax.all_gather(w_in, "dp", axis=0, tiled=True),
        lax.all_gather(w_back, "dp", axis=1, tiled=True),
    )
    mat_in, mat_back = ffn_mats
    preact = matmul_plain(hidden_full, mat_in) + bias_in
    activ_val, gelu_slope = gelu_parts(preact)
    activation = activ_val.astype(jnp.bfloat16)
    ffn_sum = lax.psum_scatter(
        matmul_plain(activation, mat_back).astype(jnp.bfloat16),
        "tensor",
        scatter_dimension=0,
        tiled=True,
    ).astype(jnp.float32)
    resid_two = hidden_one + ffn_sum + b_back
    normed_out, normed_two, inv_two = layer_norm(resid_two, gain_ffn, shift_ffn)
    output = (normed_out * live_rows).astype(jnp.bfloat16)
    grad_final = cotangent.astype(jnp.float32) * live_rows
    grad_gain_ffn = jnp.sum(grad_final * normed_two, axis=0)
    grad_shift_ffn = jnp.sum(grad_final, axis=0)
    grad_two = norm_back(grad_final, normed_two, inv_two, gain_ffn)
    grad_b_back = jnp.sum(grad_two, axis=0)
    mat_query, mat_key, mat_value, mat_out, mat_in, mat_back = (
        lax.all_gather(w_query, "dp", axis=0, tiled=True),
        lax.all_gather(w_key, "dp", axis=0, tiled=True),
        lax.all_gather(w_value, "dp", axis=0, tiled=True),
        lax.all_gather(w_out, "dp", axis=1, tiled=True),
        lax.all_gather(w_in, "dp", axis=0, tiled=True),
        lax.all_gather(w_back, "dp", axis=1, tiled=True),
    )
    grad_two_full = lax.all_gather(grad_two.astype(jnp.bfloat16), "tensor", axis=0, tiled=True)
    grad_w_back = matmul_over_rows(activation, grad_two_full)
    grad_pre = matmul_over_cols(grad_two_full, mat_back) * gelu_slope
    grad_b_in_part = jnp.sum(grad_pre, axis=0)
    grad_pre_bf = grad_pre.astype(jnp.bfloat16)
    grad_w_in = matmul_over_rows(hidden_full, grad_pre_bf)
    grad_one_out = grad_two + lax.psum_scatter(
        matmul_over_cols(grad_pre_bf, mat_in).astype(jnp.bfloat16),
        "tensor",
        scatter_dimension=0,
        tiled=True,
    ).astype(jnp.float32)
    grad_w_in, grad_w_back = (
        lax.psum_scatter(grad_w_in, "dp", scatter_dimension=0, tiled=True),
        lax.psum_scatter(grad_w_back, "dp", scatter_dimension=1, tiled=True),
    )
    grad_gain_attn = jnp.sum(grad_one_out * normed_one, axis=0)
    grad_shift_attn = jnp.sum(grad_one_out, axis=0)
    grad_one = norm_back(grad_one_out, normed_one, inv_one, gain_attn)
    grad_b_out = jnp.sum(grad_one, axis=0)
    grad_one_full = lax.all_gather(grad_one.astype(jnp.bfloat16), "tensor", axis=0, tiled=True)
    grad_w_out = matmul_over_rows(context, grad_one_full)
    grad_context = matmul_over_cols(grad_one_full, mat_out).astype(jnp.bfloat16)
    grad_query, grad_keys, grad_values = attend_backward(
        query_rows, key_rows, value_rows, context, grad_context, log_total, seg_ids, HD, block_rows
    )
    grad_b_query_part = jnp.sum(grad_query, axis=0)
    grad_b_value_part = jnp.sum(grad_values, axis=0)
    grad_query_bf = grad_query.astype(jnp.bfloat16)
    grad_keys_bf = grad_keys.astype(jnp.bfloat16)
    grad_values_bf = grad_values.astype(jnp.bfloat16)
    grad_w_query = matmul_over_rows(rows_full, grad_query_bf)
    grad_w_key = matmul_over_rows(rows_full, grad_keys_bf)
    grad_w_value = matmul_over_rows(rows_full, grad_values_bf)
    query_part = matmul_over_cols(grad_query_bf, mat_query)
    key_part = matmul_over_cols(grad_keys_bf, mat_key)
    value_part = matmul_over_cols(grad_values_bf, mat_value)
    grad_in = grad_one + lax.psum_scatter(
        (query_part + key_part + value_part).astype(jnp.bfloat16),
        "tensor",
        scatter_dimension=0,
        tiled=True,
    ).astype(jnp.float32)
    grad_w_query, grad_w_key, grad_w_value, grad_w_out = (
        lax.psum_scatter(grad_w_query, "dp", scatter_dimension=0, tiled=True),
        lax.psum_scatter(grad_w_key, "dp", scatter_dimension=0, tiled=True),
        lax.psum_scatter(grad_w_value, "dp", scatter_dimension=0, tiled=True),
        lax.psum_scatter(grad_w_out, "dp", scatter_dimension=1, tiled=True),
    )

    def widen(part_vec, full_width):
        return lax.dynamic_update_slice_in_dim(
            jnp.zeros((full_width,), jnp.float32), part_vec, tensor_index * part_vec.shape[0], 0
        )

    small_sums = lax.psum(
        (
            widen(grad_b_query_part, b_query.shape[0]),
            widen(grad_b_value_part, b_value.shape[0]),
            grad_b_out,
            grad_gain_attn,
            grad_shift_attn,
            widen(grad_b_in_part, b_in.shape[0]),
            grad_b_back,
            grad_gain_ffn,
            grad_shift_ffn,
        ),
        ("dp", "tensor"),
    )
    return (
        output,
        grad_in,
        grad_w_query,
        small_sums[0],
        grad_w_key,
        grad_w_value,
        small_sums[1],
        grad_w_out,
        small_sums[2],
        small_sums[3],
        small_sums[4],
        grad_w_in,
        small_sums[5],
        grad_w_back,
        small_sums[6],
        small_sums[7],
        small_sums[8],
    )


MESH_ID = pl.DeviceIdType.MESH
F32 = jnp.float32
BF16 = jnp.bfloat16

SLOTS = 4
BLOCK = 128
GROUP = 512
WIDTH = 1024
HEAD_COLS = 256
HIDDEN = 1024
N_SEND = 58
N_GOT = 110
HALF = BLOCK // 2
HALVES = dict(q=(128, 256), k=(128, 256), v=(128, 256), o=(256, 128), i0=(128, 512), i1=(128, 512), b0=(512, 128),
              b1=(512, 128))
VECTORS = dict(bq=1024, bv=1024, bo=1024, ga=1024, sa=1024, bi=4096, bb=1024, gf=1024, sf=1024)


def flip(bit):
    return 1 - bit


def slot_step(t, j):
    return (t % 2 + j % 2) % 2 + 2 * ((t // 2 + j // 2) % 2)


def rows_of(r, count=BLOCK):
    return pl.ds(pl.multiple_of(r * BLOCK, BLOCK), count)


def cols_of(n, count=256):
    return pl.ds(pl.multiple_of(n * count, count), count)


def dot_nn(a, b):
    return jnp.dot(a, b, preferred_element_type=F32)


def dot_nt(a, b):
    return lax.dot_general(a, b, (((1,), (1,)), ((), ())), preferred_element_type=F32)


def dot_tn(a, b):
    return lax.dot_general(a, b, (((0,), (0,)), ((), ())), preferred_element_type=F32)


def scratch_table():
    act = lambda n: pltpu.VMEM((GROUP, n), BF16)
    table = dict(
        w3=pltpu.VMEM((3 * WIDTH, HEAD_COLS), BF16),
        wo=pltpu.VMEM((4, HEAD_COLS, 256), BF16),
        wi=pltpu.VMEM((WIDTH, HIDDEN), BF16),
        wb=pltpu.VMEM((4, HIDDEN, 256), BF16),
        w3t=pltpu.VMEM((3, HEAD_COLS, WIDTH), BF16),
        wot=pltpu.VMEM((WIDTH, HEAD_COLS), BF16),
        wit=pltpu.VMEM((HIDDEN, WIDTH), BF16),
        wbt=pltpu.VMEM((WIDTH, HIDDEN), BF16),
        lens_own=pltpu.VMEM((2, 8, 128), F32),
        lens_got=pltpu.VMEM((2, 8, 128), F32),
        lens_use=pltpu.VMEM((2, 8, 128), F32),
        tk=act(WIDTH),
        tkt=pltpu.VMEM((WIDTH, GROUP), BF16),
        cot_own=pltpu.VMEM((BLOCK, WIDTH), BF16),
        bias=pltpu.VMEM((GROUP, GROUP), F32),
        q=act(HEAD_COLS),
        qt=pltpu.VMEM((HEAD_COLS, GROUP), BF16),
        k=act(HEAD_COLS),
        ks=act(HEAD_COLS),
        v=act(HEAD_COLS),
        ps=pltpu.VMEM((4, GROUP, GROUP), BF16),
        ctx=act(HEAD_COLS),
        ctxt=pltpu.VMEM((HEAD_COLS, GROUP), BF16),
        hid=act(WIDTH),
        hidt=pltpu.VMEM((WIDTH, GROUP), BF16),
        act=act(HIDDEN),
        actt=pltpu.VMEM((HIDDEN, GROUP), BF16),
        slope=pltpu.VMEM((GROUP, HIDDEN), F32),
        g2=act(WIDTH),
        gpre=act(HIDDEN),
        g1=act(WIDTH),
        gctxt=pltpu.VMEM((HEAD_COLS, GROUP), BF16),
        dq=act(HEAD_COLS),
        dkt=pltpu.VMEM((HEAD_COLS, GROUP), F32),
        dvt=pltpu.VMEM((HEAD_COLS, GROUP), F32),
        dk=act(HEAD_COLS),
        dv=act(HEAD_COLS),
        hid1=pltpu.VMEM((BLOCK, WIDTH), F32),
        normed1=pltpu.VMEM((BLOCK, WIDTH), F32),
        inv1=pltpu.VMEM((BLOCK, 128), F32),
        g2f=pltpu.VMEM((BLOCK, WIDTH), F32),
        g1f=pltpu.VMEM((BLOCK, WIDTH), F32),
        out_own=pltpu.VMEM((BLOCK, WIDTH), BF16),
        gtok_own=pltpu.VMEM((BLOCK, WIDTH), BF16),
        rs_own=pltpu.VMEM((4, BLOCK, WIDTH), BF16),
        rs_out=pltpu.VMEM((4, 3, BLOCK, WIDTH), BF16),
        rs_got=pltpu.VMEM((4, 3, BLOCK, WIDTH), BF16),
        sums=pltpu.VMEM((6, 16, WIDTH), F32),
        sums_got=pltpu.VMEM((5, 16, WIDTH), F32),
        gb_in=pltpu.VMEM((1, HIDDEN), F32),
        vectors={name: pltpu.VMEM((1, width), F32) for name, width in VECTORS.items()},
        vsem=pltpu.SemaphoreType.DMA((len(VECTORS),)),
        turn=pltpu.SemaphoreType.REGULAR((5,)),
        g3=pltpu.VMEM((3 * WIDTH, HEAD_COLS), BF16),
        go=pltpu.VMEM((4, HEAD_COLS, 256), BF16),
        gi=pltpu.VMEM((WIDTH, HIDDEN), BF16),
        gb=pltpu.VMEM((4, HIDDEN, 256), BF16),
        stage={},
        ssem=pltpu.SemaphoreType.DMA((N_SEND,)),
        rsem=pltpu.SemaphoreType.DMA((N_GOT,)),
    )
    for name, dims in HALVES.items():
        table["stage"][name] = pltpu.VMEM((10,) + dims, BF16)
    return table


def layer_kernel(tok, lens, wq, bq, wk, wv, bv, wo, bo, ga, sa, wi, bi, wb, bb, gf, sf, cot, out, gtok, sums, zq, zk, zv,
                 zo, zi0, zi1, zb0, zb1, *scratch):
    a = SimpleNamespace(tok=tok, lens=lens, wq=wq, bq=bq, wk=wk, wv=wv, bv=bv, wo=wo, bo=bo, ga=ga, sa=sa, wi=wi, bi=bi,
                        wb=wb, bb=bb, gf=gf, sf=sf, cot=cot)
    o = SimpleNamespace(out=out, gtok=gtok, sums=sums)
    landed = dict(q=zq, k=zk, v=zv, o=zo, i0=zi0, i1=zi1, b0=zb0, b1=zb1)
    s = SimpleNamespace(**jax.tree.unflatten(jax.tree.structure(scratch_table()), scratch))
    ssem, rsem, vsem, vectors = s.ssem, s.rsem, s.vsem, s.vectors

    dp = lax.axis_index("dp")
    z = lax.axis_index("tensor")
    b, c = dp // 2, dp % 2
    zl, zh = z % 2, z // 2
    t = zl * 2 + c
    sl = (z + 2 * c) % 4
    here, away = c == 0, c == 1
    bx = b + 1 - 2 * (b % 2)
    by = (b + 2) % 4
    bd = 3 - b
    t1, t2, t3 = slot_step(t, 1), slot_step(t, 2), slot_step(t, 3)

    def dev(pos, core, zz):
        return (pos * 2 + core, zz)

    partner = dev(b, flip(c), z)
    z_near = z + 1 - 2 * (z % 2)
    z_far = (z + 2) % 4
    pair = dev(b, c, z_near)
    across = dev(b, c, z_far)
    is_inner = jnp.logical_and(z >= 1, z <= 2)
    inner_away = jnp.logical_and(is_inner, away)
    outer_away = jnp.logical_and(jnp.logical_not(is_inner), away)
    x_near = dev(bx, c, z)
    y_near = dev(by, c, z)

    taken = {"s": 0, "r": 0}

    def take(kind, count=1):
        first = taken[kind]
        taken[kind] = first + count
        assert taken[kind] <= (N_SEND if kind == "s" else N_GOT)
        return first

    to_drain = []

    def make_copy(src, dst, device, sk, rk):
        return pltpu.make_async_remote_copy(
            src_ref=src, dst_ref=dst, send_sem=ssem.at[sk], recv_sem=rsem.at[rk], device_id=device,
            device_id_type=MESH_ID)

    def send(src, dst, device, sk, rk):
        make_copy(src, dst, device, sk, rk).start()

    def got(dst, rk):
        pltpu.make_async_copy(dst, dst, rsem.at[rk]).wait()

    def left(size_of, sk):
        pltpu.make_async_copy(size_of, size_of, ssem.at[sk]).wait()

    def at_end(size_of, sk, skipped=None, instead=None):
        to_drain.append((size_of, sk, skipped, instead))

    def send_or_keep(src, dst, device, is_self, sk, rk):
        copy = make_copy(src, dst, device, sk, rk)

        @pl.when(is_self)
        def _():
            pltpu.make_async_copy(src, dst, rsem.at[rk]).start()

        @pl.when(jnp.logical_not(is_self))
        def _():
            copy.start()

    barrier = pltpu.get_barrier_semaphore()
    peers = [x_near, y_near]
    for dz in range(4):
        for dc in range(2):
            if dz or dc:
                peers.append(dev(b, (c + dc) % 2, (z + dz) % 4))
    for peer in peers:
        pl.semaphore_signal(barrier, inc=1, device_id=peer, device_id_type=MESH_ID)
    pl.semaphore_wait(barrier, len(peers))

    def piece_qkv(m, home):
        base = m * WIDTH
        return SimpleNamespace(
            home=home,
            own=lambda bb, cc: s.w3.at[pl.ds(pl.multiple_of(base + bb * 256 + cc * 128, 128), 128), :],
            block=lambda bb: s.w3.at[pl.ds(pl.multiple_of(base + bb * 256, 256), 256), :],
            half=lambda bb, h: s.w3.at[pl.ds(pl.multiple_of(base + bb * 256 + h * 128, 128), 128), :])

    piece_o = SimpleNamespace(
        home=a.wo,
        own=lambda bb, cc: s.wo.at[bb, :, pl.ds(pl.multiple_of(cc * 128, 128), 128)],
        block=lambda bb: s.wo.at[bb],
        half=lambda bb, h: s.wo.at[bb, pl.ds(h * 128, 128), :])

    def piece_in(j):
        cols = pl.ds(j * 512, 512)
        return SimpleNamespace(
            home=a.wi.at[:, cols],
            own=lambda bb, cc: s.wi.at[pl.ds(pl.multiple_of(bb * 256 + cc * 128, 128), 128), cols],
            block=lambda bb: s.wi.at[pl.ds(pl.multiple_of(bb * 256, 256), 256), cols],
            half=lambda bb, h: s.wi.at[pl.ds(pl.multiple_of(bb * 256 + h * 128, 128), 128), cols])

    def piece_back(j):
        part = pl.ds(j * 512, 512)
        return SimpleNamespace(
            home=a.wb.at[part, :],
            own=lambda bb, cc: s.wb.at[bb, part, pl.ds(pl.multiple_of(cc * 128, 128), 128)],
            block=lambda bb: s.wb.at[bb, part, :],
            half=lambda bb, h: s.wb.at[bb, pl.ds(j * 512 + h * 256, 256), :])

    pieces = dict(q=piece_qkv(0, a.wq), k=piece_qkv(1, a.wk), v=piece_qkv(2, a.wv), o=piece_o,
                  i0=piece_in(0), i1=piece_in(1), b0=piece_back(0), b1=piece_back(1))
    first_size = dict(
        q=s.w3.at[0:768, :], k=s.w3.at[0:768, :], v=s.w3.at[0:768, :], o=s.wo.at[0:3], i0=s.wi.at[0:768, 0:512],
        i1=s.wi.at[0:768, 0:512], b0=s.wb.at[0:3, 0:512, :], b1=s.wb.at[0:3, 0:512, :])
    for name, piece in pieces.items():
        piece.s1, piece.r1 = take("s"), take("r")
        piece.s2, piece.r2 = take("s"), take("r", 3)
        at_end(piece.block(b), piece.s1, here, piece.own(b, 0))
        at_end(first_size[name], piece.s2)

    def to_local(name):
        piece = pieces[name]
        send_or_keep(piece.home, piece.own(b, c), dev(b, 0, z), here, piece.s1, piece.r1)

    def to_across(name):
        piece = pieces[name]
        send(piece.home, piece.own(b, c), dev(b, 1, z_far), piece.s1, piece.r1)

    def over_plane(name):
        piece = pieces[name]
        got(piece.block(b), piece.r1)
        send(piece.block(b), piece.block(b), x_near, piece.s2, piece.r2)
        send(piece.block(b), piece.block(b), y_near, piece.s2, piece.r2 + 1)

    def relay(name):
        piece = pieces[name]
        got(piece.block(bx), piece.r2)
        send(piece.half(bx, 0), piece.half(bx, 0), y_near, piece.s2, piece.r2 + 2)
        got(piece.block(by), piece.r2 + 1)
        send(piece.half(by, 1), piece.half(by, 1), x_near, piece.s2, piece.r2 + 2)

    def over_plane_now(names, chosen, relays=()):
        @pl.when(chosen)
        def _():
            for name in relays:
                relay(name)
            for name in names:
                over_plane(name)

    def arrived(name):
        piece = pieces[name]
        got(piece.block(bd), piece.r2 + 2)

    tok_s, tok_r = take("s", 2), take("r", 4)
    fwd_s = take("s", 6)
    lens_s, lens_r = take("s"), take("r")
    cot_s, cot_r = take("s"), take("r")

    def send_lens():
        first = a.lens[0, 0].astype(F32)
        s.lens_own[0] = jnp.full((8, 128), first, F32)
        s.lens_own[1] = jnp.full((8, 128), first + a.lens[0, 1].astype(F32), F32)
        send(s.lens_own, s.lens_got, partner, lens_s, lens_r)
        at_end(s.lens_own, lens_s)

    def take_lens():
        got(s.lens_got, lens_r)

        @pl.when(c == zh)
        def _():
            s.lens_use[...] = s.lens_own[...]

        @pl.when(c != zh)
        def _():
            s.lens_use[...] = s.lens_got[...]

    def tok_block(r):
        return s.tk.at[rows_of(r), :]

    inner, outer = 1 + c, 3 * c
    is_relay = jnp.logical_and(c == zh, z == inner)

    def send_tokens():
        near = z // 2 == c
        first = jnp.where(near, 2 * c, inner)
        send_or_keep(a.tok, tok_block(z), dev(b, c, first), first == z, tok_s, tok_r + z)
        at_end(tok_block(z), tok_s, first == z)
        second = make_copy(a.tok, tok_block(z), dev(b, c, 2 * c + 1), tok_s + 1, tok_r + z)
        keep = jnp.logical_and(near, z == 2 * c + 1)
        go = jnp.logical_and(near, z != 2 * c + 1)

        @pl.when(keep)
        def _():
            pltpu.make_async_copy(a.tok, tok_block(z), rsem.at[tok_r + z]).start()

        @pl.when(go)
        def _():
            second.start()

        at_end(tok_block(z), tok_s + 1, jnp.logical_not(go))

    def pass_on(half, far):
        for k in range(2):
            r = half * 2 + k
            block = tok_block(r)
            got(block, tok_r + r)
            if far:
                on = make_copy(block, block, dev(b, c, outer), fwd_s + k, tok_r + r)

                @pl.when(is_relay)
                def _():
                    on.start()
            copy = make_copy(block, block, partner, fwd_s + 2 + 2 * far + k, tok_r + r)

            @pl.when(c == zh)
            def _():
                copy.start()

    for k in range(6):
        at_end(s.tk.at[0:BLOCK, :], fwd_s + k, jnp.logical_not(is_relay) if k < 2 else c != zh)

    def send_cotangent():
        zt, ct = 2 * c + z // 2, z % 2
        is_self = jnp.logical_and(zt == z, ct == c)
        send_or_keep(a.cot, s.cot_own, dev(b, ct, zt), is_self, cot_s, cot_r)
        at_end(s.cot_own, cot_s, is_self)

    gather_s, gather_r = take("s", 3), take("r", 12)
    scatter_s, scatter_r = take("s", 4), take("r", 20)
    for k in range(3):
        at_end(s.tk.at[0:3 * BLOCK, :], gather_s + k)
    for k in range(4):
        at_end(s.tk.at[0:3 * BLOCK, :], scatter_s + k)

    def block_at(full, r):
        return full.at[rows_of(r), :]

    def half_at(full, r, k):
        return full.at[pl.ds(pl.multiple_of(r * BLOCK + k * HALF, HALF), HALF), :]

    def gather_start(which, full, k):
        mine = half_at(full, t, k)
        send(mine, mine, pair, gather_s + which, gather_r + 4 * which + 1 + k)
        send(mine, mine, partner, gather_s + which, gather_r + 4 * which)

    def gather_step(which, full, j):
        base = gather_r + 4 * which

        @pl.when(j == 1)
        def _():
            got(block_at(full, t1), base)

        @pl.when(j == 2)
        def _():
            if which == 0:
                over_plane_now((), inner_away, relays=("b0",))
            for k in range(2):
                near = half_at(full, t2, k)
                got(near, base + 1 + k)
                send(near, near, partner, gather_s + which, base + 3)

        @pl.when(j == 3)
        def _():
            if which == 0:
                over_plane_now((), inner_away, relays=("b1",))
            got(block_at(full, t3), base + 3)

    halves = [pl.ds(k * HALF, HALF) for k in range(2)]

    def scatter(which, part):
        out, back = s.rs_out, s.rs_got
        ss, rr = scatter_s + which, scatter_r + 5 * which
        part(t3 * BLOCK, BLOCK, out.at[which, 0])
        send(out.at[which, 0], back.at[which, 0], partner, ss, rr)
        part(t2 * BLOCK, BLOCK, out.at[which, 1])
        got(back.at[which, 0], rr)
        for k in range(2):
            rows = halves[k]
            total = out[which, 1, rows, :].astype(F32) + back[which, 0, rows, :].astype(F32)
            out[which, 1, rows, :] = total.astype(BF16)
            send(out.at[which, 1, rows, :], back.at[which, 1, rows, :], pair, ss, rr + 2 + k)
        part(t1 * BLOCK, BLOCK, out.at[which, 2])
        send(out.at[which, 2], back.at[which, 2], partner, ss, rr + 4)
        part(t * BLOCK, BLOCK, s.rs_own.at[which])

    def scatter_wait(which, k):
        rr = scatter_r + 5 * which
        if k == 0:
            got(s.rs_got.at[which, 2], rr + 4)
        got(s.rs_got.at[which, 1, halves[k], :], rr + 2 + k)

    def scatter_rows(which, chunk):
        total = s.rs_own[which, chunk, :].astype(F32) + s.rs_got[which, 2, chunk, :].astype(F32)
        return total + s.rs_got[which, 1, chunk, :].astype(F32)

    def by_halves(which, body, after):
        for k in range(2):
            scatter_wait(which, k)
            loop(2, lambda i: body(2 * k + i))
            after(k)

    def put_part(dst, n, value):
        dst[:, 256 * n:256 * n + 256] = value.astype(BF16)

    def loop(count, body):
        lax.fori_loop(0, count, lambda i, _: (body(i), 0)[1], 0)

    def grad_qkv(m):
        base = m * WIDTH
        return lambda bb, h: s.g3.at[pl.ds(pl.multiple_of(base + bb * 256 + h * 128, 128), 128), :]

    def grad_in_part(k):
        cols = pl.ds(k * 512, 512)
        return lambda bb, h: s.gi.at[pl.ds(pl.multiple_of(bb * 256 + h * 128, 128), 128), cols]

    def grad_back_part(k):
        part = pl.ds(k * 512, 512)
        return lambda bb, h: s.gb.at[bb, part, pl.ds(h * 128, 128)]

    grad_half = dict(
        q=grad_qkv(0), k=grad_qkv(1), v=grad_qkv(2), o=lambda bb, h: s.go.at[bb, :, pl.ds(h * 128, 128)],
        i0=grad_in_part(0), i1=grad_in_part(1), b0=grad_back_part(0), b1=grad_back_part(1))
    grad_s = {name: take("s", 2) for name in grad_half}
    grad_r = {name: take("r", 4) for name in grad_half}
    for name in grad_half:
        at_end(s.stage[name].at[0:6], grad_s[name])
        at_end(s.stage[name].at[0:2], grad_s[name] + 1, here, s.stage[name].at[0])

    def chunks(name, body):
        size = 64 if name in ("i0", "i1") else 128
        count = HALVES[name][0] // size
        loop(count, lambda i: body(pl.ds(pl.multiple_of(i * size, size), size)))

    def grad_first(name, part=2):
        half, ss, rr, st = grad_half[name], grad_s[name], grad_r[name], s.stage[name]
        if part in (0, 2):
            send(half(bd, 0), st.at[1], x_near, ss, rr)
            send(half(bd, 1), st.at[3], y_near, ss, rr + 1)
        if part == 0:
            return
        send(half(bx, 0), st.at[0], x_near, ss, rr + 2)
        send(half(by, 1), st.at[2], y_near, ss, rr + 2)

    def grad_second(name):
        half, ss, rr, st = grad_half[name], grad_s[name], grad_r[name], s.stage[name]
        for h, block, to in ((0, by, y_near), (1, bx, x_near)):
            got(st.at[1 + 2 * h], rr + h)
            mine = half(block, h)

            def add(ch):
                st[4 + h, ch, :] = (mine[ch, :].astype(F32) + st[1 + 2 * h, ch, :].astype(F32)).astype(BF16)
            chunks(name, add)
            send(st.at[4 + h], st.at[6 + h], to, ss, rr + 2)

    def grad_third(name):
        half, ss, rr, st = grad_half[name], grad_s[name], grad_r[name], s.stage[name]
        zr = landed[name]
        got(st.at[0:4], rr + 2)
        for h in range(2):
            mine = half(b, h)

            def add_all(ch):
                total = mine[ch, :].astype(F32) + st[2 * h, ch, :].astype(F32) + st[6 + h, ch, :].astype(F32)
                st[8 + h, ch, :] = total.astype(BF16)
            chunks(name, add_all)
            is_self = here if h == 0 else c < 0
            send_or_keep(st.at[8 + h], zr.at[zh], dev(b, h, sl), is_self, ss + 1, rr + 3)

    def grad_final(name):
        got(landed[name], grad_r[name] + 3)

    to_across("q")
    to_across("k")
    send_tokens()
    to_across("v")
    for name in pieces:
        to_local(name)
    send_lens()
    for name, ref in vectors.items():
        pltpu.make_async_copy(getattr(a, name), ref, vsem.at[list(vectors).index(name)]).start()
    s.sums[0] = jnp.zeros((16, WIDTH), F32)
    s.gb_in[...] = jnp.zeros((1, HIDDEN), F32)
    leads = jnp.logical_and(is_inner, away)

    def in_turn(k, inner_next, outer_next):
        @pl.when(leads)
        def _():
            for device in (partner, pair, dev(b, 0, z_near)):
                pl.semaphore_signal(s.turn.at[k], inc=1, device_id=device, device_id_type=MESH_ID)

        @pl.when(jnp.logical_not(leads))
        def _():
            pl.semaphore_wait(s.turn.at[k], 1)

        for chosen, names in ((is_inner, inner_next), (jnp.logical_not(is_inner), outer_next)):
            if names:
                @pl.when(chosen)
                def _():
                    for name in names:
                        to_across(name)

    over_plane_now(("q", "k", "v", "o"), here)
    over_plane_now(("q", "k"), away)
    relay("q")
    over_plane_now(("i0",), here, relays=("k", "v"))
    pass_on(zh, 0)
    to_across("o")

    @pl.when(is_inner)
    def _():
        pass_on(flip(zh), 1)

    in_turn(0, (), ("i0",))
    take_lens()

    def make_bias(r):
        first, end = s.lens_use[0][0:1, 0:1], s.lens_use[1][0:1, 0:1]
        row = (lax.broadcasted_iota(jnp.int32, (BLOCK, GROUP), 0) + r * BLOCK).astype(F32)
        col = lax.broadcasted_iota(jnp.int32, (BLOCK, GROUP), 1).astype(F32)
        seg = lambda p: jnp.where(p >= end, 2.0, jnp.where(p >= first, 1.0, 0.0))
        s.bias[rows_of(r), :] = jnp.where(seg(row) == seg(col), 0.0, masked_value)
    loop(SLOTS, make_bias)
    for name, ref in vectors.items():
        pltpu.make_async_copy(getattr(a, name), ref, vsem.at[list(vectors).index(name)]).wait()
        setattr(a, name, ref)
    over_plane_now(("v", "o"), away, relays=("k",))
    over_plane_now(("i1",), here, relays=("o",))
    over_plane_now((), away, relays=("v",))
    over_plane_now(("b0",), here, relays=("i0",))
    in_turn(1, ("i0", "i1"), ("i1",))

    @pl.when(jnp.logical_not(is_inner))
    def _():
        pass_on(flip(zh), 1)


    def turn_tokens(r):
        s.tkt[:, rows_of(r)] = s.tk[rows_of(r), :].T
    loop(SLOTS, turn_tokens)

    head_cols = pl.ds(pl.multiple_of(sl * HEAD_COLS, HEAD_COLS), HEAD_COLS)

    def project(m):
        acc = dot_nn(s.tk[...], s.w3[m * WIDTH:(m + 1) * WIDTH, :])
        if m == 0:
            value = (acc + a.bq[:, head_cols]).astype(BF16)
            scaled = (value.astype(F32) * 0.125).astype(BF16)
            s.q[...] = scaled
            s.qt[...] = scaled.T
        elif m == 1:
            value = acc.astype(BF16)
            s.k[...] = value
            s.ks[...] = (value.astype(F32) * 0.125).astype(BF16)
        else:
            s.v[...] = (acc + a.bv[:, head_cols]).astype(BF16)

    arrived("q")
    project(0)
    arrived("k")
    project(1)
    in_turn(2, ("b0", "b1"), ())
    arrived("v")
    project(2)

    def attend():
        parts = []
        for h in range(4):
            cols = slice(64 * h, 64 * h + 64)
            scores = dot_nt(s.q[:, cols], s.k[:, cols]) + s.bias[...]
            top = jnp.max(scores, axis=-1, keepdims=True)
            weight = jnp.exp(scores - top)
            total = jnp.sum(weight, axis=-1, keepdims=True)
            prob = (weight * (1.0 / total)).astype(BF16)
            s.ps[h] = prob
            parts.append(dot_nn(prob, s.v[:, cols]))
        context = jnp.concatenate(parts, axis=1).astype(BF16)
        s.ctx[...] = context
        s.ctxt[...] = context.T
    over_plane_now((), away, relays=("o",))
    over_plane_now(("i0",), inner_away)
    over_plane_now(("b1",), here, relays=("i1",))
    attend()
    over_plane_now(("i0",), outer_away)
    over_plane_now(("i1",), inner_away)
    arrived("o")

    def attn_part(first, count, dst):
        rows = s.ctx[pl.ds(pl.multiple_of(first, HALF), count), :]
        for n in range(4):
            put_part(dst, n, dot_nn(rows, s.wo[n]))
    scatter(0, attn_part)
    @pl.when(jnp.logical_not(is_inner))
    def _():
        to_across("b0")
        to_across("b1")

    for m in range(3):
        for n in range(4):
            s.w3t[m, :, 256 * n:256 * n + 256] = s.w3[m * WIDTH + 256 * n:m * WIDTH + 256 * n + 256, :].T
    for n in range(4):
        s.wot[256 * n:256 * n + 256, :] = s.wo[n].T

    CH = 32

    def own_chunk(i):
        return pl.ds(pl.multiple_of(i * CH, CH), CH)

    def group_chunk(i):
        return pl.ds(pl.multiple_of(t * BLOCK + i * CH, CH), CH)

    def norm_one(i):
        ch = own_chunk(i)
        resid = s.tk[group_chunk(i), :].astype(F32) + scatter_rows(0, ch) + a.bo[...]
        centered = resid - jnp.mean(resid, axis=-1, keepdims=True)
        inv = lax.rsqrt(jnp.mean(centered * centered, axis=-1, keepdims=True) + epsilon)
        normed = centered * inv
        hidden = normed * a.ga[...] + a.sa[...]
        s.normed1[ch, :] = normed
        s.inv1[ch, :] = jnp.broadcast_to(inv, (CH, 128))
        s.hid1[ch, :] = hidden
        s.hid[group_chunk(i), :] = hidden.astype(BF16)
    over_plane_now((), here, relays=("b0",))
    over_plane_now((), inner_away, relays=("i0",))
    over_plane_now(("i1", "b0", "b1"), outer_away, relays=("i0",))
    by_halves(0, norm_one, lambda k: gather_start(0, s.hid, k))
    over_plane_now((), here, relays=("b1",))
    over_plane_now((), inner_away, relays=("i1",))
    over_plane_now((), outer_away, relays=("i1", "b0", "b1"))
    over_plane_now(("b0", "b1"), inner_away)
    send_cotangent()
    arrived("i0")
    arrived("i1")

    def ffn_in(j):
        gather_step(0, s.hid, j)
        r = slot_step(t, j)
        rows = rows_of(r)
        for n in range(4):
            cols = slice(256 * n, 256 * n + 256)
            bias = a.bi[:, pl.ds(pl.multiple_of(sl * HIDDEN + n * 256, 256), 256)]
            pre = dot_nn(s.hid[rows, :], s.wi[:, cols]) + bias
            cdf = 0.5 * (1.0 + lax.erf(pre * 0.7071067811865476))
            pdf = jnp.exp(-0.5 * pre * pre) * 0.3989422804014327
            s.act[rows, cols] = (pre * cdf).astype(BF16)
            s.slope[rows, cols] = cdf + pre * pdf
    loop(SLOTS, ffn_in)

    def turn_ffn(r):
        rows = rows_of(r)
        s.actt[:, rows] = s.act[rows, :].T
        s.hidt[:, rows] = s.hid[rows, :].T
    arrived("b0")
    arrived("b1")

    def ffn_part(first, count, dst):
        rows = pl.ds(pl.multiple_of(first, HALF), count)
        for n in range(4):
            put_part(dst, n, dot_nn(s.act[rows, :], s.wb[n]))
    scatter(1, ffn_part)
    loop(SLOTS, turn_ffn)

    def turn_wi(r):
        rows = rows_of(r)
        s.wit[:, rows] = s.wi[rows, :].T
    loop(8, turn_wi)

    def turn_wb(r):
        rows = rows_of(r)
        for n in range(4):
            s.wbt[256 * n:256 * n + 256, rows] = s.wb[n, rows, :].T
    loop(8, turn_wb)
    got(s.cot_own, cot_r)

    def add_rows(row, value):
        s.sums[0, row:row + 1, :] += jnp.sum(value, axis=0, keepdims=True)

    def norm_two(i):
        ch = own_chunk(i)
        resid = s.hid1[ch, :] + scatter_rows(1, ch) + a.bb[...]
        centered = resid - jnp.mean(resid, axis=-1, keepdims=True)
        inv = lax.rsqrt(jnp.mean(centered * centered, axis=-1, keepdims=True) + epsilon)
        normed = centered * inv
        position = lax.broadcasted_iota(jnp.int32, (CH, 128), 0) + (t * BLOCK + i * CH)
        live = jnp.where(position.astype(F32) < s.lens_use[1][0:1, :], 1.0, 0.0)[:, 0:1]
        s.out_own[ch, :] = ((normed * a.gf[...] + a.sf[...]) * live).astype(BF16)
        grad = s.cot_own[ch, :].astype(F32) * live
        add_rows(4, grad * normed)
        add_rows(5, grad)
        u = grad * a.gf[...]
        first = jnp.mean(u, axis=-1, keepdims=True)
        second = jnp.mean(u * normed, axis=-1, keepdims=True)
        grad_two = inv * (u - first - normed * second)
        add_rows(3, grad_two)
        s.g2f[ch, :] = grad_two
        s.g2[group_chunk(i), :] = grad_two.astype(BF16)
    by_halves(1, norm_two, lambda k: gather_start(1, s.g2, k))
    out_s, out_r = take("s"), take("r")
    home_self = jnp.logical_and(zh == c, t == z)

    def ffn_back(j):
        @pl.when(j < 3)
        def _():
            gather_step(1, s.g2, j)
        r = slot_step(t, j)
        rows = rows_of(r)
        for n in range(4):
            cols = slice(256 * n, 256 * n + 256)
            grad = dot_nn(s.g2[rows, :], s.wbt[:, cols]) * s.slope[rows, cols]
            s.gb_in[:, cols] += jnp.sum(grad, axis=0, keepdims=True)
            s.gpre[rows, cols] = grad.astype(BF16)
    loop(SLOTS - 1, ffn_back)

    def grad_back(k):
        part = slice(512 * k, 512 * k + 512)

        def body(n):
            for e in range(2):
                block = n * 2 + e
                s.gb[block, part, :] = dot_nn(s.actt[part, :], s.g2[:, cols_of(block)]).astype(BF16)
        loop(2, body)

    def grad_in(k):
        cols = slice(512 * k, 512 * k + 512)

        def body(m):
            part = rows_of(m * 4, 512)
            s.gi[part, cols] = dot_nn(s.hidt[part, :], s.gpre[:, cols]).astype(BF16)
        loop(2, body)

    gather_step(1, s.g2, 3)
    grad_back(0)
    grad_first("b0")
    ffn_back(3)
    grad_back(1)
    grad_first("b1", 0)
    send_or_keep(s.out_own, o.out, dev(b, zh, t), home_self, out_s, out_r)
    at_end(s.out_own, out_s, home_self)

    def in_part(first, count, dst):
        rows = pl.ds(pl.multiple_of(first, HALF), count)
        for n in range(4):
            put_part(dst, n, dot_nn(s.gpre[rows, :], s.wit[:, 256 * n:256 * n + 256]))
    scatter(2, in_part)
    grad_in(0)
    grad_in(1)
    grad_second("b0")
    grad_first("b1", 1)
    grad_second("b1")
    grad_first("i0", 0)

    def norm_one_back(i):
        ch = own_chunk(i)
        grad = s.g2f[ch, :] + scatter_rows(2, ch)
        normed = s.normed1[ch, :]
        add_rows(1, grad * normed)
        add_rows(2, grad)
        u = grad * a.ga[...]
        first = jnp.mean(u, axis=-1, keepdims=True)
        second = jnp.mean(u * normed, axis=-1, keepdims=True)
        grad_one = s.inv1[ch, 0:1] * (u - first - normed * second)
        add_rows(0, grad_one)
        s.g1f[ch, :] = grad_one
        s.g1[group_chunk(i), :] = grad_one.astype(BF16)
    by_halves(2, norm_one_back, lambda k: gather_start(2, s.g1, k))
    grad_first("i0", 1)
    grad_third("b0")

    def attend_back(chip, add):
        rows = pl.ds(pl.multiple_of(chip * 2 * BLOCK, 2 * BLOCK), 2 * BLOCK)
        grad_ctx = dot_nn(s.g1[rows, :], s.wot[...]).astype(BF16)
        s.gctxt[:, rows] = grad_ctx.T
        product = grad_ctx.astype(F32) * s.ctx[rows, :].astype(F32)
        parts = []
        for h in range(4):
            cols = slice(64 * h, 64 * h + 64)
            prob = s.ps[h, rows, :]
            delta = jnp.sum(product[:, cols], axis=-1, keepdims=True)
            grad_prob = dot_nt(grad_ctx[:, cols], s.v[:, cols])
            grad_score = (prob.astype(F32) * (grad_prob - delta)).astype(BF16)
            parts.append(dot_nn(grad_score, s.ks[:, cols]))
            grad_key = dot_nn(s.qt[cols, rows], grad_score)
            grad_value = dot_nn(s.gctxt[cols, rows], prob)
            if add:
                grad_key, grad_value = s.dkt[cols, :] + grad_key, s.dvt[cols, :] + grad_value
            s.dkt[cols, :] = grad_key
            s.dvt[cols, :] = grad_value
        grad_query = jnp.concatenate(parts, axis=1)
        for k in range(4):
            @pl.when(sl == k)
            def _():
                s.sums[0, 6:7, 256 * k:256 * k + 256] += jnp.sum(grad_query, axis=0, keepdims=True)
        s.dq[rows, :] = grad_query.astype(BF16)
    gather_step(2, s.g1, 1)
    attend_back(zl, False)
    grad_third("b1")
    gather_step(2, s.g1, 2)
    gather_step(2, s.g1, 3)
    attend_back(flip(zl), True)
    grad_second("i0")
    grad_first("i1")
    s.dk[...] = s.dkt[...].T.astype(BF16)
    grad_value = s.dvt[...].T
    for k in range(4):
        @pl.when(sl == k)
        def _():
            s.sums[0, 7:8, 256 * k:256 * k + 256] += jnp.sum(grad_value, axis=0, keepdims=True)
    s.dv[...] = grad_value.astype(BF16)
    for k in range(4):
        @pl.when(sl == k)
        def _():
            s.sums[0, 8 + k:9 + k, :] = s.gb_in[...]

    sums_s, sums_r = take("s", 5), take("r", 5)
    sums_to = [partner, across, pair, x_near, y_near]

    def sums_start(k):
        send(s.sums.at[k], s.sums_got.at[k], sums_to[k], sums_s + k, sums_r + k)
        at_end(s.sums.at[k], sums_s + k)

    def sums_finish(k):
        got(s.sums_got.at[k], sums_r + k)
        total = s.sums[k] + s.sums_got[k]
        s.sums[k + 1] = total
        if k == 4:
            pltpu.make_async_copy(s.sums.at[5], o.sums, vsem.at[0]).start()

    sums_start(0)

    def tok_part(first, count, dst):
        rows = pl.ds(pl.multiple_of(first, HALF), count)
        for n in range(4):
            cols = slice(256 * n, 256 * n + 256)
            acc = dot_nn(s.dq[rows, :], s.w3t[0, :, cols])
            acc = acc + dot_nn(s.dk[rows, :], s.w3t[1, :, cols])
            acc = acc + dot_nn(s.dv[rows, :], s.w3t[2, :, cols])
            put_part(dst, n, acc)
    scatter(3, tok_part)
    sums_finish(0)
    sums_start(1)

    def grad_head(m, src):
        s.g3[m * WIDTH:(m + 1) * WIDTH, :] = dot_nn(s.tkt[...], src[...]).astype(BF16)

    grad_third("i0")
    for n in range(4):
        s.go[n] = dot_nn(s.ctxt[...], s.g1[:, 256 * n:256 * n + 256]).astype(BF16)
    grad_head(0, s.dq)
    grad_head(1, s.dk)
    grad_head(2, s.dv)
    grad_second("i1")
    grad_first("o")
    grad_first("q")
    gtok_s, gtok_r = take("s"), take("r")
    at_end(s.gtok_own, gtok_s, home_self)

    def last_rows(i):
        ch = own_chunk(i)
        s.gtok_own[ch, :] = (s.g1f[ch, :] + scatter_rows(3, ch)).astype(BF16)

    def rows_home(chosen):
        @pl.when(chosen)
        def _():
            by_halves(3, last_rows, lambda k: None)
            send_or_keep(s.gtok_own, o.gtok, dev(b, zh, t), home_self, gtok_s, gtok_r)

    rows_home(is_inner)
    grad_third("i1")
    grad_second("o")
    grad_first("k")
    grad_second("q")
    grad_first("v")
    rows_home(jnp.logical_not(is_inner))
    sums_finish(1)
    sums_start(2)
    grad_third("o")
    grad_second("k")
    grad_third("q")
    sums_finish(2)
    grad_second("v")
    sums_start(3)
    grad_third("k")
    grad_third("v")
    sums_finish(3)
    sums_start(4)
    grad_final("b0")
    grad_final("b1")
    grad_final("i0")
    grad_final("i1")
    got(o.gtok, gtok_r)
    got(o.out, out_r)
    grad_final("o")
    grad_final("q")
    sums_finish(4)
    grad_final("k")
    grad_final("v")

    pltpu.make_async_copy(s.sums.at[5], o.sums, vsem.at[0]).wait()
    for size_of, sk, skipped, instead in to_drain:
        if skipped is None:
            left(size_of, sk)
        else:
            @pl.when(jnp.logical_not(skipped))
            def _():
                left(size_of, sk)
            if instead is not None:
                @pl.when(skipped)
                def _():
                    left(instead, sk)


def result_kernel(*refs):
    out, gtok, sums, zq, zk, zv, zo, zi0, zi1, zb0, zb1 = refs[:11]
    (o_out, o_gtok, o_gq, o_gbq, o_gk, o_gv, o_gbv, o_go, o_gbo, o_gga, o_gsa, o_gi, o_gbi, o_gb, o_gbb, o_ggf,
     o_gsf) = refs[11:28]
    held, wide, lines, wide_in, in_sem, out_sem = refs[28:39], refs[39:46], refs[46:55], refs[55], refs[56], refs[57]
    arriving = [pltpu.make_async_copy(src, dst, in_sem.at[n]) for n, (src, dst) in enumerate(zip(refs[:11], held))]
    for n in (0, 1, 9, 10, 7, 8, 6, 3, 4, 5, 2):
        arriving[n].start()
    leaving = []

    def put(src, dst):
        copy = pltpu.make_async_copy(src, dst, out_sem.at[len(leaving)])
        copy.start()
        leaving.append(copy)

    arriving[0].wait()
    put(held[0], o_out)
    arriving[1].wait()
    wide[0][...] = held[1][...].astype(F32)
    put(wide[0], o_gtok)

    def both(n, dst):
        arriving[n].wait()
        dst[...] = held[n][0].astype(F32) + held[n][1].astype(F32)

    both(9, wide[1].at[0:512, :])
    both(10, wide[1].at[512:1024, :])
    put(wide[1], o_gb)
    both(7, wide_in.at[:, 0:512])
    both(8, wide_in.at[:, 512:1024])
    put(wide_in, o_gi)
    for n, buf, dst in ((6, wide[2], o_go), (3, wide[3], o_gq), (4, wide[4], o_gk), (5, wide[5], o_gv)):
        both(n, buf)
        put(buf, dst)
    arriving[2].wait()
    for row, buf, dst in ((6, 0, o_gbq), (7, 1, o_gbv), (0, 2, o_gbo), (1, 3, o_gga), (2, 4, o_gsa), (3, 5, o_gbb),
                          (4, 6, o_ggf), (5, 7, o_gsf)):
        lines[buf][...] = held[2][row:row + 1, :]
        put(lines[buf], dst)
    for k in range(4):
        lines[8][:, WIDTH * k:WIDTH * k + WIDTH] = held[2][8 + k:9 + k, :]
    put(lines[8], o_gbi)
    for copy in leaving:
        copy.wait()


def on_device_fused(tokens, lengths, w_query, b_query, w_key, w_value, b_value, w_out, b_out, gain_attn, shift_attn,
                    w_in, b_in, w_back, b_back, gain_ffn, shift_ffn, cotangent):
    row = lambda vec: vec.reshape(1, -1)
    operands = (tokens, lengths, w_query, row(b_query), w_key, w_value, row(b_value), w_out, row(b_out),
                row(gain_attn), row(shift_attn), w_in, row(b_in), w_back, row(b_back), row(gain_ffn),
                row(shift_ffn), cotangent)
    stay = pl.BlockSpec(memory_space=pl.ANY)
    in_specs = [stay] * len(operands)
    in_specs[1] = pl.BlockSpec(memory_space=pltpu.SMEM)
    shape = lambda dims, dtype: jax.ShapeDtypeStruct(dims, dtype)
    between = [shape(tokens.shape, BF16), shape(tokens.shape, BF16), shape((16, WIDTH), F32)]
    between += [shape((2,) + HALVES[name], BF16) for name in ("q", "k", "v", "o", "i0", "i1", "b0", "b1")]
    parts = pl.pallas_call(
        layer_kernel,
        out_shape=between,
        in_specs=in_specs,
        out_specs=[stay] * len(between),
        scratch_shapes=jax.tree.leaves(scratch_table()),
        compiler_params=pltpu.CompilerParams(collective_id=0, has_side_effects=True, vmem_limit_bytes=64 * 1024 * 1000),
        name="layer",
    )(*operands)
    line = shape((1, WIDTH), F32)
    results = (
        shape(tokens.shape, BF16), shape(tokens.shape, F32), shape(w_query.shape, F32), line, shape(w_key.shape, F32),
        shape(w_value.shape, F32), line, shape(w_out.shape, F32), line, line, line, shape(w_in.shape, F32),
        shape((1, b_in.shape[0]), F32), shape(w_back.shape, F32), line, line, line)
    outs = pl.pallas_call(
        result_kernel,
        out_shape=results,
        in_specs=[stay] * len(between),
        out_specs=[stay] * len(results),
        scratch_shapes=[pltpu.VMEM(part.shape, part.dtype) for part in between]
        + [pltpu.VMEM(dims, F32) for dims in (tokens.shape, w_back.shape, w_out.shape, w_query.shape, w_key.shape,
                                              w_value.shape, (8, 128))]
        + [pltpu.VMEM((1, WIDTH), F32)] * 8
        + [pltpu.VMEM((1, b_in.shape[0]), F32), pltpu.VMEM(w_in.shape, F32), pltpu.SemaphoreType.DMA((11,)),
           pltpu.SemaphoreType.DMA((17,))],
        name="results",
    )(*parts)
    return tuple(v.reshape(-1) if v.shape[0] == 1 else v for v in outs)


def fits_fused(mesh):
    return dict(mesh.shape) == {"dp": 8, "tensor": 4}


def solution(mesh):
    placed = (
        P(("dp", "tensor"), None),
        P("dp", None),
        P("dp", "tensor"),
        P(),
        P("dp", "tensor"),
        P("dp", "tensor"),
        P(),
        P("tensor", "dp"),
        P(),
        P(),
        P(),
        P("dp", "tensor"),
        P(),
        P("tensor", "dp"),
        P(),
        P(),
        P(),
        P(("dp", "tensor"), None),
    )
    on_device = on_device_fused if fits_fused(mesh) else on_device_plain
    return jax.shard_map(
        on_device,
        mesh=mesh,
        in_specs=placed,
        out_specs=(
            P(("dp", "tensor"), None),
            P(("dp", "tensor"), None),
            P("dp", "tensor"),
            P(),
            P("dp", "tensor"),
            P("dp", "tensor"),
            P(),
            P("tensor", "dp"),
            P(),
            P(),
            P(),
            P("dp", "tensor"),
            P(),
            P("tensor", "dp"),
            P(),
            P(),
            P(),
        ),
        check_vma=False,
    )
```

```python
from types import SimpleNamespace

import jax
import jax.numpy as jnp
from jax import lax
from jax.experimental import pallas as pl
from jax.experimental.pallas import tpu as pltpu
from jax.sharding import PartitionSpec as P

HD = 64


epsilon = 1e-06
masked_value = -1e30


def matmul_plain(left_side, right_side):
    return jnp.dot(left_side, right_side, preferred_element_type=jnp.float32)


def matmul_over_rows(left_side, right_side):
    return lax.dot_general(
        left_side, right_side, (((0,), (0,)), ((), ())), preferred_element_type=jnp.float32
    )


def matmul_over_cols(left_side, right_side):
    return lax.dot_general(
        left_side, right_side, (((1,), (1,)), ((), ())), preferred_element_type=jnp.float32
    )


def layer_norm(residual, gain_vec, shift_vec):
    mean_val = jnp.mean(residual, axis=-1, keepdims=True)
    centered = residual - mean_val
    inv_std = lax.rsqrt(jnp.mean(centered * centered, axis=-1, keepdims=True) + epsilon)
    normed = centered * inv_std
    return (normed * gain_vec + shift_vec, normed, inv_std)


def norm_back(grad_out, normed, inv_std, gain_vec):
    grad_norm = grad_out * gain_vec
    first_mean = jnp.mean(grad_norm, axis=-1, keepdims=True)
    second_mean = jnp.mean(grad_norm * normed, axis=-1, keepdims=True)
    return inv_std * (grad_norm - first_mean - normed * second_mean)


def gelu_parts(preact):
    cdf_val = 0.5 * (1.0 + lax.erf(preact * 0.7071067811865476))
    pdf_val = jnp.exp(-0.5 * preact * preact) * 0.3989422804014327
    return (preact * cdf_val, cdf_val + preact * pdf_val)


def attend_forward(query_rows, key_rows, value_rows, seg_ids, head_dim, block_rows):
    group_rows, head_cols = query_rows.shape
    pair_width = 2 * head_dim
    block_count = group_rows // block_rows
    pair_count = head_cols // pair_width
    score_scale = head_dim ** (-0.5)

    def attend_step(step_index, loop_carry):
        context, log_total = loop_carry
        pair_index = step_index // block_count
        row_start = step_index % block_count * block_rows
        first_col = pair_index * pair_width
        query_block = lax.dynamic_slice(
            query_rows, (row_start, first_col), (block_rows, pair_width)
        ).reshape(block_rows, 2, head_dim)
        key_pair = lax.dynamic_slice(key_rows, (0, first_col), (group_rows, pair_width)).reshape(
            group_rows, 2, head_dim
        )
        value_pair = lax.dynamic_slice(
            value_rows, (0, first_col), (group_rows, pair_width)
        ).reshape(group_rows, 2, head_dim)
        same_seg = seg_ids[:, None] == seg_ids[None, :]
        scores = (
            jnp.einsum("qhd,khd->hqk", query_block, key_pair, preferred_element_type=jnp.float32)
            * score_scale
        )
        scores = jnp.where(same_seg[None], scores, masked_value)
        row_max = jnp.max(scores, axis=-1, keepdims=True)
        block_total = row_max + jnp.log(jnp.sum(jnp.exp(scores - row_max), axis=-1, keepdims=True))
        prob_bf = jnp.exp(scores - block_total).astype(jnp.bfloat16)
        context_block = jnp.einsum(
            "hqk,khd->qhd", prob_bf, value_pair, preferred_element_type=jnp.float32
        ).astype(jnp.bfloat16)
        context = lax.dynamic_update_slice(
            context, context_block.reshape(block_rows, pair_width), (row_start, first_col)
        )
        log_total = lax.dynamic_update_slice(
            log_total, block_total[:, :, 0], (2 * pair_index, row_start)
        )
        return (context, log_total)

    start_carry = (
        jnp.zeros((group_rows, head_cols), jnp.bfloat16),
        jnp.zeros((head_cols // head_dim, group_rows), jnp.float32),
    )
    return lax.fori_loop(0, pair_count * block_count, attend_step, start_carry)


def attend_backward(
    query_rows,
    key_rows,
    value_rows,
    context,
    grad_context,
    log_total,
    seg_ids,
    head_dim,
    block_rows,
):
    group_rows, head_cols = query_rows.shape
    pair_width = 2 * head_dim
    block_count = group_rows // block_rows
    pair_count = head_cols // pair_width
    score_scale = head_dim ** (-0.5)

    def back_step(step_index, loop_carry):
        grad_query, grad_keys, grad_values = loop_carry
        pair_index = step_index // block_count
        row_start = step_index % block_count * block_rows
        first_col = pair_index * pair_width
        query_block = lax.dynamic_slice(
            query_rows, (row_start, first_col), (block_rows, pair_width)
        ).reshape(block_rows, 2, head_dim)
        key_pair = lax.dynamic_slice(key_rows, (0, first_col), (group_rows, pair_width)).reshape(
            group_rows, 2, head_dim
        )
        value_pair = lax.dynamic_slice(
            value_rows, (0, first_col), (group_rows, pair_width)
        ).reshape(group_rows, 2, head_dim)
        context_block = lax.dynamic_slice(
            context, (row_start, first_col), (block_rows, pair_width)
        ).reshape(block_rows, 2, head_dim)
        gctx_block = lax.dynamic_slice(
            grad_context, (row_start, first_col), (block_rows, pair_width)
        ).reshape(block_rows, 2, head_dim)
        total_block = lax.dynamic_slice(log_total, (2 * pair_index, row_start), (2, block_rows))
        same_seg = seg_ids[:, None] == seg_ids[None, :]
        scores = (
            jnp.einsum("qhd,khd->hqk", query_block, key_pair, preferred_element_type=jnp.float32)
            * score_scale
        )
        scores = jnp.where(same_seg[None], scores, masked_value)
        probs = jnp.exp(scores - total_block[:, :, None])
        prob_bf = probs.astype(jnp.bfloat16)
        grad_probs = jnp.einsum(
            "qhd,khd->hqk", gctx_block, value_pair, preferred_element_type=jnp.float32
        )
        delta_rows = jnp.sum(
            gctx_block.astype(jnp.float32) * context_block.astype(jnp.float32), axis=-1
        ).T[:, :, None]
        grad_scores = (probs * (grad_probs - delta_rows) * score_scale).astype(jnp.bfloat16)
        grad_q_block = jnp.einsum(
            "hqk,khd->qhd", grad_scores, key_pair, preferred_element_type=jnp.float32
        ).reshape(block_rows, pair_width)
        grad_k_pair = jnp.einsum(
            "hqk,qhd->khd", grad_scores, query_block, preferred_element_type=jnp.float32
        ).reshape(group_rows, pair_width)
        grad_v_pair = jnp.einsum(
            "hqk,qhd->khd", prob_bf, gctx_block, preferred_element_type=jnp.float32
        ).reshape(group_rows, pair_width)
        grad_query = lax.dynamic_update_slice(grad_query, grad_q_block, (row_start, first_col))
        old_keys = lax.dynamic_slice(grad_keys, (0, first_col), (group_rows, pair_width))
        grad_keys = lax.dynamic_update_slice(grad_keys, old_keys + grad_k_pair, (0, first_col))
        old_values = lax.dynamic_slice(grad_values, (0, first_col), (group_rows, pair_width))
        grad_values = lax.dynamic_update_slice(
            grad_values, old_values + grad_v_pair, (0, first_col)
        )
        return (grad_query, grad_keys, grad_values)

    zero_grad = jnp.zeros((group_rows, head_cols), jnp.float32)
    return lax.fori_loop(0, pair_count * block_count, back_step, (zero_grad, zero_grad, zero_grad))


def on_device_plain(
    tokens,
    lengths,
    w_query,
    b_query,
    w_key,
    w_value,
    b_value,
    w_out,
    b_out,
    gain_attn,
    shift_attn,
    w_in,
    b_in,
    w_back,
    b_back,
    gain_ffn,
    shift_ffn,
    cotangent,
):
    tensor_size = lax.axis_size("tensor")
    tensor_index = lax.axis_index("tensor")
    local_rows = tokens.shape[0]
    group_rows = local_rows * tensor_size
    head_cols = w_query.shape[1]
    hidden_cols = w_in.shape[1]
    block_rows = min(512, group_rows)
    seq_lens = lengths[0]
    live_end = seq_lens[0] + seq_lens[1]
    positions = jnp.arange(group_rows, dtype=jnp.int32)
    seg_ids = (positions >= seq_lens[0]).astype(jnp.int32) + (positions >= live_end).astype(
        jnp.int32
    )
    local_pos = tensor_index * local_rows + jnp.arange(local_rows, dtype=jnp.int32)
    live_rows = (local_pos < live_end).astype(jnp.float32)[:, None]
    rows_full = lax.all_gather(tokens, "tensor", axis=0, tiled=True)
    attn_mats = (
        lax.all_gather(w_query, "dp", axis=0, tiled=True),
        lax.all_gather(w_key, "dp", axis=0, tiled=True),
        lax.all_gather(w_value, "dp", axis=0, tiled=True),
        lax.all_gather(w_out, "dp", axis=1, tiled=True),
    )
    mat_query, mat_key, mat_value, mat_out = attn_mats
    bias_query = lax.dynamic_slice_in_dim(b_query, tensor_index * head_cols, head_cols)
    bias_value = lax.dynamic_slice_in_dim(b_value, tensor_index * head_cols, head_cols)
    bias_in = lax.dynamic_slice_in_dim(b_in, tensor_index * hidden_cols, hidden_cols)
    query_rows = (matmul_plain(rows_full, mat_query) + bias_query).astype(jnp.bfloat16)
    key_rows = matmul_plain(rows_full, mat_key).astype(jnp.bfloat16)
    value_rows = (matmul_plain(rows_full, mat_value) + bias_value).astype(jnp.bfloat16)
    context, log_total = attend_forward(query_rows, key_rows, value_rows, seg_ids, HD, block_rows)
    attn_sum = lax.psum_scatter(
        matmul_plain(context, mat_out).astype(jnp.bfloat16),
        "tensor",
        scatter_dimension=0,
        tiled=True,
    ).astype(jnp.float32)
    resid_one = tokens.astype(jnp.float32) + attn_sum + b_out
    hidden_one, normed_one, inv_one = layer_norm(resid_one, gain_attn, shift_attn)
    hidden_bf = hidden_one.astype(jnp.bfloat16)
    hidden_full = lax.all_gather(hidden_bf, "tensor", axis=0, tiled=True)
    ffn_mats = (
        lax.all_gather(w_in, "dp", axis=0, tiled=True),
        lax.all_gather(w_back, "dp", axis=1, tiled=True),
    )
    mat_in, mat_back = ffn_mats
    preact = matmul_plain(hidden_full, mat_in) + bias_in
    activ_val, gelu_slope = gelu_parts(preact)
    activation = activ_val.astype(jnp.bfloat16)
    ffn_sum = lax.psum_scatter(
        matmul_plain(activation, mat_back).astype(jnp.bfloat16),
        "tensor",
        scatter_dimension=0,
        tiled=True,
    ).astype(jnp.float32)
    resid_two = hidden_one + ffn_sum + b_back
    normed_out, normed_two, inv_two = layer_norm(resid_two, gain_ffn, shift_ffn)
    output = (normed_out * live_rows).astype(jnp.bfloat16)
    grad_final = cotangent.astype(jnp.float32) * live_rows
    grad_gain_ffn = jnp.sum(grad_final * normed_two, axis=0)
    grad_shift_ffn = jnp.sum(grad_final, axis=0)
    grad_two = norm_back(grad_final, normed_two, inv_two, gain_ffn)
    grad_b_back = jnp.sum(grad_two, axis=0)
    mat_query, mat_key, mat_value, mat_out, mat_in, mat_back = (
        lax.all_gather(w_query, "dp", axis=0, tiled=True),
        lax.all_gather(w_key, "dp", axis=0, tiled=True),
        lax.all_gather(w_value, "dp", axis=0, tiled=True),
        lax.all_gather(w_out, "dp", axis=1, tiled=True),
        lax.all_gather(w_in, "dp", axis=0, tiled=True),
        lax.all_gather(w_back, "dp", axis=1, tiled=True),
    )
    grad_two_full = lax.all_gather(grad_two.astype(jnp.bfloat16), "tensor", axis=0, tiled=True)
    grad_w_back = matmul_over_rows(activation, grad_two_full)
    grad_pre = matmul_over_cols(grad_two_full, mat_back) * gelu_slope
    grad_b_in_part = jnp.sum(grad_pre, axis=0)
    grad_pre_bf = grad_pre.astype(jnp.bfloat16)
    grad_w_in = matmul_over_rows(hidden_full, grad_pre_bf)
    grad_one_out = grad_two + lax.psum_scatter(
        matmul_over_cols(grad_pre_bf, mat_in).astype(jnp.bfloat16),
        "tensor",
        scatter_dimension=0,
        tiled=True,
    ).astype(jnp.float32)
    grad_w_in, grad_w_back = (
        lax.psum_scatter(grad_w_in, "dp", scatter_dimension=0, tiled=True),
        lax.psum_scatter(grad_w_back, "dp", scatter_dimension=1, tiled=True),
    )
    grad_gain_attn = jnp.sum(grad_one_out * normed_one, axis=0)
    grad_shift_attn = jnp.sum(grad_one_out, axis=0)
    grad_one = norm_back(grad_one_out, normed_one, inv_one, gain_attn)
    grad_b_out = jnp.sum(grad_one, axis=0)
    grad_one_full = lax.all_gather(grad_one.astype(jnp.bfloat16), "tensor", axis=0, tiled=True)
    grad_w_out = matmul_over_rows(context, grad_one_full)
    grad_context = matmul_over_cols(grad_one_full, mat_out).astype(jnp.bfloat16)
    grad_query, grad_keys, grad_values = attend_backward(
        query_rows, key_rows, value_rows, context, grad_context, log_total, seg_ids, HD, block_rows
    )
    grad_b_query_part = jnp.sum(grad_query, axis=0)
    grad_b_value_part = jnp.sum(grad_values, axis=0)
    grad_query_bf = grad_query.astype(jnp.bfloat16)
    grad_keys_bf = grad_keys.astype(jnp.bfloat16)
    grad_values_bf = grad_values.astype(jnp.bfloat16)
    grad_w_query = matmul_over_rows(rows_full, grad_query_bf)
    grad_w_key = matmul_over_rows(rows_full, grad_keys_bf)
    grad_w_value = matmul_over_rows(rows_full, grad_values_bf)
    query_part = matmul_over_cols(grad_query_bf, mat_query)
    key_part = matmul_over_cols(grad_keys_bf, mat_key)
    value_part = matmul_over_cols(grad_values_bf, mat_value)
    grad_in = grad_one + lax.psum_scatter(
        (query_part + key_part + value_part).astype(jnp.bfloat16),
        "tensor",
        scatter_dimension=0,
        tiled=True,
    ).astype(jnp.float32)
    grad_w_query, grad_w_key, grad_w_value, grad_w_out = (
        lax.psum_scatter(grad_w_query, "dp", scatter_dimension=0, tiled=True),
        lax.psum_scatter(grad_w_key, "dp", scatter_dimension=0, tiled=True),
        lax.psum_scatter(grad_w_value, "dp", scatter_dimension=0, tiled=True),
        lax.psum_scatter(grad_w_out, "dp", scatter_dimension=1, tiled=True),
    )

    def widen(part_vec, full_width):
        return lax.dynamic_update_slice_in_dim(
            jnp.zeros((full_width,), jnp.float32), part_vec, tensor_index * part_vec.shape[0], 0
        )

    small_sums = lax.psum(
        (
            widen(grad_b_query_part, b_query.shape[0]),
            widen(grad_b_value_part, b_value.shape[0]),
            grad_b_out,
            grad_gain_attn,
            grad_shift_attn,
            widen(grad_b_in_part, b_in.shape[0]),
            grad_b_back,
            grad_gain_ffn,
            grad_shift_ffn,
        ),
        ("dp", "tensor"),
    )
    return (
        output,
        grad_in,
        grad_w_query,
        small_sums[0],
        grad_w_key,
        grad_w_value,
        small_sums[1],
        grad_w_out,
        small_sums[2],
        small_sums[3],
        small_sums[4],
        grad_w_in,
        small_sums[5],
        grad_w_back,
        small_sums[6],
        small_sums[7],
        small_sums[8],
    )


MESH_ID = pl.DeviceIdType.MESH
F32 = jnp.float32
BF16 = jnp.bfloat16

SLOTS = 4
BLOCK = 128
GROUP = 512
WIDTH = 1024
HEAD_COLS = 256
HIDDEN = 1024
N_SEND = 58
N_GOT = 110
HALF = BLOCK // 2
HALVES = dict(q=(128, 256), k=(128, 256), v=(128, 256), o=(256, 128), i0=(128, 512), i1=(128, 512), b0=(512, 128),
              b1=(512, 128))
VECTORS = dict(bq=1024, bv=1024, bo=1024, ga=1024, sa=1024, bi=4096, bb=1024, gf=1024, sf=1024)


def flip(bit):
    return 1 - bit


def slot_step(t, j):
    return (t % 2 + j % 2) % 2 + 2 * ((t // 2 + j // 2) % 2)


def rows_of(r, count=BLOCK):
    return pl.ds(pl.multiple_of(r * BLOCK, BLOCK), count)


def cols_of(n, count=256):
    return pl.ds(pl.multiple_of(n * count, count), count)


def dot_nn(a, b):
    return jnp.dot(a, b, preferred_element_type=F32)


def dot_nt(a, b):
    return lax.dot_general(a, b, (((1,), (1,)), ((), ())), preferred_element_type=F32)


def dot_tn(a, b):
    return lax.dot_general(a, b, (((0,), (0,)), ((), ())), preferred_element_type=F32)


def scratch_table():
    act = lambda n: pltpu.VMEM((GROUP, n), BF16)
    table = dict(
        w3=pltpu.VMEM((3 * WIDTH, HEAD_COLS), BF16),
        wo=pltpu.VMEM((4, HEAD_COLS, 256), BF16),
        wi=pltpu.VMEM((WIDTH, HIDDEN), BF16),
        wb=pltpu.VMEM((4, HIDDEN, 256), BF16),
        w3t=pltpu.VMEM((3, HEAD_COLS, WIDTH), BF16),
        wot=pltpu.VMEM((WIDTH, HEAD_COLS), BF16),
        wit=pltpu.VMEM((HIDDEN, WIDTH), BF16),
        wbt=pltpu.VMEM((WIDTH, HIDDEN), BF16),
        lens_own=pltpu.VMEM((2, 8, 128), F32),
        lens_got=pltpu.VMEM((2, 8, 128), F32),
        lens_use=pltpu.VMEM((2, 8, 128), F32),
        tk=act(WIDTH),
        tkt=pltpu.VMEM((WIDTH, GROUP), BF16),
        cot_own=pltpu.VMEM((BLOCK, WIDTH), BF16),
        bias=pltpu.VMEM((GROUP, GROUP), F32),
        q=act(HEAD_COLS),
        qt=pltpu.VMEM((HEAD_COLS, GROUP), BF16),
        k=act(HEAD_COLS),
        ks=act(HEAD_COLS),
        v=act(HEAD_COLS),
        ps=pltpu.VMEM((4, GROUP, GROUP), BF16),
        ctx=act(HEAD_COLS),
        ctxt=pltpu.VMEM((HEAD_COLS, GROUP), BF16),
        hid=act(WIDTH),
        hidt=pltpu.VMEM((WIDTH, GROUP), BF16),
        act=act(HIDDEN),
        actt=pltpu.VMEM((HIDDEN, GROUP), BF16),
        slope=pltpu.VMEM((GROUP, HIDDEN), F32),
        g2=act(WIDTH),
        gpre=act(HIDDEN),
        g1=act(WIDTH),
        gctxt=pltpu.VMEM((HEAD_COLS, GROUP), BF16),
        dq=act(HEAD_COLS),
        dkt=pltpu.VMEM((HEAD_COLS, GROUP), F32),
        dvt=pltpu.VMEM((HEAD_COLS, GROUP), F32),
        dk=act(HEAD_COLS),
        dv=act(HEAD_COLS),
        hid1=pltpu.VMEM((BLOCK, WIDTH), F32),
        normed1=pltpu.VMEM((BLOCK, WIDTH), F32),
        inv1=pltpu.VMEM((BLOCK, 128), F32),
        g2f=pltpu.VMEM((BLOCK, WIDTH), F32),
        g1f=pltpu.VMEM((BLOCK, WIDTH), F32),
        out_own=pltpu.VMEM((BLOCK, WIDTH), BF16),
        gtok_own=pltpu.VMEM((BLOCK, WIDTH), BF16),
        rs_own=pltpu.VMEM((4, BLOCK, WIDTH), BF16),
        rs_out=pltpu.VMEM((4, 3, BLOCK, WIDTH), BF16),
        rs_got=pltpu.VMEM((4, 3, BLOCK, WIDTH), BF16),
        sums=pltpu.VMEM((6, 16, WIDTH), F32),
        sums_got=pltpu.VMEM((5, 16, WIDTH), F32),
        gb_in=pltpu.VMEM((1, HIDDEN), F32),
        vectors={name: pltpu.VMEM((1, width), F32) for name, width in VECTORS.items()},
        vsem=pltpu.SemaphoreType.DMA((len(VECTORS),)),
        turn=pltpu.SemaphoreType.REGULAR((5,)),
        g3=pltpu.VMEM((3 * WIDTH, HEAD_COLS), BF16),
        go=pltpu.VMEM((4, HEAD_COLS, 256), BF16),
        gi=pltpu.VMEM((WIDTH, HIDDEN), BF16),
        gb=pltpu.VMEM((4, HIDDEN, 256), BF16),
        stage={},
        ssem=pltpu.SemaphoreType.DMA((N_SEND,)),
        rsem=pltpu.SemaphoreType.DMA((N_GOT,)),
    )
    for name, dims in HALVES.items():
        table["stage"][name] = pltpu.VMEM((10,) + dims, BF16)
    return table


def layer_kernel(tok, lens, wq, bq, wk, wv, bv, wo, bo, ga, sa, wi, bi, wb, bb, gf, sf, cot, out, gtok, sums, zq, zk, zv,
                 zo, zi0, zi1, zb0, zb1, *scratch):
    a = SimpleNamespace(tok=tok, lens=lens, wq=wq, bq=bq, wk=wk, wv=wv, bv=bv, wo=wo, bo=bo, ga=ga, sa=sa, wi=wi, bi=bi,
                        wb=wb, bb=bb, gf=gf, sf=sf, cot=cot)
    o = SimpleNamespace(out=out, gtok=gtok, sums=sums)
    landed = dict(q=zq, k=zk, v=zv, o=zo, i0=zi0, i1=zi1, b0=zb0, b1=zb1)
    s = SimpleNamespace(**jax.tree.unflatten(jax.tree.structure(scratch_table()), scratch))
    ssem, rsem, vsem, vectors = s.ssem, s.rsem, s.vsem, s.vectors

    dp = lax.axis_index("dp")
    z = lax.axis_index("tensor")
    b, c = dp // 2, dp % 2
    zl, zh = z % 2, z // 2
    t = zl * 2 + c
    sl = (z + 2 * c) % 4
    here, away = c == 0, c == 1
    bx = b + 1 - 2 * (b % 2)
    by = (b + 2) % 4
    bd = 3 - b
    t1, t2, t3 = slot_step(t, 1), slot_step(t, 2), slot_step(t, 3)

    def dev(pos, core, zz):
        return (pos * 2 + core, zz)

    partner = dev(b, flip(c), z)
    z_near = z + 1 - 2 * (z % 2)
    z_far = (z + 2) % 4
    pair = dev(b, c, z_near)
    across = dev(b, c, z_far)
    is_inner = jnp.logical_and(z >= 1, z <= 2)
    inner_away = jnp.logical_and(is_inner, away)
    outer_away = jnp.logical_and(jnp.logical_not(is_inner), away)
    x_near = dev(bx, c, z)
    y_near = dev(by, c, z)

    taken = {"s": 0, "r": 0}

    def take(kind, count=1):
        first = taken[kind]
        taken[kind] = first + count
        assert taken[kind] <= (N_SEND if kind == "s" else N_GOT)
        return first

    to_drain = []

    def make_copy(src, dst, device, sk, rk):
        return pltpu.make_async_remote_copy(
            src_ref=src, dst_ref=dst, send_sem=ssem.at[sk], recv_sem=rsem.at[rk], device_id=device,
            device_id_type=MESH_ID)

    def send(src, dst, device, sk, rk):
        make_copy(src, dst, device, sk, rk).start()

    def got(dst, rk):
        pltpu.make_async_copy(dst, dst, rsem.at[rk]).wait()

    def left(size_of, sk):
        pltpu.make_async_copy(size_of, size_of, ssem.at[sk]).wait()

    def at_end(size_of, sk, skipped=None, instead=None):
        to_drain.append((size_of, sk, skipped, instead))

    def send_or_keep(src, dst, device, is_self, sk, rk):
        copy = make_copy(src, dst, device, sk, rk)

        @pl.when(is_self)
        def _():
            pltpu.make_async_copy(src, dst, rsem.at[rk]).start()

        @pl.when(jnp.logical_not(is_self))
        def _():
            copy.start()

    barrier = pltpu.get_barrier_semaphore()
    peers = [x_near, y_near]
    for dz in range(4):
        for dc in range(2):
            if dz or dc:
                peers.append(dev(b, (c + dc) % 2, (z + dz) % 4))
    for peer in peers:
        pl.semaphore_signal(barrier, inc=1, device_id=peer, device_id_type=MESH_ID)
    pl.semaphore_wait(barrier, len(peers))

    def piece_qkv(m, home):
        base = m * WIDTH
        return SimpleNamespace(
            home=home,
            own=lambda bb, cc: s.w3.at[pl.ds(pl.multiple_of(base + bb * 256 + cc * 128, 128), 128), :],
            block=lambda bb: s.w3.at[pl.ds(pl.multiple_of(base + bb * 256, 256), 256), :],
            half=lambda bb, h: s.w3.at[pl.ds(pl.multiple_of(base + bb * 256 + h * 128, 128), 128), :])

    piece_o = SimpleNamespace(
        home=a.wo,
        own=lambda bb, cc: s.wo.at[bb, :, pl.ds(pl.multiple_of(cc * 128, 128), 128)],
        block=lambda bb: s.wo.at[bb],
        half=lambda bb, h: s.wo.at[bb, pl.ds(h * 128, 128), :])

    def piece_in(j):
        cols = pl.ds(j * 512, 512)
        return SimpleNamespace(
            home=a.wi.at[:, cols],
            own=lambda bb, cc: s.wi.at[pl.ds(pl.multiple_of(bb * 256 + cc * 128, 128), 128), cols],
            block=lambda bb: s.wi.at[pl.ds(pl.multiple_of(bb * 256, 256), 256), cols],
            half=lambda bb, h: s.wi.at[pl.ds(pl.multiple_of(bb * 256 + h * 128, 128), 128), cols])

    def piece_back(j):
        part = pl.ds(j * 512, 512)
        return SimpleNamespace(
            home=a.wb.at[part, :],
            own=lambda bb, cc: s.wb.at[bb, part, pl.ds(pl.multiple_of(cc * 128, 128), 128)],
            block=lambda bb: s.wb.at[bb, part, :],
            half=lambda bb, h: s.wb.at[bb, pl.ds(j * 512 + h * 256, 256), :])

    pieces = dict(q=piece_qkv(0, a.wq), k=piece_qkv(1, a.wk), v=piece_qkv(2, a.wv), o=piece_o,
                  i0=piece_in(0), i1=piece_in(1), b0=piece_back(0), b1=piece_back(1))
    first_size = dict(
        q=s.w3.at[0:768, :], k=s.w3.at[0:768, :], v=s.w3.at[0:768, :], o=s.wo.at[0:3], i0=s.wi.at[0:768, 0:512],
        i1=s.wi.at[0:768, 0:512], b0=s.wb.at[0:3, 0:512, :], b1=s.wb.at[0:3, 0:512, :])
    for name, piece in pieces.items():
        piece.s1, piece.r1 = take("s"), take("r")
        piece.s2, piece.r2 = take("s"), take("r", 3)
        at_end(piece.block(b), piece.s1, here, piece.own(b, 0))
        at_end(first_size[name], piece.s2)

    def to_local(name):
        piece = pieces[name]
        send_or_keep(piece.home, piece.own(b, c), dev(b, 0, z), here, piece.s1, piece.r1)

    def to_across(name):
        piece = pieces[name]
        send(piece.home, piece.own(b, c), dev(b, 1, z_far), piece.s1, piece.r1)

    def over_plane(name):
        piece = pieces[name]
        got(piece.block(b), piece.r1)
        send(piece.block(b), piece.block(b), x_near, piece.s2, piece.r2)
        send(piece.block(b), piece.block(b), y_near, piece.s2, piece.r2 + 1)

    def relay(name):
        piece = pieces[name]
        got(piece.block(bx), piece.r2)
        send(piece.half(bx, 0), piece.half(bx, 0), y_near, piece.s2, piece.r2 + 2)
        got(piece.block(by), piece.r2 + 1)
        send(piece.half(by, 1), piece.half(by, 1), x_near, piece.s2, piece.r2 + 2)

    def over_plane_now(names, chosen, relays=()):
        @pl.when(chosen)
        def _():
            for name in relays:
                relay(name)
            for name in names:
                over_plane(name)

    def arrived(name):
        piece = pieces[name]
        got(piece.block(bd), piece.r2 + 2)

    tok_s, tok_r = take("s", 2), take("r", 4)
    fwd_s = take("s", 6)
    lens_s, lens_r = take("s"), take("r")
    cot_s, cot_r = take("s"), take("r")

    def send_lens():
        first = a.lens[0, 0].astype(F32)
        s.lens_own[0] = jnp.full((8, 128), first, F32)
        s.lens_own[1] = jnp.full((8, 128), first + a.lens[0, 1].astype(F32), F32)
        send(s.lens_own, s.lens_got, partner, lens_s, lens_r)
        at_end(s.lens_own, lens_s)

    def take_lens():
        got(s.lens_got, lens_r)

        @pl.when(c == zh)
        def _():
            s.lens_use[...] = s.lens_own[...]

        @pl.when(c != zh)
        def _():
            s.lens_use[...] = s.lens_got[...]

    def tok_block(r):
        return s.tk.at[rows_of(r), :]

    inner, outer = 1 + c, 3 * c
    is_relay = jnp.logical_and(c == zh, z == inner)

    def send_tokens():
        near = z // 2 == c
        first = jnp.where(near, 2 * c, inner)
        send_or_keep(a.tok, tok_block(z), dev(b, c, first), first == z, tok_s, tok_r + z)
        at_end(tok_block(z), tok_s, first == z)
        second = make_copy(a.tok, tok_block(z), dev(b, c, 2 * c + 1), tok_s + 1, tok_r + z)
        keep = jnp.logical_and(near, z == 2 * c + 1)
        go = jnp.logical_and(near, z != 2 * c + 1)

        @pl.when(keep)
        def _():
            pltpu.make_async_copy(a.tok, tok_block(z), rsem.at[tok_r + z]).start()

        @pl.when(go)
        def _():
            second.start()

        at_end(tok_block(z), tok_s + 1, jnp.logical_not(go))

    def pass_on(half, far):
        for k in range(2):
            r = half * 2 + k
            block = tok_block(r)
            got(block, tok_r + r)
            if far:
                on = make_copy(block, block, dev(b, c, outer), fwd_s + k, tok_r + r)

                @pl.when(is_relay)
                def _():
                    on.start()
            copy = make_copy(block, block, partner, fwd_s + 2 + 2 * far + k, tok_r + r)

            @pl.when(c == zh)
            def _():
                copy.start()

    for k in range(6):
        at_end(s.tk.at[0:BLOCK, :], fwd_s + k, jnp.logical_not(is_relay) if k < 2 else c != zh)

    def send_cotangent():
        zt, ct = 2 * c + z // 2, z % 2
        is_self = jnp.logical_and(zt == z, ct == c)
        send_or_keep(a.cot, s.cot_own, dev(b, ct, zt), is_self, cot_s, cot_r)
        at_end(s.cot_own, cot_s, is_self)

    gather_s, gather_r = take("s", 3), take("r", 12)
    scatter_s, scatter_r = take("s", 4), take("r", 20)
    for k in range(3):
        at_end(s.tk.at[0:3 * BLOCK, :], gather_s + k)
    for k in range(4):
        at_end(s.tk.at[0:3 * BLOCK, :], scatter_s + k)

    def block_at(full, r):
        return full.at[rows_of(r), :]

    def half_at(full, r, k):
        return full.at[pl.ds(pl.multiple_of(r * BLOCK + k * HALF, HALF), HALF), :]

    def gather_start(which, full, k):
        mine = half_at(full, t, k)
        send(mine, mine, pair, gather_s + which, gather_r + 4 * which + 1 + k)
        send(mine, mine, partner, gather_s + which, gather_r + 4 * which)

    def gather_step(which, full, j):
        base = gather_r + 4 * which

        @pl.when(j == 1)
        def _():
            got(block_at(full, t1), base)

        @pl.when(j == 2)
        def _():
            if which == 0:
                over_plane_now((), away, relays=("b0",))
            for k in range(2):
                near = half_at(full, t2, k)
                got(near, base + 1 + k)
                send(near, near, partner, gather_s + which, base + 3)

        @pl.when(j == 3)
        def _():
            if which == 0:
                over_plane_now((), away, relays=("b1",))
            got(block_at(full, t3), base + 3)

    halves = [pl.ds(k * HALF, HALF) for k in range(2)]

    def scatter(which, part):
        out, back = s.rs_out, s.rs_got
        ss, rr = scatter_s + which, scatter_r + 5 * which
        part(t3 * BLOCK, BLOCK, out.at[which, 0])
        send(out.at[which, 0], back.at[which, 0], partner, ss, rr)
        part(t2 * BLOCK, BLOCK, out.at[which, 1])
        got(back.at[which, 0], rr)
        for k in range(2):
            rows = halves[k]
            total = out[which, 1, rows, :].astype(F32) + back[which, 0, rows, :].astype(F32)
            out[which, 1, rows, :] = total.astype(BF16)
            send(out.at[which, 1, rows, :], back.at[which, 1, rows, :], pair, ss, rr + 2 + k)
        part(t1 * BLOCK, BLOCK, out.at[which, 2])
        send(out.at[which, 2], back.at[which, 2], partner, ss, rr + 4)
        part(t * BLOCK, BLOCK, s.rs_own.at[which])

    def scatter_cols(which, blocks, k):
        out, back = s.rs_out, s.rs_got
        ss, rr = scatter_s + which, scatter_r + 5 * which
        slots = [pl.ds(pl.multiple_of(block * 256, 256), 256) for block in blocks]
        size = s.rs_got.at[which, 0, :, 0:256 * len(blocks)]

        def product(row, block):
            rows = pl.ds(pl.multiple_of(row * BLOCK, BLOCK), BLOCK)
            return dot_nn(s.act[rows, :], s.wb[block])

        def cast(row, slot):
            for block, cols in zip(blocks, slots):
                out[which, slot, :, cols] = product(row, block).astype(BF16)

        cast(t3, 0)
        for cols in slots:
            send(out.at[which, 0, :, cols], back.at[which, 0, :, cols], partner, ss, rr + k)
        cast(t1, 2)
        for cols in slots:
            send(out.at[which, 2, :, cols], back.at[which, 2, :, cols], partner, ss, rr + 4)
        got(size, rr + k)
        for block, cols in zip(blocks, slots):
            total = product(t2, block).astype(BF16).astype(F32) + back[which, 0, :, cols].astype(F32)
            out[which, 1, :, cols] = total.astype(BF16)
            send(out.at[which, 1, :, cols], back.at[which, 1, :, cols], pair, ss, rr + 2)
        for block, cols in zip(blocks, slots):
            s.rs_own[which, :, cols] = product(t, block).astype(BF16)

    def scatter_cols_wait(which):
        rr = scatter_r + 5 * which
        got(s.rs_got.at[which, 2], rr + 4)
        got(s.rs_got.at[which, 1], rr + 2)

    def scatter_wait(which, k):
        rr = scatter_r + 5 * which
        if k == 0:
            got(s.rs_got.at[which, 2], rr + 4)
        got(s.rs_got.at[which, 1, halves[k], :], rr + 2 + k)

    def scatter_rows(which, chunk):
        total = s.rs_own[which, chunk, :].astype(F32) + s.rs_got[which, 2, chunk, :].astype(F32)
        return total + s.rs_got[which, 1, chunk, :].astype(F32)

    def by_halves(which, body, after):
        if which == 1:
            scatter_cols_wait(which)
        for k in range(2):
            if which != 1:
                scatter_wait(which, k)
            loop(2, lambda i: body(2 * k + i))
            after(k)

    def put_part(dst, n, value):
        dst[:, 256 * n:256 * n + 256] = value.astype(BF16)

    def loop(count, body):
        lax.fori_loop(0, count, lambda i, _: (body(i), 0)[1], 0)

    def grad_qkv(m):
        base = m * WIDTH
        return lambda bb, h: s.g3.at[pl.ds(pl.multiple_of(base + bb * 256 + h * 128, 128), 128), :]

    def grad_in_part(k):
        cols = pl.ds(k * 512, 512)
        return lambda bb, h: s.gi.at[pl.ds(pl.multiple_of(bb * 256 + h * 128, 128), 128), cols]

    def grad_back_part(k):
        part = pl.ds(k * 512, 512)
        return lambda bb, h: s.gb.at[bb, part, pl.ds(h * 128, 128)]

    grad_half = dict(
        q=grad_qkv(0), k=grad_qkv(1), v=grad_qkv(2), o=lambda bb, h: s.go.at[bb, :, pl.ds(h * 128, 128)],
        i0=grad_in_part(0), i1=grad_in_part(1), b0=grad_back_part(0), b1=grad_back_part(1))
    grad_s = {name: take("s", 2) for name in grad_half}
    grad_r = {name: take("r", 4) for name in grad_half}
    for name in grad_half:
        at_end(s.stage[name].at[0:6], grad_s[name])
        at_end(s.stage[name].at[0:2], grad_s[name] + 1, here, s.stage[name].at[0])

    def chunks(name, body):
        size = 64 if name in ("i0", "i1") else 128
        count = HALVES[name][0] // size
        loop(count, lambda i: body(pl.ds(pl.multiple_of(i * size, size), size)))

    def grad_first(name, part=2):
        half, ss, rr, st = grad_half[name], grad_s[name], grad_r[name], s.stage[name]
        if part in (0, 2):
            send(half(bd, 0), st.at[1], x_near, ss, rr)
            send(half(bd, 1), st.at[3], y_near, ss, rr + 1)
        if part == 0:
            return
        send(half(bx, 0), st.at[0], x_near, ss, rr + 2)
        send(half(by, 1), st.at[2], y_near, ss, rr + 2)

    def grad_second(name):
        half, ss, rr, st = grad_half[name], grad_s[name], grad_r[name], s.stage[name]
        for h, block, to in ((0, by, y_near), (1, bx, x_near)):
            got(st.at[1 + 2 * h], rr + h)
            mine = half(block, h)

            def add(ch):
                st[4 + h, ch, :] = (mine[ch, :].astype(F32) + st[1 + 2 * h, ch, :].astype(F32)).astype(BF16)
            chunks(name, add)
            send(st.at[4 + h], st.at[6 + h], to, ss, rr + 2)

    def grad_third(name):
        half, ss, rr, st = grad_half[name], grad_s[name], grad_r[name], s.stage[name]
        zr = landed[name]
        got(st.at[0:4], rr + 2)
        for h in range(2):
            mine = half(b, h)

            def add_all(ch):
                total = mine[ch, :].astype(F32) + st[2 * h, ch, :].astype(F32) + st[6 + h, ch, :].astype(F32)
                st[8 + h, ch, :] = total.astype(BF16)
            chunks(name, add_all)
            is_self = here if h == 0 else c < 0
            send_or_keep(st.at[8 + h], zr.at[zh], dev(b, h, sl), is_self, ss + 1, rr + 3)

    def grad_final(name):
        got(landed[name], grad_r[name] + 3)

    to_across("q")
    to_across("k")
    send_tokens()
    to_across("v")
    for name in pieces:
        to_local(name)
    send_lens()
    for name, ref in vectors.items():
        pltpu.make_async_copy(getattr(a, name), ref, vsem.at[list(vectors).index(name)]).start()
    s.sums[0] = jnp.zeros((16, WIDTH), F32)
    s.gb_in[...] = jnp.zeros((1, HIDDEN), F32)
    leads = jnp.logical_and(is_inner, away)

    def in_turn(k, inner_next, outer_next):
        @pl.when(leads)
        def _():
            for device in (partner, pair, dev(b, 0, z_near)):
                pl.semaphore_signal(s.turn.at[k], inc=1, device_id=device, device_id_type=MESH_ID)

        @pl.when(jnp.logical_not(leads))
        def _():
            pl.semaphore_wait(s.turn.at[k], 1)

        for chosen, names in ((is_inner, inner_next), (jnp.logical_not(is_inner), outer_next)):
            if names:
                @pl.when(chosen)
                def _():
                    for name in names:
                        to_across(name)

    over_plane_now(("q", "k", "v", "o"), here)
    over_plane_now(("q", "k"), away)
    relay("q")
    over_plane_now(("i0",), here, relays=("k", "v"))
    pass_on(zh, 0)
    to_across("o")

    @pl.when(is_inner)
    def _():
        pass_on(flip(zh), 1)

    in_turn(0, (), ("i0",))
    take_lens()

    def make_bias(r):
        first, end = s.lens_use[0][0:1, 0:1], s.lens_use[1][0:1, 0:1]
        row = (lax.broadcasted_iota(jnp.int32, (BLOCK, GROUP), 0) + r * BLOCK).astype(F32)
        col = lax.broadcasted_iota(jnp.int32, (BLOCK, GROUP), 1).astype(F32)
        seg = lambda p: jnp.where(p >= end, 2.0, jnp.where(p >= first, 1.0, 0.0))
        s.bias[rows_of(r), :] = jnp.where(seg(row) == seg(col), 0.0, masked_value)
    loop(SLOTS, make_bias)
    for name, ref in vectors.items():
        pltpu.make_async_copy(getattr(a, name), ref, vsem.at[list(vectors).index(name)]).wait()
        setattr(a, name, ref)
    over_plane_now(("v", "o"), away, relays=("k",))
    over_plane_now(("i1",), here, relays=("o",))
    over_plane_now((), away, relays=("v",))
    over_plane_now(("b0",), here, relays=("i0",))
    in_turn(1, ("i0", "i1"), ("i1",))

    @pl.when(jnp.logical_not(is_inner))
    def _():
        pass_on(flip(zh), 1)


    def turn_tokens(r):
        s.tkt[:, rows_of(r)] = s.tk[rows_of(r), :].T
    loop(SLOTS, turn_tokens)

    head_cols = pl.ds(pl.multiple_of(sl * HEAD_COLS, HEAD_COLS), HEAD_COLS)

    def project(m):
        acc = dot_nn(s.tk[...], s.w3[m * WIDTH:(m + 1) * WIDTH, :])
        if m == 0:
            value = (acc + a.bq[:, head_cols]).astype(BF16)
            scaled = (value.astype(F32) * 0.125).astype(BF16)
            s.q[...] = scaled
            s.qt[...] = scaled.T
        elif m == 1:
            value = acc.astype(BF16)
            s.k[...] = value
            s.ks[...] = (value.astype(F32) * 0.125).astype(BF16)
        else:
            s.v[...] = (acc + a.bv[:, head_cols]).astype(BF16)

    arrived("q")
    project(0)
    arrived("k")
    project(1)
    in_turn(2, ("b0", "b1"), ())
    arrived("v")
    project(2)

    def attend():
        parts = []
        for h in range(4):
            cols = slice(64 * h, 64 * h + 64)
            scores = dot_nt(s.q[:, cols], s.k[:, cols]) + s.bias[...]
            top = jnp.max(scores, axis=-1, keepdims=True)
            weight = jnp.exp(scores - top)
            total = jnp.sum(weight, axis=-1, keepdims=True)
            prob = (weight * (1.0 / total)).astype(BF16)
            s.ps[h] = prob
            parts.append(dot_nn(prob, s.v[:, cols]))
        context = jnp.concatenate(parts, axis=1).astype(BF16)
        s.ctx[...] = context
        s.ctxt[...] = context.T
    over_plane_now((), away, relays=("o",))
    over_plane_now(("i0",), inner_away)
    over_plane_now(("b1",), here, relays=("i1",))
    attend()
    @pl.when(jnp.logical_not(is_inner))
    def _():
        to_across("b0")

    over_plane_now(("i0",), outer_away)
    over_plane_now(("i1",), inner_away)
    arrived("o")

    def attn_part(first, count, dst):
        rows = s.ctx[pl.ds(pl.multiple_of(first, HALF), count), :]
        for n in range(4):
            put_part(dst, n, dot_nn(rows, s.wo[n]))
    scatter(0, attn_part)
    @pl.when(jnp.logical_not(is_inner))
    def _():
        to_across("b1")

    for m in range(3):
        for n in range(4):
            s.w3t[m, :, 256 * n:256 * n + 256] = s.w3[m * WIDTH + 256 * n:m * WIDTH + 256 * n + 256, :].T
    for n in range(4):
        s.wot[256 * n:256 * n + 256, :] = s.wo[n].T

    CH = 32

    def own_chunk(i):
        return pl.ds(pl.multiple_of(i * CH, CH), CH)

    def group_chunk(i):
        return pl.ds(pl.multiple_of(t * BLOCK + i * CH, CH), CH)

    def norm_one(i):
        ch = own_chunk(i)
        resid = s.tk[group_chunk(i), :].astype(F32) + scatter_rows(0, ch) + a.bo[...]
        centered = resid - jnp.mean(resid, axis=-1, keepdims=True)
        inv = lax.rsqrt(jnp.mean(centered * centered, axis=-1, keepdims=True) + epsilon)
        normed = centered * inv
        hidden = normed * a.ga[...] + a.sa[...]
        s.normed1[ch, :] = normed
        s.inv1[ch, :] = jnp.broadcast_to(inv, (CH, 128))
        s.hid1[ch, :] = hidden
        s.hid[group_chunk(i), :] = hidden.astype(BF16)
    over_plane_now((), here, relays=("b0",))
    over_plane_now((), inner_away, relays=("i0",))
    over_plane_now(("i1", "b0"), outer_away, relays=("i0",))
    by_halves(0, norm_one, lambda k: gather_start(0, s.hid, k))
    over_plane_now((), here, relays=("b1",))
    over_plane_now((), inner_away, relays=("i1",))
    over_plane_now(("b1",), outer_away, relays=("i1",))
    over_plane_now(("b0", "b1"), inner_away)
    send_cotangent()
    arrived("i0")
    arrived("i1")

    def ffn_in(j):
        gather_step(0, s.hid, j)
        r = slot_step(t, j)
        rows = rows_of(r)
        for n in range(4):
            cols = slice(256 * n, 256 * n + 256)
            bias = a.bi[:, pl.ds(pl.multiple_of(sl * HIDDEN + n * 256, 256), 256)]
            pre = dot_nn(s.hid[rows, :], s.wi[:, cols]) + bias
            cdf = 0.5 * (1.0 + lax.erf(pre * 0.7071067811865476))
            pdf = jnp.exp(-0.5 * pre * pre) * 0.3989422804014327
            s.act[rows, cols] = (pre * cdf).astype(BF16)
            s.slope[rows, cols] = cdf + pre * pdf
    loop(SLOTS, ffn_in)

    def turn_ffn(r):
        rows = rows_of(r)
        s.actt[:, rows] = s.act[rows, :].T
        s.hidt[:, rows] = s.hid[rows, :].T
    scatter_cols(1, (b, bx, by), 0)
    arrived("b0")
    arrived("b1")
    scatter_cols(1, (bd,), 1)
    loop(SLOTS, turn_ffn)

    def turn_wi(r):
        rows = rows_of(r)
        s.wit[:, rows] = s.wi[rows, :].T
    loop(8, turn_wi)

    def turn_wb(r):
        rows = rows_of(r)
        for n in range(4):
            s.wbt[256 * n:256 * n + 256, rows] = s.wb[n, rows, :].T
    loop(8, turn_wb)
    got(s.cot_own, cot_r)

    def add_rows(row, value):
        s.sums[0, row:row + 1, :] += jnp.sum(value, axis=0, keepdims=True)

    def norm_two(i):
        ch = own_chunk(i)
        resid = s.hid1[ch, :] + scatter_rows(1, ch) + a.bb[...]
        centered = resid - jnp.mean(resid, axis=-1, keepdims=True)
        inv = lax.rsqrt(jnp.mean(centered * centered, axis=-1, keepdims=True) + epsilon)
        normed = centered * inv
        position = lax.broadcasted_iota(jnp.int32, (CH, 128), 0) + (t * BLOCK + i * CH)
        live = jnp.where(position.astype(F32) < s.lens_use[1][0:1, :], 1.0, 0.0)[:, 0:1]
        s.out_own[ch, :] = ((normed * a.gf[...] + a.sf[...]) * live).astype(BF16)
        grad = s.cot_own[ch, :].astype(F32) * live
        add_rows(4, grad * normed)
        add_rows(5, grad)
        u = grad * a.gf[...]
        first = jnp.mean(u, axis=-1, keepdims=True)
        second = jnp.mean(u * normed, axis=-1, keepdims=True)
        grad_two = inv * (u - first - normed * second)
        add_rows(3, grad_two)
        s.g2f[ch, :] = grad_two
        s.g2[group_chunk(i), :] = grad_two.astype(BF16)
    by_halves(1, norm_two, lambda k: gather_start(1, s.g2, k))
    out_s, out_r = take("s"), take("r")
    home_self = jnp.logical_and(zh == c, t == z)

    def ffn_back(j):
        @pl.when(j < 3)
        def _():
            gather_step(1, s.g2, j)
        r = slot_step(t, j)
        rows = rows_of(r)
        for n in range(4):
            cols = slice(256 * n, 256 * n + 256)
            grad = dot_nn(s.g2[rows, :], s.wbt[:, cols]) * s.slope[rows, cols]
            s.gb_in[:, cols] += jnp.sum(grad, axis=0, keepdims=True)
            s.gpre[rows, cols] = grad.astype(BF16)
    loop(SLOTS - 1, ffn_back)

    def grad_back(k):
        part = slice(512 * k, 512 * k + 512)

        def body(n):
            for e in range(2):
                block = n * 2 + e
                s.gb[block, part, :] = dot_nn(s.actt[part, :], s.g2[:, cols_of(block)]).astype(BF16)
        loop(2, body)

    def grad_in(k):
        cols = slice(512 * k, 512 * k + 512)

        def body(m):
            part = rows_of(m * 4, 512)
            s.gi[part, cols] = dot_nn(s.hidt[part, :], s.gpre[:, cols]).astype(BF16)
        loop(2, body)

    gather_step(1, s.g2, 3)
    grad_back(0)
    grad_first("b0")
    ffn_back(3)
    grad_back(1)
    grad_first("b1", 0)
    send_or_keep(s.out_own, o.out, dev(b, zh, t), home_self, out_s, out_r)
    at_end(s.out_own, out_s, home_self)

    def in_part(first, count, dst):
        rows = pl.ds(pl.multiple_of(first, HALF), count)
        for n in range(4):
            put_part(dst, n, dot_nn(s.gpre[rows, :], s.wit[:, 256 * n:256 * n + 256]))
    scatter(2, in_part)
    grad_in(0)
    grad_in(1)
    grad_second("b0")
    grad_first("b1", 1)
    grad_second("b1")
    grad_first("i0", 0)

    def norm_one_back(i):
        ch = own_chunk(i)
        grad = s.g2f[ch, :] + scatter_rows(2, ch)
        normed = s.normed1[ch, :]
        add_rows(1, grad * normed)
        add_rows(2, grad)
        u = grad * a.ga[...]
        first = jnp.mean(u, axis=-1, keepdims=True)
        second = jnp.mean(u * normed, axis=-1, keepdims=True)
        grad_one = s.inv1[ch, 0:1] * (u - first - normed * second)
        add_rows(0, grad_one)
        s.g1f[ch, :] = grad_one
        s.g1[group_chunk(i), :] = grad_one.astype(BF16)
    by_halves(2, norm_one_back, lambda k: gather_start(2, s.g1, k))
    grad_first("i0", 1)
    grad_third("b0")

    def attend_back(chip, add):
        rows = pl.ds(pl.multiple_of(chip * 2 * BLOCK, 2 * BLOCK), 2 * BLOCK)
        grad_ctx = dot_nn(s.g1[rows, :], s.wot[...]).astype(BF16)
        s.gctxt[:, rows] = grad_ctx.T
        product = grad_ctx.astype(F32) * s.ctx[rows, :].astype(F32)
        parts = []
        for h in range(4):
            cols = slice(64 * h, 64 * h + 64)
            prob = s.ps[h, rows, :]
            delta = jnp.sum(product[:, cols], axis=-1, keepdims=True)
            grad_prob = dot_nt(grad_ctx[:, cols], s.v[:, cols])
            grad_score = (prob.astype(F32) * (grad_prob - delta)).astype(BF16)
            parts.append(dot_nn(grad_score, s.ks[:, cols]))
            grad_key = dot_nn(s.qt[cols, rows], grad_score)
            grad_value = dot_nn(s.gctxt[cols, rows], prob)
            if add:
                grad_key, grad_value = s.dkt[cols, :] + grad_key, s.dvt[cols, :] + grad_value
            s.dkt[cols, :] = grad_key
            s.dvt[cols, :] = grad_value
        grad_query = jnp.concatenate(parts, axis=1)
        for k in range(4):
            @pl.when(sl == k)
            def _():
                s.sums[0, 6:7, 256 * k:256 * k + 256] += jnp.sum(grad_query, axis=0, keepdims=True)
        s.dq[rows, :] = grad_query.astype(BF16)
    gather_step(2, s.g1, 1)
    attend_back(zl, False)
    grad_third("b1")
    gather_step(2, s.g1, 2)
    gather_step(2, s.g1, 3)
    attend_back(flip(zl), True)
    grad_second("i0")
    grad_first("i1")
    s.dk[...] = s.dkt[...].T.astype(BF16)
    grad_value = s.dvt[...].T
    for k in range(4):
        @pl.when(sl == k)
        def _():
            s.sums[0, 7:8, 256 * k:256 * k + 256] += jnp.sum(grad_value, axis=0, keepdims=True)
    s.dv[...] = grad_value.astype(BF16)
    for k in range(4):
        @pl.when(sl == k)
        def _():
            s.sums[0, 8 + k:9 + k, :] = s.gb_in[...]

    sums_s, sums_r = take("s", 5), take("r", 5)
    sums_to = [partner, across, pair, x_near, y_near]

    def sums_start(k):
        send(s.sums.at[k], s.sums_got.at[k], sums_to[k], sums_s + k, sums_r + k)
        at_end(s.sums.at[k], sums_s + k)

    def sums_finish(k):
        got(s.sums_got.at[k], sums_r + k)
        total = s.sums[k] + s.sums_got[k]
        s.sums[k + 1] = total
        if k == 4:
            pltpu.make_async_copy(s.sums.at[5], o.sums, vsem.at[0]).start()

    sums_start(0)

    def tok_part(first, count, dst):
        rows = pl.ds(pl.multiple_of(first, HALF), count)
        for n in range(4):
            cols = slice(256 * n, 256 * n + 256)
            acc = dot_nn(s.dq[rows, :], s.w3t[0, :, cols])
            acc = acc + dot_nn(s.dk[rows, :], s.w3t[1, :, cols])
            acc = acc + dot_nn(s.dv[rows, :], s.w3t[2, :, cols])
            put_part(dst, n, acc)
    scatter(3, tok_part)
    sums_finish(0)
    sums_start(1)

    def grad_head(m, src):
        s.g3[m * WIDTH:(m + 1) * WIDTH, :] = dot_nn(s.tkt[...], src[...]).astype(BF16)

    grad_third("i0")
    for n in range(4):
        s.go[n] = dot_nn(s.ctxt[...], s.g1[:, 256 * n:256 * n + 256]).astype(BF16)
    grad_head(0, s.dq)
    grad_head(1, s.dk)
    grad_head(2, s.dv)
    grad_second("i1")
    grad_first("o")
    grad_first("q")
    gtok_s, gtok_r = take("s"), take("r")
    at_end(s.gtok_own, gtok_s, home_self)

    def last_rows(i):
        ch = own_chunk(i)
        s.gtok_own[ch, :] = (s.g1f[ch, :] + scatter_rows(3, ch)).astype(BF16)

    def rows_home(chosen):
        @pl.when(chosen)
        def _():
            by_halves(3, last_rows, lambda k: None)
            send_or_keep(s.gtok_own, o.gtok, dev(b, zh, t), home_self, gtok_s, gtok_r)

    rows_home(is_inner)
    grad_third("i1")
    grad_second("o")
    grad_first("k")
    grad_second("q")
    grad_first("v")
    rows_home(jnp.logical_not(is_inner))
    sums_finish(1)
    sums_start(2)
    grad_third("o")
    grad_second("k")
    grad_third("q")
    sums_finish(2)
    grad_second("v")
    sums_start(3)
    grad_third("k")
    grad_third("v")
    sums_finish(3)
    sums_start(4)
    grad_final("b0")
    grad_final("b1")
    grad_final("i0")
    grad_final("i1")
    got(o.gtok, gtok_r)
    got(o.out, out_r)
    grad_final("o")
    grad_final("q")
    sums_finish(4)
    grad_final("k")
    grad_final("v")

    pltpu.make_async_copy(s.sums.at[5], o.sums, vsem.at[0]).wait()
    for size_of, sk, skipped, instead in to_drain:
        if skipped is None:
            left(size_of, sk)
        else:
            @pl.when(jnp.logical_not(skipped))
            def _():
                left(size_of, sk)
            if instead is not None:
                @pl.when(skipped)
                def _():
                    left(instead, sk)


def result_kernel(*refs):
    out, gtok, sums, zq, zk, zv, zo, zi0, zi1, zb0, zb1 = refs[:11]
    (o_out, o_gtok, o_gq, o_gbq, o_gk, o_gv, o_gbv, o_go, o_gbo, o_gga, o_gsa, o_gi, o_gbi, o_gb, o_gbb, o_ggf,
     o_gsf) = refs[11:28]
    held, wide, lines, wide_in, in_sem, out_sem = refs[28:39], refs[39:46], refs[46:55], refs[55], refs[56], refs[57]
    arriving = [pltpu.make_async_copy(src, dst, in_sem.at[n]) for n, (src, dst) in enumerate(zip(refs[:11], held))]
    for n in (0, 1, 9, 10, 7, 8, 6, 3, 4, 5, 2):
        arriving[n].start()
    leaving = []

    def put(src, dst):
        copy = pltpu.make_async_copy(src, dst, out_sem.at[len(leaving)])
        copy.start()
        leaving.append(copy)

    arriving[0].wait()
    put(held[0], o_out)
    arriving[1].wait()
    wide[0][...] = held[1][...].astype(F32)
    put(wide[0], o_gtok)

    def both(n, dst):
        arriving[n].wait()
        dst[...] = held[n][0].astype(F32) + held[n][1].astype(F32)

    both(9, wide[1].at[0:512, :])
    both(10, wide[1].at[512:1024, :])
    put(wide[1], o_gb)
    both(7, wide_in.at[:, 0:512])
    both(8, wide_in.at[:, 512:1024])
    put(wide_in, o_gi)
    for n, buf, dst in ((6, wide[2], o_go), (3, wide[3], o_gq), (4, wide[4], o_gk), (5, wide[5], o_gv)):
        both(n, buf)
        put(buf, dst)
    arriving[2].wait()
    for row, buf, dst in ((6, 0, o_gbq), (7, 1, o_gbv), (0, 2, o_gbo), (1, 3, o_gga), (2, 4, o_gsa), (3, 5, o_gbb),
                          (4, 6, o_ggf), (5, 7, o_gsf)):
        lines[buf][...] = held[2][row:row + 1, :]
        put(lines[buf], dst)
    for k in range(4):
        lines[8][:, WIDTH * k:WIDTH * k + WIDTH] = held[2][8 + k:9 + k, :]
    put(lines[8], o_gbi)
    for copy in leaving:
        copy.wait()


def on_device_fused(tokens, lengths, w_query, b_query, w_key, w_value, b_value, w_out, b_out, gain_attn, shift_attn,
                    w_in, b_in, w_back, b_back, gain_ffn, shift_ffn, cotangent):
    row = lambda vec: vec.reshape(1, -1)
    operands = (tokens, lengths, w_query, row(b_query), w_key, w_value, row(b_value), w_out, row(b_out),
                row(gain_attn), row(shift_attn), w_in, row(b_in), w_back, row(b_back), row(gain_ffn),
                row(shift_ffn), cotangent)
    stay = pl.BlockSpec(memory_space=pl.ANY)
    in_specs = [stay] * len(operands)
    in_specs[1] = pl.BlockSpec(memory_space=pltpu.SMEM)
    shape = lambda dims, dtype: jax.ShapeDtypeStruct(dims, dtype)
    between = [shape(tokens.shape, BF16), shape(tokens.shape, BF16), shape((16, WIDTH), F32)]
    between += [shape((2,) + HALVES[name], BF16) for name in ("q", "k", "v", "o", "i0", "i1", "b0", "b1")]
    parts = pl.pallas_call(
        layer_kernel,
        out_shape=between,
        in_specs=in_specs,
        out_specs=[stay] * len(between),
        scratch_shapes=jax.tree.leaves(scratch_table()),
        compiler_params=pltpu.CompilerParams(collective_id=0, has_side_effects=True, vmem_limit_bytes=64 * 1024 * 1000),
        name="layer",
    )(*operands)
    line = shape((1, WIDTH), F32)
    results = (
        shape(tokens.shape, BF16), shape(tokens.shape, F32), shape(w_query.shape, F32), line, shape(w_key.shape, F32),
        shape(w_value.shape, F32), line, shape(w_out.shape, F32), line, line, line, shape(w_in.shape, F32),
        shape((1, b_in.shape[0]), F32), shape(w_back.shape, F32), line, line, line)
    outs = pl.pallas_call(
        result_kernel,
        out_shape=results,
        in_specs=[stay] * len(between),
        out_specs=[stay] * len(results),
        scratch_shapes=[pltpu.VMEM(part.shape, part.dtype) for part in between]
        + [pltpu.VMEM(dims, F32) for dims in (tokens.shape, w_back.shape, w_out.shape, w_query.shape, w_key.shape,
                                              w_value.shape, (8, 128))]
        + [pltpu.VMEM((1, WIDTH), F32)] * 8
        + [pltpu.VMEM((1, b_in.shape[0]), F32), pltpu.VMEM(w_in.shape, F32), pltpu.SemaphoreType.DMA((11,)),
           pltpu.SemaphoreType.DMA((17,))],
        name="results",
    )(*parts)
    return tuple(v.reshape(-1) if v.shape[0] == 1 else v for v in outs)


def fits_fused(mesh):
    return dict(mesh.shape) == {"dp": 8, "tensor": 4}


def solution(mesh):
    placed = (
        P(("dp", "tensor"), None),
        P("dp", None),
        P("dp", "tensor"),
        P(),
        P("dp", "tensor"),
        P("dp", "tensor"),
        P(),
        P("tensor", "dp"),
        P(),
        P(),
        P(),
        P("dp", "tensor"),
        P(),
        P("tensor", "dp"),
        P(),
        P(),
        P(),
        P(("dp", "tensor"), None),
    )
    on_device = on_device_fused if fits_fused(mesh) else on_device_plain
    return jax.shard_map(
        on_device,
        mesh=mesh,
        in_specs=placed,
        out_specs=(
            P(("dp", "tensor"), None),
            P(("dp", "tensor"), None),
            P("dp", "tensor"),
            P(),
            P("dp", "tensor"),
            P("dp", "tensor"),
            P(),
            P("tensor", "dp"),
            P(),
            P(),
            P(),
            P("dp", "tensor"),
            P(),
            P("tensor", "dp"),
            P(),
            P(),
            P(),
        ),
        check_vma=False,
    )
```

```python
from types import SimpleNamespace

import jax
import jax.numpy as jnp
from jax import lax
from jax.experimental import pallas as pl
from jax.experimental.pallas import tpu as pltpu
from jax.sharding import PartitionSpec as P

HD = 64


epsilon = 1e-06
masked_value = -1e30


def matmul_plain(left_side, right_side):
    return jnp.dot(left_side, right_side, preferred_element_type=jnp.float32)


def matmul_over_rows(left_side, right_side):
    return lax.dot_general(
        left_side, right_side, (((0,), (0,)), ((), ())), preferred_element_type=jnp.float32
    )


def matmul_over_cols(left_side, right_side):
    return lax.dot_general(
        left_side, right_side, (((1,), (1,)), ((), ())), preferred_element_type=jnp.float32
    )


def layer_norm(residual, gain_vec, shift_vec):
    mean_val = jnp.mean(residual, axis=-1, keepdims=True)
    centered = residual - mean_val
    inv_std = lax.rsqrt(jnp.mean(centered * centered, axis=-1, keepdims=True) + epsilon)
    normed = centered * inv_std
    return (normed * gain_vec + shift_vec, normed, inv_std)


def norm_back(grad_out, normed, inv_std, gain_vec):
    grad_norm = grad_out * gain_vec
    first_mean = jnp.mean(grad_norm, axis=-1, keepdims=True)
    second_mean = jnp.mean(grad_norm * normed, axis=-1, keepdims=True)
    return inv_std * (grad_norm - first_mean - normed * second_mean)


def gelu_parts(preact):
    cdf_val = 0.5 * (1.0 + lax.erf(preact * 0.7071067811865476))
    pdf_val = jnp.exp(-0.5 * preact * preact) * 0.3989422804014327
    return (preact * cdf_val, cdf_val + preact * pdf_val)


def attend_forward(query_rows, key_rows, value_rows, seg_ids, head_dim, block_rows):
    group_rows, head_cols = query_rows.shape
    pair_width = 2 * head_dim
    block_count = group_rows // block_rows
    pair_count = head_cols // pair_width
    score_scale = head_dim ** (-0.5)

    def attend_step(step_index, loop_carry):
        context, log_total = loop_carry
        pair_index = step_index // block_count
        row_start = step_index % block_count * block_rows
        first_col = pair_index * pair_width
        query_block = lax.dynamic_slice(
            query_rows, (row_start, first_col), (block_rows, pair_width)
        ).reshape(block_rows, 2, head_dim)
        key_pair = lax.dynamic_slice(key_rows, (0, first_col), (group_rows, pair_width)).reshape(
            group_rows, 2, head_dim
        )
        value_pair = lax.dynamic_slice(
            value_rows, (0, first_col), (group_rows, pair_width)
        ).reshape(group_rows, 2, head_dim)
        same_seg = seg_ids[:, None] == seg_ids[None, :]
        scores = (
            jnp.einsum("qhd,khd->hqk", query_block, key_pair, preferred_element_type=jnp.float32)
            * score_scale
        )
        scores = jnp.where(same_seg[None], scores, masked_value)
        row_max = jnp.max(scores, axis=-1, keepdims=True)
        block_total = row_max + jnp.log(jnp.sum(jnp.exp(scores - row_max), axis=-1, keepdims=True))
        prob_bf = jnp.exp(scores - block_total).astype(jnp.bfloat16)
        context_block = jnp.einsum(
            "hqk,khd->qhd", prob_bf, value_pair, preferred_element_type=jnp.float32
        ).astype(jnp.bfloat16)
        context = lax.dynamic_update_slice(
            context, context_block.reshape(block_rows, pair_width), (row_start, first_col)
        )
        log_total = lax.dynamic_update_slice(
            log_total, block_total[:, :, 0], (2 * pair_index, row_start)
        )
        return (context, log_total)

    start_carry = (
        jnp.zeros((group_rows, head_cols), jnp.bfloat16),
        jnp.zeros((head_cols // head_dim, group_rows), jnp.float32),
    )
    return lax.fori_loop(0, pair_count * block_count, attend_step, start_carry)


def attend_backward(
    query_rows,
    key_rows,
    value_rows,
    context,
    grad_context,
    log_total,
    seg_ids,
    head_dim,
    block_rows,
):
    group_rows, head_cols = query_rows.shape
    pair_width = 2 * head_dim
    block_count = group_rows // block_rows
    pair_count = head_cols // pair_width
    score_scale = head_dim ** (-0.5)

    def back_step(step_index, loop_carry):
        grad_query, grad_keys, grad_values = loop_carry
        pair_index = step_index // block_count
        row_start = step_index % block_count * block_rows
        first_col = pair_index * pair_width
        query_block = lax.dynamic_slice(
            query_rows, (row_start, first_col), (block_rows, pair_width)
        ).reshape(block_rows, 2, head_dim)
        key_pair = lax.dynamic_slice(key_rows, (0, first_col), (group_rows, pair_width)).reshape(
            group_rows, 2, head_dim
        )
        value_pair = lax.dynamic_slice(
            value_rows, (0, first_col), (group_rows, pair_width)
        ).reshape(group_rows, 2, head_dim)
        context_block = lax.dynamic_slice(
            context, (row_start, first_col), (block_rows, pair_width)
        ).reshape(block_rows, 2, head_dim)
        gctx_block = lax.dynamic_slice(
            grad_context, (row_start, first_col), (block_rows, pair_width)
        ).reshape(block_rows, 2, head_dim)
        total_block = lax.dynamic_slice(log_total, (2 * pair_index, row_start), (2, block_rows))
        same_seg = seg_ids[:, None] == seg_ids[None, :]
        scores = (
            jnp.einsum("qhd,khd->hqk", query_block, key_pair, preferred_element_type=jnp.float32)
            * score_scale
        )
        scores = jnp.where(same_seg[None], scores, masked_value)
        probs = jnp.exp(scores - total_block[:, :, None])
        prob_bf = probs.astype(jnp.bfloat16)
        grad_probs = jnp.einsum(
            "qhd,khd->hqk", gctx_block, value_pair, preferred_element_type=jnp.float32
        )
        delta_rows = jnp.sum(
            gctx_block.astype(jnp.float32) * context_block.astype(jnp.float32), axis=-1
        ).T[:, :, None]
        grad_scores = (probs * (grad_probs - delta_rows) * score_scale).astype(jnp.bfloat16)
        grad_q_block = jnp.einsum(
            "hqk,khd->qhd", grad_scores, key_pair, preferred_element_type=jnp.float32
        ).reshape(block_rows, pair_width)
        grad_k_pair = jnp.einsum(
            "hqk,qhd->khd", grad_scores, query_block, preferred_element_type=jnp.float32
        ).reshape(group_rows, pair_width)
        grad_v_pair = jnp.einsum(
            "hqk,qhd->khd", prob_bf, gctx_block, preferred_element_type=jnp.float32
        ).reshape(group_rows, pair_width)
        grad_query = lax.dynamic_update_slice(grad_query, grad_q_block, (row_start, first_col))
        old_keys = lax.dynamic_slice(grad_keys, (0, first_col), (group_rows, pair_width))
        grad_keys = lax.dynamic_update_slice(grad_keys, old_keys + grad_k_pair, (0, first_col))
        old_values = lax.dynamic_slice(grad_values, (0, first_col), (group_rows, pair_width))
        grad_values = lax.dynamic_update_slice(
            grad_values, old_values + grad_v_pair, (0, first_col)
        )
        return (grad_query, grad_keys, grad_values)

    zero_grad = jnp.zeros((group_rows, head_cols), jnp.float32)
    return lax.fori_loop(0, pair_count * block_count, back_step, (zero_grad, zero_grad, zero_grad))


def on_device_plain(
    tokens,
    lengths,
    w_query,
    b_query,
    w_key,
    w_value,
    b_value,
    w_out,
    b_out,
    gain_attn,
    shift_attn,
    w_in,
    b_in,
    w_back,
    b_back,
    gain_ffn,
    shift_ffn,
    cotangent,
):
    tensor_size = lax.axis_size("tensor")
    tensor_index = lax.axis_index("tensor")
    local_rows = tokens.shape[0]
    group_rows = local_rows * tensor_size
    head_cols = w_query.shape[1]
    hidden_cols = w_in.shape[1]
    block_rows = min(512, group_rows)
    seq_lens = lengths[0]
    live_end = seq_lens[0] + seq_lens[1]
    positions = jnp.arange(group_rows, dtype=jnp.int32)
    seg_ids = (positions >= seq_lens[0]).astype(jnp.int32) + (positions >= live_end).astype(
        jnp.int32
    )
    local_pos = tensor_index * local_rows + jnp.arange(local_rows, dtype=jnp.int32)
    live_rows = (local_pos < live_end).astype(jnp.float32)[:, None]
    rows_full = lax.all_gather(tokens, "tensor", axis=0, tiled=True)
    attn_mats = (
        lax.all_gather(w_query, "dp", axis=0, tiled=True),
        lax.all_gather(w_key, "dp", axis=0, tiled=True),
        lax.all_gather(w_value, "dp", axis=0, tiled=True),
        lax.all_gather(w_out, "dp", axis=1, tiled=True),
    )
    mat_query, mat_key, mat_value, mat_out = attn_mats
    bias_query = lax.dynamic_slice_in_dim(b_query, tensor_index * head_cols, head_cols)
    bias_value = lax.dynamic_slice_in_dim(b_value, tensor_index * head_cols, head_cols)
    bias_in = lax.dynamic_slice_in_dim(b_in, tensor_index * hidden_cols, hidden_cols)
    query_rows = (matmul_plain(rows_full, mat_query) + bias_query).astype(jnp.bfloat16)
    key_rows = matmul_plain(rows_full, mat_key).astype(jnp.bfloat16)
    value_rows = (matmul_plain(rows_full, mat_value) + bias_value).astype(jnp.bfloat16)
    context, log_total = attend_forward(query_rows, key_rows, value_rows, seg_ids, HD, block_rows)
    attn_sum = lax.psum_scatter(
        matmul_plain(context, mat_out).astype(jnp.bfloat16),
        "tensor",
        scatter_dimension=0,
        tiled=True,
    ).astype(jnp.float32)
    resid_one = tokens.astype(jnp.float32) + attn_sum + b_out
    hidden_one, normed_one, inv_one = layer_norm(resid_one, gain_attn, shift_attn)
    hidden_bf = hidden_one.astype(jnp.bfloat16)
    hidden_full = lax.all_gather(hidden_bf, "tensor", axis=0, tiled=True)
    ffn_mats = (
        lax.all_gather(w_in, "dp", axis=0, tiled=True),
        lax.all_gather(w_back, "dp", axis=1, tiled=True),
    )
    mat_in, mat_back = ffn_mats
    preact = matmul_plain(hidden_full, mat_in) + bias_in
    activ_val, gelu_slope = gelu_parts(preact)
    activation = activ_val.astype(jnp.bfloat16)
    ffn_sum = lax.psum_scatter(
        matmul_plain(activation, mat_back).astype(jnp.bfloat16),
        "tensor",
        scatter_dimension=0,
        tiled=True,
    ).astype(jnp.float32)
    resid_two = hidden_one + ffn_sum + b_back
    normed_out, normed_two, inv_two = layer_norm(resid_two, gain_ffn, shift_ffn)
    output = (normed_out * live_rows).astype(jnp.bfloat16)
    grad_final = cotangent.astype(jnp.float32) * live_rows
    grad_gain_ffn = jnp.sum(grad_final * normed_two, axis=0)
    grad_shift_ffn = jnp.sum(grad_final, axis=0)
    grad_two = norm_back(grad_final, normed_two, inv_two, gain_ffn)
    grad_b_back = jnp.sum(grad_two, axis=0)
    mat_query, mat_key, mat_value, mat_out, mat_in, mat_back = (
        lax.all_gather(w_query, "dp", axis=0, tiled=True),
        lax.all_gather(w_key, "dp", axis=0, tiled=True),
        lax.all_gather(w_value, "dp", axis=0, tiled=True),
        lax.all_gather(w_out, "dp", axis=1, tiled=True),
        lax.all_gather(w_in, "dp", axis=0, tiled=True),
        lax.all_gather(w_back, "dp", axis=1, tiled=True),
    )
    grad_two_full = lax.all_gather(grad_two.astype(jnp.bfloat16), "tensor", axis=0, tiled=True)
    grad_w_back = matmul_over_rows(activation, grad_two_full)
    grad_pre = matmul_over_cols(grad_two_full, mat_back) * gelu_slope
    grad_b_in_part = jnp.sum(grad_pre, axis=0)
    grad_pre_bf = grad_pre.astype(jnp.bfloat16)
    grad_w_in = matmul_over_rows(hidden_full, grad_pre_bf)
    grad_one_out = grad_two + lax.psum_scatter(
        matmul_over_cols(grad_pre_bf, mat_in).astype(jnp.bfloat16),
        "tensor",
        scatter_dimension=0,
        tiled=True,
    ).astype(jnp.float32)
    grad_w_in, grad_w_back = (
        lax.psum_scatter(grad_w_in, "dp", scatter_dimension=0, tiled=True),
        lax.psum_scatter(grad_w_back, "dp", scatter_dimension=1, tiled=True),
    )
    grad_gain_attn = jnp.sum(grad_one_out * normed_one, axis=0)
    grad_shift_attn = jnp.sum(grad_one_out, axis=0)
    grad_one = norm_back(grad_one_out, normed_one, inv_one, gain_attn)
    grad_b_out = jnp.sum(grad_one, axis=0)
    grad_one_full = lax.all_gather(grad_one.astype(jnp.bfloat16), "tensor", axis=0, tiled=True)
    grad_w_out = matmul_over_rows(context, grad_one_full)
    grad_context = matmul_over_cols(grad_one_full, mat_out).astype(jnp.bfloat16)
    grad_query, grad_keys, grad_values = attend_backward(
        query_rows, key_rows, value_rows, context, grad_context, log_total, seg_ids, HD, block_rows
    )
    grad_b_query_part = jnp.sum(grad_query, axis=0)
    grad_b_value_part = jnp.sum(grad_values, axis=0)
    grad_query_bf = grad_query.astype(jnp.bfloat16)
    grad_keys_bf = grad_keys.astype(jnp.bfloat16)
    grad_values_bf = grad_values.astype(jnp.bfloat16)
    grad_w_query = matmul_over_rows(rows_full, grad_query_bf)
    grad_w_key = matmul_over_rows(rows_full, grad_keys_bf)
    grad_w_value = matmul_over_rows(rows_full, grad_values_bf)
    query_part = matmul_over_cols(grad_query_bf, mat_query)
    key_part = matmul_over_cols(grad_keys_bf, mat_key)
    value_part = matmul_over_cols(grad_values_bf, mat_value)
    grad_in = grad_one + lax.psum_scatter(
        (query_part + key_part + value_part).astype(jnp.bfloat16),
        "tensor",
        scatter_dimension=0,
        tiled=True,
    ).astype(jnp.float32)
    grad_w_query, grad_w_key, grad_w_value, grad_w_out = (
        lax.psum_scatter(grad_w_query, "dp", scatter_dimension=0, tiled=True),
        lax.psum_scatter(grad_w_key, "dp", scatter_dimension=0, tiled=True),
        lax.psum_scatter(grad_w_value, "dp", scatter_dimension=0, tiled=True),
        lax.psum_scatter(grad_w_out, "dp", scatter_dimension=1, tiled=True),
    )

    def widen(part_vec, full_width):
        return lax.dynamic_update_slice_in_dim(
            jnp.zeros((full_width,), jnp.float32), part_vec, tensor_index * part_vec.shape[0], 0
        )

    small_sums = lax.psum(
        (
            widen(grad_b_query_part, b_query.shape[0]),
            widen(grad_b_value_part, b_value.shape[0]),
            grad_b_out,
            grad_gain_attn,
            grad_shift_attn,
            widen(grad_b_in_part, b_in.shape[0]),
            grad_b_back,
            grad_gain_ffn,
            grad_shift_ffn,
        ),
        ("dp", "tensor"),
    )
    return (
        output,
        grad_in,
        grad_w_query,
        small_sums[0],
        grad_w_key,
        grad_w_value,
        small_sums[1],
        grad_w_out,
        small_sums[2],
        small_sums[3],
        small_sums[4],
        grad_w_in,
        small_sums[5],
        grad_w_back,
        small_sums[6],
        small_sums[7],
        small_sums[8],
    )


MESH_ID = pl.DeviceIdType.MESH
F32 = jnp.float32
BF16 = jnp.bfloat16

SLOTS = 4
BLOCK = 128
GROUP = 512
WIDTH = 1024
HEAD_COLS = 256
HIDDEN = 1024
N_SEND = 58
N_GOT = 110
HALF = BLOCK // 2
HALVES = dict(q=(128, 256), k=(128, 256), v=(128, 256), o=(256, 128), i0=(128, 512), i1=(128, 512), b0=(512, 128),
              b1=(512, 128))
VECTORS = dict(bq=1024, bv=1024, bo=1024, ga=1024, sa=1024, bi=4096, bb=1024, gf=1024, sf=1024)


def flip(bit):
    return 1 - bit


def slot_step(t, j):
    return (t % 2 + j % 2) % 2 + 2 * ((t // 2 + j // 2) % 2)


def rows_of(r, count=BLOCK):
    return pl.ds(pl.multiple_of(r * BLOCK, BLOCK), count)


def cols_of(n, count=256):
    return pl.ds(pl.multiple_of(n * count, count), count)


def dot_nn(a, b):
    return jnp.dot(a, b, preferred_element_type=F32)


def dot_nt(a, b):
    return lax.dot_general(a, b, (((1,), (1,)), ((), ())), preferred_element_type=F32)


def dot_tn(a, b):
    return lax.dot_general(a, b, (((0,), (0,)), ((), ())), preferred_element_type=F32)


def scratch_table():
    act = lambda n: pltpu.VMEM((GROUP, n), BF16)
    table = dict(
        w3=pltpu.VMEM((3 * WIDTH, HEAD_COLS), BF16),
        wo=pltpu.VMEM((4, HEAD_COLS, 256), BF16),
        wi=pltpu.VMEM((WIDTH, HIDDEN), BF16),
        wb=pltpu.VMEM((4, HIDDEN, 256), BF16),
        w3t=pltpu.VMEM((3, HEAD_COLS, WIDTH), BF16),
        wot=pltpu.VMEM((WIDTH, HEAD_COLS), BF16),
        wit=pltpu.VMEM((HIDDEN, WIDTH), BF16),
        wbt=pltpu.VMEM((WIDTH, HIDDEN), BF16),
        lens_own=pltpu.VMEM((2, 8, 128), F32),
        lens_got=pltpu.VMEM((2, 8, 128), F32),
        lens_use=pltpu.VMEM((2, 8, 128), F32),
        tk=act(WIDTH),
        tkt=pltpu.VMEM((WIDTH, GROUP), BF16),
        cot_own=pltpu.VMEM((BLOCK, WIDTH), BF16),
        bias=pltpu.VMEM((GROUP, GROUP), F32),
        q=act(HEAD_COLS),
        qt=pltpu.VMEM((HEAD_COLS, GROUP), BF16),
        k=act(HEAD_COLS),
        ks=act(HEAD_COLS),
        v=act(HEAD_COLS),
        ps=pltpu.VMEM((4, GROUP, GROUP), BF16),
        ctx=act(HEAD_COLS),
        ctxt=pltpu.VMEM((HEAD_COLS, GROUP), BF16),
        hid=act(WIDTH),
        hidt=pltpu.VMEM((WIDTH, GROUP), BF16),
        act=act(HIDDEN),
        actt=pltpu.VMEM((HIDDEN, GROUP), BF16),
        slope=pltpu.VMEM((GROUP, HIDDEN), F32),
        g2=act(WIDTH),
        gpre=act(HIDDEN),
        g1=act(WIDTH),
        gctxt=pltpu.VMEM((HEAD_COLS, GROUP), BF16),
        dq=act(HEAD_COLS),
        dkt=pltpu.VMEM((HEAD_COLS, GROUP), F32),
        dvt=pltpu.VMEM((HEAD_COLS, GROUP), F32),
        dk=act(HEAD_COLS),
        dv=act(HEAD_COLS),
        hid1=pltpu.VMEM((BLOCK, WIDTH), F32),
        normed1=pltpu.VMEM((BLOCK, WIDTH), F32),
        inv1=pltpu.VMEM((BLOCK, 128), F32),
        g2f=pltpu.VMEM((BLOCK, WIDTH), F32),
        g1f=pltpu.VMEM((BLOCK, WIDTH), F32),
        out_own=pltpu.VMEM((BLOCK, WIDTH), BF16),
        gtok_own=pltpu.VMEM((BLOCK, WIDTH), BF16),
        rs_own=pltpu.VMEM((4, BLOCK, WIDTH), BF16),
        rs_out=pltpu.VMEM((4, 3, BLOCK, WIDTH), BF16),
        rs_got=pltpu.VMEM((4, 3, BLOCK, WIDTH), BF16),
        sums=pltpu.VMEM((6, 16, WIDTH), F32),
        sums_got=pltpu.VMEM((5, 16, WIDTH), F32),
        gb_in=pltpu.VMEM((1, HIDDEN), F32),
        vectors={name: pltpu.VMEM((1, width), F32) for name, width in VECTORS.items()},
        vsem=pltpu.SemaphoreType.DMA((len(VECTORS),)),
        turn=pltpu.SemaphoreType.REGULAR((5,)),
        g3=pltpu.VMEM((3 * WIDTH, HEAD_COLS), BF16),
        go=pltpu.VMEM((4, HEAD_COLS, 256), BF16),
        gi=pltpu.VMEM((WIDTH, HIDDEN), BF16),
        gb=pltpu.VMEM((4, HIDDEN, 256), BF16),
        stage={},
        ssem=pltpu.SemaphoreType.DMA((N_SEND,)),
        rsem=pltpu.SemaphoreType.DMA((N_GOT,)),
    )
    for name, dims in HALVES.items():
        table["stage"][name] = pltpu.VMEM((10,) + dims, BF16)
    return table


def layer_kernel(tok, lens, wq, bq, wk, wv, bv, wo, bo, ga, sa, wi, bi, wb, bb, gf, sf, cot, out, gtok, sums, zq, zk, zv,
                 zo, zi0, zi1, zb0, zb1, *scratch):
    a = SimpleNamespace(tok=tok, lens=lens, wq=wq, bq=bq, wk=wk, wv=wv, bv=bv, wo=wo, bo=bo, ga=ga, sa=sa, wi=wi, bi=bi,
                        wb=wb, bb=bb, gf=gf, sf=sf, cot=cot)
    o = SimpleNamespace(out=out, gtok=gtok, sums=sums)
    landed = dict(q=zq, k=zk, v=zv, o=zo, i0=zi0, i1=zi1, b0=zb0, b1=zb1)
    s = SimpleNamespace(**jax.tree.unflatten(jax.tree.structure(scratch_table()), scratch))
    ssem, rsem, vsem, vectors = s.ssem, s.rsem, s.vsem, s.vectors

    dp = lax.axis_index("dp")
    z = lax.axis_index("tensor")
    b, c = dp // 2, dp % 2
    zl, zh = z % 2, z // 2
    t = zl * 2 + c
    sl = (z + 2 * c) % 4
    here, away = c == 0, c == 1
    bx = b + 1 - 2 * (b % 2)
    by = (b + 2) % 4
    bd = 3 - b
    t1, t2, t3 = slot_step(t, 1), slot_step(t, 2), slot_step(t, 3)

    def dev(pos, core, zz):
        return (pos * 2 + core, zz)

    partner = dev(b, flip(c), z)
    z_near = z + 1 - 2 * (z % 2)
    z_far = (z + 2) % 4
    pair = dev(b, c, z_near)
    across = dev(b, c, z_far)
    is_inner = jnp.logical_and(z >= 1, z <= 2)
    inner_away = jnp.logical_and(is_inner, away)
    outer_away = jnp.logical_and(jnp.logical_not(is_inner), away)
    x_near = dev(bx, c, z)
    y_near = dev(by, c, z)

    taken = {"s": 0, "r": 0}

    def take(kind, count=1):
        first = taken[kind]
        taken[kind] = first + count
        assert taken[kind] <= (N_SEND if kind == "s" else N_GOT)
        return first

    to_drain = []

    def make_copy(src, dst, device, sk, rk):
        return pltpu.make_async_remote_copy(
            src_ref=src, dst_ref=dst, send_sem=ssem.at[sk], recv_sem=rsem.at[rk], device_id=device,
            device_id_type=MESH_ID)

    def send(src, dst, device, sk, rk):
        make_copy(src, dst, device, sk, rk).start()

    def got(dst, rk):
        pltpu.make_async_copy(dst, dst, rsem.at[rk]).wait()

    def left(size_of, sk):
        pltpu.make_async_copy(size_of, size_of, ssem.at[sk]).wait()

    def at_end(size_of, sk, skipped=None, instead=None):
        to_drain.append((size_of, sk, skipped, instead))

    def send_or_keep(src, dst, device, is_self, sk, rk):
        copy = make_copy(src, dst, device, sk, rk)

        @pl.when(is_self)
        def _():
            pltpu.make_async_copy(src, dst, rsem.at[rk]).start()

        @pl.when(jnp.logical_not(is_self))
        def _():
            copy.start()

    barrier = pltpu.get_barrier_semaphore()
    peers = [x_near, y_near]
    for dz in range(4):
        for dc in range(2):
            if dz or dc:
                peers.append(dev(b, (c + dc) % 2, (z + dz) % 4))
    for peer in peers:
        pl.semaphore_signal(barrier, inc=1, device_id=peer, device_id_type=MESH_ID)
    pl.semaphore_wait(barrier, len(peers))

    def piece_qkv(m, home):
        base = m * WIDTH
        return SimpleNamespace(
            home=home,
            own=lambda bb, cc: s.w3.at[pl.ds(pl.multiple_of(base + bb * 256 + cc * 128, 128), 128), :],
            block=lambda bb: s.w3.at[pl.ds(pl.multiple_of(base + bb * 256, 256), 256), :],
            half=lambda bb, h: s.w3.at[pl.ds(pl.multiple_of(base + bb * 256 + h * 128, 128), 128), :])

    piece_o = SimpleNamespace(
        home=a.wo,
        own=lambda bb, cc: s.wo.at[bb, :, pl.ds(pl.multiple_of(cc * 128, 128), 128)],
        block=lambda bb: s.wo.at[bb],
        half=lambda bb, h: s.wo.at[bb, pl.ds(h * 128, 128), :])

    def piece_in(j):
        cols = pl.ds(j * 512, 512)
        return SimpleNamespace(
            home=a.wi.at[:, cols],
            own=lambda bb, cc: s.wi.at[pl.ds(pl.multiple_of(bb * 256 + cc * 128, 128), 128), cols],
            block=lambda bb: s.wi.at[pl.ds(pl.multiple_of(bb * 256, 256), 256), cols],
            half=lambda bb, h: s.wi.at[pl.ds(pl.multiple_of(bb * 256 + h * 128, 128), 128), cols])

    def piece_back(j):
        part = pl.ds(j * 512, 512)
        return SimpleNamespace(
            home=a.wb.at[part, :],
            own=lambda bb, cc: s.wb.at[bb, part, pl.ds(pl.multiple_of(cc * 128, 128), 128)],
            block=lambda bb: s.wb.at[bb, part, :],
            half=lambda bb, h: s.wb.at[bb, pl.ds(j * 512 + h * 256, 256), :])

    pieces = dict(q=piece_qkv(0, a.wq), k=piece_qkv(1, a.wk), v=piece_qkv(2, a.wv), o=piece_o,
                  i0=piece_in(0), i1=piece_in(1), b0=piece_back(0), b1=piece_back(1))
    first_size = dict(
        q=s.w3.at[0:768, :], k=s.w3.at[0:768, :], v=s.w3.at[0:768, :], o=s.wo.at[0:3], i0=s.wi.at[0:768, 0:512],
        i1=s.wi.at[0:768, 0:512], b0=s.wb.at[0:3, 0:512, :], b1=s.wb.at[0:3, 0:512, :])
    for name, piece in pieces.items():
        piece.s1, piece.r1 = take("s"), take("r")
        piece.s2, piece.r2 = take("s"), take("r", 3)
        at_end(piece.block(b), piece.s1, here, piece.own(b, 0))
        at_end(first_size[name], piece.s2)

    def to_local(name):
        piece = pieces[name]
        send_or_keep(piece.home, piece.own(b, c), dev(b, 0, z), here, piece.s1, piece.r1)

    def to_across(name):
        piece = pieces[name]
        send(piece.home, piece.own(b, c), dev(b, 1, z_far), piece.s1, piece.r1)

    def over_plane(name):
        piece = pieces[name]
        got(piece.block(b), piece.r1)
        send(piece.block(b), piece.block(b), x_near, piece.s2, piece.r2)
        send(piece.block(b), piece.block(b), y_near, piece.s2, piece.r2 + 1)

    def relay(name):
        piece = pieces[name]
        got(piece.block(bx), piece.r2)
        send(piece.half(bx, 0), piece.half(bx, 0), y_near, piece.s2, piece.r2 + 2)
        got(piece.block(by), piece.r2 + 1)
        send(piece.half(by, 1), piece.half(by, 1), x_near, piece.s2, piece.r2 + 2)

    def over_plane_now(names, chosen, relays=()):
        @pl.when(chosen)
        def _():
            for name in relays:
                relay(name)
            for name in names:
                over_plane(name)

    def arrived(name):
        piece = pieces[name]
        got(piece.block(bd), piece.r2 + 2)

    tok_s, tok_r = take("s", 2), take("r", 4)
    fwd_s = take("s", 6)
    lens_s, lens_r = take("s"), take("r")
    cot_s, cot_r = take("s"), take("r")

    def send_lens():
        first = a.lens[0, 0].astype(F32)
        s.lens_own[0] = jnp.full((8, 128), first, F32)
        s.lens_own[1] = jnp.full((8, 128), first + a.lens[0, 1].astype(F32), F32)
        send(s.lens_own, s.lens_got, partner, lens_s, lens_r)
        at_end(s.lens_own, lens_s)

    def take_lens():
        got(s.lens_got, lens_r)

        @pl.when(c == zh)
        def _():
            s.lens_use[...] = s.lens_own[...]

        @pl.when(c != zh)
        def _():
            s.lens_use[...] = s.lens_got[...]

    def tok_block(r):
        return s.tk.at[rows_of(r), :]

    inner, outer = 1 + c, 3 * c
    is_relay = jnp.logical_and(c == zh, z == inner)

    def send_tokens():
        near = z // 2 == c
        first = jnp.where(near, 2 * c, inner)
        send_or_keep(a.tok, tok_block(z), dev(b, c, first), first == z, tok_s, tok_r + z)
        at_end(tok_block(z), tok_s, first == z)
        second = make_copy(a.tok, tok_block(z), dev(b, c, 2 * c + 1), tok_s + 1, tok_r + z)
        keep = jnp.logical_and(near, z == 2 * c + 1)
        go = jnp.logical_and(near, z != 2 * c + 1)

        @pl.when(keep)
        def _():
            pltpu.make_async_copy(a.tok, tok_block(z), rsem.at[tok_r + z]).start()

        @pl.when(go)
        def _():
            second.start()

        at_end(tok_block(z), tok_s + 1, jnp.logical_not(go))

    def pass_on(half, far):
        for k in range(2):
            r = half * 2 + k
            block = tok_block(r)
            got(block, tok_r + r)
            if far:
                on = make_copy(block, block, dev(b, c, outer), fwd_s + k, tok_r + r)

                @pl.when(is_relay)
                def _():
                    on.start()
            copy = make_copy(block, block, partner, fwd_s + 2 + 2 * far + k, tok_r + r)

            @pl.when(c == zh)
            def _():
                copy.start()

    for k in range(6):
        at_end(s.tk.at[0:BLOCK, :], fwd_s + k, jnp.logical_not(is_relay) if k < 2 else c != zh)

    def send_cotangent():
        zt, ct = 2 * c + z // 2, z % 2
        is_self = jnp.logical_and(zt == z, ct == c)
        send_or_keep(a.cot, s.cot_own, dev(b, ct, zt), is_self, cot_s, cot_r)
        at_end(s.cot_own, cot_s, is_self)

    gather_s, gather_r = take("s", 3), take("r", 12)
    scatter_s, scatter_r = take("s", 4), take("r", 20)
    for k in range(3):
        at_end(s.tk.at[0:3 * BLOCK, :], gather_s + k)
    for k in range(4):
        at_end(s.tk.at[0:3 * BLOCK, :], scatter_s + k)

    def block_at(full, r):
        return full.at[rows_of(r), :]

    def half_at(full, r, k):
        return full.at[pl.ds(pl.multiple_of(r * BLOCK + k * HALF, HALF), HALF), :]

    def gather_start(which, full, k):
        mine = half_at(full, t, k)
        send(mine, mine, pair, gather_s + which, gather_r + 4 * which + 1 + k)
        send(mine, mine, partner, gather_s + which, gather_r + 4 * which)

    def gather_step(which, full, j):
        base = gather_r + 4 * which

        @pl.when(j == 1)
        def _():
            got(block_at(full, t1), base)

        @pl.when(j == 2)
        def _():
            if which == 0:
                over_plane_now((), away, relays=("b0",))
            for k in range(2):
                near = half_at(full, t2, k)
                got(near, base + 1 + k)
                send(near, near, partner, gather_s + which, base + 3)

        @pl.when(j == 3)
        def _():
            if which == 0:
                over_plane_now((), away, relays=("b1",))
            got(block_at(full, t3), base + 3)

    halves = [pl.ds(k * HALF, HALF) for k in range(2)]

    def scatter(which, part):
        out, back = s.rs_out, s.rs_got
        ss, rr = scatter_s + which, scatter_r + 5 * which
        part(t3 * BLOCK, BLOCK, out.at[which, 0])
        send(out.at[which, 0], back.at[which, 0], partner, ss, rr)
        part(t2 * BLOCK, BLOCK, out.at[which, 1])
        got(back.at[which, 0], rr)
        for k in range(2):
            rows = halves[k]
            total = out[which, 1, rows, :].astype(F32) + back[which, 0, rows, :].astype(F32)
            out[which, 1, rows, :] = total.astype(BF16)
            send(out.at[which, 1, rows, :], back.at[which, 1, rows, :], pair, ss, rr + 2 + k)
        part(t1 * BLOCK, BLOCK, out.at[which, 2])
        send(out.at[which, 2], back.at[which, 2], partner, ss, rr + 4)
        part(t * BLOCK, BLOCK, s.rs_own.at[which])

    def scatter_cols(which, blocks, k):
        out, back = s.rs_out, s.rs_got
        ss, rr = scatter_s + which, scatter_r + 5 * which
        slots = [pl.ds(pl.multiple_of(block * 256, 256), 256) for block in blocks]
        size = s.rs_got.at[which, 0, :, 0:256 * len(blocks)]

        def product(row, block):
            rows = pl.ds(pl.multiple_of(row * BLOCK, BLOCK), BLOCK)
            return dot_nn(s.act[rows, :], s.wb[block])

        def cast(row, slot):
            for block, cols in zip(blocks, slots):
                out[which, slot, :, cols] = product(row, block).astype(BF16)

        cast(t3, 0)
        for cols in slots:
            send(out.at[which, 0, :, cols], back.at[which, 0, :, cols], partner, ss, rr + k)
        cast(t1, 2)
        for cols in slots:
            send(out.at[which, 2, :, cols], back.at[which, 2, :, cols], partner, ss, rr + 4)
        got(size, rr + k)
        for block, cols in zip(blocks, slots):
            total = product(t2, block).astype(BF16).astype(F32) + back[which, 0, :, cols].astype(F32)
            out[which, 1, :, cols] = total.astype(BF16)
            send(out.at[which, 1, :, cols], back.at[which, 1, :, cols], pair, ss, rr + 2)
        for block, cols in zip(blocks, slots):
            s.rs_own[which, :, cols] = product(t, block).astype(BF16)

    def scatter_cols_wait(which):
        rr = scatter_r + 5 * which
        got(s.rs_got.at[which, 2], rr + 4)
        got(s.rs_got.at[which, 1], rr + 2)

    def scatter_wait(which, k):
        rr = scatter_r + 5 * which
        if k == 0:
            got(s.rs_got.at[which, 2], rr + 4)
        got(s.rs_got.at[which, 1, halves[k], :], rr + 2 + k)

    def scatter_rows(which, chunk):
        total = s.rs_own[which, chunk, :].astype(F32) + s.rs_got[which, 2, chunk, :].astype(F32)
        return total + s.rs_got[which, 1, chunk, :].astype(F32)

    def by_halves(which, body, after):
        if which == 1:
            scatter_cols_wait(which)
        for k in range(2):
            if which != 1:
                scatter_wait(which, k)
            loop(2, lambda i: body(2 * k + i))
            after(k)

    def put_part(dst, n, value):
        dst[:, 256 * n:256 * n + 256] = value.astype(BF16)

    def loop(count, body):
        lax.fori_loop(0, count, lambda i, _: (body(i), 0)[1], 0)

    def grad_qkv(m):
        base = m * WIDTH
        return lambda bb, h: s.g3.at[pl.ds(pl.multiple_of(base + bb * 256 + h * 128, 128), 128), :]

    def grad_in_part(k):
        cols = pl.ds(k * 512, 512)
        return lambda bb, h: s.gi.at[pl.ds(pl.multiple_of(bb * 256 + h * 128, 128), 128), cols]

    def grad_back_part(k):
        part = pl.ds(k * 512, 512)
        return lambda bb, h: s.gb.at[bb, part, pl.ds(h * 128, 128)]

    grad_half = dict(
        q=grad_qkv(0), k=grad_qkv(1), v=grad_qkv(2), o=lambda bb, h: s.go.at[bb, :, pl.ds(h * 128, 128)],
        i0=grad_in_part(0), i1=grad_in_part(1), b0=grad_back_part(0), b1=grad_back_part(1))
    grad_s = {name: take("s", 2) for name in grad_half}
    grad_r = {name: take("r", 4) for name in grad_half}
    for name in grad_half:
        at_end(s.stage[name].at[0:6], grad_s[name])
        at_end(s.stage[name].at[0:2], grad_s[name] + 1, here, s.stage[name].at[0])

    def chunks(name, body):
        size = 64 if name in ("i0", "i1") else 128
        count = HALVES[name][0] // size
        loop(count, lambda i: body(pl.ds(pl.multiple_of(i * size, size), size)))

    def grad_first(name, part=2):
        half, ss, rr, st = grad_half[name], grad_s[name], grad_r[name], s.stage[name]
        if part in (0, 2):
            send(half(bd, 0), st.at[1], x_near, ss, rr)
            send(half(bd, 1), st.at[3], y_near, ss, rr + 1)
        if part == 0:
            return
        send(half(bx, 0), st.at[0], x_near, ss, rr + 2)
        send(half(by, 1), st.at[2], y_near, ss, rr + 2)

    def grad_second(name):
        half, ss, rr, st = grad_half[name], grad_s[name], grad_r[name], s.stage[name]
        for h, block, to in ((0, by, y_near), (1, bx, x_near)):
            got(st.at[1 + 2 * h], rr + h)
            mine = half(block, h)

            def add(ch):
                st[4 + h, ch, :] = (mine[ch, :].astype(F32) + st[1 + 2 * h, ch, :].astype(F32)).astype(BF16)
            chunks(name, add)
            send(st.at[4 + h], st.at[6 + h], to, ss, rr + 2)

    def grad_third(name):
        half, ss, rr, st = grad_half[name], grad_s[name], grad_r[name], s.stage[name]
        zr = landed[name]
        got(st.at[0:4], rr + 2)
        for h in range(2):
            mine = half(b, h)

            def add_all(ch):
                total = mine[ch, :].astype(F32) + st[2 * h, ch, :].astype(F32) + st[6 + h, ch, :].astype(F32)
                st[8 + h, ch, :] = total.astype(BF16)
            chunks(name, add_all)
            is_self = here if h == 0 else c < 0
            send_or_keep(st.at[8 + h], zr.at[zh], dev(b, h, sl), is_self, ss + 1, rr + 3)

    def grad_final(name):
        got(landed[name], grad_r[name] + 3)

    to_across("q")
    to_across("k")
    send_tokens()
    to_across("v")
    for name in pieces:
        to_local(name)
    send_lens()
    for name, ref in vectors.items():
        pltpu.make_async_copy(getattr(a, name), ref, vsem.at[list(vectors).index(name)]).start()
    s.sums[0] = jnp.zeros((16, WIDTH), F32)
    s.gb_in[...] = jnp.zeros((1, HIDDEN), F32)
    leads = jnp.logical_and(is_inner, away)

    def in_turn(k, inner_next, outer_next):
        @pl.when(leads)
        def _():
            for device in (partner, pair, dev(b, 0, z_near)):
                pl.semaphore_signal(s.turn.at[k], inc=1, device_id=device, device_id_type=MESH_ID)

        @pl.when(jnp.logical_not(leads))
        def _():
            pl.semaphore_wait(s.turn.at[k], 1)

        for chosen, names in ((is_inner, inner_next), (jnp.logical_not(is_inner), outer_next)):
            if names:
                @pl.when(chosen)
                def _():
                    for name in names:
                        to_across(name)

    over_plane_now(("q", "k", "v", "o"), here)
    over_plane_now(("q", "k"), away)
    relay("q")
    over_plane_now(("i0",), here, relays=("k", "v"))
    pass_on(zh, 0)
    to_across("o")

    @pl.when(is_inner)
    def _():
        pass_on(flip(zh), 1)

    in_turn(0, (), ("i0",))
    take_lens()

    def make_bias(r):
        first, end = s.lens_use[0][0:1, 0:1], s.lens_use[1][0:1, 0:1]
        row = (lax.broadcasted_iota(jnp.int32, (BLOCK, GROUP), 0) + r * BLOCK).astype(F32)
        col = lax.broadcasted_iota(jnp.int32, (BLOCK, GROUP), 1).astype(F32)
        seg = lambda p: jnp.where(p >= end, 2.0, jnp.where(p >= first, 1.0, 0.0))
        s.bias[rows_of(r), :] = jnp.where(seg(row) == seg(col), 0.0, masked_value)
    loop(SLOTS, make_bias)
    for name, ref in vectors.items():
        pltpu.make_async_copy(getattr(a, name), ref, vsem.at[list(vectors).index(name)]).wait()
        setattr(a, name, ref)
    over_plane_now(("v", "o"), away, relays=("k",))
    over_plane_now(("i1",), here, relays=("o",))
    over_plane_now((), away, relays=("v",))
    over_plane_now(("b0",), here, relays=("i0",))
    in_turn(1, ("i0", "i1"), ("i1",))

    @pl.when(jnp.logical_not(is_inner))
    def _():
        pass_on(flip(zh), 1)


    def turn_tokens(r):
        s.tkt[:, rows_of(r)] = s.tk[rows_of(r), :].T
    loop(SLOTS, turn_tokens)

    head_cols = pl.ds(pl.multiple_of(sl * HEAD_COLS, HEAD_COLS), HEAD_COLS)

    def project(m):
        acc = dot_nn(s.tk[...], s.w3[m * WIDTH:(m + 1) * WIDTH, :])
        if m == 0:
            value = (acc + a.bq[:, head_cols]).astype(BF16)
            scaled = (value.astype(F32) * 0.125).astype(BF16)
            s.q[...] = scaled
            s.qt[...] = scaled.T
        elif m == 1:
            value = acc.astype(BF16)
            s.k[...] = value
            s.ks[...] = (value.astype(F32) * 0.125).astype(BF16)
        else:
            s.v[...] = (acc + a.bv[:, head_cols]).astype(BF16)

    arrived("q")
    project(0)
    arrived("k")
    project(1)
    in_turn(2, ("b0", "b1"), ())
    arrived("v")
    project(2)

    def attend():
        parts = []
        for h in range(4):
            cols = slice(64 * h, 64 * h + 64)
            scores = dot_nt(s.q[:, cols], s.k[:, cols]) + s.bias[...]
            top = jnp.max(scores, axis=-1, keepdims=True)
            weight = jnp.exp(scores - top)
            total = jnp.sum(weight, axis=-1, keepdims=True)
            prob = (weight * (1.0 / total)).astype(BF16)
            s.ps[h] = prob
            parts.append(dot_nn(prob, s.v[:, cols]))
        context = jnp.concatenate(parts, axis=1).astype(BF16)
        s.ctx[...] = context
        s.ctxt[...] = context.T
    over_plane_now((), away, relays=("o",))
    over_plane_now(("i0",), inner_away)
    over_plane_now(("b1",), here, relays=("i1",))
    attend()
    @pl.when(jnp.logical_not(is_inner))
    def _():
        to_across("b0")

    over_plane_now(("i0",), outer_away)
    over_plane_now(("i1",), inner_away)
    arrived("o")

    def attn_part(first, count, dst):
        rows = s.ctx[pl.ds(pl.multiple_of(first, HALF), count), :]
        for n in range(4):
            put_part(dst, n, dot_nn(rows, s.wo[n]))
    scatter(0, attn_part)
    @pl.when(jnp.logical_not(is_inner))
    def _():
        to_across("b1")

    for m in range(3):
        for n in range(4):
            s.w3t[m, :, 256 * n:256 * n + 256] = s.w3[m * WIDTH + 256 * n:m * WIDTH + 256 * n + 256, :].T
    for n in range(4):
        s.wot[256 * n:256 * n + 256, :] = s.wo[n].T

    CH = 32

    def own_chunk(i):
        return pl.ds(pl.multiple_of(i * CH, CH), CH)

    def group_chunk(i):
        return pl.ds(pl.multiple_of(t * BLOCK + i * CH, CH), CH)

    def norm_one(i):
        ch = own_chunk(i)
        resid = s.tk[group_chunk(i), :].astype(F32) + scatter_rows(0, ch) + a.bo[...]
        centered = resid - jnp.mean(resid, axis=-1, keepdims=True)
        inv = lax.rsqrt(jnp.mean(centered * centered, axis=-1, keepdims=True) + epsilon)
        normed = centered * inv
        hidden = normed * a.ga[...] + a.sa[...]
        s.normed1[ch, :] = normed
        s.inv1[ch, :] = jnp.broadcast_to(inv, (CH, 128))
        s.hid1[ch, :] = hidden
        s.hid[group_chunk(i), :] = hidden.astype(BF16)
    over_plane_now((), here, relays=("b0",))
    over_plane_now((), inner_away, relays=("i0",))
    over_plane_now(("i1", "b0"), outer_away, relays=("i0",))
    by_halves(0, norm_one, lambda k: gather_start(0, s.hid, k))
    over_plane_now((), here, relays=("b1",))
    over_plane_now((), inner_away, relays=("i1",))
    over_plane_now(("b1",), outer_away, relays=("i1",))
    over_plane_now(("b0", "b1"), inner_away)
    send_cotangent()
    arrived("i0")
    arrived("i1")

    def ffn_in(j):
        gather_step(0, s.hid, j)
        r = slot_step(t, j)
        rows = rows_of(r)
        for n in range(4):
            cols = slice(256 * n, 256 * n + 256)
            bias = a.bi[:, pl.ds(pl.multiple_of(sl * HIDDEN + n * 256, 256), 256)]
            pre = dot_nn(s.hid[rows, :], s.wi[:, cols]) + bias
            cdf = 0.5 * (1.0 + lax.erf(pre * 0.7071067811865476))
            pdf = jnp.exp(-0.5 * pre * pre) * 0.3989422804014327
            s.act[rows, cols] = (pre * cdf).astype(BF16)
            s.slope[rows, cols] = cdf + pre * pdf
    loop(SLOTS, ffn_in)

    def turn_ffn(r):
        rows = rows_of(r)
        s.actt[:, rows] = s.act[rows, :].T
        s.hidt[:, rows] = s.hid[rows, :].T
    scatter_cols(1, (b, bx, by), 0)
    arrived("b0")
    arrived("b1")
    scatter_cols(1, (bd,), 1)
    loop(SLOTS, turn_ffn)

    def turn_wi(r):
        rows = rows_of(r)
        s.wit[:, rows] = s.wi[rows, :].T
    loop(8, turn_wi)

    def turn_wb(r):
        rows = rows_of(r)
        for n in range(4):
            s.wbt[256 * n:256 * n + 256, rows] = s.wb[n, rows, :].T
    loop(8, turn_wb)
    got(s.cot_own, cot_r)

    def add_rows(row, value):
        s.sums[0, row:row + 1, :] += jnp.sum(value, axis=0, keepdims=True)

    def norm_two(i):
        ch = own_chunk(i)
        resid = s.hid1[ch, :] + scatter_rows(1, ch) + a.bb[...]
        centered = resid - jnp.mean(resid, axis=-1, keepdims=True)
        inv = lax.rsqrt(jnp.mean(centered * centered, axis=-1, keepdims=True) + epsilon)
        normed = centered * inv
        position = lax.broadcasted_iota(jnp.int32, (CH, 128), 0) + (t * BLOCK + i * CH)
        live = jnp.where(position.astype(F32) < s.lens_use[1][0:1, :], 1.0, 0.0)[:, 0:1]
        s.out_own[ch, :] = ((normed * a.gf[...] + a.sf[...]) * live).astype(BF16)
        grad = s.cot_own[ch, :].astype(F32) * live
        add_rows(4, grad * normed)
        add_rows(5, grad)
        u = grad * a.gf[...]
        first = jnp.mean(u, axis=-1, keepdims=True)
        second = jnp.mean(u * normed, axis=-1, keepdims=True)
        grad_two = inv * (u - first - normed * second)
        add_rows(3, grad_two)
        s.g2f[ch, :] = grad_two
        s.g2[group_chunk(i), :] = grad_two.astype(BF16)
    by_halves(1, norm_two, lambda k: gather_start(1, s.g2, k))
    out_s, out_r = take("s"), take("r")
    home_self = jnp.logical_and(zh == c, t == z)

    def ffn_back(j):
        @pl.when(j < 3)
        def _():
            gather_step(1, s.g2, j)
        r = slot_step(t, j)
        rows = rows_of(r)
        for n in range(4):
            cols = slice(256 * n, 256 * n + 256)
            grad = dot_nn(s.g2[rows, :], s.wbt[:, cols]) * s.slope[rows, cols]
            s.gb_in[:, cols] += jnp.sum(grad, axis=0, keepdims=True)
            s.gpre[rows, cols] = grad.astype(BF16)
    loop(SLOTS - 1, ffn_back)

    def grad_back(k):
        part = slice(512 * k, 512 * k + 512)

        def body(n):
            for e in range(2):
                block = n * 2 + e
                s.gb[block, part, :] = dot_nn(s.actt[part, :], s.g2[:, cols_of(block)]).astype(BF16)
        loop(2, body)

    def grad_in(k):
        cols = slice(512 * k, 512 * k + 512)

        def body(m):
            part = rows_of(m * 4, 512)
            s.gi[part, cols] = dot_nn(s.hidt[part, :], s.gpre[:, cols]).astype(BF16)
        loop(2, body)

    gather_step(1, s.g2, 3)
    grad_back(0)
    grad_first("b0")
    ffn_back(3)
    grad_back(1)
    grad_first("b1", 0)
    send_or_keep(s.out_own, o.out, dev(b, zh, t), home_self, out_s, out_r)
    at_end(s.out_own, out_s, home_self)

    def in_part(first, count, dst):
        rows = pl.ds(pl.multiple_of(first, HALF), count)
        for n in range(4):
            put_part(dst, n, dot_nn(s.gpre[rows, :], s.wit[:, 256 * n:256 * n + 256]))
    scatter(2, in_part)
    grad_in(0)
    grad_in(1)
    grad_second("b0")
    grad_first("b1", 1)
    grad_second("b1")
    grad_first("i0", 0)

    def norm_one_back(i):
        ch = own_chunk(i)
        grad = s.g2f[ch, :] + scatter_rows(2, ch)
        normed = s.normed1[ch, :]
        add_rows(1, grad * normed)
        add_rows(2, grad)
        u = grad * a.ga[...]
        first = jnp.mean(u, axis=-1, keepdims=True)
        second = jnp.mean(u * normed, axis=-1, keepdims=True)
        grad_one = s.inv1[ch, 0:1] * (u - first - normed * second)
        add_rows(0, grad_one)
        s.g1f[ch, :] = grad_one
        s.g1[group_chunk(i), :] = grad_one.astype(BF16)
    by_halves(2, norm_one_back, lambda k: gather_start(2, s.g1, k))
    grad_first("i0", 1)
    grad_third("b0")

    def attend_back(chip, add):
        rows = pl.ds(pl.multiple_of(chip * 2 * BLOCK, 2 * BLOCK), 2 * BLOCK)
        grad_ctx = dot_nn(s.g1[rows, :], s.wot[...]).astype(BF16)
        s.gctxt[:, rows] = grad_ctx.T
        product = grad_ctx.astype(F32) * s.ctx[rows, :].astype(F32)
        parts = []
        for h in range(4):
            cols = slice(64 * h, 64 * h + 64)
            prob = s.ps[h, rows, :]
            delta = jnp.sum(product[:, cols], axis=-1, keepdims=True)
            grad_prob = dot_nt(grad_ctx[:, cols], s.v[:, cols])
            grad_score = (prob.astype(F32) * (grad_prob - delta)).astype(BF16)
            parts.append(dot_nn(grad_score, s.ks[:, cols]))
            grad_key = dot_nn(s.qt[cols, rows], grad_score)
            grad_value = dot_nn(s.gctxt[cols, rows], prob)
            if add:
                grad_key, grad_value = s.dkt[cols, :] + grad_key, s.dvt[cols, :] + grad_value
            s.dkt[cols, :] = grad_key
            s.dvt[cols, :] = grad_value
        grad_query = jnp.concatenate(parts, axis=1)
        for k in range(4):
            @pl.when(sl == k)
            def _():
                s.sums[0, 6:7, 256 * k:256 * k + 256] += jnp.sum(grad_query, axis=0, keepdims=True)
        s.dq[rows, :] = grad_query.astype(BF16)
    gather_step(2, s.g1, 1)
    attend_back(zl, False)
    grad_third("b1")
    gather_step(2, s.g1, 2)
    gather_step(2, s.g1, 3)
    attend_back(flip(zl), True)
    grad_second("i0")
    grad_first("i1")
    s.dk[...] = s.dkt[...].T.astype(BF16)
    grad_value = s.dvt[...].T
    for k in range(4):
        @pl.when(sl == k)
        def _():
            s.sums[0, 7:8, 256 * k:256 * k + 256] += jnp.sum(grad_value, axis=0, keepdims=True)
    s.dv[...] = grad_value.astype(BF16)
    for k in range(4):
        @pl.when(sl == k)
        def _():
            s.sums[0, 8 + k:9 + k, :] = s.gb_in[...]

    sums_s, sums_r = take("s", 6), take("r", 6)
    sums_to = [partner, across, pair, x_near, y_near]
    sum_rows = pl.ds(pl.multiple_of(c * 8, 8), 8)
    other_rows = pl.ds(pl.multiple_of(flip(c) * 8, 8), 8)

    def sums_part(ref, k):
        return ref.at[k] if k == 0 else ref.at[k, sum_rows, :]

    def sums_start(k):
        mine = sums_part(s.sums, k)
        send(mine, sums_part(s.sums_got, k), sums_to[k], sums_s + k, sums_r + k)
        at_end(mine, sums_s + k)

    def sums_finish(k):
        got(sums_part(s.sums_got, k), sums_r + k)
        if k == 0:
            s.sums[1] = s.sums[0] + s.sums_got[0]
        else:
            s.sums[k + 1, sum_rows, :] = s.sums[k, sum_rows, :] + s.sums_got[k, sum_rows, :]
        if k == 4:
            done = s.sums.at[5, sum_rows, :]
            send(done, done, partner, sums_s + 5, sums_r + 5)
            at_end(done, sums_s + 5)

    def sums_out():
        got(s.sums.at[5, other_rows, :], sums_r + 5)
        pltpu.make_async_copy(s.sums.at[5], o.sums, vsem.at[0]).start()

    sums_start(0)

    def tok_part(first, count, dst):
        rows = pl.ds(pl.multiple_of(first, HALF), count)
        for n in range(4):
            cols = slice(256 * n, 256 * n + 256)
            acc = dot_nn(s.dq[rows, :], s.w3t[0, :, cols])
            acc = acc + dot_nn(s.dk[rows, :], s.w3t[1, :, cols])
            acc = acc + dot_nn(s.dv[rows, :], s.w3t[2, :, cols])
            put_part(dst, n, acc)
    scatter(3, tok_part)
    sums_finish(0)
    sums_start(1)

    def grad_head(m, src):
        s.g3[m * WIDTH:(m + 1) * WIDTH, :] = dot_nn(s.tkt[...], src[...]).astype(BF16)

    grad_third("i0")
    for n in range(4):
        s.go[n] = dot_nn(s.ctxt[...], s.g1[:, 256 * n:256 * n + 256]).astype(BF16)
    grad_head(0, s.dq)
    grad_head(1, s.dk)
    grad_head(2, s.dv)
    grad_second("i1")
    grad_first("o")
    grad_first("q")
    gtok_s, gtok_r = take("s"), take("r")
    at_end(s.gtok_own, gtok_s, home_self)

    def last_rows(i):
        ch = own_chunk(i)
        s.gtok_own[ch, :] = (s.g1f[ch, :] + scatter_rows(3, ch)).astype(BF16)

    def rows_home(chosen):
        @pl.when(chosen)
        def _():
            by_halves(3, last_rows, lambda k: None)
            send_or_keep(s.gtok_own, o.gtok, dev(b, zh, t), home_self, gtok_s, gtok_r)

    rows_home(is_inner)
    grad_third("i1")
    grad_second("o")
    grad_first("k")
    grad_second("q")
    grad_first("v")
    rows_home(jnp.logical_not(is_inner))
    sums_finish(1)
    sums_start(2)
    grad_third("o")
    grad_second("k")
    grad_third("q")
    sums_finish(2)
    grad_second("v")
    sums_start(3)
    grad_third("k")
    grad_third("v")
    sums_finish(3)
    sums_start(4)
    grad_final("b0")
    grad_final("b1")
    grad_final("i0")
    grad_final("i1")
    got(o.gtok, gtok_r)
    got(o.out, out_r)
    grad_final("o")
    grad_final("q")
    sums_finish(4)
    grad_final("k")
    sums_out()
    grad_final("v")

    pltpu.make_async_copy(s.sums.at[5], o.sums, vsem.at[0]).wait()
    for size_of, sk, skipped, instead in to_drain:
        if skipped is None:
            left(size_of, sk)
        else:
            @pl.when(jnp.logical_not(skipped))
            def _():
                left(size_of, sk)
            if instead is not None:
                @pl.when(skipped)
                def _():
                    left(instead, sk)


def result_kernel(*refs):
    out, gtok, sums, zq, zk, zv, zo, zi0, zi1, zb0, zb1 = refs[:11]
    (o_out, o_gtok, o_gq, o_gbq, o_gk, o_gv, o_gbv, o_go, o_gbo, o_gga, o_gsa, o_gi, o_gbi, o_gb, o_gbb, o_ggf,
     o_gsf) = refs[11:28]
    held, wide, lines, wide_in, in_sem, out_sem = refs[28:39], refs[39:46], refs[46:55], refs[55], refs[56], refs[57]
    arriving = [pltpu.make_async_copy(src, dst, in_sem.at[n]) for n, (src, dst) in enumerate(zip(refs[:11], held))]
    for n in (0, 1, 9, 10, 7, 8, 6, 3, 4, 5, 2):
        arriving[n].start()
    leaving = []

    def put(src, dst):
        copy = pltpu.make_async_copy(src, dst, out_sem.at[len(leaving)])
        copy.start()
        leaving.append(copy)

    arriving[0].wait()
    put(held[0], o_out)
    arriving[1].wait()
    wide[0][...] = held[1][...].astype(F32)
    put(wide[0], o_gtok)

    def both(n, dst):
        arriving[n].wait()
        dst[...] = held[n][0].astype(F32) + held[n][1].astype(F32)

    both(9, wide[1].at[0:512, :])
    both(10, wide[1].at[512:1024, :])
    put(wide[1], o_gb)
    both(7, wide_in.at[:, 0:512])
    both(8, wide_in.at[:, 512:1024])
    put(wide_in, o_gi)
    for n, buf, dst in ((6, wide[2], o_go), (3, wide[3], o_gq), (4, wide[4], o_gk), (5, wide[5], o_gv)):
        both(n, buf)
        put(buf, dst)
    arriving[2].wait()
    for row, buf, dst in ((6, 0, o_gbq), (7, 1, o_gbv), (0, 2, o_gbo), (1, 3, o_gga), (2, 4, o_gsa), (3, 5, o_gbb),
                          (4, 6, o_ggf), (5, 7, o_gsf)):
        lines[buf][...] = held[2][row:row + 1, :]
        put(lines[buf], dst)
    for k in range(4):
        lines[8][:, WIDTH * k:WIDTH * k + WIDTH] = held[2][8 + k:9 + k, :]
    put(lines[8], o_gbi)
    for copy in leaving:
        copy.wait()


def on_device_fused(tokens, lengths, w_query, b_query, w_key, w_value, b_value, w_out, b_out, gain_attn, shift_attn,
                    w_in, b_in, w_back, b_back, gain_ffn, shift_ffn, cotangent):
    row = lambda vec: vec.reshape(1, -1)
    operands = (tokens, lengths, w_query, row(b_query), w_key, w_value, row(b_value), w_out, row(b_out),
                row(gain_attn), row(shift_attn), w_in, row(b_in), w_back, row(b_back), row(gain_ffn),
                row(shift_ffn), cotangent)
    stay = pl.BlockSpec(memory_space=pl.ANY)
    in_specs = [stay] * len(operands)
    in_specs[1] = pl.BlockSpec(memory_space=pltpu.SMEM)
    shape = lambda dims, dtype: jax.ShapeDtypeStruct(dims, dtype)
    between = [shape(tokens.shape, BF16), shape(tokens.shape, BF16), shape((16, WIDTH), F32)]
    between += [shape((2,) + HALVES[name], BF16) for name in ("q", "k", "v", "o", "i0", "i1", "b0", "b1")]
    parts = pl.pallas_call(
        layer_kernel,
        out_shape=between,
        in_specs=in_specs,
        out_specs=[stay] * len(between),
        scratch_shapes=jax.tree.leaves(scratch_table()),
        compiler_params=pltpu.CompilerParams(collective_id=0, has_side_effects=True, vmem_limit_bytes=64 * 1024 * 1000),
        name="layer",
    )(*operands)
    line = shape((1, WIDTH), F32)
    results = (
        shape(tokens.shape, BF16), shape(tokens.shape, F32), shape(w_query.shape, F32), line, shape(w_key.shape, F32),
        shape(w_value.shape, F32), line, shape(w_out.shape, F32), line, line, line, shape(w_in.shape, F32),
        shape((1, b_in.shape[0]), F32), shape(w_back.shape, F32), line, line, line)
    outs = pl.pallas_call(
        result_kernel,
        out_shape=results,
        in_specs=[stay] * len(between),
        out_specs=[stay] * len(results),
        scratch_shapes=[pltpu.VMEM(part.shape, part.dtype) for part in between]
        + [pltpu.VMEM(dims, F32) for dims in (tokens.shape, w_back.shape, w_out.shape, w_query.shape, w_key.shape,
                                              w_value.shape, (8, 128))]
        + [pltpu.VMEM((1, WIDTH), F32)] * 8
        + [pltpu.VMEM((1, b_in.shape[0]), F32), pltpu.VMEM(w_in.shape, F32), pltpu.SemaphoreType.DMA((11,)),
           pltpu.SemaphoreType.DMA((17,))],
        name="results",
    )(*parts)
    return tuple(v.reshape(-1) if v.shape[0] == 1 else v for v in outs)


def fits_fused(mesh):
    return dict(mesh.shape) == {"dp": 8, "tensor": 4}


def solution(mesh):
    placed = (
        P(("dp", "tensor"), None),
        P("dp", None),
        P("dp", "tensor"),
        P(),
        P("dp", "tensor"),
        P("dp", "tensor"),
        P(),
        P("tensor", "dp"),
        P(),
        P(),
        P(),
        P("dp", "tensor"),
        P(),
        P("tensor", "dp"),
        P(),
        P(),
        P(),
        P(("dp", "tensor"), None),
    )
    on_device = on_device_fused if fits_fused(mesh) else on_device_plain
    return jax.shard_map(
        on_device,
        mesh=mesh,
        in_specs=placed,
        out_specs=(
            P(("dp", "tensor"), None),
            P(("dp", "tensor"), None),
            P("dp", "tensor"),
            P(),
            P("dp", "tensor"),
            P("dp", "tensor"),
            P(),
            P("tensor", "dp"),
            P(),
            P(),
            P(),
            P("dp", "tensor"),
            P(),
            P("tensor", "dp"),
            P(),
            P(),
            P(),
        ),
        check_vma=False,
    )
```

```python
from types import SimpleNamespace

import jax
import jax.numpy as jnp
from jax import lax
from jax.experimental import pallas as pl
from jax.experimental.pallas import tpu as pltpu
from jax.sharding import PartitionSpec as P

HD = 64


epsilon = 1e-06
masked_value = -1e30


def matmul_plain(left_side, right_side):
    return jnp.dot(left_side, right_side, preferred_element_type=jnp.float32)


def matmul_over_rows(left_side, right_side):
    return lax.dot_general(
        left_side, right_side, (((0,), (0,)), ((), ())), preferred_element_type=jnp.float32
    )


def matmul_over_cols(left_side, right_side):
    return lax.dot_general(
        left_side, right_side, (((1,), (1,)), ((), ())), preferred_element_type=jnp.float32
    )


def layer_norm(residual, gain_vec, shift_vec):
    mean_val = jnp.mean(residual, axis=-1, keepdims=True)
    centered = residual - mean_val
    inv_std = lax.rsqrt(jnp.mean(centered * centered, axis=-1, keepdims=True) + epsilon)
    normed = centered * inv_std
    return (normed * gain_vec + shift_vec, normed, inv_std)


def norm_back(grad_out, normed, inv_std, gain_vec):
    grad_norm = grad_out * gain_vec
    first_mean = jnp.mean(grad_norm, axis=-1, keepdims=True)
    second_mean = jnp.mean(grad_norm * normed, axis=-1, keepdims=True)
    return inv_std * (grad_norm - first_mean - normed * second_mean)


def gelu_parts(preact):
    cdf_val = 0.5 * (1.0 + lax.erf(preact * 0.7071067811865476))
    pdf_val = jnp.exp(-0.5 * preact * preact) * 0.3989422804014327
    return (preact * cdf_val, cdf_val + preact * pdf_val)


def attend_forward(query_rows, key_rows, value_rows, seg_ids, head_dim, block_rows):
    group_rows, head_cols = query_rows.shape
    pair_width = 2 * head_dim
    block_count = group_rows // block_rows
    pair_count = head_cols // pair_width
    score_scale = head_dim ** (-0.5)

    def attend_step(step_index, loop_carry):
        context, log_total = loop_carry
        pair_index = step_index // block_count
        row_start = step_index % block_count * block_rows
        first_col = pair_index * pair_width
        query_block = lax.dynamic_slice(
            query_rows, (row_start, first_col), (block_rows, pair_width)
        ).reshape(block_rows, 2, head_dim)
        key_pair = lax.dynamic_slice(key_rows, (0, first_col), (group_rows, pair_width)).reshape(
            group_rows, 2, head_dim
        )
        value_pair = lax.dynamic_slice(
            value_rows, (0, first_col), (group_rows, pair_width)
        ).reshape(group_rows, 2, head_dim)
        same_seg = seg_ids[:, None] == seg_ids[None, :]
        scores = (
            jnp.einsum("qhd,khd->hqk", query_block, key_pair, preferred_element_type=jnp.float32)
            * score_scale
        )
        scores = jnp.where(same_seg[None], scores, masked_value)
        row_max = jnp.max(scores, axis=-1, keepdims=True)
        block_total = row_max + jnp.log(jnp.sum(jnp.exp(scores - row_max), axis=-1, keepdims=True))
        prob_bf = jnp.exp(scores - block_total).astype(jnp.bfloat16)
        context_block = jnp.einsum(
            "hqk,khd->qhd", prob_bf, value_pair, preferred_element_type=jnp.float32
        ).astype(jnp.bfloat16)
        context = lax.dynamic_update_slice(
            context, context_block.reshape(block_rows, pair_width), (row_start, first_col)
        )
        log_total = lax.dynamic_update_slice(
            log_total, block_total[:, :, 0], (2 * pair_index, row_start)
        )
        return (context, log_total)

    start_carry = (
        jnp.zeros((group_rows, head_cols), jnp.bfloat16),
        jnp.zeros((head_cols // head_dim, group_rows), jnp.float32),
    )
    return lax.fori_loop(0, pair_count * block_count, attend_step, start_carry)


def attend_backward(
    query_rows,
    key_rows,
    value_rows,
    context,
    grad_context,
    log_total,
    seg_ids,
    head_dim,
    block_rows,
):
    group_rows, head_cols = query_rows.shape
    pair_width = 2 * head_dim
    block_count = group_rows // block_rows
    pair_count = head_cols // pair_width
    score_scale = head_dim ** (-0.5)

    def back_step(step_index, loop_carry):
        grad_query, grad_keys, grad_values = loop_carry
        pair_index = step_index // block_count
        row_start = step_index % block_count * block_rows
        first_col = pair_index * pair_width
        query_block = lax.dynamic_slice(
            query_rows, (row_start, first_col), (block_rows, pair_width)
        ).reshape(block_rows, 2, head_dim)
        key_pair = lax.dynamic_slice(key_rows, (0, first_col), (group_rows, pair_width)).reshape(
            group_rows, 2, head_dim
        )
        value_pair = lax.dynamic_slice(
            value_rows, (0, first_col), (group_rows, pair_width)
        ).reshape(group_rows, 2, head_dim)
        context_block = lax.dynamic_slice(
            context, (row_start, first_col), (block_rows, pair_width)
        ).reshape(block_rows, 2, head_dim)
        gctx_block = lax.dynamic_slice(
            grad_context, (row_start, first_col), (block_rows, pair_width)
        ).reshape(block_rows, 2, head_dim)
        total_block = lax.dynamic_slice(log_total, (2 * pair_index, row_start), (2, block_rows))
        same_seg = seg_ids[:, None] == seg_ids[None, :]
        scores = (
            jnp.einsum("qhd,khd->hqk", query_block, key_pair, preferred_element_type=jnp.float32)
            * score_scale
        )
        scores = jnp.where(same_seg[None], scores, masked_value)
        probs = jnp.exp(scores - total_block[:, :, None])
        prob_bf = probs.astype(jnp.bfloat16)
        grad_probs = jnp.einsum(
            "qhd,khd->hqk", gctx_block, value_pair, preferred_element_type=jnp.float32
        )
        delta_rows = jnp.sum(
            gctx_block.astype(jnp.float32) * context_block.astype(jnp.float32), axis=-1
        ).T[:, :, None]
        grad_scores = (probs * (grad_probs - delta_rows) * score_scale).astype(jnp.bfloat16)
        grad_q_block = jnp.einsum(
            "hqk,khd->qhd", grad_scores, key_pair, preferred_element_type=jnp.float32
        ).reshape(block_rows, pair_width)
        grad_k_pair = jnp.einsum(
            "hqk,qhd->khd", grad_scores, query_block, preferred_element_type=jnp.float32
        ).reshape(group_rows, pair_width)
        grad_v_pair = jnp.einsum(
            "hqk,qhd->khd", prob_bf, gctx_block, preferred_element_type=jnp.float32
        ).reshape(group_rows, pair_width)
        grad_query = lax.dynamic_update_slice(grad_query, grad_q_block, (row_start, first_col))
        old_keys = lax.dynamic_slice(grad_keys, (0, first_col), (group_rows, pair_width))
        grad_keys = lax.dynamic_update_slice(grad_keys, old_keys + grad_k_pair, (0, first_col))
        old_values = lax.dynamic_slice(grad_values, (0, first_col), (group_rows, pair_width))
        grad_values = lax.dynamic_update_slice(
            grad_values, old_values + grad_v_pair, (0, first_col)
        )
        return (grad_query, grad_keys, grad_values)

    zero_grad = jnp.zeros((group_rows, head_cols), jnp.float32)
    return lax.fori_loop(0, pair_count * block_count, back_step, (zero_grad, zero_grad, zero_grad))


def on_device_plain(
    tokens,
    lengths,
    w_query,
    b_query,
    w_key,
    w_value,
    b_value,
    w_out,
    b_out,
    gain_attn,
    shift_attn,
    w_in,
    b_in,
    w_back,
    b_back,
    gain_ffn,
    shift_ffn,
    cotangent,
):
    tensor_size = lax.axis_size("tensor")
    tensor_index = lax.axis_index("tensor")
    local_rows = tokens.shape[0]
    group_rows = local_rows * tensor_size
    head_cols = w_query.shape[1]
    hidden_cols = w_in.shape[1]
    block_rows = min(512, group_rows)
    seq_lens = lengths[0]
    live_end = seq_lens[0] + seq_lens[1]
    positions = jnp.arange(group_rows, dtype=jnp.int32)
    seg_ids = (positions >= seq_lens[0]).astype(jnp.int32) + (positions >= live_end).astype(
        jnp.int32
    )
    local_pos = tensor_index * local_rows + jnp.arange(local_rows, dtype=jnp.int32)
    live_rows = (local_pos < live_end).astype(jnp.float32)[:, None]
    rows_full = lax.all_gather(tokens, "tensor", axis=0, tiled=True)
    attn_mats = (
        lax.all_gather(w_query, "dp", axis=0, tiled=True),
        lax.all_gather(w_key, "dp", axis=0, tiled=True),
        lax.all_gather(w_value, "dp", axis=0, tiled=True),
        lax.all_gather(w_out, "dp", axis=1, tiled=True),
    )
    mat_query, mat_key, mat_value, mat_out = attn_mats
    bias_query = lax.dynamic_slice_in_dim(b_query, tensor_index * head_cols, head_cols)
    bias_value = lax.dynamic_slice_in_dim(b_value, tensor_index * head_cols, head_cols)
    bias_in = lax.dynamic_slice_in_dim(b_in, tensor_index * hidden_cols, hidden_cols)
    query_rows = (matmul_plain(rows_full, mat_query) + bias_query).astype(jnp.bfloat16)
    key_rows = matmul_plain(rows_full, mat_key).astype(jnp.bfloat16)
    value_rows = (matmul_plain(rows_full, mat_value) + bias_value).astype(jnp.bfloat16)
    context, log_total = attend_forward(query_rows, key_rows, value_rows, seg_ids, HD, block_rows)
    attn_sum = lax.psum_scatter(
        matmul_plain(context, mat_out).astype(jnp.bfloat16),
        "tensor",
        scatter_dimension=0,
        tiled=True,
    ).astype(jnp.float32)
    resid_one = tokens.astype(jnp.float32) + attn_sum + b_out
    hidden_one, normed_one, inv_one = layer_norm(resid_one, gain_attn, shift_attn)
    hidden_bf = hidden_one.astype(jnp.bfloat16)
    hidden_full = lax.all_gather(hidden_bf, "tensor", axis=0, tiled=True)
    ffn_mats = (
        lax.all_gather(w_in, "dp", axis=0, tiled=True),
        lax.all_gather(w_back, "dp", axis=1, tiled=True),
    )
    mat_in, mat_back = ffn_mats
    preact = matmul_plain(hidden_full, mat_in) + bias_in
    activ_val, gelu_slope = gelu_parts(preact)
    activation = activ_val.astype(jnp.bfloat16)
    ffn_sum = lax.psum_scatter(
        matmul_plain(activation, mat_back).astype(jnp.bfloat16),
        "tensor",
        scatter_dimension=0,
        tiled=True,
    ).astype(jnp.float32)
    resid_two = hidden_one + ffn_sum + b_back
    normed_out, normed_two, inv_two = layer_norm(resid_two, gain_ffn, shift_ffn)
    output = (normed_out * live_rows).astype(jnp.bfloat16)
    grad_final = cotangent.astype(jnp.float32) * live_rows
    grad_gain_ffn = jnp.sum(grad_final * normed_two, axis=0)
    grad_shift_ffn = jnp.sum(grad_final, axis=0)
    grad_two = norm_back(grad_final, normed_two, inv_two, gain_ffn)
    grad_b_back = jnp.sum(grad_two, axis=0)
    mat_query, mat_key, mat_value, mat_out, mat_in, mat_back = (
        lax.all_gather(w_query, "dp", axis=0, tiled=True),
        lax.all_gather(w_key, "dp", axis=0, tiled=True),
        lax.all_gather(w_value, "dp", axis=0, tiled=True),
        lax.all_gather(w_out, "dp", axis=1, tiled=True),
        lax.all_gather(w_in, "dp", axis=0, tiled=True),
        lax.all_gather(w_back, "dp", axis=1, tiled=True),
    )
    grad_two_full = lax.all_gather(grad_two.astype(jnp.bfloat16), "tensor", axis=0, tiled=True)
    grad_w_back = matmul_over_rows(activation, grad_two_full)
    grad_pre = matmul_over_cols(grad_two_full, mat_back) * gelu_slope
    grad_b_in_part = jnp.sum(grad_pre, axis=0)
    grad_pre_bf = grad_pre.astype(jnp.bfloat16)
    grad_w_in = matmul_over_rows(hidden_full, grad_pre_bf)
    grad_one_out = grad_two + lax.psum_scatter(
        matmul_over_cols(grad_pre_bf, mat_in).astype(jnp.bfloat16),
        "tensor",
        scatter_dimension=0,
        tiled=True,
    ).astype(jnp.float32)
    grad_w_in, grad_w_back = (
        lax.psum_scatter(grad_w_in, "dp", scatter_dimension=0, tiled=True),
        lax.psum_scatter(grad_w_back, "dp", scatter_dimension=1, tiled=True),
    )
    grad_gain_attn = jnp.sum(grad_one_out * normed_one, axis=0)
    grad_shift_attn = jnp.sum(grad_one_out, axis=0)
    grad_one = norm_back(grad_one_out, normed_one, inv_one, gain_attn)
    grad_b_out = jnp.sum(grad_one, axis=0)
    grad_one_full = lax.all_gather(grad_one.astype(jnp.bfloat16), "tensor", axis=0, tiled=True)
    grad_w_out = matmul_over_rows(context, grad_one_full)
    grad_context = matmul_over_cols(grad_one_full, mat_out).astype(jnp.bfloat16)
    grad_query, grad_keys, grad_values = attend_backward(
        query_rows, key_rows, value_rows, context, grad_context, log_total, seg_ids, HD, block_rows
    )
    grad_b_query_part = jnp.sum(grad_query, axis=0)
    grad_b_value_part = jnp.sum(grad_values, axis=0)
    grad_query_bf = grad_query.astype(jnp.bfloat16)
    grad_keys_bf = grad_keys.astype(jnp.bfloat16)
    grad_values_bf = grad_values.astype(jnp.bfloat16)
    grad_w_query = matmul_over_rows(rows_full, grad_query_bf)
    grad_w_key = matmul_over_rows(rows_full, grad_keys_bf)
    grad_w_value = matmul_over_rows(rows_full, grad_values_bf)
    query_part = matmul_over_cols(grad_query_bf, mat_query)
    key_part = matmul_over_cols(grad_keys_bf, mat_key)
    value_part = matmul_over_cols(grad_values_bf, mat_value)
    grad_in = grad_one + lax.psum_scatter(
        (query_part + key_part + value_part).astype(jnp.bfloat16),
        "tensor",
        scatter_dimension=0,
        tiled=True,
    ).astype(jnp.float32)
    grad_w_query, grad_w_key, grad_w_value, grad_w_out = (
        lax.psum_scatter(grad_w_query, "dp", scatter_dimension=0, tiled=True),
        lax.psum_scatter(grad_w_key, "dp", scatter_dimension=0, tiled=True),
        lax.psum_scatter(grad_w_value, "dp", scatter_dimension=0, tiled=True),
        lax.psum_scatter(grad_w_out, "dp", scatter_dimension=1, tiled=True),
    )

    def widen(part_vec, full_width):
        return lax.dynamic_update_slice_in_dim(
            jnp.zeros((full_width,), jnp.float32), part_vec, tensor_index * part_vec.shape[0], 0
        )

    small_sums = lax.psum(
        (
            widen(grad_b_query_part, b_query.shape[0]),
            widen(grad_b_value_part, b_value.shape[0]),
            grad_b_out,
            grad_gain_attn,
            grad_shift_attn,
            widen(grad_b_in_part, b_in.shape[0]),
            grad_b_back,
            grad_gain_ffn,
            grad_shift_ffn,
        ),
        ("dp", "tensor"),
    )
    return (
        output,
        grad_in,
        grad_w_query,
        small_sums[0],
        grad_w_key,
        grad_w_value,
        small_sums[1],
        grad_w_out,
        small_sums[2],
        small_sums[3],
        small_sums[4],
        grad_w_in,
        small_sums[5],
        grad_w_back,
        small_sums[6],
        small_sums[7],
        small_sums[8],
    )


MESH_ID = pl.DeviceIdType.MESH
F32 = jnp.float32
BF16 = jnp.bfloat16

SLOTS = 4
BLOCK = 128
GROUP = 512
WIDTH = 1024
HEAD_COLS = 256
HIDDEN = 1024
N_SEND = 58
N_GOT = 110
HALF = BLOCK // 2
HALVES = dict(q=(128, 256), k=(128, 256), v=(128, 256), o=(256, 128), i0=(128, 512), i1=(128, 512), b0=(512, 128),
              b1=(512, 128))
VECTORS = dict(bq=1024, bv=1024, bo=1024, ga=1024, sa=1024, bi=4096, bb=1024, gf=1024, sf=1024)


def flip(bit):
    return 1 - bit


def slot_step(t, j):
    return (t % 2 + j % 2) % 2 + 2 * ((t // 2 + j // 2) % 2)


def rows_of(r, count=BLOCK):
    return pl.ds(pl.multiple_of(r * BLOCK, BLOCK), count)


def cols_of(n, count=256):
    return pl.ds(pl.multiple_of(n * count, count), count)


def dot_nn(a, b):
    return jnp.dot(a, b, preferred_element_type=F32)


def dot_nt(a, b):
    return lax.dot_general(a, b, (((1,), (1,)), ((), ())), preferred_element_type=F32)


def dot_tn(a, b):
    return lax.dot_general(a, b, (((0,), (0,)), ((), ())), preferred_element_type=F32)


def scratch_table():
    act = lambda n: pltpu.VMEM((GROUP, n), BF16)
    table = dict(
        w3=pltpu.VMEM((3 * WIDTH, HEAD_COLS), BF16),
        wo=pltpu.VMEM((4, HEAD_COLS, 256), BF16),
        wi=pltpu.VMEM((WIDTH, HIDDEN), BF16),
        wb=pltpu.VMEM((4, HIDDEN, 256), BF16),
        w3t=pltpu.VMEM((3, HEAD_COLS, WIDTH), BF16),
        wot=pltpu.VMEM((WIDTH, HEAD_COLS), BF16),
        wit=pltpu.VMEM((HIDDEN, WIDTH), BF16),
        wbt=pltpu.VMEM((WIDTH, HIDDEN), BF16),
        lens_own=pltpu.VMEM((2, 8, 128), F32),
        lens_got=pltpu.VMEM((2, 8, 128), F32),
        lens_use=pltpu.VMEM((2, 8, 128), F32),
        tk=act(WIDTH),
        tkt=pltpu.VMEM((WIDTH, GROUP), BF16),
        cot_own=pltpu.VMEM((BLOCK, WIDTH), BF16),
        bias=pltpu.VMEM((GROUP, GROUP), F32),
        q=act(HEAD_COLS),
        qt=pltpu.VMEM((HEAD_COLS, GROUP), BF16),
        k=act(HEAD_COLS),
        ks=act(HEAD_COLS),
        v=act(HEAD_COLS),
        ps=pltpu.VMEM((4, GROUP, GROUP), BF16),
        ctx=act(HEAD_COLS),
        ctxt=pltpu.VMEM((HEAD_COLS, GROUP), BF16),
        hid=act(WIDTH),
        hidt=pltpu.VMEM((WIDTH, GROUP), BF16),
        act=act(HIDDEN),
        actt=pltpu.VMEM((HIDDEN, GROUP), BF16),
        slope=pltpu.VMEM((GROUP, HIDDEN), F32),
        g2=act(WIDTH),
        gpre=act(HIDDEN),
        g1=act(WIDTH),
        gctxt=pltpu.VMEM((HEAD_COLS, GROUP), BF16),
        dq=act(HEAD_COLS),
        dkt=pltpu.VMEM((HEAD_COLS, GROUP), F32),
        dvt=pltpu.VMEM((HEAD_COLS, GROUP), F32),
        dk=act(HEAD_COLS),
        dv=act(HEAD_COLS),
        hid1=pltpu.VMEM((BLOCK, WIDTH), F32),
        normed1=pltpu.VMEM((BLOCK, WIDTH), F32),
        inv1=pltpu.VMEM((BLOCK, 128), F32),
        g2f=pltpu.VMEM((BLOCK, WIDTH), F32),
        g1f=pltpu.VMEM((BLOCK, WIDTH), F32),
        out_own=pltpu.VMEM((BLOCK, WIDTH), BF16),
        gtok_own=pltpu.VMEM((BLOCK, WIDTH), BF16),
        rs_own=pltpu.VMEM((4, BLOCK, WIDTH), BF16),
        rs_out=pltpu.VMEM((4, 3, BLOCK, WIDTH), BF16),
        rs_got=pltpu.VMEM((4, 3, BLOCK, WIDTH), BF16),
        sums=pltpu.VMEM((6, 16, WIDTH), F32),
        sums_got=pltpu.VMEM((5, 16, WIDTH), F32),
        gb_in=pltpu.VMEM((1, HIDDEN), F32),
        vectors={name: pltpu.VMEM((1, width), F32) for name, width in VECTORS.items()},
        vsem=pltpu.SemaphoreType.DMA((len(VECTORS),)),
        turn=pltpu.SemaphoreType.REGULAR((5,)),
        g3=pltpu.VMEM((3 * WIDTH, HEAD_COLS), BF16),
        go=pltpu.VMEM((4, HEAD_COLS, 256), BF16),
        gi=pltpu.VMEM((WIDTH, HIDDEN), BF16),
        gb=pltpu.VMEM((4, HIDDEN, 256), BF16),
        stage={},
        ssem=pltpu.SemaphoreType.DMA((N_SEND,)),
        rsem=pltpu.SemaphoreType.DMA((N_GOT,)),
    )
    for name, dims in HALVES.items():
        table["stage"][name] = pltpu.VMEM((10,) + dims, BF16)
    return table


def layer_kernel(tok, lens, wq, bq, wk, wv, bv, wo, bo, ga, sa, wi, bi, wb, bb, gf, sf, cot, out, gtok, sums, zq, zk, zv,
                 zo, zi0, zi1, zb0, zb1, *scratch):
    a = SimpleNamespace(tok=tok, lens=lens, wq=wq, bq=bq, wk=wk, wv=wv, bv=bv, wo=wo, bo=bo, ga=ga, sa=sa, wi=wi, bi=bi,
                        wb=wb, bb=bb, gf=gf, sf=sf, cot=cot)
    o = SimpleNamespace(out=out, gtok=gtok, sums=sums)
    landed = dict(q=zq, k=zk, v=zv, o=zo, i0=zi0, i1=zi1, b0=zb0, b1=zb1)
    s = SimpleNamespace(**jax.tree.unflatten(jax.tree.structure(scratch_table()), scratch))
    ssem, rsem, vsem, vectors = s.ssem, s.rsem, s.vsem, s.vectors

    dp = lax.axis_index("dp")
    z = lax.axis_index("tensor")
    b, c = dp // 2, dp % 2
    zl, zh = z % 2, z // 2
    t = zl * 2 + c
    sl = (z + 2 * c) % 4
    here, away = c == 0, c == 1
    bx = b + 1 - 2 * (b % 2)
    by = (b + 2) % 4
    bd = 3 - b
    t1, t2, t3 = slot_step(t, 1), slot_step(t, 2), slot_step(t, 3)

    def dev(pos, core, zz):
        return (pos * 2 + core, zz)

    partner = dev(b, flip(c), z)
    z_near = z + 1 - 2 * (z % 2)
    z_far = (z + 2) % 4
    pair = dev(b, c, z_near)
    across = dev(b, c, z_far)
    is_inner = jnp.logical_and(z >= 1, z <= 2)
    inner_away = jnp.logical_and(is_inner, away)
    outer_away = jnp.logical_and(jnp.logical_not(is_inner), away)
    x_near = dev(bx, c, z)
    y_near = dev(by, c, z)

    taken = {"s": 0, "r": 0}

    def take(kind, count=1):
        first = taken[kind]
        taken[kind] = first + count
        assert taken[kind] <= (N_SEND if kind == "s" else N_GOT)
        return first

    to_drain = []

    def make_copy(src, dst, device, sk, rk):
        return pltpu.make_async_remote_copy(
            src_ref=src, dst_ref=dst, send_sem=ssem.at[sk], recv_sem=rsem.at[rk], device_id=device,
            device_id_type=MESH_ID)

    def send(src, dst, device, sk, rk):
        make_copy(src, dst, device, sk, rk).start()

    def got(dst, rk):
        pltpu.make_async_copy(dst, dst, rsem.at[rk]).wait()

    def left(size_of, sk):
        pltpu.make_async_copy(size_of, size_of, ssem.at[sk]).wait()

    def at_end(size_of, sk, skipped=None, instead=None):
        to_drain.append((size_of, sk, skipped, instead))

    def send_or_keep(src, dst, device, is_self, sk, rk):
        copy = make_copy(src, dst, device, sk, rk)

        @pl.when(is_self)
        def _():
            pltpu.make_async_copy(src, dst, rsem.at[rk]).start()

        @pl.when(jnp.logical_not(is_self))
        def _():
            copy.start()

    barrier = pltpu.get_barrier_semaphore()
    peers = [x_near, y_near]
    for dz in range(4):
        for dc in range(2):
            if dz or dc:
                peers.append(dev(b, (c + dc) % 2, (z + dz) % 4))
    for peer in peers:
        pl.semaphore_signal(barrier, inc=1, device_id=peer, device_id_type=MESH_ID)
    pl.semaphore_wait(barrier, len(peers))

    def piece_qkv(m, home):
        base = m * WIDTH
        return SimpleNamespace(
            home=home,
            own=lambda bb, cc: s.w3.at[pl.ds(pl.multiple_of(base + bb * 256 + cc * 128, 128), 128), :],
            block=lambda bb: s.w3.at[pl.ds(pl.multiple_of(base + bb * 256, 256), 256), :],
            half=lambda bb, h: s.w3.at[pl.ds(pl.multiple_of(base + bb * 256 + h * 128, 128), 128), :])

    piece_o = SimpleNamespace(
        home=a.wo,
        own=lambda bb, cc: s.wo.at[bb, :, pl.ds(pl.multiple_of(cc * 128, 128), 128)],
        block=lambda bb: s.wo.at[bb],
        half=lambda bb, h: s.wo.at[bb, pl.ds(h * 128, 128), :])

    def piece_in(j):
        cols = pl.ds(j * 512, 512)
        return SimpleNamespace(
            home=a.wi.at[:, cols],
            own=lambda bb, cc: s.wi.at[pl.ds(pl.multiple_of(bb * 256 + cc * 128, 128), 128), cols],
            block=lambda bb: s.wi.at[pl.ds(pl.multiple_of(bb * 256, 256), 256), cols],
            half=lambda bb, h: s.wi.at[pl.ds(pl.multiple_of(bb * 256 + h * 128, 128), 128), cols])

    def piece_back(j):
        part = pl.ds(j * 512, 512)
        return SimpleNamespace(
            home=a.wb.at[part, :],
            own=lambda bb, cc: s.wb.at[bb, part, pl.ds(pl.multiple_of(cc * 128, 128), 128)],
            block=lambda bb: s.wb.at[bb, part, :],
            half=lambda bb, h: s.wb.at[bb, pl.ds(j * 512 + h * 256, 256), :])

    pieces = dict(q=piece_qkv(0, a.wq), k=piece_qkv(1, a.wk), v=piece_qkv(2, a.wv), o=piece_o,
                  i0=piece_in(0), i1=piece_in(1), b0=piece_back(0), b1=piece_back(1))
    first_size = dict(
        q=s.w3.at[0:768, :], k=s.w3.at[0:768, :], v=s.w3.at[0:768, :], o=s.wo.at[0:3], i0=s.wi.at[0:768, 0:512],
        i1=s.wi.at[0:768, 0:512], b0=s.wb.at[0:3, 0:512, :], b1=s.wb.at[0:3, 0:512, :])
    for name, piece in pieces.items():
        piece.s1, piece.r1 = take("s"), take("r")
        piece.s2, piece.r2 = take("s"), take("r", 3)
        at_end(piece.block(b), piece.s1, here, piece.own(b, 0))
        at_end(first_size[name], piece.s2)

    def to_local(name):
        piece = pieces[name]
        send_or_keep(piece.home, piece.own(b, c), dev(b, 0, z), here, piece.s1, piece.r1)

    def to_across(name):
        piece = pieces[name]
        send(piece.home, piece.own(b, c), dev(b, 1, z_far), piece.s1, piece.r1)

    def over_plane(name):
        piece = pieces[name]
        got(piece.block(b), piece.r1)
        send(piece.block(b), piece.block(b), x_near, piece.s2, piece.r2)
        send(piece.block(b), piece.block(b), y_near, piece.s2, piece.r2 + 1)

    def relay(name):
        piece = pieces[name]
        got(piece.block(bx), piece.r2)
        send(piece.half(bx, 0), piece.half(bx, 0), y_near, piece.s2, piece.r2 + 2)
        got(piece.block(by), piece.r2 + 1)
        send(piece.half(by, 1), piece.half(by, 1), x_near, piece.s2, piece.r2 + 2)

    def over_plane_now(names, chosen, relays=()):
        @pl.when(chosen)
        def _():
            for name in relays:
                relay(name)
            for name in names:
                over_plane(name)

    def arrived(name):
        piece = pieces[name]
        got(piece.block(bd), piece.r2 + 2)

    tok_s, tok_r = take("s", 2), take("r", 4)
    fwd_s = take("s", 6)
    lens_s, lens_r = take("s"), take("r")
    cot_s, cot_r = take("s"), take("r")

    def send_lens():
        first = a.lens[0, 0].astype(F32)
        s.lens_own[0] = jnp.full((8, 128), first, F32)
        s.lens_own[1] = jnp.full((8, 128), first + a.lens[0, 1].astype(F32), F32)
        send(s.lens_own, s.lens_got, partner, lens_s, lens_r)
        at_end(s.lens_own, lens_s)

    def take_lens():
        got(s.lens_got, lens_r)

        @pl.when(c == zh)
        def _():
            s.lens_use[...] = s.lens_own[...]

        @pl.when(c != zh)
        def _():
            s.lens_use[...] = s.lens_got[...]

    def tok_block(r):
        return s.tk.at[rows_of(r), :]

    inner, outer = 1 + c, 3 * c
    is_relay = jnp.logical_and(c == zh, z == inner)

    def send_tokens():
        near = z // 2 == c
        first = jnp.where(near, 2 * c, inner)
        send_or_keep(a.tok, tok_block(z), dev(b, c, first), first == z, tok_s, tok_r + z)
        at_end(tok_block(z), tok_s, first == z)
        second = make_copy(a.tok, tok_block(z), dev(b, c, 2 * c + 1), tok_s + 1, tok_r + z)
        keep = jnp.logical_and(near, z == 2 * c + 1)
        go = jnp.logical_and(near, z != 2 * c + 1)

        @pl.when(keep)
        def _():
            pltpu.make_async_copy(a.tok, tok_block(z), rsem.at[tok_r + z]).start()

        @pl.when(go)
        def _():
            second.start()

        at_end(tok_block(z), tok_s + 1, jnp.logical_not(go))

    def pass_on(half, far):
        for k in range(2):
            r = half * 2 + k
            block = tok_block(r)
            got(block, tok_r + r)
            if far:
                on = make_copy(block, block, dev(b, c, outer), fwd_s + k, tok_r + r)

                @pl.when(is_relay)
                def _():
                    on.start()
            copy = make_copy(block, block, partner, fwd_s + 2 + 2 * far + k, tok_r + r)

            @pl.when(c == zh)
            def _():
                copy.start()

    for k in range(6):
        at_end(s.tk.at[0:BLOCK, :], fwd_s + k, jnp.logical_not(is_relay) if k < 2 else c != zh)

    def send_cotangent():
        zt, ct = 2 * c + z // 2, z % 2
        is_self = jnp.logical_and(zt == z, ct == c)
        send_or_keep(a.cot, s.cot_own, dev(b, ct, zt), is_self, cot_s, cot_r)
        at_end(s.cot_own, cot_s, is_self)

    gather_s, gather_r = take("s", 3), take("r", 12)
    scatter_s, scatter_r = take("s", 4), take("r", 20)
    for k in range(3):
        at_end(s.tk.at[0:3 * BLOCK, :], gather_s + k)
    for k in range(4):
        at_end(s.tk.at[0:3 * BLOCK, :], scatter_s + k)

    def block_at(full, r):
        return full.at[rows_of(r), :]

    def half_at(full, r, k):
        return full.at[pl.ds(pl.multiple_of(r * BLOCK + k * HALF, HALF), HALF), :]

    def gather_start(which, full, k):
        mine = half_at(full, t, k)
        send(mine, mine, pair, gather_s + which, gather_r + 4 * which + 1 + k)
        send(mine, mine, partner, gather_s + which, gather_r + 4 * which)

    def gather_step(which, full, j):
        base = gather_r + 4 * which

        @pl.when(j == 1)
        def _():
            got(block_at(full, t1), base)

        @pl.when(j == 2)
        def _():
            if which == 0:
                over_plane_now((), away, relays=("b0",))
            for k in range(2):
                near = half_at(full, t2, k)
                got(near, base + 1 + k)
                send(near, near, partner, gather_s + which, base + 3)

        @pl.when(j == 3)
        def _():
            if which == 0:
                over_plane_now((), away, relays=("b1",))
            got(block_at(full, t3), base + 3)

    halves = [pl.ds(k * HALF, HALF) for k in range(2)]

    def scatter(which, part):
        out, back = s.rs_out, s.rs_got
        ss, rr = scatter_s + which, scatter_r + 5 * which
        part(t3 * BLOCK, BLOCK, out.at[which, 0])
        send(out.at[which, 0], back.at[which, 0], partner, ss, rr)
        part(t2 * BLOCK, BLOCK, out.at[which, 1])
        got(back.at[which, 0], rr)
        for k in range(2):
            rows = halves[k]
            total = out[which, 1, rows, :].astype(F32) + back[which, 0, rows, :].astype(F32)
            out[which, 1, rows, :] = total.astype(BF16)
            send(out.at[which, 1, rows, :], back.at[which, 1, rows, :], pair, ss, rr + 2 + k)
        part(t1 * BLOCK, BLOCK, out.at[which, 2])
        send(out.at[which, 2], back.at[which, 2], partner, ss, rr + 4)
        part(t * BLOCK, BLOCK, s.rs_own.at[which])

    def scatter_cols(which, blocks, k):
        out, back = s.rs_out, s.rs_got
        ss, rr = scatter_s + which, scatter_r + 5 * which
        slots = [pl.ds(pl.multiple_of(block * 256, 256), 256) for block in blocks]
        size = s.rs_got.at[which, 0, :, 0:256 * len(blocks)]

        def product(row, block):
            rows = pl.ds(pl.multiple_of(row * BLOCK, BLOCK), BLOCK)
            return dot_nn(s.act[rows, :], s.wb[block])

        def cast(row, slot):
            for block, cols in zip(blocks, slots):
                out[which, slot, :, cols] = product(row, block).astype(BF16)

        cast(t3, 0)
        for cols in slots:
            send(out.at[which, 0, :, cols], back.at[which, 0, :, cols], partner, ss, rr + k)
        cast(t1, 2)
        for cols in slots:
            send(out.at[which, 2, :, cols], back.at[which, 2, :, cols], partner, ss, rr + 4)
        got(size, rr + k)
        for block, cols in zip(blocks, slots):
            total = product(t2, block).astype(BF16).astype(F32) + back[which, 0, :, cols].astype(F32)
            out[which, 1, :, cols] = total.astype(BF16)
            send(out.at[which, 1, :, cols], back.at[which, 1, :, cols], pair, ss, rr + 2)
        for block, cols in zip(blocks, slots):
            s.rs_own[which, :, cols] = product(t, block).astype(BF16)

    def scatter_cols_wait(which):
        rr = scatter_r + 5 * which
        got(s.rs_got.at[which, 2], rr + 4)
        got(s.rs_got.at[which, 1], rr + 2)

    def scatter_wait(which, k):
        rr = scatter_r + 5 * which
        if k == 0:
            got(s.rs_got.at[which, 2], rr + 4)
        got(s.rs_got.at[which, 1, halves[k], :], rr + 2 + k)

    def scatter_rows(which, chunk):
        total = s.rs_own[which, chunk, :].astype(F32) + s.rs_got[which, 2, chunk, :].astype(F32)
        return total + s.rs_got[which, 1, chunk, :].astype(F32)

    def by_halves(which, body, after):
        if which == 1:
            scatter_cols_wait(which)
        for k in range(2):
            if which != 1:
                scatter_wait(which, k)
            loop(2, lambda i: body(2 * k + i))
            after(k)

    def put_part(dst, n, value):
        dst[:, 256 * n:256 * n + 256] = value.astype(BF16)

    def loop(count, body):
        lax.fori_loop(0, count, lambda i, _: (body(i), 0)[1], 0)

    def grad_qkv(m):
        base = m * WIDTH
        return lambda bb, h: s.g3.at[pl.ds(pl.multiple_of(base + bb * 256 + h * 128, 128), 128), :]

    def grad_in_part(k):
        cols = pl.ds(k * 512, 512)
        return lambda bb, h: s.gi.at[pl.ds(pl.multiple_of(bb * 256 + h * 128, 128), 128), cols]

    def grad_back_part(k):
        part = pl.ds(k * 512, 512)
        return lambda bb, h: s.gb.at[bb, part, pl.ds(h * 128, 128)]

    grad_half = dict(
        q=grad_qkv(0), k=grad_qkv(1), v=grad_qkv(2), o=lambda bb, h: s.go.at[bb, :, pl.ds(h * 128, 128)],
        i0=grad_in_part(0), i1=grad_in_part(1), b0=grad_back_part(0), b1=grad_back_part(1))
    grad_s = {name: take("s", 2) for name in grad_half}
    grad_r = {name: take("r", 4) for name in grad_half}
    for name in grad_half:
        at_end(s.stage[name].at[0:6], grad_s[name])
        at_end(s.stage[name].at[0:2], grad_s[name] + 1, here, s.stage[name].at[0])

    def chunks(name, body):
        size = min(HALVES[name][0], 256)
        count = HALVES[name][0] // size
        loop(count, lambda i: body(pl.ds(pl.multiple_of(i * size, size), size)))

    def grad_first(name, part=2):
        half, ss, rr, st = grad_half[name], grad_s[name], grad_r[name], s.stage[name]
        if part in (0, 2):
            send(half(bd, 0), st.at[1], x_near, ss, rr)
            send(half(bd, 1), st.at[3], y_near, ss, rr + 1)
        if part == 0:
            return
        send(half(bx, 0), st.at[0], x_near, ss, rr + 2)
        send(half(by, 1), st.at[2], y_near, ss, rr + 2)

    def grad_second(name):
        half, ss, rr, st = grad_half[name], grad_s[name], grad_r[name], s.stage[name]
        for h, block, to in ((0, by, y_near), (1, bx, x_near)):
            got(st.at[1 + 2 * h], rr + h)
            mine = half(block, h)

            def add(ch):
                st[4 + h, ch, :] = (mine[ch, :].astype(F32) + st[1 + 2 * h, ch, :].astype(F32)).astype(BF16)
            chunks(name, add)
            send(st.at[4 + h], st.at[6 + h], to, ss, rr + 2)

    def grad_third(name):
        half, ss, rr, st = grad_half[name], grad_s[name], grad_r[name], s.stage[name]
        zr = landed[name]
        got(st.at[0:4], rr + 2)
        for h in range(2):
            mine = half(b, h)

            def add_all(ch):
                total = mine[ch, :].astype(F32) + st[2 * h, ch, :].astype(F32) + st[6 + h, ch, :].astype(F32)
                st[8 + h, ch, :] = total.astype(BF16)
            chunks(name, add_all)
            is_self = here if h == 0 else c < 0
            send_or_keep(st.at[8 + h], zr.at[zh], dev(b, h, sl), is_self, ss + 1, rr + 3)

    def grad_final(name):
        got(landed[name], grad_r[name] + 3)

    to_across("q")
    to_across("k")
    send_tokens()
    to_across("v")
    for name in pieces:
        to_local(name)
    send_lens()
    for name, ref in vectors.items():
        pltpu.make_async_copy(getattr(a, name), ref, vsem.at[list(vectors).index(name)]).start()
    s.sums[0] = jnp.zeros((16, WIDTH), F32)
    s.gb_in[...] = jnp.zeros((1, HIDDEN), F32)
    leads = jnp.logical_and(is_inner, away)

    def in_turn(k, inner_next, outer_next):
        @pl.when(leads)
        def _():
            for device in (partner, pair, dev(b, 0, z_near)):
                pl.semaphore_signal(s.turn.at[k], inc=1, device_id=device, device_id_type=MESH_ID)

        @pl.when(jnp.logical_not(leads))
        def _():
            pl.semaphore_wait(s.turn.at[k], 1)

        for chosen, names in ((is_inner, inner_next), (jnp.logical_not(is_inner), outer_next)):
            if names:
                @pl.when(chosen)
                def _():
                    for name in names:
                        to_across(name)

    over_plane_now(("q", "k", "v", "o"), here)
    over_plane_now(("q", "k"), away)
    relay("q")
    over_plane_now(("i0",), here, relays=("k", "v"))
    pass_on(zh, 0)
    to_across("o")

    @pl.when(is_inner)
    def _():
        pass_on(flip(zh), 1)

    in_turn(0, (), ("i0",))
    take_lens()

    def make_bias(r):
        first, end = s.lens_use[0][0:1, 0:1], s.lens_use[1][0:1, 0:1]
        row = (lax.broadcasted_iota(jnp.int32, (BLOCK, GROUP), 0) + r * BLOCK).astype(F32)
        col = lax.broadcasted_iota(jnp.int32, (BLOCK, GROUP), 1).astype(F32)
        seg = lambda p: jnp.where(p >= end, 2.0, jnp.where(p >= first, 1.0, 0.0))
        s.bias[rows_of(r), :] = jnp.where(seg(row) == seg(col), 0.0, masked_value)
    loop(SLOTS, make_bias)
    for name, ref in vectors.items():
        pltpu.make_async_copy(getattr(a, name), ref, vsem.at[list(vectors).index(name)]).wait()
        setattr(a, name, ref)
    over_plane_now(("v", "o"), away, relays=("k",))
    over_plane_now(("i1",), here, relays=("o",))
    over_plane_now((), away, relays=("v",))
    over_plane_now(("b0",), here, relays=("i0",))
    in_turn(1, ("i0", "i1"), ("i1",))

    @pl.when(jnp.logical_not(is_inner))
    def _():
        pass_on(flip(zh), 1)


    def turn_tokens(r):
        s.tkt[:, rows_of(r)] = s.tk[rows_of(r), :].T
    loop(SLOTS, turn_tokens)

    head_cols = pl.ds(pl.multiple_of(sl * HEAD_COLS, HEAD_COLS), HEAD_COLS)

    def project(m):
        acc = dot_nn(s.tk[...], s.w3[m * WIDTH:(m + 1) * WIDTH, :])
        if m == 0:
            value = (acc + a.bq[:, head_cols]).astype(BF16)
            scaled = (value.astype(F32) * 0.125).astype(BF16)
            s.q[...] = scaled
            s.qt[...] = scaled.T
        elif m == 1:
            value = acc.astype(BF16)
            s.k[...] = value
            s.ks[...] = (value.astype(F32) * 0.125).astype(BF16)
        else:
            s.v[...] = (acc + a.bv[:, head_cols]).astype(BF16)

    arrived("q")
    project(0)
    arrived("k")
    project(1)
    in_turn(2, ("b0", "b1"), ())
    arrived("v")
    project(2)

    def attend():
        parts = []
        for h in range(4):
            cols = slice(64 * h, 64 * h + 64)
            scores = dot_nt(s.q[:, cols], s.k[:, cols]) + s.bias[...]
            top = jnp.max(scores, axis=-1, keepdims=True)
            weight = jnp.exp(scores - top)
            total = jnp.sum(weight, axis=-1, keepdims=True)
            prob = (weight * (1.0 / total)).astype(BF16)
            s.ps[h] = prob
            parts.append(dot_nn(prob, s.v[:, cols]))
        context = jnp.concatenate(parts, axis=1).astype(BF16)
        s.ctx[...] = context
        s.ctxt[...] = context.T
    over_plane_now((), away, relays=("o",))
    over_plane_now(("i0",), inner_away)
    over_plane_now(("b1",), here, relays=("i1",))
    attend()
    @pl.when(jnp.logical_not(is_inner))
    def _():
        to_across("b0")

    over_plane_now(("i0",), outer_away)
    over_plane_now(("i1",), inner_away)
    arrived("o")

    def attn_part(first, count, dst):
        rows = s.ctx[pl.ds(pl.multiple_of(first, HALF), count), :]
        for n in range(4):
            put_part(dst, n, dot_nn(rows, s.wo[n]))
    scatter(0, attn_part)
    @pl.when(jnp.logical_not(is_inner))
    def _():
        to_across("b1")

    for m in range(3):
        for n in range(4):
            s.w3t[m, :, 256 * n:256 * n + 256] = s.w3[m * WIDTH + 256 * n:m * WIDTH + 256 * n + 256, :].T
    for n in range(4):
        s.wot[256 * n:256 * n + 256, :] = s.wo[n].T

    CH = 32

    def own_chunk(i):
        return pl.ds(pl.multiple_of(i * CH, CH), CH)

    def group_chunk(i):
        return pl.ds(pl.multiple_of(t * BLOCK + i * CH, CH), CH)

    def norm_one(i):
        ch = own_chunk(i)
        resid = s.tk[group_chunk(i), :].astype(F32) + scatter_rows(0, ch) + a.bo[...]
        centered = resid - jnp.mean(resid, axis=-1, keepdims=True)
        inv = lax.rsqrt(jnp.mean(centered * centered, axis=-1, keepdims=True) + epsilon)
        normed = centered * inv
        hidden = normed * a.ga[...] + a.sa[...]
        s.normed1[ch, :] = normed
        s.inv1[ch, :] = jnp.broadcast_to(inv, (CH, 128))
        s.hid1[ch, :] = hidden
        s.hid[group_chunk(i), :] = hidden.astype(BF16)
    over_plane_now((), here, relays=("b0",))
    over_plane_now((), inner_away, relays=("i0",))
    over_plane_now(("i1", "b0"), outer_away, relays=("i0",))
    by_halves(0, norm_one, lambda k: gather_start(0, s.hid, k))
    over_plane_now((), here, relays=("b1",))
    over_plane_now((), inner_away, relays=("i1",))
    over_plane_now(("b1",), outer_away, relays=("i1",))
    over_plane_now(("b0", "b1"), inner_away)
    send_cotangent()
    arrived("i0")
    arrived("i1")

    def ffn_in(j):
        gather_step(0, s.hid, j)
        r = slot_step(t, j)
        rows = rows_of(r)
        for n in range(4):
            cols = slice(256 * n, 256 * n + 256)
            bias = a.bi[:, pl.ds(pl.multiple_of(sl * HIDDEN + n * 256, 256), 256)]
            pre = dot_nn(s.hid[rows, :], s.wi[:, cols]) + bias
            cdf = 0.5 * (1.0 + lax.erf(pre * 0.7071067811865476))
            pdf = jnp.exp(-0.5 * pre * pre) * 0.3989422804014327
            s.act[rows, cols] = (pre * cdf).astype(BF16)
            s.slope[rows, cols] = cdf + pre * pdf
    loop(SLOTS, ffn_in)

    def turn_ffn(r):
        rows = rows_of(r)
        s.actt[:, rows] = s.act[rows, :].T
        s.hidt[:, rows] = s.hid[rows, :].T
    scatter_cols(1, (b, bx, by), 0)
    arrived("b0")
    arrived("b1")
    scatter_cols(1, (bd,), 1)
    loop(SLOTS, turn_ffn)

    def turn_wi(r):
        rows = rows_of(r)
        s.wit[:, rows] = s.wi[rows, :].T
    loop(8, turn_wi)

    def turn_wb(r):
        rows = rows_of(r)
        for n in range(4):
            s.wbt[256 * n:256 * n + 256, rows] = s.wb[n, rows, :].T
    loop(8, turn_wb)
    got(s.cot_own, cot_r)

    def add_rows(row, value):
        s.sums[0, row:row + 1, :] += jnp.sum(value, axis=0, keepdims=True)

    def norm_two(i):
        ch = own_chunk(i)
        resid = s.hid1[ch, :] + scatter_rows(1, ch) + a.bb[...]
        centered = resid - jnp.mean(resid, axis=-1, keepdims=True)
        inv = lax.rsqrt(jnp.mean(centered * centered, axis=-1, keepdims=True) + epsilon)
        normed = centered * inv
        position = lax.broadcasted_iota(jnp.int32, (CH, 128), 0) + (t * BLOCK + i * CH)
        live = jnp.where(position.astype(F32) < s.lens_use[1][0:1, :], 1.0, 0.0)[:, 0:1]
        s.out_own[ch, :] = ((normed * a.gf[...] + a.sf[...]) * live).astype(BF16)
        grad = s.cot_own[ch, :].astype(F32) * live
        add_rows(4, grad * normed)
        add_rows(5, grad)
        u = grad * a.gf[...]
        first = jnp.mean(u, axis=-1, keepdims=True)
        second = jnp.mean(u * normed, axis=-1, keepdims=True)
        grad_two = inv * (u - first - normed * second)
        add_rows(3, grad_two)
        s.g2f[ch, :] = grad_two
        s.g2[group_chunk(i), :] = grad_two.astype(BF16)
    by_halves(1, norm_two, lambda k: gather_start(1, s.g2, k))
    out_s, out_r = take("s"), take("r")
    home_self = jnp.logical_and(zh == c, t == z)

    def ffn_back(j):
        @pl.when(j < 3)
        def _():
            gather_step(1, s.g2, j)
        r = slot_step(t, j)
        rows = rows_of(r)
        for n in range(4):
            cols = slice(256 * n, 256 * n + 256)
            grad = dot_nn(s.g2[rows, :], s.wbt[:, cols]) * s.slope[rows, cols]
            s.gb_in[:, cols] += jnp.sum(grad, axis=0, keepdims=True)
            s.gpre[rows, cols] = grad.astype(BF16)
    loop(SLOTS - 1, ffn_back)

    def grad_back(k):
        part = slice(512 * k, 512 * k + 512)

        def body(n):
            for e in range(2):
                block = n * 2 + e
                s.gb[block, part, :] = dot_nn(s.actt[part, :], s.g2[:, cols_of(block)]).astype(BF16)
        loop(2, body)

    def grad_in(k):
        cols = slice(512 * k, 512 * k + 512)

        def body(m):
            part = rows_of(m * 4, 512)
            s.gi[part, cols] = dot_nn(s.hidt[part, :], s.gpre[:, cols]).astype(BF16)
        loop(2, body)

    gather_step(1, s.g2, 3)
    grad_back(0)
    grad_first("b0")
    ffn_back(3)
    grad_back(1)
    grad_first("b1", 0)
    send_or_keep(s.out_own, o.out, dev(b, zh, t), home_self, out_s, out_r)
    at_end(s.out_own, out_s, home_self)

    def in_part(first, count, dst):
        rows = pl.ds(pl.multiple_of(first, HALF), count)
        for n in range(4):
            put_part(dst, n, dot_nn(s.gpre[rows, :], s.wit[:, 256 * n:256 * n + 256]))
    scatter(2, in_part)
    grad_in(0)
    grad_in(1)
    grad_second("b0")
    grad_first("b1", 1)
    grad_second("b1")
    grad_first("i0", 0)

    def norm_one_back(i):
        ch = own_chunk(i)
        grad = s.g2f[ch, :] + scatter_rows(2, ch)
        normed = s.normed1[ch, :]
        add_rows(1, grad * normed)
        add_rows(2, grad)
        u = grad * a.ga[...]
        first = jnp.mean(u, axis=-1, keepdims=True)
        second = jnp.mean(u * normed, axis=-1, keepdims=True)
        grad_one = s.inv1[ch, 0:1] * (u - first - normed * second)
        add_rows(0, grad_one)
        s.g1f[ch, :] = grad_one
        s.g1[group_chunk(i), :] = grad_one.astype(BF16)
    by_halves(2, norm_one_back, lambda k: gather_start(2, s.g1, k))
    grad_first("i0", 1)
    grad_third("b0")

    def attend_back(chip, add):
        rows = pl.ds(pl.multiple_of(chip * 2 * BLOCK, 2 * BLOCK), 2 * BLOCK)
        grad_ctx = dot_nn(s.g1[rows, :], s.wot[...]).astype(BF16)
        s.gctxt[:, rows] = grad_ctx.T
        product = grad_ctx.astype(F32) * s.ctx[rows, :].astype(F32)
        parts = []
        for h in range(4):
            cols = slice(64 * h, 64 * h + 64)
            prob = s.ps[h, rows, :]
            delta = jnp.sum(product[:, cols], axis=-1, keepdims=True)
            grad_prob = dot_nt(grad_ctx[:, cols], s.v[:, cols])
            grad_score = (prob.astype(F32) * (grad_prob - delta)).astype(BF16)
            parts.append(dot_nn(grad_score, s.ks[:, cols]))
            grad_key = dot_nn(s.qt[cols, rows], grad_score)
            grad_value = dot_nn(s.gctxt[cols, rows], prob)
            if add:
                grad_key, grad_value = s.dkt[cols, :] + grad_key, s.dvt[cols, :] + grad_value
            s.dkt[cols, :] = grad_key
            s.dvt[cols, :] = grad_value
        grad_query = jnp.concatenate(parts, axis=1)
        for k in range(4):
            @pl.when(sl == k)
            def _():
                s.sums[0, 6:7, 256 * k:256 * k + 256] += jnp.sum(grad_query, axis=0, keepdims=True)
        s.dq[rows, :] = grad_query.astype(BF16)
    gather_step(2, s.g1, 1)
    attend_back(zl, False)
    grad_third("b1")
    gather_step(2, s.g1, 2)
    gather_step(2, s.g1, 3)
    attend_back(flip(zl), True)
    grad_second("i0")
    grad_first("i1")
    s.dk[...] = s.dkt[...].T.astype(BF16)
    grad_value = s.dvt[...].T
    for k in range(4):
        @pl.when(sl == k)
        def _():
            s.sums[0, 7:8, 256 * k:256 * k + 256] += jnp.sum(grad_value, axis=0, keepdims=True)
    s.dv[...] = grad_value.astype(BF16)
    for k in range(4):
        @pl.when(sl == k)
        def _():
            s.sums[0, 8 + k:9 + k, :] = s.gb_in[...]

    sums_s, sums_r = take("s", 6), take("r", 6)
    sums_to = [partner, across, pair, x_near, y_near]
    sum_rows = pl.ds(pl.multiple_of(c * 8, 8), 8)
    other_rows = pl.ds(pl.multiple_of(flip(c) * 8, 8), 8)

    def sums_part(ref, k):
        return ref.at[k] if k == 0 else ref.at[k, sum_rows, :]

    def sums_start(k):
        mine = sums_part(s.sums, k)
        send(mine, sums_part(s.sums_got, k), sums_to[k], sums_s + k, sums_r + k)
        at_end(mine, sums_s + k)

    def sums_finish(k):
        got(sums_part(s.sums_got, k), sums_r + k)
        if k == 0:
            s.sums[1] = s.sums[0] + s.sums_got[0]
        else:
            s.sums[k + 1, sum_rows, :] = s.sums[k, sum_rows, :] + s.sums_got[k, sum_rows, :]
        if k == 4:
            done = s.sums.at[5, sum_rows, :]
            send(done, done, partner, sums_s + 5, sums_r + 5)
            at_end(done, sums_s + 5)

    def sums_out():
        got(s.sums.at[5, other_rows, :], sums_r + 5)
        pltpu.make_async_copy(s.sums.at[5], o.sums, vsem.at[0]).start()

    sums_start(0)

    def tok_part(first, count, dst):
        rows = pl.ds(pl.multiple_of(first, HALF), count)
        for n in range(4):
            cols = slice(256 * n, 256 * n + 256)
            acc = dot_nn(s.dq[rows, :], s.w3t[0, :, cols])
            acc = acc + dot_nn(s.dk[rows, :], s.w3t[1, :, cols])
            acc = acc + dot_nn(s.dv[rows, :], s.w3t[2, :, cols])
            put_part(dst, n, acc)
    scatter(3, tok_part)
    sums_finish(0)
    sums_start(1)

    def grad_head(m, src):
        s.g3[m * WIDTH:(m + 1) * WIDTH, :] = dot_nn(s.tkt[...], src[...]).astype(BF16)

    grad_third("i0")
    for n in range(4):
        s.go[n] = dot_nn(s.ctxt[...], s.g1[:, 256 * n:256 * n + 256]).astype(BF16)
    grad_head(0, s.dq)
    grad_head(1, s.dk)
    grad_head(2, s.dv)
    grad_second("i1")
    grad_first("o")
    grad_first("q")
    gtok_s, gtok_r = take("s"), take("r")
    at_end(s.gtok_own, gtok_s, home_self)

    def last_rows(i):
        ch = own_chunk(i)
        s.gtok_own[ch, :] = (s.g1f[ch, :] + scatter_rows(3, ch)).astype(BF16)

    def rows_home(chosen):
        @pl.when(chosen)
        def _():
            by_halves(3, last_rows, lambda k: None)
            send_or_keep(s.gtok_own, o.gtok, dev(b, zh, t), home_self, gtok_s, gtok_r)

    rows_home(is_inner)
    grad_third("i1")
    grad_second("o")
    grad_first("k")
    grad_second("q")
    grad_first("v")
    rows_home(jnp.logical_not(is_inner))
    sums_finish(1)
    sums_start(2)
    grad_third("o")
    grad_second("k")
    grad_third("q")
    sums_finish(2)
    grad_second("v")
    sums_start(3)
    grad_third("k")
    grad_third("v")
    sums_finish(3)
    sums_start(4)
    grad_final("b0")
    grad_final("b1")
    grad_final("i0")
    grad_final("i1")
    got(o.gtok, gtok_r)
    got(o.out, out_r)
    grad_final("o")
    grad_final("q")
    sums_finish(4)
    grad_final("k")
    sums_out()
    grad_final("v")

    pltpu.make_async_copy(s.sums.at[5], o.sums, vsem.at[0]).wait()
    for size_of, sk, skipped, instead in to_drain:
        if skipped is None:
            left(size_of, sk)
        else:
            @pl.when(jnp.logical_not(skipped))
            def _():
                left(size_of, sk)
            if instead is not None:
                @pl.when(skipped)
                def _():
                    left(instead, sk)


def result_kernel(*refs):
    out, gtok, sums, zq, zk, zv, zo, zi0, zi1, zb0, zb1 = refs[:11]
    (o_out, o_gtok, o_gq, o_gbq, o_gk, o_gv, o_gbv, o_go, o_gbo, o_gga, o_gsa, o_gi, o_gbi, o_gb, o_gbb, o_ggf,
     o_gsf) = refs[11:28]
    held, wide, lines, wide_in, in_sem, out_sem = refs[28:39], refs[39:46], refs[46:55], refs[55], refs[56], refs[57]
    arriving = [pltpu.make_async_copy(src, dst, in_sem.at[n]) for n, (src, dst) in enumerate(zip(refs[:11], held))]
    for n in (0, 1, 9, 10, 7, 8, 6, 3, 4, 5, 2):
        arriving[n].start()
    leaving = []

    def put(src, dst):
        copy = pltpu.make_async_copy(src, dst, out_sem.at[len(leaving)])
        copy.start()
        leaving.append(copy)

    arriving[0].wait()
    put(held[0], o_out)
    arriving[1].wait()
    wide[0][...] = held[1][...].astype(F32)
    put(wide[0], o_gtok)

    def both(n, dst):
        arriving[n].wait()
        dst[...] = held[n][0].astype(F32) + held[n][1].astype(F32)

    both(9, wide[1].at[0:512, :])
    both(10, wide[1].at[512:1024, :])
    put(wide[1], o_gb)
    both(7, wide_in.at[:, 0:512])
    both(8, wide_in.at[:, 512:1024])
    put(wide_in, o_gi)
    for n, buf, dst in ((6, wide[2], o_go), (3, wide[3], o_gq), (4, wide[4], o_gk), (5, wide[5], o_gv)):
        both(n, buf)
        put(buf, dst)
    arriving[2].wait()
    for row, buf, dst in ((6, 0, o_gbq), (7, 1, o_gbv), (0, 2, o_gbo), (1, 3, o_gga), (2, 4, o_gsa), (3, 5, o_gbb),
                          (4, 6, o_ggf), (5, 7, o_gsf)):
        lines[buf][...] = held[2][row:row + 1, :]
        put(lines[buf], dst)
    for k in range(4):
        lines[8][:, WIDTH * k:WIDTH * k + WIDTH] = held[2][8 + k:9 + k, :]
    put(lines[8], o_gbi)
    for copy in leaving:
        copy.wait()


def on_device_fused(tokens, lengths, w_query, b_query, w_key, w_value, b_value, w_out, b_out, gain_attn, shift_attn,
                    w_in, b_in, w_back, b_back, gain_ffn, shift_ffn, cotangent):
    row = lambda vec: vec.reshape(1, -1)
    operands = (tokens, lengths, w_query, row(b_query), w_key, w_value, row(b_value), w_out, row(b_out),
                row(gain_attn), row(shift_attn), w_in, row(b_in), w_back, row(b_back), row(gain_ffn),
                row(shift_ffn), cotangent)
    stay = pl.BlockSpec(memory_space=pl.ANY)
    in_specs = [stay] * len(operands)
    in_specs[1] = pl.BlockSpec(memory_space=pltpu.SMEM)
    shape = lambda dims, dtype: jax.ShapeDtypeStruct(dims, dtype)
    between = [shape(tokens.shape, BF16), shape(tokens.shape, BF16), shape((16, WIDTH), F32)]
    between += [shape((2,) + HALVES[name], BF16) for name in ("q", "k", "v", "o", "i0", "i1", "b0", "b1")]
    parts = pl.pallas_call(
        layer_kernel,
        out_shape=between,
        in_specs=in_specs,
        out_specs=[stay] * len(between),
        scratch_shapes=jax.tree.leaves(scratch_table()),
        compiler_params=pltpu.CompilerParams(collective_id=0, has_side_effects=True, vmem_limit_bytes=64 * 1024 * 1000),
        name="layer",
    )(*operands)
    line = shape((1, WIDTH), F32)
    results = (
        shape(tokens.shape, BF16), shape(tokens.shape, F32), shape(w_query.shape, F32), line, shape(w_key.shape, F32),
        shape(w_value.shape, F32), line, shape(w_out.shape, F32), line, line, line, shape(w_in.shape, F32),
        shape((1, b_in.shape[0]), F32), shape(w_back.shape, F32), line, line, line)
    outs = pl.pallas_call(
        result_kernel,
        out_shape=results,
        in_specs=[stay] * len(between),
        out_specs=[stay] * len(results),
        scratch_shapes=[pltpu.VMEM(part.shape, part.dtype) for part in between]
        + [pltpu.VMEM(dims, F32) for dims in (tokens.shape, w_back.shape, w_out.shape, w_query.shape, w_key.shape,
                                              w_value.shape, (8, 128))]
        + [pltpu.VMEM((1, WIDTH), F32)] * 8
        + [pltpu.VMEM((1, b_in.shape[0]), F32), pltpu.VMEM(w_in.shape, F32), pltpu.SemaphoreType.DMA((11,)),
           pltpu.SemaphoreType.DMA((17,))],
        name="results",
    )(*parts)
    return tuple(v.reshape(-1) if v.shape[0] == 1 else v for v in outs)


def fits_fused(mesh):
    return dict(mesh.shape) == {"dp": 8, "tensor": 4}


def solution(mesh):
    placed = (
        P(("dp", "tensor"), None),
        P("dp", None),
        P("dp", "tensor"),
        P(),
        P("dp", "tensor"),
        P("dp", "tensor"),
        P(),
        P("tensor", "dp"),
        P(),
        P(),
        P(),
        P("dp", "tensor"),
        P(),
        P("tensor", "dp"),
        P(),
        P(),
        P(),
        P(("dp", "tensor"), None),
    )
    on_device = on_device_fused if fits_fused(mesh) else on_device_plain
    return jax.shard_map(
        on_device,
        mesh=mesh,
        in_specs=placed,
        out_specs=(
            P(("dp", "tensor"), None),
            P(("dp", "tensor"), None),
            P("dp", "tensor"),
            P(),
            P("dp", "tensor"),
            P("dp", "tensor"),
            P(),
            P("tensor", "dp"),
            P(),
            P(),
            P(),
            P("dp", "tensor"),
            P(),
            P("tensor", "dp"),
            P(),
            P(),
            P(),
        ),
        check_vma=False,
    )
```
